32 devices in a mesh: dp: 2 (over x), row: 4 (over y, core), col: 4 (over z).
Axes of the slice: x: 2, y: 2, z: 4, core: 2. Of those that a mesh axis runs over, the one named last changes fastest.
Arguments:
- inputs: bfloat16 [4096, 2048], P(('dp', 'row'), 'col'), may hold values from -6 to 6
- cotangent: bfloat16 [4096, 2048], P(('dp', 'row'), 'col'), may hold values from -6 to 6
- segments: int32 [4096], P('dp'), may hold values from 1999 to 4095, as said below
- positions: int32 [4096], P('dp'), may hold values from 0 to 1999, as said below
- w_qkv: bfloat16 [2048, 3, 2048], P('col', None, 'row'), may hold values from -1 to 1
- w_out: bfloat16 [2048, 2048], P('row', 'col'), may hold values from -0.5 to 0.5
- w_up: bfloat16 [2048, 8192], P('col', 'row'), may hold values from -1 to 1
- w_down: bfloat16 [8192, 2048], P('row', 'col'), may hold values from -0.0625 to 0.0625
- vectors: float32 [11, 2048], replicated, may hold values from -1.5 to 3
- tile_moment: float32 [4, 4, 24, 512, 256], P('row', 'col', 'dp'), may hold values from -40 to 40
- vector_moment: float32 [11, 2048], replicated, may hold values from -3 to 3
Outputs:
- result: float32 [4096, 2048], P(('dp', 'row'), 'col')
- grad_input: float32 [4096, 2048], P(('dp', 'row'), 'col')
- tile_grads: float32 [4, 4, 24, 512, 256], P('row', 'col', 'dp')
- new_tiles: float32 [4, 4, 24, 512, 256], P('row', 'col', 'dp')
- new_tile_moment: float32 [4, 4, 24, 512, 256], P('row', 'col', 'dp')
- vector_grads: float32 [11, 2048], replicated
- new_vectors: float32 [11, 2048], replicated
- new_vector_moment: float32 [11, 2048], replicated
The draws below stay inside these ranges and needn't reach their ends.
Inputs may be any that keep to these rules, and one draw needn't show every extreme that they name: `segments`: each token's document label, the index in the whole array of its document's last token (the last document's label is 4095); labels never fall; every document but the last has 200 to 2000 tokens, documents run on across sequence ends, and the first has exactly 2000. `positions`: each token's place in its document, counted from 0 and running on across sequence ends.
All inputs are finite; a program needn't handle non-finite values.
Results may differ from the reference program's by a relative error of at most 0.015.
The reference program's roundings to bfloat16 on the way count: a program that leaves them out, or rounds other values in their place, can miss the bound.
Values may be sent and summed in bfloat16 or wider, within the bound.
A program may use at most 256 MiB of HBM per device.

```python
import math
import jax
import jax.numpy as jnp
from jax import lax

D = 2048
FF = 8192
HEADS = 32
HEAD_DIM = 64
ROTARY = 32
SEQ_LEN = 512
DOC_MIN = 200
DOC_MAX = 2000
TILES = 24
TOK_DP = 2048
TOKENS = 4096
TILE_R = 512
TILE_C = 256
N_DP = 2
N_ROW = 4
N_COL = 4


def document_layout(key):
    inner_key = jax.random.fold_in(key, 17)
    doc_count = TOKENS // DOC_MIN + 1
    doc_lengths = jax.random.randint(inner_key, (doc_count,), DOC_MIN, DOC_MAX + 1, dtype=jnp.int32)
    doc_lengths = doc_lengths.at[0].set(DOC_MAX)
    doc_ends = jnp.cumsum(doc_lengths).astype(jnp.int32)
    doc_starts = doc_ends - doc_lengths
    token_place = jnp.arange(TOKENS, dtype=jnp.int32)
    doc_index = jnp.sum((doc_ends[None, :] <= token_place[:, None]).astype(jnp.int32), axis=1).astype(jnp.int32)
    doc_last = jnp.minimum(doc_ends - 1, TOKENS - 1).astype(jnp.int32)
    return (jnp.take(doc_last, doc_index).astype(jnp.int32), (token_place - jnp.take(doc_starts, doc_index)).astype(jnp.int32))


def draw_segments(key, part):
    return document_layout(key)[0]


def draw_positions(key, part):
    return document_layout(key)[1]


def draw_w_qkv(key, part):
    base_draw = jax.random.normal(key, (D, 3, D), jnp.float32) * (1.0 / math.sqrt(D))
    return jnp.clip(base_draw, -1.0, 1.0).astype(jnp.bfloat16)


def draw_w_up(key, part):
    base_draw = jax.random.normal(key, (D, FF), jnp.float32) * (1.0 / math.sqrt(D))
    shared_row = jax.random.normal(jax.random.fold_in(key, 31), (FF,), jnp.float32) * (2.0 / math.sqrt(FF))
    return jnp.clip(base_draw + shared_row[None, :], -1.0, 1.0).astype(jnp.bfloat16)


def draw_vectors(key, part):
    vec_rows = 7 + FF // D
    row_id = jnp.arange(vec_rows)[:, None]
    feature_frac = jnp.arange(D, dtype=jnp.float32)[None, :] / D
    spread = jnp.clip(jax.random.normal(key, (vec_rows, D), jnp.float32), -3.0, 3.0) * 0.5
    jitter = jax.random.uniform(jax.random.fold_in(key, 5), (vec_rows, D), jnp.float32, 0.8, 1.2)
    gains = (0.4 + 1.6 * feature_frac) * jitter
    return jnp.where(row_id == 5, gains, spread)


def shard_levels(rng, dims, cuts, least, high):
    def one(dim, parts):
        steps = jax.random.uniform(jax.random.fold_in(jax.random.fold_in(rng, 6), dim), (parts,), jnp.float32, least / len(cuts), high / len(cuts))
        return jnp.repeat(jnp.exp(steps), dims[dim] // parts).reshape((-1,) + (1,) * (len(dims) - dim - 1))

    level = one(*cuts[0])
    for cut in cuts[1:]:
        level = level * one(*cut)
    return level


def centred(own_key, dims, scale, limit, cuts=(), held_as=jnp.bfloat16):
    loudness = shard_levels(own_key, dims, cuts, -0.22, 0.18) if cuts else 1.0
    array = jax.random.normal(own_key, dims, jnp.float32) * scale * loudness
    return jnp.minimum(jnp.maximum(array, -limit), limit).astype(held_as)


def setup_inputs(seed: int = 0) -> dict:
    key_of = jax.random.split(jax.random.key(seed), 12)
    return {
        "inputs": centred(key_of[0], (TOKENS, D), 1.0, 6.0, ((0, 8), (1, 4))),
        "cotangent": centred(key_of[1], (TOKENS, D), 1.0, 6.0, ((0, 8), (1, 4))),
        "segments": draw_segments(jax.random.fold_in(key_of[11], 71), 0),
        "positions": draw_positions(jax.random.fold_in(key_of[11], 71), 0),
        "w_qkv": draw_w_qkv(jax.random.fold_in(key_of[11], 71), 0),
        "w_out": centred(key_of[5], (D, D), (D // 16) ** -0.5, 0.5, ((0, 4), (1, 4))),
        "w_up": draw_w_up(jax.random.fold_in(key_of[11], 71), 0),
        "w_down": centred(key_of[7], (FF, D), FF ** -0.5, 0.0625, ((0, 4), (1, 4))),
        "vectors": draw_vectors(jax.random.fold_in(key_of[11], 71), 0),
        "tile_moment": centred(key_of[9], (N_ROW, N_COL, TILES, TILE_R, TILE_C), (0.1 * TOKENS ** 0.5), 40.0, ((0, 4), (1, 4), (2, 2)), jnp.float32),
        "vector_moment": centred(key_of[10], (7 + FF // D, D), 0.5, 3.0, (), jnp.float32),
    }


MOMENTUM_RATE = 0.95
MUON_RATE = 0.05
VECTOR_RATE = 0.12
NEWTON_A = 3.4445
NEWTON_B = -4.775
NEWTON_C = 2.0315
GELU_SCALE = 0.7978845608028654
GELU_CUBIC = 0.044715
NORM_EPS = 1e-05
STAT_EPS = 1e-06
MASKED_SCORE = -1e+30

def to_low(tensor_in):
    return lax.optimization_barrier(tensor_in.astype(jnp.bfloat16))

def gelu_value(pre_act):
    inner_arg = GELU_SCALE * (pre_act + GELU_CUBIC * pre_act * pre_act * pre_act)
    return 0.5 * pre_act * (1.0 + jnp.tanh(inner_arg))

def gelu_slope(pre_act):
    tanh_val = jnp.tanh(GELU_SCALE * (pre_act + GELU_CUBIC * pre_act * pre_act * pre_act))
    return 0.5 * (1.0 + tanh_val) + 0.5 * pre_act * (1.0 - tanh_val * tanh_val) * GELU_SCALE * (1.0 + 3.0 * GELU_CUBIC * pre_act * pre_act)

def rotary_tables(positions):
    half_dims = ROTARY // 2
    frequency = jnp.exp(jnp.arange(half_dims, dtype=jnp.float32) * (-2.0 * math.log(10000.0) / ROTARY))
    angles = positions.astype(jnp.float32)[:, None] * frequency[None, :]
    return (jnp.cos(angles), jnp.sin(angles))

def rotate(tensor_in, cosine, sine_tab, direction_sign):
    half_dims = ROTARY // 2
    first_half = tensor_in[..., :half_dims]
    second_half = tensor_in[..., half_dims:ROTARY]
    cos_wide = cosine[:, None, :]
    sin_wide = sine_tab[:, None, :] * direction_sign
    return jnp.concatenate([first_half * cos_wide - second_half * sin_wide, second_half * cos_wide + first_half * sin_wide, tensor_in[..., ROTARY:]], axis=-1)

def causal_allowed(segment):
    token_order = jnp.arange(segment.shape[0])
    return (segment[:, None] == segment[None, :]) & (token_order[:, None] >= token_order[None, :])

def masked_scores(queries, key_vecs, segment, score_scale):
    scores = jnp.einsum('lhe,mhe->hlm', queries.astype(jnp.float32), key_vecs.astype(jnp.float32)) * score_scale
    return jnp.where(causal_allowed(segment)[None], scores, MASKED_SCORE)

def attend_forward(queries, key_vecs, values, segment, score_scale):
    scores = masked_scores(queries, key_vecs, segment, score_scale)
    row_max = lax.optimization_barrier(jnp.max(scores, axis=-1, keepdims=True))
    exp_scores = jnp.exp(scores - row_max)
    row_total = lax.optimization_barrier(jnp.sum(exp_scores, axis=-1, keepdims=True))
    probs_low = to_low(exp_scores / row_total)
    attended = jnp.einsum('hlm,mhe->lhe', probs_low.astype(jnp.float32), values.astype(jnp.float32))
    return (attended, (row_max + jnp.log(row_total))[..., 0])

def attend_backward(queries, key_vecs, values, output_low, grad_low, logsum, segment, score_scale):
    scores = masked_scores(queries, key_vecs, segment, score_scale)
    probs = jnp.exp(scores - logsum[..., None])
    grad_values = jnp.einsum('hlm,lhe->mhe', to_low(probs).astype(jnp.float32), grad_low.astype(jnp.float32))
    grad_probs = jnp.einsum('lhe,mhe->hlm', grad_low.astype(jnp.float32), values.astype(jnp.float32))
    row_delta = lax.optimization_barrier(jnp.sum(grad_low.astype(jnp.float32) * output_low.astype(jnp.float32), axis=-1))
    grad_scores = to_low(probs * (grad_probs - row_delta.T[:, :, None]) * score_scale).astype(jnp.float32)
    grad_queries = jnp.einsum('hlm,mhe->lhe', grad_scores, key_vecs.astype(jnp.float32))
    grad_keys = jnp.einsum('hlm,lhe->mhe', grad_scores, queries.astype(jnp.float32))
    return (grad_queries, grad_keys, grad_values)

def newton_schulz(moment):
    iterate = to_low(moment * lax.rsqrt(jnp.sum(moment * moment) + STAT_EPS))
    for newton_step in range(5):
        gram = to_low(jnp.dot(iterate.T, iterate, preferred_element_type=jnp.float32))
        square = jnp.dot(gram, gram, preferred_element_type=jnp.float32)
        poly = to_low(NEWTON_B * gram.astype(jnp.float32) + NEWTON_C * square)
        iterate = to_low(NEWTON_A * iterate.astype(jnp.float32) + jnp.dot(iterate, poly, preferred_element_type=jnp.float32))
    return iterate

def tile_all(w_qkv, w_out, w_up, w_down):

    def attention_tiles(matrix):
        blocks = matrix.reshape(N_COL, TILE_R, N_ROW, 2 * TILE_C).transpose(2, 0, 1, 3)
        return blocks.reshape(N_ROW, N_COL, TILE_R, 2, TILE_C).transpose(0, 1, 3, 2, 4)
    out_blocks = w_out.reshape(N_ROW, D // N_ROW, N_COL, 2 * TILE_C).transpose(0, 2, 1, 3)
    out_tiles = out_blocks.reshape(N_ROW, N_COL, D // N_ROW, 2, TILE_C).transpose(0, 1, 3, 2, 4)
    up_blocks = w_up.reshape(N_COL, TILE_R, N_ROW, FF // N_ROW).transpose(2, 0, 1, 3)
    up_tiles = up_blocks.reshape(N_ROW, N_COL, TILE_R, FF // (N_ROW * TILE_C), TILE_C).transpose(0, 1, 3, 2, 4)
    down_blocks = w_down.reshape(N_ROW, FF // N_ROW, N_COL, D // N_COL).transpose(0, 2, 1, 3)
    down_tiles = down_blocks.reshape(N_ROW, N_COL, FF // (N_ROW * TILE_R), TILE_R, D // N_COL // TILE_C, TILE_C)
    down_tiles = down_tiles.transpose(0, 1, 2, 4, 3, 5).reshape(N_ROW, N_COL, -1, TILE_R, TILE_C)
    return jnp.concatenate([attention_tiles(w_qkv[:, 0]), attention_tiles(w_qkv[:, 1]), attention_tiles(w_qkv[:, 2]), out_tiles, up_tiles, down_tiles], axis=2)

def block_pass(x_low, grad_low, segment, position, w_qkv, w_out, w_up, w_down, vectors):
    row_count = x_low.shape[0]
    seq_count = row_count // SEQ_LEN
    score_scale = HEAD_DIM ** (-0.5)

    def by_seq(tensor_in):
        return tensor_in.reshape((seq_count, SEQ_LEN) + tensor_in.shape[1:])
    x_val = x_low.astype(jnp.float32)
    mean_x = lax.optimization_barrier(jnp.mean(x_val, axis=1, keepdims=True))
    var_x = lax.optimization_barrier(jnp.mean(x_val * x_val, axis=1, keepdims=True)) - mean_x * mean_x
    inv_std = lax.rsqrt(var_x + NORM_EPS)
    x_hat = (x_val - mean_x) * inv_std
    normed = (x_hat * vectors[5] + vectors[6]).astype(jnp.bfloat16)
    qkv_flat = w_qkv.reshape(D, 3 * D)
    mixed_out = jnp.dot(normed, qkv_flat, preferred_element_type=jnp.float32).reshape(row_count, 3, D) + vectors[0:3][None]
    cosine, sine_tab = rotary_tables(position)
    queries = to_low(rotate(mixed_out[:, 0].reshape(row_count, HEADS, HEAD_DIM), cosine, sine_tab, 1.0))
    key_vecs = to_low(rotate(mixed_out[:, 1].reshape(row_count, HEADS, HEAD_DIM), cosine, sine_tab, 1.0))
    values = to_low(mixed_out[:, 2].reshape(row_count, HEADS, HEAD_DIM))
    attended, logsum = lax.map(lambda items: attend_forward(items[0], items[1], items[2], items[3], score_scale), (by_seq(queries), by_seq(key_vecs), by_seq(values), by_seq(segment)))
    attn_low = to_low(attended.reshape(row_count, D))
    up_pre = jnp.dot(normed, w_up, preferred_element_type=jnp.float32) + vectors[7:].reshape(FF)
    act_low = gelu_value(up_pre).astype(jnp.bfloat16)
    branch = jnp.dot(attn_low, w_out, preferred_element_type=jnp.float32) + jnp.dot(act_low, w_down, preferred_element_type=jnp.float32)
    result = x_val + branch + vectors[3] + vectors[4]
    grad_y = grad_low.astype(jnp.float32)
    grad_w_out = jnp.dot(attn_low.T, grad_low, preferred_element_type=jnp.float32)
    grad_w_down = jnp.dot(act_low.T, grad_low, preferred_element_type=jnp.float32)
    grad_attn_low = to_low(jnp.dot(grad_low, w_out.T, preferred_element_type=jnp.float32))
    grad_act = jnp.dot(grad_low, w_down.T, preferred_element_type=jnp.float32)
    grad_up = grad_act * gelu_slope(up_pre)
    grad_up_low = grad_up.astype(jnp.bfloat16)
    g_queries, g_keys, g_values = lax.map(lambda items: attend_backward(items[0], items[1], items[2], items[3], items[4], items[5], items[6], score_scale), (by_seq(queries), by_seq(key_vecs), by_seq(values), by_seq(attn_low.reshape(row_count, HEADS, HEAD_DIM)), by_seq(grad_attn_low.reshape(row_count, HEADS, HEAD_DIM)), logsum, by_seq(segment)))
    g_queries = rotate(g_queries.reshape(row_count, HEADS, HEAD_DIM), cosine, sine_tab, -1.0).reshape(row_count, D)
    g_keys = rotate(g_keys.reshape(row_count, HEADS, HEAD_DIM), cosine, sine_tab, -1.0).reshape(row_count, D)
    g_values = g_values.reshape(row_count, D)
    grad_mixed = jnp.stack([g_queries, g_keys, g_values], axis=1)
    grad_mixed_low = grad_mixed.reshape(row_count, 3 * D).astype(jnp.bfloat16)
    grad_w_qkv = jnp.dot(normed.T, grad_mixed_low, preferred_element_type=jnp.float32).reshape(D, 3, D)
    grad_w_up = jnp.dot(normed.T, grad_up_low, preferred_element_type=jnp.float32)
    grad_norm = jnp.dot(grad_mixed_low, qkv_flat.T, preferred_element_type=jnp.float32) + jnp.dot(grad_up_low, w_up.T, preferred_element_type=jnp.float32)
    grad_hat = grad_norm * vectors[5]
    grad_x = inv_std * (grad_hat - lax.optimization_barrier(jnp.mean(grad_hat, axis=1, keepdims=True)) - x_hat * lax.optimization_barrier(jnp.mean(grad_hat * x_hat, axis=1, keepdims=True)))
    grad_total = grad_y + grad_x
    out_sums = lax.optimization_barrier(jnp.sum(grad_y, axis=0))
    vec_grad = jnp.concatenate([lax.optimization_barrier(jnp.sum(grad_mixed, axis=0)), out_sums[None], out_sums[None], lax.optimization_barrier(jnp.sum(grad_norm * x_hat, axis=0))[None], lax.optimization_barrier(jnp.sum(grad_norm, axis=0))[None], lax.optimization_barrier(jnp.sum(grad_up, axis=0)).reshape(FF // D, D)], axis=0)
    return (result, grad_total, (grad_w_qkv, grad_w_out, grad_w_up, grad_w_down, vec_grad))

def reference(inputs, cotangent, segments, positions, w_qkv, w_out, w_up, w_down, vectors, tile_moment, vector_moment):

    def scan_step(carry, items):
        result, grad_total, grads = block_pass(items[0], items[1], items[2], items[3], w_qkv, w_out, w_up, w_down, vectors)
        return (jax.tree.map(lambda running, fresh: running + fresh, carry, grads), (result, grad_total))
    start_sums = (jnp.zeros((D, 3, D), jnp.float32), jnp.zeros((D, D), jnp.float32), jnp.zeros((D, FF), jnp.float32), jnp.zeros((FF, D), jnp.float32), jnp.zeros((7 + FF // D, D), jnp.float32))
    pieces = (inputs.reshape(N_DP, TOK_DP, D), cotangent.reshape(N_DP, TOK_DP, D), segments.reshape(N_DP, TOK_DP), positions.reshape(N_DP, TOK_DP))
    sums, (result, grad_total) = lax.scan(scan_step, start_sums, pieces)
    grad_tiles = tile_all(sums[0], sums[1], sums[2], sums[3])
    weight_tiles = tile_all(w_qkv.astype(jnp.float32), w_out.astype(jnp.float32), w_up.astype(jnp.float32), w_down.astype(jnp.float32))
    moment_new = MOMENTUM_RATE * tile_moment + grad_tiles
    ortho = lax.map(newton_schulz, moment_new.reshape(-1, TILE_R, TILE_C)).reshape(moment_new.shape)
    tile_ratio = math.sqrt(max(1.0, TILE_R / TILE_C))
    tiles_new = weight_tiles - MUON_RATE * tile_ratio * ortho.astype(jnp.float32)
    vec_grad = sums[4]
    scaled = vec_grad * lax.rsqrt(lax.optimization_barrier(jnp.mean(vec_grad * vec_grad, axis=1, keepdims=True)) + STAT_EPS)
    vec_moment_new = MOMENTUM_RATE * vector_moment + scaled
    vectors_new = vectors - VECTOR_RATE * vec_moment_new
    return (result.reshape(TOKENS, D), grad_total.reshape(TOKENS, D), grad_tiles, tiles_new, moment_new, vec_grad, vectors_new, vec_moment_new)
```

```python
import functools
import math

import jax
import jax.numpy as jnp
from jax import lax
from jax.experimental import pallas as pl
from jax.experimental.pallas import tpu as pltpu
from jax.sharding import PartitionSpec as P

HEAD_DIM = 64
ROTARY = 32
SEQ_LEN = 512

MOMENTUM_RATE = 0.95
MUON_RATE = 0.05
VECTOR_RATE = 0.12
NEWTON_A = 3.4445
NEWTON_B = -4.775
NEWTON_C = 2.0315
GELU_SCALE = 0.7978845608028654
GELU_CUBIC = 0.044715
NORM_EPS = 1e-05
STAT_EPS = 1e-06
MASKED_SCORE = -1e30

MESH = pl.DeviceIdType.MESH
ANY = pl.BlockSpec(memory_space=pl.ANY)
F32 = jnp.float32
BF16 = jnp.bfloat16


def to_low(tensor_in):
    return lax.optimization_barrier(tensor_in.astype(BF16))


def gelu_value(pre_act):
    inner_arg = GELU_SCALE * (pre_act + GELU_CUBIC * pre_act * pre_act * pre_act)
    return 0.5 * pre_act * (1.0 + jnp.tanh(inner_arg))


def gelu_slope(pre_act):
    tanh_val = jnp.tanh(GELU_SCALE * (pre_act + GELU_CUBIC * pre_act * pre_act * pre_act))
    return 0.5 * (1.0 + tanh_val) + 0.5 * pre_act * (1.0 - tanh_val * tanh_val) * GELU_SCALE * (
        1.0 + 3.0 * GELU_CUBIC * pre_act * pre_act
    )


def rotary_tables(positions):
    half_dims = ROTARY // 2
    frequency = jnp.exp(jnp.arange(half_dims, dtype=F32) * (-2.0 * math.log(10000.0) / ROTARY))
    angles = positions.astype(F32)[:, None] * frequency[None, :]
    return (jnp.cos(angles), jnp.sin(angles))


def rotate(tensor_in, cosine, sine_tab, direction_sign):
    half_dims = ROTARY // 2
    first_half = tensor_in[..., :half_dims]
    second_half = tensor_in[..., half_dims:ROTARY]
    cos_wide = cosine[:, None, :]
    sin_wide = sine_tab[:, None, :] * direction_sign
    return jnp.concatenate(
        [
            first_half * cos_wide - second_half * sin_wide,
            second_half * cos_wide + first_half * sin_wide,
            tensor_in[..., ROTARY:],
        ],
        axis=-1,
    )


def causal_allowed(segment):
    token_order = jnp.arange(segment.shape[0])
    return (segment[:, None] == segment[None, :]) & (token_order[:, None] >= token_order[None, :])


def masked_scores(queries, key_vecs, segment, score_scale):
    scores = (
        jnp.einsum("lhe,mhe->hlm", queries, key_vecs, preferred_element_type=F32) * score_scale
    )
    return jnp.where(causal_allowed(segment)[None], scores, MASKED_SCORE)


def attend_forward(queries, key_vecs, values, segment, score_scale):
    scores = masked_scores(queries, key_vecs, segment, score_scale)
    row_max = jnp.max(scores, axis=-1, keepdims=True)
    exp_scores = jnp.exp(scores - row_max)
    row_total = jnp.sum(exp_scores, axis=-1, keepdims=True)
    probs_low = to_low(exp_scores / row_total)
    attended = jnp.einsum("hlm,mhe->lhe", probs_low, values, preferred_element_type=F32)
    return (attended, (row_max + jnp.log(row_total))[..., 0])


def attend_backward(queries, key_vecs, values, output_low, grad_low, logsum, segment, score_scale):
    scores = masked_scores(queries, key_vecs, segment, score_scale)
    probs = jnp.exp(scores - logsum[..., None])
    grad_values = jnp.einsum("hlm,lhe->mhe", to_low(probs), grad_low, preferred_element_type=F32)
    grad_probs = jnp.einsum("lhe,mhe->hlm", grad_low, values, preferred_element_type=F32)
    row_delta = jnp.sum(grad_low.astype(F32) * output_low.astype(F32), axis=-1)
    grad_scores = to_low(probs * (grad_probs - row_delta.T[:, :, None]) * score_scale)
    grad_queries = jnp.einsum("hlm,mhe->lhe", grad_scores, key_vecs, preferred_element_type=F32)
    grad_keys = jnp.einsum("hlm,lhe->mhe", grad_scores, queries, preferred_element_type=F32)
    return (grad_queries, grad_keys, grad_values)


def newton_schulz(moment):
    iterate = to_low(moment * lax.rsqrt(jnp.sum(moment * moment) + STAT_EPS))
    for newton_step in range(5):
        gram = to_low(jnp.dot(iterate.T, iterate, preferred_element_type=F32))
        square = jnp.dot(gram, gram, preferred_element_type=F32)
        poly = to_low(NEWTON_B * gram.astype(F32) + NEWTON_C * square)
        iterate = to_low(
            NEWTON_A * iterate.astype(F32) + jnp.dot(iterate, poly, preferred_element_type=F32)
        )
    return iterate


def tile_blocks(qkv_block, out_block, up_block, down_block):
    tile_rows = qkv_block.shape[0]
    tile_cols = qkv_block.shape[2] // 2

    def split_cols(block_in):
        return block_in.reshape(
            block_in.shape[0], block_in.shape[1] // tile_cols, tile_cols
        ).transpose(1, 0, 2)

    down_part = down_block.reshape(
        down_block.shape[0] // tile_rows, tile_rows, down_block.shape[1] // tile_cols, tile_cols
    )
    down_part = down_part.transpose(0, 2, 1, 3).reshape(-1, tile_rows, tile_cols)
    return jnp.concatenate(
        [
            split_cols(qkv_block[:, 0]),
            split_cols(qkv_block[:, 1]),
            split_cols(qkv_block[:, 2]),
            split_cols(out_block),
            split_cols(up_block),
            down_part,
        ],
        axis=0,
    )


def gather_kernel(n_dp, n_row, n_col, dims, x_ref, g_ref, wq_ref, wu_ref, wo_ref, wd_ref,
                  xf, gf, wi, wf, stage_x, stage_q, stage_u, stage_o, stage_d,
                  zs, zr, ys, yr, cs, cr, ws, wr, ds, dr, ls, lo):
    T, C, HF, UT = dims
    d, r, c = lax.axis_index("dp"), lax.axis_index("row"), lax.axis_index("col")
    chunks = 2
    tc = T // chunks
    qw = 3 * HF
    acts = ((x_ref, xf), (g_ref, gf))

    def blk(a, rr, cc, t):
        return acts[a][1].at[pl.ds(rr * T + t * tc, tc), pl.ds(cc * C, C)]

    barrier = pltpu.get_barrier_semaphore()
    peers = [{"row": r ^ 1}, {"row": r ^ 2}]
    peers += [{"col": lax.rem(c + k, n_col)} for k in range(1, n_col)]
    peers += [{"dp": lax.rem(d + k, n_dp)} for k in range(1, n_dp)]
    for peer in peers:
        pl.semaphore_signal(barrier, inc=1, device_id=peer, device_id_type=MESH)
    pl.semaphore_wait(barrier, len(peers))

    def own(a, t):
        return acts[a][0].at[pl.ds(t * tc, tc), :]

    def copy(src, dst, s, rcv, peer):
        return pltpu.make_async_remote_copy(
            src_ref=src, dst_ref=dst, send_sem=s, recv_sem=rcv, device_id=peer, device_id_type=MESH
        )

    def z_copy(a, t, cc, src, right):
        peer = {"col": c + 1} if right else {"col": c - 1}
        return copy(src, blk(a, r, cc, t), zs.at[a, t, int(right), cc], zr.at[a, t, cc], peer)

    def y_copy(a, t, cc, src):
        return copy(src, blk(a, r, cc, t), ys.at[a, t, cc], yr.at[a, t, cc], {"row": r ^ 2})

    def c_copy(a, t, cc, src, rr, which):
        return copy(
            src, blk(a, rr, cc, t), cs.at[a, t, which, cc], cr.at[a, t, which, cc], {"row": r ^ 1}
        )

    order = [(a, t) for a in range(2) for t in range(chunks)]

    for a, t in order:
        @pl.when(c < n_col - 1)
        def _(a=a, t=t):
            z_copy(a, t, c, own(a, t), True).start()

        @pl.when(c > 0)
        def _(a=a, t=t):
            z_copy(a, t, c, own(a, t), False).start()

        y_copy(a, t, c, own(a, t)).start()
        c_copy(a, t, c, own(a, t), r, 0).start()

    loads = [
        pltpu.make_async_copy(x_ref, stage_x.at[0], ls.at[0]),
        pltpu.make_async_copy(g_ref, stage_x.at[1], ls.at[1]),
        pltpu.make_async_copy(wq_ref.at[c], stage_q, ls.at[2]),
        pltpu.make_async_copy(wu_ref.at[:, pl.ds(c * UT, UT)], stage_u.at[0], ls.at[3]),
        pltpu.make_async_copy(
            wu_ref.at[:, pl.ds((n_col + c) * UT, UT)], stage_u.at[1], ls.at[4]
        ),
        pltpu.make_async_copy(wo_ref.at[pl.ds(c * HF, HF), :], stage_o, ls.at[5]),
        pltpu.make_async_copy(wd_ref.at[pl.ds(c * UT, UT), :], stage_d.at[0], ls.at[6]),
        pltpu.make_async_copy(wd_ref.at[pl.ds((n_col + c) * UT, UT), :], stage_d.at[1], ls.at[7]),
    ]
    for item in loads:
        item.start()
    stores = [
        pltpu.make_async_copy(stage_x.at[0], xf.at[pl.ds(r * T, T), pl.ds(c * C, C)], lo.at[0]),
        pltpu.make_async_copy(stage_x.at[1], gf.at[pl.ds(r * T, T), pl.ds(c * C, C)], lo.at[1]),
        pltpu.make_async_copy(stage_q, wi.at[pl.ds(c * C, C), pl.ds(0, qw)], lo.at[2]),
        pltpu.make_async_copy(stage_u.at[0], wi.at[pl.ds(c * C, C), pl.ds(qw, UT)], lo.at[3]),
        pltpu.make_async_copy(stage_u.at[1], wi.at[pl.ds(c * C, C), pl.ds(qw + UT, UT)], lo.at[4]),
        pltpu.make_async_copy(stage_o, wf.at[pl.ds(0, HF), pl.ds(c * C, C)], lo.at[5]),
        pltpu.make_async_copy(stage_d.at[0], wf.at[pl.ds(HF, UT), pl.ds(c * C, C)], lo.at[6]),
        pltpu.make_async_copy(stage_d.at[1], wf.at[pl.ds(HF + UT, UT), pl.ds(c * C, C)], lo.at[7]),
    ]
    for load, store in zip(loads, stores):
        load.wait()
        store.start()

    ck, hk, uk = C // n_dp, HF // n_dp, UT // n_dp

    def w_dst(part, dd, cc):
        if part == 0:
            return wi.at[pl.ds(cc * C + dd * ck, ck), pl.ds(0, qw)]
        if part == 1:
            return wi.at[pl.ds(cc * C + dd * ck, ck), pl.ds(qw, UT)]
        if part == 2:
            return wi.at[pl.ds(cc * C + dd * ck, ck), pl.ds(qw + UT, UT)]
        if part == 3:
            return wf.at[pl.ds(dd * hk, hk), pl.ds(cc * C, C)]
        if part == 4:
            return wf.at[pl.ds(HF + dd * uk, uk), pl.ds(cc * C, C)]
        return wf.at[pl.ds(HF + UT + dd * uk, uk), pl.ds(cc * C, C)]

    def w_src(part, cc):
        if part == 0:
            return wq_ref.at[cc, pl.ds(d * ck, ck), :]
        if part == 1:
            return wu_ref.at[pl.ds(d * ck, ck), pl.ds(cc * UT, UT)]
        if part == 2:
            return wu_ref.at[pl.ds(d * ck, ck), pl.ds((n_col + cc) * UT, UT)]
        if part == 3:
            return wo_ref.at[pl.ds(cc * HF + d * hk, hk), :]
        if part == 4:
            return wd_ref.at[pl.ds(cc * UT + d * uk, uk), :]
        return wd_ref.at[pl.ds((n_col + cc) * UT + d * uk, uk), :]

    def w_copy(part, k):
        dest = lax.rem(c + k, n_col)
        return copy(
            w_src(part, dest), w_dst(part, d, c), ws.at[part, k], wr.at[part, k], {"col": dest}
        )

    def w_got(part, k):
        return w_dst(part, d, lax.rem(c + n_col - k, n_col))

    def x_copy(part, k, j):
        return copy(
            w_got(part, k), w_got(part, k), ds.at[part, k, j], dr.at[part, k, j],
            {"dp": lax.rem(d + j, n_dp)},
        )

    parts = range(6)

    for s in range(1, n_col):
        for a, t in order:
            @pl.when(c - s >= 0)
            def _(a=a, t=t, s=s):
                cc = c - s
                z_copy(a, t, cc, blk(a, r, cc, t), True).wait_recv()

                @pl.when(c < n_col - 1)
                def _():
                    z_copy(a, t, cc, blk(a, r, cc, t), True).start()

                y_copy(a, t, cc, blk(a, r, cc, t)).start()
                c_copy(a, t, cc, blk(a, r, cc, t), r, 0).start()

            @pl.when(c + s < n_col)
            def _(a=a, t=t, s=s):
                cc = c + s
                z_copy(a, t, cc, blk(a, r, cc, t), False).wait_recv()

                @pl.when(c > 0)
                def _():
                    z_copy(a, t, cc, blk(a, r, cc, t), False).start()

                y_copy(a, t, cc, blk(a, r, cc, t)).start()
                c_copy(a, t, cc, blk(a, r, cc, t), r, 0).start()

        for part in parts:
            w_copy(part, s).start()

    for s in range(n_col):
        for a, t in order:
            for cc in ((c,) if s == 0 else (c - s, c + s)):
                @pl.when((cc >= 0) & (cc < n_col))
                def _(a=a, t=t, cc=cc):
                    y_copy(a, t, cc, blk(a, r, cc, t)).wait_recv()
                    c_copy(a, t, cc, blk(a, r ^ 2, cc, t), r ^ 2, 1).start()

    for k in range(1, n_col):
        for part in parts:
            w_copy(part, k).wait_recv()
            for j in range(1, n_dp):
                x_copy(part, k, j).start()

    for a, t in order:
        for cc in range(n_col):
            c_copy(a, t, cc, blk(a, r, cc, t), r, 0).wait_recv()
            c_copy(a, t, cc, blk(a, r, cc, t), r, 1).wait_recv()
    for k in range(1, n_col):
        for part in parts:
            for j in range(1, n_dp):
                x_copy(part, k, j).wait_recv()
    for a, t in order:
        for cc in range(n_col):
            @pl.when((cc <= c) & (c < n_col - 1))
            def _(a=a, t=t, cc=cc):
                z_copy(a, t, cc, blk(a, r, cc, t), True).wait_send()

            @pl.when((cc >= c) & (c > 0))
            def _(a=a, t=t, cc=cc):
                z_copy(a, t, cc, blk(a, r, cc, t), False).wait_send()

            y_copy(a, t, cc, blk(a, r, cc, t)).wait_send()
            c_copy(a, t, cc, blk(a, r, cc, t), r, 0).wait_send()
            c_copy(a, t, cc, blk(a, r, cc, t), r, 1).wait_send()
    for k in range(1, n_col):
        for part in parts:
            w_copy(part, k).wait_send()
            for j in range(1, n_dp):
                x_copy(part, k, j).wait_send()
    for store in stores:
        store.wait()


def gather_all(x, g, w_q, w_up, w_out, w_down, n_dp, n_row, n_col):
    T, C = x.shape
    HF = w_q.shape[2] // 3
    UT = w_up.shape[1] // (2 * n_col)
    n_in, n_out = 3 * HF + 2 * UT, HF + 2 * UT
    dma = pltpu.SemaphoreType.DMA
    return pl.pallas_call(
        functools.partial(gather_kernel, n_dp, n_row, n_col, (T, C, HF, UT)),
        name="gather_all",
        out_shape=(
            jax.ShapeDtypeStruct((n_row * T, n_col * C), BF16),
            jax.ShapeDtypeStruct((n_row * T, n_col * C), BF16),
            jax.ShapeDtypeStruct((n_col * C, n_in), BF16),
            jax.ShapeDtypeStruct((n_out, n_col * C), BF16),
        ),
        in_specs=[ANY] * 6,
        out_specs=(ANY,) * 4,
        scratch_shapes=[
            pltpu.VMEM((2, T, C), BF16),
            pltpu.VMEM((C, 3 * HF), BF16),
            pltpu.VMEM((2, C, UT), BF16),
            pltpu.VMEM((HF, C), BF16),
            pltpu.VMEM((2, UT, C), BF16),
            dma((2, 2, 2, n_col)),
            dma((2, 2, n_col)),
            dma((2, 2, n_col)),
            dma((2, 2, n_col)),
            dma((2, 2, 2, n_col)),
            dma((2, 2, 2, n_col)),
            dma((6, n_col)),
            dma((6, n_col)),
            dma((6, n_col, n_dp)),
            dma((6, n_col, n_dp)),
            dma((8,)),
            dma((8,)),
        ],
        compiler_params=pltpu.CompilerParams(collective_id=0, has_side_effects=True),
    )(x, g, w_q, w_up, w_out, w_down)


def body(
    inputs,
    cotangent,
    segments,
    positions,
    w_qkv,
    w_out,
    w_up,
    w_down,
    vectors,
    tile_moment,
    vector_moment,
):
    d_index = lax.axis_index("dp")
    row_index = lax.axis_index("row")
    col_index = lax.axis_index("col")
    n_dp, n_row, n_col = lax.axis_size("dp"), lax.axis_size("row"), lax.axis_size("col")
    T, C = inputs.shape
    D = vectors.shape[1]
    row_width = w_qkv.shape[2]
    HF = row_width // n_col
    UT = w_up.shape[1] // (2 * n_col)
    score_scale = HEAD_DIM ** (-0.5)
    feat_start = (row_index * n_col + col_index) * HF
    unit_a = (row_index * 2 * n_col + col_index) * UT
    unit_b = unit_a + n_col * UT
    col_start = col_index * C
    gain, shift = vectors[5], vectors[6]
    norm_gain = lax.dynamic_slice_in_dim(gain, col_start, C)
    out_bias = lax.dynamic_slice_in_dim(vectors[3] + vectors[4], col_start, C)
    qkv_bias = lax.dynamic_slice_in_dim(vectors[0:3], feat_start, HF, axis=1)
    up_flat = vectors[7:].reshape(-1)
    up_bias = jnp.concatenate(
        [
            lax.dynamic_slice_in_dim(up_flat, unit_a, UT),
            lax.dynamic_slice_in_dim(up_flat, unit_b, UT),
        ]
    )
    w_q = (
        w_qkv.reshape(C, 3, n_col, HF).transpose(2, 0, 1, 3).reshape(n_col, C, 3 * HF)
    )
    x_full, cot_rows, w_in, w_fin = gather_all(
        inputs, cotangent, w_q, w_up, w_out, w_down, n_dp, n_row, n_col
    )
    seq_rows = x_full.shape[0]

    x_wide = x_full.astype(F32)
    mean_all = jnp.mean(x_wide, axis=1, keepdims=True)
    var_all = jnp.mean(x_wide * x_wide, axis=1, keepdims=True) - mean_all * mean_all
    rstd_all = lax.rsqrt(var_all + NORM_EPS)
    normed = ((x_wide - mean_all) * rstd_all * gain + shift).astype(BF16)

    mixed_out = jnp.dot(normed, w_in, preferred_element_type=F32)
    qkv_part = mixed_out[:, : 3 * HF].reshape(seq_rows, 3, HF) + qkv_bias[None]
    up_pre = mixed_out[:, 3 * HF :] + up_bias
    heads_here = HF // HEAD_DIM
    seq_count = seq_rows // SEQ_LEN

    def by_seq(tensor_in):
        return tensor_in.reshape((seq_count, SEQ_LEN) + tensor_in.shape[1:])

    cosine, sine_tab = rotary_tables(positions)
    queries = rotate(
        qkv_part[:, 0].reshape(seq_rows, heads_here, HEAD_DIM), cosine, sine_tab, 1.0
    ).astype(BF16)
    key_vecs = rotate(
        qkv_part[:, 1].reshape(seq_rows, heads_here, HEAD_DIM), cosine, sine_tab, 1.0
    ).astype(BF16)
    values = qkv_part[:, 2].reshape(seq_rows, heads_here, HEAD_DIM).astype(BF16)
    attended, logsum = jax.vmap(attend_forward, in_axes=(0, 0, 0, 0, None))(
        by_seq(queries), by_seq(key_vecs), by_seq(values), by_seq(segments), score_scale
    )
    attn_low = attended.reshape(seq_rows, HF).astype(BF16)
    act_low = gelu_value(up_pre).astype(BF16)
    hidden = jnp.concatenate([attn_low, act_low], axis=1)

    partial_out = jnp.dot(hidden, w_fin, preferred_element_type=F32).astype(BF16)
    branch = lax.psum_scatter(partial_out, "row", scatter_dimension=0, tiled=True)
    branch = lax.psum_scatter(branch, "col", scatter_dimension=1, tiled=True).astype(F32)
    x_val = inputs.astype(F32)
    result = x_val + branch + out_bias

    cot_val = cotangent.astype(F32)
    grad_w_fin = jnp.einsum("ti,tj->ij", hidden, cot_rows, preferred_element_type=F32).astype(BF16)
    back = jnp.einsum("tj,ij->ti", cot_rows, w_fin, preferred_element_type=F32)
    grad_attn_low = back[:, :HF].astype(BF16)
    grad_up = back[:, HF:] * gelu_slope(up_pre)
    g_queries, g_keys, g_values = jax.vmap(attend_backward, in_axes=(0, 0, 0, 0, 0, 0, 0, None))(
        by_seq(queries),
        by_seq(key_vecs),
        by_seq(values),
        by_seq(attn_low.reshape(seq_rows, heads_here, HEAD_DIM)),
        by_seq(grad_attn_low.reshape(seq_rows, heads_here, HEAD_DIM)),
        logsum,
        by_seq(segments),
        score_scale,
    )
    g_queries = rotate(
        g_queries.reshape(seq_rows, heads_here, HEAD_DIM), cosine, sine_tab, -1.0
    ).reshape(seq_rows, HF)
    g_keys = rotate(g_keys.reshape(seq_rows, heads_here, HEAD_DIM), cosine, sine_tab, -1.0).reshape(
        seq_rows, HF
    )
    g_values = g_values.reshape(seq_rows, HF)
    grad_mixed = jnp.concatenate([g_queries, g_keys, g_values, grad_up], axis=1)
    grad_mixed_low = grad_mixed.astype(BF16)
    grad_w_in = jnp.einsum(
        "ti,tj->ij", normed, grad_mixed_low, preferred_element_type=F32
    ).astype(BF16)
    partial_norm = jnp.einsum(
        "tj,ij->ti", grad_mixed_low, w_in, preferred_element_type=F32
    ).astype(BF16)
    grad_norm = lax.psum_scatter(partial_norm, "row", scatter_dimension=0, tiled=True)
    grad_norm = lax.psum_scatter(grad_norm, "col", scatter_dimension=1, tiled=True).astype(F32)

    mean_x = lax.dynamic_slice_in_dim(mean_all, row_index * T, T)
    inv_std = lax.dynamic_slice_in_dim(rstd_all, row_index * T, T)
    x_hat = (x_val - mean_x) * inv_std
    grad_hat = grad_norm * norm_gain
    back_stats = lax.psum((jnp.sum(grad_hat, axis=1), jnp.sum(grad_hat * x_hat, axis=1)), "col")
    grad_x = inv_std * (
        grad_hat - (back_stats[0] / D)[:, None] - x_hat * (back_stats[1] / D)[:, None]
    )
    grad_input = cot_val + grad_x

    sums = jnp.sum(grad_mixed, axis=0)
    qkv_sums = sums[: 3 * HF].reshape(3, HF)
    out_sums = jnp.sum(cot_val, axis=0)
    norm_sums = jnp.stack(
        [out_sums, out_sums, jnp.sum(grad_norm * x_hat, axis=0), jnp.sum(grad_norm, axis=0)]
    )
    qkv_rows = lax.dynamic_update_slice_in_dim(
        jnp.zeros((3, D), F32), qkv_sums, feat_start, axis=1
    )
    norm_rows = lax.dynamic_update_slice_in_dim(
        jnp.zeros((4, D), F32), norm_sums, col_start, axis=1
    )
    up_rows = jnp.zeros((up_flat.shape[0],), F32)
    up_rows = lax.dynamic_update_slice_in_dim(up_rows, sums[3 * HF : 3 * HF + UT], unit_a, axis=0)
    up_rows = lax.dynamic_update_slice_in_dim(up_rows, sums[3 * HF + UT :], unit_b, axis=0)
    local_vec = jnp.concatenate([qkv_rows, norm_rows, up_rows.reshape(-1, D)], axis=0)
    vec_grad = lax.psum(local_vec, ("dp", "row", "col"))
    scaled = vec_grad * lax.rsqrt(jnp.mean(vec_grad * vec_grad, axis=1, keepdims=True) + STAT_EPS)
    vec_moment_new = MOMENTUM_RATE * vector_moment + scaled
    vectors_new = vectors - VECTOR_RATE * vec_moment_new

    wi4 = lax.all_to_all(grad_w_in.reshape(n_col, C, -1), "col", 0, 0)
    wf4 = lax.all_to_all(
        grad_w_fin.reshape(-1, n_col, C).transpose(1, 0, 2), "col", 0, 0
    )
    grad_qkv = (
        wi4[:, :, : 3 * HF].reshape(n_col, C, 3, HF).transpose(1, 2, 0, 3).reshape(C, 3, row_width)
    )
    grad_up_w = (
        wi4[:, :, 3 * HF :].reshape(n_col, C, 2, UT).transpose(1, 2, 0, 3).reshape(C, -1)
    )
    grad_w_out = wf4[:, :HF].reshape(-1, C)
    grad_w_down = wf4[:, HF:].reshape(n_col, 2, UT, C).transpose(1, 0, 2, 3).reshape(-1, C)
    grad_tiles = tile_blocks(grad_qkv, grad_w_out, grad_up_w, grad_w_down)
    owned_grads = lax.psum_scatter(grad_tiles, "dp", scatter_dimension=0, tiled=True).astype(F32)
    owned_count = owned_grads.shape[0]
    weight_tiles = lax.dynamic_slice_in_dim(
        tile_blocks(w_qkv, w_out, w_up, w_down), d_index * owned_count, owned_count, 0
    ).astype(F32)
    moment_new = MOMENTUM_RATE * tile_moment[0, 0] + owned_grads
    ortho_tiles = jax.vmap(newton_schulz)(moment_new)
    tile_ratio = math.sqrt(max(1.0, moment_new.shape[1] / moment_new.shape[2]))
    tiles_new = weight_tiles - MUON_RATE * tile_ratio * ortho_tiles.astype(F32)
    return (
        result,
        grad_input,
        owned_grads[None, None],
        tiles_new[None, None],
        moment_new[None, None],
        vec_grad,
        vectors_new,
        vec_moment_new,
    )


def solution(mesh):
    placed = (
        P(("dp", "row"), "col"),
        P(("dp", "row"), "col"),
        P("dp"),
        P("dp"),
        P("col", None, "row"),
        P("row", "col"),
        P("col", "row"),
        P("row", "col"),
        P(),
        P("row", "col", "dp", None, None),
        P(),
    )
    return jax.shard_map(
        body,
        mesh=mesh,
        in_specs=placed,
        out_specs=(
            P(("dp", "row"), "col"),
            P(("dp", "row"), "col"),
            P("row", "col", "dp", None, None),
            P("row", "col", "dp", None, None),
            P("row", "col", "dp", None, None),
            P(),
            P(),
            P(),
        ),
        check_vma=False,
    )
```

```python
import functools
import math

import jax
import jax.numpy as jnp
from jax import lax
from jax.experimental import pallas as pl
from jax.experimental.pallas import tpu as pltpu
from jax.sharding import PartitionSpec as P

HEAD_DIM = 64
ROTARY = 32
SEQ_LEN = 512

MOMENTUM_RATE = 0.95
MUON_RATE = 0.05
VECTOR_RATE = 0.12
NEWTON_A = 3.4445
NEWTON_B = -4.775
NEWTON_C = 2.0315
GELU_SCALE = 0.7978845608028654
GELU_CUBIC = 0.044715
NORM_EPS = 1e-05
STAT_EPS = 1e-06
MASKED_SCORE = -1e30

MESH = pl.DeviceIdType.MESH
ANY = pl.BlockSpec(memory_space=pl.ANY)
F32 = jnp.float32
BF16 = jnp.bfloat16


def to_low(tensor_in):
    return lax.optimization_barrier(tensor_in.astype(BF16))


def gelu_value(pre_act):
    inner_arg = GELU_SCALE * (pre_act + GELU_CUBIC * pre_act * pre_act * pre_act)
    return 0.5 * pre_act * (1.0 + jnp.tanh(inner_arg))


def gelu_slope(pre_act):
    tanh_val = jnp.tanh(GELU_SCALE * (pre_act + GELU_CUBIC * pre_act * pre_act * pre_act))
    return 0.5 * (1.0 + tanh_val) + 0.5 * pre_act * (1.0 - tanh_val * tanh_val) * GELU_SCALE * (
        1.0 + 3.0 * GELU_CUBIC * pre_act * pre_act
    )


def rotary_tables(positions):
    half_dims = ROTARY // 2
    frequency = jnp.exp(jnp.arange(half_dims, dtype=F32) * (-2.0 * math.log(10000.0) / ROTARY))
    angles = positions.astype(F32)[:, None] * frequency[None, :]
    return (jnp.cos(angles), jnp.sin(angles))


def rotate(tensor_in, cosine, sine_tab, direction_sign):
    half_dims = ROTARY // 2
    first_half = tensor_in[..., :half_dims]
    second_half = tensor_in[..., half_dims:ROTARY]
    cos_wide = cosine[:, None, :]
    sin_wide = sine_tab[:, None, :] * direction_sign
    return jnp.concatenate(
        [
            first_half * cos_wide - second_half * sin_wide,
            second_half * cos_wide + first_half * sin_wide,
            tensor_in[..., ROTARY:],
        ],
        axis=-1,
    )


def causal_allowed(segment):
    token_order = jnp.arange(segment.shape[0])
    return (segment[:, None] == segment[None, :]) & (token_order[:, None] >= token_order[None, :])


def masked_scores(queries, key_vecs, segment, score_scale):
    scores = (
        jnp.einsum("lhe,mhe->hlm", queries, key_vecs, preferred_element_type=F32) * score_scale
    )
    return jnp.where(causal_allowed(segment)[None], scores, MASKED_SCORE)


def attend_forward(queries, key_vecs, values, segment, score_scale):
    scores = masked_scores(queries, key_vecs, segment, score_scale)
    row_max = jnp.max(scores, axis=-1, keepdims=True)
    exp_scores = jnp.exp(scores - row_max)
    row_total = jnp.sum(exp_scores, axis=-1, keepdims=True)
    probs_low = to_low(exp_scores / row_total)
    attended = jnp.einsum("hlm,mhe->lhe", probs_low, values, preferred_element_type=F32)
    return (attended, (row_max + jnp.log(row_total))[..., 0])


def attend_backward(queries, key_vecs, values, output_low, grad_low, logsum, segment, score_scale):
    scores = masked_scores(queries, key_vecs, segment, score_scale)
    probs = jnp.exp(scores - logsum[..., None])
    grad_values = jnp.einsum("hlm,lhe->mhe", to_low(probs), grad_low, preferred_element_type=F32)
    grad_probs = jnp.einsum("lhe,mhe->hlm", grad_low, values, preferred_element_type=F32)
    row_delta = jnp.sum(grad_low.astype(F32) * output_low.astype(F32), axis=-1)
    grad_scores = to_low(probs * (grad_probs - row_delta.T[:, :, None]) * score_scale)
    grad_queries = jnp.einsum("hlm,mhe->lhe", grad_scores, key_vecs, preferred_element_type=F32)
    grad_keys = jnp.einsum("hlm,lhe->mhe", grad_scores, queries, preferred_element_type=F32)
    return (grad_queries, grad_keys, grad_values)


def newton_schulz(moment):
    iterate = to_low(moment * lax.rsqrt(jnp.sum(moment * moment) + STAT_EPS))
    for newton_step in range(5):
        gram = to_low(jnp.dot(iterate.T, iterate, preferred_element_type=F32))
        square = jnp.dot(gram, gram, preferred_element_type=F32)
        poly = to_low(NEWTON_B * gram.astype(F32) + NEWTON_C * square)
        iterate = to_low(
            NEWTON_A * iterate.astype(F32) + jnp.dot(iterate, poly, preferred_element_type=F32)
        )
    return iterate


def tile_blocks(qkv_block, out_block, up_block, down_block):
    tile_rows = qkv_block.shape[0]
    tile_cols = qkv_block.shape[2] // 2

    def split_cols(block_in):
        return block_in.reshape(
            block_in.shape[0], block_in.shape[1] // tile_cols, tile_cols
        ).transpose(1, 0, 2)

    down_part = down_block.reshape(
        down_block.shape[0] // tile_rows, tile_rows, down_block.shape[1] // tile_cols, tile_cols
    )
    down_part = down_part.transpose(0, 2, 1, 3).reshape(-1, tile_rows, tile_cols)
    return jnp.concatenate(
        [
            split_cols(qkv_block[:, 0]),
            split_cols(qkv_block[:, 1]),
            split_cols(qkv_block[:, 2]),
            split_cols(out_block),
            split_cols(up_block),
            down_part,
        ],
        axis=0,
    )


def gather_kernel(n_dp, n_row, n_col, dims, x_ref, g_ref, wq_ref, wu_ref, wo_ref, wd_ref,
                  xf, gf, wi, wf, stage_x, stage_q, stage_u, stage_o, stage_d,
                  zs, zr, ys, yr, cs, cr, ws, wr, ds, dr, ls, lo):
    T, C, HF, UT = dims
    d, r, c = lax.axis_index("dp"), lax.axis_index("row"), lax.axis_index("col")
    r1 = r + 1 - 2 * lax.rem(r, 2)
    r2 = lax.rem(r + 2, n_row)
    chunks = 2
    tc = T // chunks
    qw = 3 * HF
    acts = ((x_ref, xf), (g_ref, gf))

    def blk(a, rr, cc, t):
        return acts[a][1].at[pl.ds(rr * T + t * tc, tc), pl.ds(cc * C, C)]

    barrier = pltpu.get_barrier_semaphore()
    peers = [{"row": r1}, {"row": r2}]
    peers += [{"col": lax.rem(c + k, n_col)} for k in range(1, n_col)]
    peers += [{"dp": lax.rem(d + k, n_dp)} for k in range(1, n_dp)]
    for peer in peers:
        pl.semaphore_signal(barrier, inc=1, device_id=peer, device_id_type=MESH)
    pl.semaphore_wait(barrier, len(peers))

    def own(a, t):
        return acts[a][0].at[pl.ds(t * tc, tc), :]

    def copy(src, dst, s, rcv, peer):
        return pltpu.make_async_remote_copy(
            src_ref=src, dst_ref=dst, send_sem=s, recv_sem=rcv, device_id=peer, device_id_type=MESH
        )

    def z_copy(a, t, cc, src, right):
        peer = {"col": c + 1} if right else {"col": c - 1}
        return copy(src, blk(a, r, cc, t), zs.at[a, t, int(right), cc], zr.at[a, t, cc], peer)

    def y_copy(a, t, cc, src):
        return copy(src, blk(a, r, cc, t), ys.at[a, t, cc], yr.at[a, t, cc], {"row": r2})

    def c_copy(a, t, cc, src, rr, which):
        return copy(
            src, blk(a, rr, cc, t), cs.at[a, t, which, cc], cr.at[a, t, which, cc], {"row": r1}
        )

    order = [(a, t) for a in range(2) for t in range(chunks)]

    for a, t in order:
        @pl.when(c < n_col - 1)
        def _(a=a, t=t):
            z_copy(a, t, c, own(a, t), True).start()

        @pl.when(c > 0)
        def _(a=a, t=t):
            z_copy(a, t, c, own(a, t), False).start()

        y_copy(a, t, c, own(a, t)).start()
        c_copy(a, t, c, own(a, t), r, 0).start()

    loads = [
        pltpu.make_async_copy(x_ref, stage_x.at[0], ls.at[0]),
        pltpu.make_async_copy(g_ref, stage_x.at[1], ls.at[1]),
        pltpu.make_async_copy(wq_ref.at[c], stage_q, ls.at[2]),
        pltpu.make_async_copy(wu_ref.at[:, pl.ds(c * UT, UT)], stage_u.at[0], ls.at[3]),
        pltpu.make_async_copy(
            wu_ref.at[:, pl.ds((n_col + c) * UT, UT)], stage_u.at[1], ls.at[4]
        ),
        pltpu.make_async_copy(wo_ref.at[pl.ds(c * HF, HF), :], stage_o, ls.at[5]),
        pltpu.make_async_copy(wd_ref.at[pl.ds(c * UT, UT), :], stage_d.at[0], ls.at[6]),
        pltpu.make_async_copy(wd_ref.at[pl.ds((n_col + c) * UT, UT), :], stage_d.at[1], ls.at[7]),
    ]
    for item in loads:
        item.start()
    stores = [
        pltpu.make_async_copy(stage_x.at[0], xf.at[pl.ds(r * T, T), pl.ds(c * C, C)], lo.at[0]),
        pltpu.make_async_copy(stage_x.at[1], gf.at[pl.ds(r * T, T), pl.ds(c * C, C)], lo.at[1]),
        pltpu.make_async_copy(stage_q, wi.at[pl.ds(c * C, C), pl.ds(0, qw)], lo.at[2]),
        pltpu.make_async_copy(stage_u.at[0], wi.at[pl.ds(c * C, C), pl.ds(qw, UT)], lo.at[3]),
        pltpu.make_async_copy(stage_u.at[1], wi.at[pl.ds(c * C, C), pl.ds(qw + UT, UT)], lo.at[4]),
        pltpu.make_async_copy(stage_o, wf.at[pl.ds(0, HF), pl.ds(c * C, C)], lo.at[5]),
        pltpu.make_async_copy(stage_d.at[0], wf.at[pl.ds(HF, UT), pl.ds(c * C, C)], lo.at[6]),
        pltpu.make_async_copy(stage_d.at[1], wf.at[pl.ds(HF + UT, UT), pl.ds(c * C, C)], lo.at[7]),
    ]
    for load, store in zip(loads, stores):
        load.wait()
        store.start()

    ck, hk, uk = C // n_dp, HF // n_dp, UT // n_dp

    def w_dst(part, dd, cc):
        if part == 0:
            return wi.at[pl.ds(cc * C + dd * ck, ck), pl.ds(0, qw)]
        if part == 1:
            return wi.at[pl.ds(cc * C + dd * ck, ck), pl.ds(qw, UT)]
        if part == 2:
            return wi.at[pl.ds(cc * C + dd * ck, ck), pl.ds(qw + UT, UT)]
        if part == 3:
            return wf.at[pl.ds(dd * hk, hk), pl.ds(cc * C, C)]
        if part == 4:
            return wf.at[pl.ds(HF + dd * uk, uk), pl.ds(cc * C, C)]
        return wf.at[pl.ds(HF + UT + dd * uk, uk), pl.ds(cc * C, C)]

    def w_src(part, cc):
        if part == 0:
            return wq_ref.at[cc, pl.ds(d * ck, ck), :]
        if part == 1:
            return wu_ref.at[pl.ds(d * ck, ck), pl.ds(cc * UT, UT)]
        if part == 2:
            return wu_ref.at[pl.ds(d * ck, ck), pl.ds((n_col + cc) * UT, UT)]
        if part == 3:
            return wo_ref.at[pl.ds(cc * HF + d * hk, hk), :]
        if part == 4:
            return wd_ref.at[pl.ds(cc * UT + d * uk, uk), :]
        return wd_ref.at[pl.ds((n_col + cc) * UT + d * uk, uk), :]

    def w_copy(part, k):
        dest = lax.rem(c + k, n_col)
        return copy(
            w_src(part, dest), w_dst(part, d, c), ws.at[part, k], wr.at[part, k], {"col": dest}
        )

    def w_got(part, k):
        return w_dst(part, d, lax.rem(c + n_col - k, n_col))

    def x_copy(part, k, j):
        return copy(
            w_got(part, k), w_got(part, k), ds.at[part, k, j], dr.at[part, k, j],
            {"dp": lax.rem(d + j, n_dp)},
        )

    parts = range(6)

    for s in range(1, n_col):
        for a, t in order:
            @pl.when(c - s >= 0)
            def _(a=a, t=t, s=s):
                cc = c - s
                z_copy(a, t, cc, blk(a, r, cc, t), True).wait_recv()

                @pl.when(c < n_col - 1)
                def _():
                    z_copy(a, t, cc, blk(a, r, cc, t), True).start()

                y_copy(a, t, cc, blk(a, r, cc, t)).start()
                c_copy(a, t, cc, blk(a, r, cc, t), r, 0).start()

            @pl.when(c + s < n_col)
            def _(a=a, t=t, s=s):
                cc = c + s
                z_copy(a, t, cc, blk(a, r, cc, t), False).wait_recv()

                @pl.when(c > 0)
                def _():
                    z_copy(a, t, cc, blk(a, r, cc, t), False).start()

                y_copy(a, t, cc, blk(a, r, cc, t)).start()
                c_copy(a, t, cc, blk(a, r, cc, t), r, 0).start()

        for part in parts:
            w_copy(part, s).start()

    for s in range(n_col):
        for a, t in order:
            for cc in ((c,) if s == 0 else (c - s, c + s)):
                @pl.when((cc >= 0) & (cc < n_col))
                def _(a=a, t=t, cc=cc):
                    y_copy(a, t, cc, blk(a, r, cc, t)).wait_recv()
                    c_copy(a, t, cc, blk(a, r2, cc, t), r2, 1).start()

    for k in range(1, n_col):
        for part in parts:
            w_copy(part, k).wait_recv()
            for j in range(1, n_dp):
                x_copy(part, k, j).start()

    for a, t in order:
        for cc in range(n_col):
            c_copy(a, t, cc, blk(a, r, cc, t), r, 0).wait_recv()
            c_copy(a, t, cc, blk(a, r, cc, t), r, 1).wait_recv()
    for k in range(1, n_col):
        for part in parts:
            for j in range(1, n_dp):
                x_copy(part, k, j).wait_recv()
    for a, t in order:
        for cc in range(n_col):
            @pl.when((cc <= c) & (c < n_col - 1))
            def _(a=a, t=t, cc=cc):
                z_copy(a, t, cc, blk(a, r, cc, t), True).wait_send()

            @pl.when((cc >= c) & (c > 0))
            def _(a=a, t=t, cc=cc):
                z_copy(a, t, cc, blk(a, r, cc, t), False).wait_send()

            y_copy(a, t, cc, blk(a, r, cc, t)).wait_send()
            c_copy(a, t, cc, blk(a, r, cc, t), r, 0).wait_send()
            c_copy(a, t, cc, blk(a, r, cc, t), r, 1).wait_send()
    for k in range(1, n_col):
        for part in parts:
            w_copy(part, k).wait_send()
            for j in range(1, n_dp):
                x_copy(part, k, j).wait_send()
    for store in stores:
        store.wait()


def gather_all(x, g, w_q, w_up, w_out, w_down, n_dp, n_row, n_col):
    T, C = x.shape
    HF = w_q.shape[2] // 3
    UT = w_up.shape[1] // (2 * n_col)
    n_in, n_out = 3 * HF + 2 * UT, HF + 2 * UT
    dma = pltpu.SemaphoreType.DMA
    return pl.pallas_call(
        functools.partial(gather_kernel, n_dp, n_row, n_col, (T, C, HF, UT)),
        name="gather_all",
        out_shape=(
            jax.ShapeDtypeStruct((n_row * T, n_col * C), BF16),
            jax.ShapeDtypeStruct((n_row * T, n_col * C), BF16),
            jax.ShapeDtypeStruct((n_col * C, n_in), BF16),
            jax.ShapeDtypeStruct((n_out, n_col * C), BF16),
        ),
        in_specs=[ANY] * 6,
        out_specs=(ANY,) * 4,
        scratch_shapes=[
            pltpu.VMEM((2, T, C), BF16),
            pltpu.VMEM((C, 3 * HF), BF16),
            pltpu.VMEM((2, C, UT), BF16),
            pltpu.VMEM((HF, C), BF16),
            pltpu.VMEM((2, UT, C), BF16),
            dma((2, 2, 2, n_col)),
            dma((2, 2, n_col)),
            dma((2, 2, n_col)),
            dma((2, 2, n_col)),
            dma((2, 2, 2, n_col)),
            dma((2, 2, 2, n_col)),
            dma((6, n_col)),
            dma((6, n_col)),
            dma((6, n_col, n_dp)),
            dma((6, n_col, n_dp)),
            dma((8,)),
            dma((8,)),
        ],
        compiler_params=pltpu.CompilerParams(collective_id=0, has_side_effects=True),
    )(x, g, w_q, w_up, w_out, w_down)


def pick(index, table):
    out = jnp.int32(table[0])
    for k in range(1, len(table)):
        out = jnp.where(index == k, jnp.int32(table[k]), out)
    return out


def reduce_kernel(n_row, n_col, dims, p_ref, q_ref, dwi_ref, dwf_ref,
                  res_ref, gn_ref, tiles_ref,
                  abuf, obuf, sbuf, bbuf, zsb, zin, gi, gf, oi, of,
                  a_s, a_r, o_l, y_s, y_r, z_s, z_r, x_s, x_r, g_l, t_s, t_r):
    T, C, HF, UT, chunks = dims
    tc = T // chunks
    step_rows = 64
    d, r, c = lax.axis_index("dp"), lax.axis_index("row"), lax.axis_index("col")
    r1 = r + 1 - 2 * lax.rem(r, 2)
    r2 = lax.rem(r + 2, n_row)
    r12 = lax.rem(r1 + 2, n_row)
    srcs = (p_ref, q_ref)
    outs = (res_ref, gn_ref)
    far = [
        sorted(range(n_col), key=lambda f: (-abs(f - cc), f < cc if cc < n_col // 2 else f > cc))
        for cc in range(n_col)
    ]
    forder = [pick(c, [far[cc][i] for cc in range(n_col)]) for i in range(n_col)]

    barrier = pltpu.get_barrier_semaphore()
    peers = [{"row": r1}, {"row": r2}, {"dp": 1 - d}]
    peers += [{"col": lax.rem(c + k, n_col)} for k in range(1, n_col)]
    for peer in peers:
        pl.semaphore_signal(barrier, inc=1, device_id=peer, device_id_type=MESH)
    pl.semaphore_wait(barrier, len(peers))

    def copy(src, dst, s, rcv, peer):
        return pltpu.make_async_remote_copy(
            src_ref=src, dst_ref=dst, send_sem=s, recv_sem=rcv, device_id=peer, device_id_type=MESH
        )

    def unit(v, rr, f, t):
        return srcs[v].at[pl.ds(rr * T + t * tc, tc), pl.ds(f * C, C)]

    def a_copy(v, h, f, t):
        return copy(
            unit(v, r12 if h else r1, f, t), abuf.at[v, h, f, t],
            a_s.at[v, h, f, t], a_r.at[v, h, f, t], {"row": r1},
        )

    def o_copy(v, h, f, t):
        return pltpu.make_async_copy(
            unit(v, r2 if h else r, f, t), obuf.at[v, h, f, t], o_l.at[v, h, f, t]
        )

    def y_copy(v, f, t):
        return copy(sbuf.at[v, f, t], bbuf.at[v, f, t], y_s.at[v, f, t], y_r.at[v, f, t],
                    {"row": r2})

    def z_copy(v, f, t, slot, step):
        return copy(zsb.at[v, f, t], zin.at[v, slot, t], z_s.at[v, f, t], z_r.at[v, slot, t],
                    {"col": c + step})

    for v in range(2):
        for i in range(n_col):
            for t in range(chunks):
                for h in (1, 0):
                    a_copy(v, h, forder[i], t).start()
                    o_copy(v, h, forder[i], t).start()

    qw, n_in, n_out = 3 * HF, 3 * HF + 2 * UT, HF + 2 * UT
    wide = (qw + UT, UT)
    lane0 = (0, qw + UT)
    tall = (HF, 2 * UT)
    row0 = (0, HF)

    def gi_src(own, cc):
        return dwi_ref.at[pl.ds(cc * C, C), pl.ds(lane0[own], wide[own])]

    def gf_src(own, cc):
        return dwf_ref.at[pl.ds(row0[own], tall[own]), pl.ds(cc * C, C)]

    def xi_copy(own, cc):
        return copy(gi_src(own, cc), gi.at[cc, :, pl.ds(0, wide[own])], x_s.at[0, cc],
                    x_r.at[0, cc], {"dp": 1 - d})

    def xf_copy(own, cc):
        return copy(gf_src(own, cc), gf.at[cc, pl.ds(0, tall[own]), :], x_s.at[1, cc],
                    x_r.at[1, cc], {"dp": 1 - d})

    def li_copy(own, cc):
        return pltpu.make_async_copy(gi_src(own, cc), oi.at[cc, :, pl.ds(0, wide[own])],
                                     g_l.at[0, cc])

    def lf_copy(own, cc):
        return pltpu.make_async_copy(gf_src(own, cc), of.at[cc, pl.ds(0, tall[own]), :],
                                     g_l.at[1, cc])

    def tile_parts(own, cc, source):
        half, odd = source // 2, lax.rem(source, 2)
        lw = 2 * HF
        if own == 0:
            parts = [
                (oi.at[cc, :, pl.ds(j * HF, HF)], tiles_ref.at[2 * j + half, :, pl.ds(odd * HF, HF)])
                for j in range(3)
            ]
            parts += [(oi.at[cc, :, pl.ds(qw, UT)], tiles_ref.at[8 + source])]
            parts += [
                (of.at[cc, pl.ds(0, HF), pl.ds(j * lw, lw)],
                 tiles_ref.at[6 + j, pl.ds(source * HF, HF), :])
                for j in range(2)
            ]
            return parts
        parts = [(oi.at[cc, :, pl.ds(0, UT)], tiles_ref.at[source])]
        for m in range(2):
            for j in range(2):
                parts.append(
                    (of.at[cc, pl.ds(m * UT, UT), pl.ds(j * lw, lw)],
                     tiles_ref.at[4 + 2 * (2 * m + half) + j, pl.ds(odd * UT, UT), :])
                )
        return parts

    def t_copies(own, cc):
        return [
            copy(src, dst, t_s.at[n, cc], t_r.at[n, c], {"col": cc})
            for n, (src, dst) in enumerate(tile_parts(own, cc, c))
        ]

    def t_waits(own, source):
        return [
            copy(src, dst, t_s.at[n, source], t_r.at[n, source], {"col": source})
            for n, (src, dst) in enumerate(tile_parts(own, source, source))
        ]

    def t_local(own):
        return [
            pltpu.make_async_copy(src, dst, t_s.at[n, c])
            for n, (src, dst) in enumerate(tile_parts(own, c, c))
        ]

    for i in range(n_col):
        for own in range(2):
            @pl.when(d == own)
            def _(own=own, i=i):
                xi_copy(1 - own, forder[i]).start()
                xf_copy(1 - own, forder[i]).start()
                li_copy(own, forder[i]).start()
                lf_copy(own, forder[i]).start()

    def looped(rows, fn):
        def one(k, carry):
            fn(pl.ds(pl.multiple_of(k * step_rows, step_rows), step_rows))
            return carry
        lax.fori_loop(0, rows // step_rows, one, 0)

    def first_sum(v, i):
        f = forder[i]
        for t in range(chunks):
            a_copy(v, 1, f, t).wait_recv()
            o_copy(v, 1, f, t).wait()

            def add(rows, t=t):
                sbuf[v, f, t, rows, :] = (
                    obuf[v, 1, f, t, rows, :].astype(F32) + abuf[v, 1, f, t, rows, :].astype(F32)
                ).astype(BF16)

            looped(tc, add)
            y_copy(v, f, t).start()

    def second_sum(v, i):
        f = forder[i]
        for t in range(chunks):
            a_copy(v, 0, f, t).wait_recv()
            o_copy(v, 0, f, t).wait()
            y_copy(v, f, t).wait_recv()

            def base(rows, t=t):
                return (
                    obuf[v, 0, f, t, rows, :].astype(F32)
                    + abuf[v, 0, f, t, rows, :].astype(F32)
                    + bbuf[v, f, t, rows, :].astype(F32)
                )

            if i < n_col - 1:
                right = f > c
                step = jnp.where(right, jnp.int32(1), jnp.int32(-1))
                landed = jnp.where(f == c + step, jnp.where(right, f, jnp.int32(n_col)), f)
                inner = jnp.where(right, c, n_col - 1 - c) > 0

                @pl.when(inner)
                def _(t=t):
                    z_copy(v, f, t, f, 0).wait_recv()

                    def add(rows):
                        zsb[v, f, t, rows, :] = (
                            base(rows) + zin[v, f, t, rows, :].astype(F32)
                        ).astype(BF16)

                    looped(tc, add)

                @pl.when(jnp.logical_not(inner))
                def _(t=t):
                    def add(rows):
                        zsb[v, f, t, rows, :] = base(rows).astype(BF16)

                    looped(tc, add)

                z_copy(v, f, t, landed, step).start()
            else:
                out = outs[v]

                def put(rows, value, t=t):
                    out[pl.ds(pl.multiple_of(rows.start + t * tc, step_rows), step_rows), :] = value

                @pl.when(c > 0)
                def _(t=t):
                    z_copy(v, f, t, f, 0).wait_recv()

                @pl.when(c < n_col - 1)
                def _(t=t):
                    z_copy(v, f, t, n_col, 0).wait_recv()

                @pl.when(c == 0)
                def _(t=t):
                    looped(tc, lambda rows: put(
                        rows, base(rows) + zin[v, n_col, t, rows, :].astype(F32)))

                @pl.when(c == n_col - 1)
                def _(t=t):
                    looped(tc, lambda rows: put(
                        rows, base(rows) + zin[v, f, t, rows, :].astype(F32)))

                @pl.when((c > 0) & (c < n_col - 1))
                def _(t=t):
                    looped(tc, lambda rows: put(
                        rows, base(rows) + zin[v, f, t, rows, :].astype(F32)
                        + zin[v, n_col, t, rows, :].astype(F32)))

    def grad_piece(i):
        cc = forder[i]
        for own in range(2):
            @pl.when(d == own)
            def _(own=own):
                xi_copy(own, cc).wait_recv()
                xf_copy(own, cc).wait_recv()
                li_copy(own, cc).wait()
                lf_copy(own, cc).wait()

                def add_i(rows):
                    at = (cc, rows, pl.ds(0, wide[own]))
                    oi[at] = (oi[at].astype(F32) + gi[at].astype(F32)).astype(BF16)

                def add_f(rows):
                    at = (cc, rows, slice(None))
                    of[at] = (of[at].astype(F32) + gf[at].astype(F32)).astype(BF16)

                looped(C, add_i)
                looped(tall[own], add_f)
                for item in t_local(own) if i == n_col - 1 else t_copies(own, cc):
                    item.start()

    for i in range(n_col):
        first_sum(0, i)
    for i in range(n_col):
        second_sum(0, i)
        first_sum(1, i)
        grad_piece(i)
    for i in range(n_col):
        second_sum(1, i)

    for own in range(2):
        @pl.when(d == own)
        def _(own=own):
            for k in range(1, n_col):
                for item in t_waits(own, lax.rem(c + k, n_col)):
                    item.wait_recv()
            for i in range(n_col - 1):
                for item in t_copies(own, forder[i]):
                    item.wait_send()
            for item in t_local(own):
                item.wait()
            for cc in range(n_col):
                xi_copy(1 - own, cc).wait_send()
                xf_copy(1 - own, cc).wait_send()
    for v in range(2):
        for t in range(chunks):
            for f in range(n_col):
                a_copy(v, 0, f, t).wait_send()
                a_copy(v, 1, f, t).wait_send()
                y_copy(v, f, t).wait_send()
            for i in range(n_col - 1):
                z_copy(v, forder[i], t, forder[i], 0).wait_send()


def reduce_all(p, q, dwi, dwf, T, C, HF, UT, n_row, n_col):
    dma = pltpu.SemaphoreType.DMA
    chunks = 2
    tc = T // chunks
    unit = (chunks, tc, C)
    vm = pl.BlockSpec(memory_space=pltpu.VMEM)
    return pl.pallas_call(
        functools.partial(reduce_kernel, n_row, n_col, (T, C, HF, UT, chunks)),
        name="reduce_all",
        out_shape=(
            jax.ShapeDtypeStruct((T, C), F32),
            jax.ShapeDtypeStruct((T, C), F32),
            jax.ShapeDtypeStruct((12, C, UT), BF16),
        ),
        in_specs=[ANY] * 4,
        out_specs=(vm, vm, ANY),
        scratch_shapes=[
            pltpu.VMEM((2, 2, n_col) + unit, BF16),
            pltpu.VMEM((2, 2, n_col) + unit, BF16),
            pltpu.VMEM((2, n_col) + unit, BF16),
            pltpu.VMEM((2, n_col) + unit, BF16),
            pltpu.VMEM((2, n_col) + unit, BF16),
            pltpu.VMEM((2, n_col + 1) + unit, BF16),
            pltpu.VMEM((n_col, C, 3 * HF + UT), BF16),
            pltpu.VMEM((n_col, 2 * UT, C), BF16),
            pltpu.VMEM((n_col, C, 3 * HF + UT), BF16),
            pltpu.VMEM((n_col, 2 * UT, C), BF16),
            dma((2, 2, n_col, chunks)),
            dma((2, 2, n_col, chunks)),
            dma((2, 2, n_col, chunks)),
            dma((2, n_col, chunks)),
            dma((2, n_col, chunks)),
            dma((2, n_col, chunks)),
            dma((2, n_col + 1, chunks)),
            dma((2, n_col)),
            dma((2, n_col)),
            dma((2, n_col)),
            dma((6, n_col)),
            dma((6, n_col)),
        ],
        compiler_params=pltpu.CompilerParams(
            collective_id=1, has_side_effects=True, vmem_limit_bytes=62 * 1024 * 1024
        ),
    )(p, q, dwi, dwf)


def finish_kernel(n_dp, n_row, n_col, width, gn_ref, x_ref, g_ref, mean_ref, rstd_ref, gain_ref, part_ref,
                  gx_ref, va_ref, vb_ref,
                  st, da, db, ra, rb,
                  st_s, st_r, d_s, d_r, r_s, r_r, c_s, c_r):
    d, r, c = lax.axis_index("dp"), lax.axis_index("row"), lax.axis_index("col")
    T, C = gn_ref.shape

    barrier = pltpu.get_barrier_semaphore()
    dps = [lax.rem(d + k, n_dp) for k in range(1, n_dp)]
    rows = [lax.rem(r + k, n_row) for k in range(1, n_row)]
    cols = [lax.rem(c + k, n_col) for k in range(1, n_col)]
    peers = [{"dp": k} for k in dps] + [{"row": k} for k in rows] + [{"col": k} for k in cols]
    for peer in peers:
        pl.semaphore_signal(barrier, inc=1, device_id=peer, device_id_type=MESH)
    pl.semaphore_wait(barrier, len(peers))

    def copy(src, dst, s, rcv, peer):
        return pltpu.make_async_remote_copy(
            src_ref=src, dst_ref=dst, send_sem=s, recv_sem=rcv, device_id=peer, device_id_type=MESH
        )

    gain = gain_ref[...]

    def fold(value):
        total = value[:, 0:128]
        for k in range(1, C // 128):
            total = total + value[:, k * 128 : (k + 1) * 128]
        return jnp.sum(jnp.transpose(total), axis=0, keepdims=True)

    gn = gn_ref[...]
    x_hat = (x_ref[...].astype(F32) - mean_ref[...]) * rstd_ref[...]
    gh = gn * gain
    st[c, 0:1, :] = fold(gh)
    st[c, 1:2, :] = fold(gh * x_hat)

    def st_copy(k):
        return copy(st.at[c], st.at[c], st_s.at[k], st_r.at[c], {"col": k})

    def st_wait(k):
        return copy(st.at[k], st.at[k], st_s.at[k], st_r.at[k], {"col": k})

    for k in cols:
        st_copy(k).start()

    da[d] = part_ref[...]
    db[d, 0:1, :] = jnp.sum(gn * x_hat, axis=0, keepdims=True)
    db[d, 1:2, :] = jnp.sum(gn, axis=0, keepdims=True)
    db[d, 2:3, :] = jnp.sum(g_ref[...].astype(F32), axis=0, keepdims=True)

    def pair(a_src, b_src, a_dst, b_dst, s, rcv, peer):
        return [copy(a_src, a_dst, s.at[0], rcv.at[0], peer),
                copy(b_src, b_dst, s.at[1], rcv.at[1], peer)]

    def d_pair(slot, peer):
        return pair(da.at[slot], db.at[slot], da.at[slot], db.at[slot],
                    d_s.at[peer], d_r.at[slot], {"dp": peer})

    def r_pair(slot, peer):
        return pair(ra.at[slot], rb.at[slot], ra.at[slot], rb.at[slot],
                    r_s.at[peer], r_r.at[slot], {"row": peer})

    def c_pair(slot, peer):
        return pair(va_ref.at[slot], vb_ref.at[slot], va_ref.at[slot], vb_ref.at[slot],
                    c_s.at[peer], c_r.at[slot], {"col": peer})

    for k in dps:
        for item in d_pair(d, k):
            item.start()
    for k in dps:
        for item in d_pair(k, k):
            item.wait_recv()
    a_sum, b_sum = da[0], db[0]
    for k in range(1, n_dp):
        a_sum = a_sum + da[k]
        b_sum = b_sum + db[k]
    ra[r] = a_sum
    rb[r] = b_sum
    for k in rows:
        for item in r_pair(r, k):
            item.start()

    for k in cols:
        st_wait(k).wait_recv()
    stats = st[0]
    for k in range(1, n_col):
        stats = stats + st[k]
    stats = stats / width
    m1 = jnp.transpose(jnp.broadcast_to(stats[0:1, :], (128, T)))[:, 0:1]
    m2 = jnp.transpose(jnp.broadcast_to(stats[1:2, :], (128, T)))[:, 0:1]
    gx_ref[...] = g_ref[...].astype(F32) + rstd_ref[...] * (gh - m1 - x_hat * m2)

    for k in rows:
        for item in r_pair(k, k):
            item.wait_recv()
    b_sum = rb[0]
    for k in range(1, n_row):
        b_sum = b_sum + rb[k]
    for k in range(n_row):
        va_ref[c, k] = ra[k]
    vb_ref[c] = b_sum
    for k in cols:
        for item in c_pair(c, k):
            item.start()
    for k in cols:
        for item in c_pair(k, k):
            item.wait_recv()
    for k in cols:
        st_copy(k).wait_send()
        for item in c_pair(c, k):
            item.wait_send()
    for k in dps:
        for item in d_pair(d, k):
            item.wait_send()
    for k in rows:
        for item in r_pair(r, k):
            item.wait_send()


def finish_all(gn, x, g, mean, rstd, gain, part, width, n_dp, n_row, n_col):
    T, C = gn.shape
    dma = pltpu.SemaphoreType.DMA
    vm = pl.BlockSpec(memory_space=pltpu.VMEM)
    return pl.pallas_call(
        functools.partial(finish_kernel, n_dp, n_row, n_col, width),
        name="finish_all",
        out_shape=(
            jax.ShapeDtypeStruct((T, C), F32),
            jax.ShapeDtypeStruct((n_col, n_row, 8, 128), F32),
            jax.ShapeDtypeStruct((n_col, 8, C), F32),
        ),
        in_specs=[vm] * 7,
        out_specs=(vm,) * 3,
        scratch_shapes=[
            pltpu.VMEM((n_col, 8, T), F32),
            pltpu.VMEM((n_dp, 8, 128), F32),
            pltpu.VMEM((n_dp, 8, C), F32),
            pltpu.VMEM((n_row, 8, 128), F32),
            pltpu.VMEM((n_row, 8, C), F32),
            dma((n_col,)),
            dma((n_col,)),
            dma((n_dp, 2)),
            dma((n_dp, 2)),
            dma((n_row, 2)),
            dma((n_row, 2)),
            dma((n_col, 2)),
            dma((n_col, 2)),
        ],
        compiler_params=pltpu.CompilerParams(
            collective_id=2, has_side_effects=True, vmem_limit_bytes=48 * 1024 * 1024
        ),
    )(gn, x, g, mean, rstd, gain, part)


def reduce_plain(p, q, dwi, dwf, C, HF, UT, n_col, row_width):
    def block(part):
        part = lax.psum_scatter(part, "row", scatter_dimension=0, tiled=True)
        return lax.psum_scatter(part, "col", scatter_dimension=1, tiled=True).astype(F32)

    wi4 = lax.all_to_all(dwi.reshape(n_col, C, -1), "col", 0, 0)
    wf4 = lax.all_to_all(dwf.reshape(-1, n_col, C).transpose(1, 0, 2), "col", 0, 0)
    grad_qkv = (
        wi4[:, :, : 3 * HF].reshape(n_col, C, 3, HF).transpose(1, 2, 0, 3).reshape(C, 3, row_width)
    )
    grad_up_w = wi4[:, :, 3 * HF :].reshape(n_col, C, 2, UT).transpose(1, 2, 0, 3).reshape(C, -1)
    grad_w_out = wf4[:, :HF].reshape(-1, C)
    grad_w_down = wf4[:, HF:].reshape(n_col, 2, UT, C).transpose(1, 0, 2, 3).reshape(-1, C)
    grad_tiles = tile_blocks(grad_qkv, grad_w_out, grad_up_w, grad_w_down)
    owned = lax.psum_scatter(grad_tiles, "dp", scatter_dimension=0, tiled=True)
    return block(p), block(q), owned


def body(
    inputs,
    cotangent,
    segments,
    positions,
    w_qkv,
    w_out,
    w_up,
    w_down,
    vectors,
    tile_moment,
    vector_moment,
):
    d_index = lax.axis_index("dp")
    row_index = lax.axis_index("row")
    col_index = lax.axis_index("col")
    n_dp, n_row, n_col = lax.axis_size("dp"), lax.axis_size("row"), lax.axis_size("col")
    T, C = inputs.shape
    D = vectors.shape[1]
    row_width = w_qkv.shape[2]
    HF = row_width // n_col
    UT = w_up.shape[1] // (2 * n_col)
    score_scale = HEAD_DIM ** (-0.5)
    feat_start = (row_index * n_col + col_index) * HF
    unit_a = (row_index * 2 * n_col + col_index) * UT
    unit_b = unit_a + n_col * UT
    col_start = col_index * C
    gain, shift = vectors[5], vectors[6]
    norm_gain = lax.dynamic_slice_in_dim(gain, col_start, C)
    out_bias = lax.dynamic_slice_in_dim(vectors[3] + vectors[4], col_start, C)
    qkv_bias = lax.dynamic_slice_in_dim(vectors[0:3], feat_start, HF, axis=1)
    up_flat = vectors[7:].reshape(-1)
    up_bias = jnp.concatenate(
        [
            lax.dynamic_slice_in_dim(up_flat, unit_a, UT),
            lax.dynamic_slice_in_dim(up_flat, unit_b, UT),
        ]
    )
    w_q = (
        w_qkv.reshape(C, 3, n_col, HF).transpose(2, 0, 1, 3).reshape(n_col, C, 3 * HF)
    )
    x_full, cot_rows, w_in, w_fin = gather_all(
        inputs, cotangent, w_q, w_up, w_out, w_down, n_dp, n_row, n_col
    )
    seq_rows = x_full.shape[0]

    x_wide = x_full.astype(F32)
    mean_all = jnp.mean(x_wide, axis=1, keepdims=True)
    var_all = jnp.mean(x_wide * x_wide, axis=1, keepdims=True) - mean_all * mean_all
    rstd_all = lax.rsqrt(var_all + NORM_EPS)
    normed = ((x_wide - mean_all) * rstd_all * gain + shift).astype(BF16)

    mixed_out = jnp.dot(normed, w_in, preferred_element_type=F32)
    qkv_part = mixed_out[:, : 3 * HF].reshape(seq_rows, 3, HF) + qkv_bias[None]
    up_pre = mixed_out[:, 3 * HF :] + up_bias
    heads_here = HF // HEAD_DIM
    seq_count = seq_rows // SEQ_LEN

    def by_seq(tensor_in):
        return tensor_in.reshape((seq_count, SEQ_LEN) + tensor_in.shape[1:])

    cosine, sine_tab = rotary_tables(positions)
    queries = rotate(
        qkv_part[:, 0].reshape(seq_rows, heads_here, HEAD_DIM), cosine, sine_tab, 1.0
    ).astype(BF16)
    key_vecs = rotate(
        qkv_part[:, 1].reshape(seq_rows, heads_here, HEAD_DIM), cosine, sine_tab, 1.0
    ).astype(BF16)
    values = qkv_part[:, 2].reshape(seq_rows, heads_here, HEAD_DIM).astype(BF16)
    attended, logsum = jax.vmap(attend_forward, in_axes=(0, 0, 0, 0, None))(
        by_seq(queries), by_seq(key_vecs), by_seq(values), by_seq(segments), score_scale
    )
    attn_low = attended.reshape(seq_rows, HF).astype(BF16)
    act_low = gelu_value(up_pre).astype(BF16)
    hidden = jnp.concatenate([attn_low, act_low], axis=1)

    partial_out = jnp.dot(hidden, w_fin, preferred_element_type=F32).astype(BF16)
    x_val = inputs.astype(F32)

    grad_w_fin = jnp.einsum("ti,tj->ij", hidden, cot_rows, preferred_element_type=F32).astype(BF16)
    back = jnp.einsum("tj,ij->ti", cot_rows, w_fin, preferred_element_type=F32)
    grad_attn_low = back[:, :HF].astype(BF16)
    grad_up = back[:, HF:] * gelu_slope(up_pre)
    g_queries, g_keys, g_values = jax.vmap(attend_backward, in_axes=(0, 0, 0, 0, 0, 0, 0, None))(
        by_seq(queries),
        by_seq(key_vecs),
        by_seq(values),
        by_seq(attn_low.reshape(seq_rows, heads_here, HEAD_DIM)),
        by_seq(grad_attn_low.reshape(seq_rows, heads_here, HEAD_DIM)),
        logsum,
        by_seq(segments),
        score_scale,
    )
    g_queries = rotate(
        g_queries.reshape(seq_rows, heads_here, HEAD_DIM), cosine, sine_tab, -1.0
    ).reshape(seq_rows, HF)
    g_keys = rotate(g_keys.reshape(seq_rows, heads_here, HEAD_DIM), cosine, sine_tab, -1.0).reshape(
        seq_rows, HF
    )
    g_values = g_values.reshape(seq_rows, HF)
    grad_mixed = jnp.concatenate([g_queries, g_keys, g_values, grad_up], axis=1)
    grad_mixed_low = grad_mixed.astype(BF16)
    grad_w_in = jnp.einsum(
        "ti,tj->ij", normed, grad_mixed_low, preferred_element_type=F32
    ).astype(BF16)
    partial_norm = jnp.einsum(
        "tj,ij->ti", grad_mixed_low, w_in, preferred_element_type=F32
    ).astype(BF16)

    if n_dp == 2:
        branch, grad_norm, owned_low = reduce_all(
            partial_out, partial_norm, grad_w_in, grad_w_fin, T, C, HF, UT, n_row, n_col
        )
    else:
        branch, grad_norm, owned_low = reduce_plain(
            partial_out, partial_norm, grad_w_in, grad_w_fin, C, HF, UT, n_col, row_width
        )
    result = x_val + branch + out_bias
    owned_grads = owned_low.astype(F32)

    sums = jnp.sum(grad_mixed, axis=0)
    part = jnp.pad(sums.reshape(-1, 128), ((0, 1), (0, 0)))
    grad_input, vec_a, vec_b = finish_all(
        grad_norm,
        inputs,
        cotangent,
        lax.dynamic_slice_in_dim(mean_all, row_index * T, T),
        lax.dynamic_slice_in_dim(rstd_all, row_index * T, T),
        norm_gain[None],
        part,
        D,
        n_dp,
        n_row,
        n_col,
    )
    vec_a = vec_a.transpose(2, 1, 0, 3)
    qkv_rows = vec_a[:3].reshape(3, D)
    up_rows = vec_a[3:7].reshape(2, UT // 128, n_row, n_col, 128).transpose(2, 0, 3, 1, 4)
    norm_rows = vec_b.transpose(1, 0, 2).reshape(8, D)
    vec_grad = jnp.concatenate(
        [qkv_rows, norm_rows[2:3], norm_rows[2:3], norm_rows[:2], up_rows.reshape(-1, D)], axis=0
    )
    scaled = vec_grad * lax.rsqrt(jnp.mean(vec_grad * vec_grad, axis=1, keepdims=True) + STAT_EPS)
    vec_moment_new = MOMENTUM_RATE * vector_moment + scaled
    vectors_new = vectors - VECTOR_RATE * vec_moment_new

    owned_count = owned_grads.shape[0]
    weight_tiles = lax.dynamic_slice_in_dim(
        tile_blocks(w_qkv, w_out, w_up, w_down), d_index * owned_count, owned_count, 0
    ).astype(F32)
    moment_new = MOMENTUM_RATE * tile_moment[0, 0] + owned_grads
    ortho_tiles = jax.vmap(newton_schulz)(moment_new)
    tile_ratio = math.sqrt(max(1.0, moment_new.shape[1] / moment_new.shape[2]))
    tiles_new = weight_tiles - MUON_RATE * tile_ratio * ortho_tiles.astype(F32)
    return (
        result,
        grad_input,
        owned_grads[None, None],
        tiles_new[None, None],
        moment_new[None, None],
        vec_grad,
        vectors_new,
        vec_moment_new,
    )


def solution(mesh):
    placed = (
        P(("dp", "row"), "col"),
        P(("dp", "row"), "col"),
        P("dp"),
        P("dp"),
        P("col", None, "row"),
        P("row", "col"),
        P("col", "row"),
        P("row", "col"),
        P(),
        P("row", "col", "dp", None, None),
        P(),
    )
    return jax.shard_map(
        body,
        mesh=mesh,
        in_specs=placed,
        out_specs=(
            P(("dp", "row"), "col"),
            P(("dp", "row"), "col"),
            P("row", "col", "dp", None, None),
            P("row", "col", "dp", None, None),
            P("row", "col", "dp", None, None),
            P(),
            P(),
            P(),
        ),
        check_vma=False,
    )
```

```python
import functools
import math

import jax
import jax.numpy as jnp
from jax import lax
from jax.experimental import pallas as pl
from jax.experimental.pallas import tpu as pltpu
from jax.sharding import PartitionSpec as P

HEAD_DIM = 64
ROTARY = 32
SEQ_LEN = 512

MOMENTUM_RATE = 0.95
MUON_RATE = 0.05
VECTOR_RATE = 0.12
NEWTON_A = 3.4445
NEWTON_B = -4.775
NEWTON_C = 2.0315
GELU_SCALE = 0.7978845608028654
GELU_CUBIC = 0.044715
NORM_EPS = 1e-05
STAT_EPS = 1e-06
MASKED_SCORE = -1e30

MESH = pl.DeviceIdType.MESH
ANY = pl.BlockSpec(memory_space=pl.ANY)
F32 = jnp.float32
BF16 = jnp.bfloat16


def to_low(tensor_in):
    return lax.optimization_barrier(tensor_in.astype(BF16))


def gelu_value(pre_act):
    inner_arg = GELU_SCALE * (pre_act + GELU_CUBIC * pre_act * pre_act * pre_act)
    return 0.5 * pre_act * (1.0 + jnp.tanh(inner_arg))


def gelu_slope(pre_act):
    tanh_val = jnp.tanh(GELU_SCALE * (pre_act + GELU_CUBIC * pre_act * pre_act * pre_act))
    return 0.5 * (1.0 + tanh_val) + 0.5 * pre_act * (1.0 - tanh_val * tanh_val) * GELU_SCALE * (
        1.0 + 3.0 * GELU_CUBIC * pre_act * pre_act
    )


def rotary_tables(positions):
    half_dims = ROTARY // 2
    frequency = jnp.exp(jnp.arange(half_dims, dtype=F32) * (-2.0 * math.log(10000.0) / ROTARY))
    angles = positions.astype(F32)[:, None] * frequency[None, :]
    return (jnp.cos(angles), jnp.sin(angles))


def rotate(tensor_in, cosine, sine_tab, direction_sign):
    half_dims = ROTARY // 2
    first_half = tensor_in[..., :half_dims]
    second_half = tensor_in[..., half_dims:ROTARY]
    cos_wide = cosine[:, None, :]
    sin_wide = sine_tab[:, None, :] * direction_sign
    return jnp.concatenate(
        [
            first_half * cos_wide - second_half * sin_wide,
            second_half * cos_wide + first_half * sin_wide,
            tensor_in[..., ROTARY:],
        ],
        axis=-1,
    )


def causal_allowed(segment):
    token_order = jnp.arange(segment.shape[0])
    return (segment[:, None] == segment[None, :]) & (token_order[:, None] >= token_order[None, :])


def masked_scores(queries, key_vecs, segment, score_scale):
    scores = (
        jnp.einsum("lhe,mhe->hlm", queries, key_vecs, preferred_element_type=F32) * score_scale
    )
    return jnp.where(causal_allowed(segment)[None], scores, MASKED_SCORE)


def attend_forward(queries, key_vecs, values, segment, score_scale):
    scores = masked_scores(queries, key_vecs, segment, score_scale)
    row_max = jnp.max(scores, axis=-1, keepdims=True)
    exp_scores = jnp.exp(scores - row_max)
    row_total = jnp.sum(exp_scores, axis=-1, keepdims=True)
    probs_low = to_low(exp_scores / row_total)
    attended = jnp.einsum("hlm,mhe->lhe", probs_low, values, preferred_element_type=F32)
    return (attended, (row_max + jnp.log(row_total))[..., 0])


def attend_backward(queries, key_vecs, values, output_low, grad_low, logsum, segment, score_scale):
    scores = masked_scores(queries, key_vecs, segment, score_scale)
    probs = jnp.exp(scores - logsum[..., None])
    grad_values = jnp.einsum("hlm,lhe->mhe", to_low(probs), grad_low, preferred_element_type=F32)
    grad_probs = jnp.einsum("lhe,mhe->hlm", grad_low, values, preferred_element_type=F32)
    row_delta = jnp.sum(grad_low.astype(F32) * output_low.astype(F32), axis=-1)
    grad_scores = to_low(probs * (grad_probs - row_delta.T[:, :, None]) * score_scale)
    grad_queries = jnp.einsum("hlm,mhe->lhe", grad_scores, key_vecs, preferred_element_type=F32)
    grad_keys = jnp.einsum("hlm,lhe->mhe", grad_scores, queries, preferred_element_type=F32)
    return (grad_queries, grad_keys, grad_values)


def tile_blocks(qkv_block, out_block, up_block, down_block):
    tile_rows = qkv_block.shape[0]
    tile_cols = qkv_block.shape[2] // 2

    def split_cols(block_in):
        return block_in.reshape(
            block_in.shape[0], block_in.shape[1] // tile_cols, tile_cols
        ).transpose(1, 0, 2)

    down_part = down_block.reshape(
        down_block.shape[0] // tile_rows, tile_rows, down_block.shape[1] // tile_cols, tile_cols
    )
    down_part = down_part.transpose(0, 2, 1, 3).reshape(-1, tile_rows, tile_cols)
    return jnp.concatenate(
        [
            split_cols(qkv_block[:, 0]),
            split_cols(qkv_block[:, 1]),
            split_cols(qkv_block[:, 2]),
            split_cols(out_block),
            split_cols(up_block),
            down_part,
        ],
        axis=0,
    )


def gather_kernel(n_dp, n_row, n_col, dims, x_ref, g_ref, wq_ref, wu_ref, wo_ref, wd_ref,
                  xf, gf, wi, wf, stage_x, stage_q, stage_u, stage_o, stage_d,
                  zs, zr, ys, yr, cs, cr, ws, wr, ds, dr, ls, lo):
    T, C, HF, UT = dims
    d, r, c = lax.axis_index("dp"), lax.axis_index("row"), lax.axis_index("col")
    r1 = r + 1 - 2 * lax.rem(r, 2)
    r2 = lax.rem(r + 2, n_row)
    chunks = 2
    tc = T // chunks
    qw = 3 * HF
    acts = ((x_ref, xf), (g_ref, gf))

    def blk(a, rr, cc, t):
        return acts[a][1].at[pl.ds(rr * T + t * tc, tc), pl.ds(cc * C, C)]

    barrier = pltpu.get_barrier_semaphore()
    peers = [{"row": r1}, {"row": r2}]
    peers += [{"col": lax.rem(c + k, n_col)} for k in range(1, n_col)]
    peers += [{"dp": lax.rem(d + k, n_dp)} for k in range(1, n_dp)]
    for peer in peers:
        pl.semaphore_signal(barrier, inc=1, device_id=peer, device_id_type=MESH)
    pl.semaphore_wait(barrier, len(peers))

    def own(a, t):
        return acts[a][0].at[pl.ds(t * tc, tc), :]

    def copy(src, dst, s, rcv, peer):
        return pltpu.make_async_remote_copy(
            src_ref=src, dst_ref=dst, send_sem=s, recv_sem=rcv, device_id=peer, device_id_type=MESH
        )

    def z_copy(a, t, cc, src, right):
        peer = {"col": c + 1} if right else {"col": c - 1}
        return copy(src, blk(a, r, cc, t), zs.at[a, t, int(right), cc], zr.at[a, t, cc], peer)

    def y_copy(a, t, cc, src):
        return copy(src, blk(a, r, cc, t), ys.at[a, t, cc], yr.at[a, t, cc], {"row": r2})

    def c_copy(a, t, cc, src, rr, which):
        return copy(
            src, blk(a, rr, cc, t), cs.at[a, t, which, cc], cr.at[a, t, which, cc], {"row": r1}
        )

    order = [(a, t) for a in range(2) for t in range(chunks)]

    for a, t in order:
        @pl.when(c < n_col - 1)
        def _(a=a, t=t):
            z_copy(a, t, c, own(a, t), True).start()

        @pl.when(c > 0)
        def _(a=a, t=t):
            z_copy(a, t, c, own(a, t), False).start()

        y_copy(a, t, c, own(a, t)).start()
        c_copy(a, t, c, own(a, t), r, 0).start()

    loads = [
        pltpu.make_async_copy(x_ref, stage_x.at[0], ls.at[0]),
        pltpu.make_async_copy(g_ref, stage_x.at[1], ls.at[1]),
        pltpu.make_async_copy(wq_ref.at[c], stage_q, ls.at[2]),
        pltpu.make_async_copy(wu_ref.at[:, pl.ds(c * UT, UT)], stage_u.at[0], ls.at[3]),
        pltpu.make_async_copy(
            wu_ref.at[:, pl.ds((n_col + c) * UT, UT)], stage_u.at[1], ls.at[4]
        ),
        pltpu.make_async_copy(wo_ref.at[pl.ds(c * HF, HF), :], stage_o, ls.at[5]),
        pltpu.make_async_copy(wd_ref.at[pl.ds(c * UT, UT), :], stage_d.at[0], ls.at[6]),
        pltpu.make_async_copy(wd_ref.at[pl.ds((n_col + c) * UT, UT), :], stage_d.at[1], ls.at[7]),
    ]
    for item in loads:
        item.start()
    stores = [
        pltpu.make_async_copy(stage_x.at[0], xf.at[pl.ds(r * T, T), pl.ds(c * C, C)], lo.at[0]),
        pltpu.make_async_copy(stage_x.at[1], gf.at[pl.ds(r * T, T), pl.ds(c * C, C)], lo.at[1]),
        pltpu.make_async_copy(stage_q, wi.at[pl.ds(c * C, C), pl.ds(0, qw)], lo.at[2]),
        pltpu.make_async_copy(stage_u.at[0], wi.at[pl.ds(c * C, C), pl.ds(qw, UT)], lo.at[3]),
        pltpu.make_async_copy(stage_u.at[1], wi.at[pl.ds(c * C, C), pl.ds(qw + UT, UT)], lo.at[4]),
        pltpu.make_async_copy(stage_o, wf.at[pl.ds(0, HF), pl.ds(c * C, C)], lo.at[5]),
        pltpu.make_async_copy(stage_d.at[0], wf.at[pl.ds(HF, UT), pl.ds(c * C, C)], lo.at[6]),
        pltpu.make_async_copy(stage_d.at[1], wf.at[pl.ds(HF + UT, UT), pl.ds(c * C, C)], lo.at[7]),
    ]
    for load, store in zip(loads, stores):
        load.wait()
        store.start()

    ck, hk, uk = C // n_dp, HF // n_dp, UT // n_dp

    def w_dst(part, dd, cc):
        if part == 0:
            return wi.at[pl.ds(cc * C + dd * ck, ck), pl.ds(0, qw)]
        if part == 1:
            return wi.at[pl.ds(cc * C + dd * ck, ck), pl.ds(qw, UT)]
        if part == 2:
            return wi.at[pl.ds(cc * C + dd * ck, ck), pl.ds(qw + UT, UT)]
        if part == 3:
            return wf.at[pl.ds(dd * hk, hk), pl.ds(cc * C, C)]
        if part == 4:
            return wf.at[pl.ds(HF + dd * uk, uk), pl.ds(cc * C, C)]
        return wf.at[pl.ds(HF + UT + dd * uk, uk), pl.ds(cc * C, C)]

    def w_src(part, cc):
        if part == 0:
            return wq_ref.at[cc, pl.ds(d * ck, ck), :]
        if part == 1:
            return wu_ref.at[pl.ds(d * ck, ck), pl.ds(cc * UT, UT)]
        if part == 2:
            return wu_ref.at[pl.ds(d * ck, ck), pl.ds((n_col + cc) * UT, UT)]
        if part == 3:
            return wo_ref.at[pl.ds(cc * HF + d * hk, hk), :]
        if part == 4:
            return wd_ref.at[pl.ds(cc * UT + d * uk, uk), :]
        return wd_ref.at[pl.ds((n_col + cc) * UT + d * uk, uk), :]

    def w_copy(part, k):
        dest = lax.rem(c + k, n_col)
        return copy(
            w_src(part, dest), w_dst(part, d, c), ws.at[part, k], wr.at[part, k], {"col": dest}
        )

    def w_got(part, k):
        return w_dst(part, d, lax.rem(c + n_col - k, n_col))

    def x_copy(part, k, j):
        return copy(
            w_got(part, k), w_got(part, k), ds.at[part, k, j], dr.at[part, k, j],
            {"dp": lax.rem(d + j, n_dp)},
        )

    parts = range(6)

    for s in range(1, n_col):
        for a, t in order:
            @pl.when(c - s >= 0)
            def _(a=a, t=t, s=s):
                cc = c - s
                z_copy(a, t, cc, blk(a, r, cc, t), True).wait_recv()

                @pl.when(c < n_col - 1)
                def _():
                    z_copy(a, t, cc, blk(a, r, cc, t), True).start()

                y_copy(a, t, cc, blk(a, r, cc, t)).start()
                c_copy(a, t, cc, blk(a, r, cc, t), r, 0).start()

            @pl.when(c + s < n_col)
            def _(a=a, t=t, s=s):
                cc = c + s
                z_copy(a, t, cc, blk(a, r, cc, t), False).wait_recv()

                @pl.when(c > 0)
                def _():
                    z_copy(a, t, cc, blk(a, r, cc, t), False).start()

                y_copy(a, t, cc, blk(a, r, cc, t)).start()
                c_copy(a, t, cc, blk(a, r, cc, t), r, 0).start()

        for part in parts:
            w_copy(part, s).start()

    for s in range(n_col):
        for a, t in order:
            for cc in ((c,) if s == 0 else (c - s, c + s)):
                @pl.when((cc >= 0) & (cc < n_col))
                def _(a=a, t=t, cc=cc):
                    y_copy(a, t, cc, blk(a, r, cc, t)).wait_recv()
                    c_copy(a, t, cc, blk(a, r2, cc, t), r2, 1).start()

    for k in range(1, n_col):
        for part in parts:
            w_copy(part, k).wait_recv()
            for j in range(1, n_dp):
                x_copy(part, k, j).start()

    for a, t in order:
        for cc in range(n_col):
            c_copy(a, t, cc, blk(a, r, cc, t), r, 0).wait_recv()
            c_copy(a, t, cc, blk(a, r, cc, t), r, 1).wait_recv()
    for k in range(1, n_col):
        for part in parts:
            for j in range(1, n_dp):
                x_copy(part, k, j).wait_recv()
    for a, t in order:
        for cc in range(n_col):
            @pl.when((cc <= c) & (c < n_col - 1))
            def _(a=a, t=t, cc=cc):
                z_copy(a, t, cc, blk(a, r, cc, t), True).wait_send()

            @pl.when((cc >= c) & (c > 0))
            def _(a=a, t=t, cc=cc):
                z_copy(a, t, cc, blk(a, r, cc, t), False).wait_send()

            y_copy(a, t, cc, blk(a, r, cc, t)).wait_send()
            c_copy(a, t, cc, blk(a, r, cc, t), r, 0).wait_send()
            c_copy(a, t, cc, blk(a, r, cc, t), r, 1).wait_send()
    for k in range(1, n_col):
        for part in parts:
            w_copy(part, k).wait_send()
            for j in range(1, n_dp):
                x_copy(part, k, j).wait_send()
    for store in stores:
        store.wait()


def gather_all(x, g, w_q, w_up, w_out, w_down, n_dp, n_row, n_col):
    T, C = x.shape
    HF = w_q.shape[2] // 3
    UT = w_up.shape[1] // (2 * n_col)
    n_in, n_out = 3 * HF + 2 * UT, HF + 2 * UT
    dma = pltpu.SemaphoreType.DMA
    return pl.pallas_call(
        functools.partial(gather_kernel, n_dp, n_row, n_col, (T, C, HF, UT)),
        name="gather_all",
        out_shape=(
            jax.ShapeDtypeStruct((n_row * T, n_col * C), BF16),
            jax.ShapeDtypeStruct((n_row * T, n_col * C), BF16),
            jax.ShapeDtypeStruct((n_col * C, n_in), BF16),
            jax.ShapeDtypeStruct((n_out, n_col * C), BF16),
        ),
        in_specs=[ANY] * 6,
        out_specs=(ANY,) * 4,
        scratch_shapes=[
            pltpu.VMEM((2, T, C), BF16),
            pltpu.VMEM((C, 3 * HF), BF16),
            pltpu.VMEM((2, C, UT), BF16),
            pltpu.VMEM((HF, C), BF16),
            pltpu.VMEM((2, UT, C), BF16),
            dma((2, 2, 2, n_col)),
            dma((2, 2, n_col)),
            dma((2, 2, n_col)),
            dma((2, 2, n_col)),
            dma((2, 2, 2, n_col)),
            dma((2, 2, 2, n_col)),
            dma((6, n_col)),
            dma((6, n_col)),
            dma((6, n_col, n_dp)),
            dma((6, n_col, n_dp)),
            dma((8,)),
            dma((8,)),
        ],
        compiler_params=pltpu.CompilerParams(collective_id=0, has_side_effects=True),
    )(x, g, w_q, w_up, w_out, w_down)


def pick(index, table):
    out = jnp.int32(table[0])
    for k in range(1, len(table)):
        out = jnp.where(index == k, jnp.int32(table[k]), out)
    return out


def reduce_kernel(n_row, n_col, dims, p_ref, q_ref, dwi_ref, dwf_ref,
                  res_ref, gn_ref, tiles_ref,
                  abuf, obuf, sbuf, bbuf, zsb, zin, gi, gf, oi, of,
                  a_s, a_r, o_l, y_s, y_r, z_s, z_r, x_s, x_r, g_l, t_s, t_r):
    T, C, HF, UT, chunks = dims
    tc = T // chunks
    step_rows = 64
    d, r, c = lax.axis_index("dp"), lax.axis_index("row"), lax.axis_index("col")
    r1 = r + 1 - 2 * lax.rem(r, 2)
    r2 = lax.rem(r + 2, n_row)
    r12 = lax.rem(r1 + 2, n_row)
    srcs = (p_ref, q_ref)
    outs = (res_ref, gn_ref)
    far = [
        sorted(range(n_col), key=lambda f: (-abs(f - cc), f < cc if cc < n_col // 2 else f > cc))
        for cc in range(n_col)
    ]
    forder = [pick(c, [far[cc][i] for cc in range(n_col)]) for i in range(n_col)]

    barrier = pltpu.get_barrier_semaphore()
    peers = [{"row": r1}, {"row": r2}, {"dp": 1 - d}]
    peers += [{"col": lax.rem(c + k, n_col)} for k in range(1, n_col)]
    for peer in peers:
        pl.semaphore_signal(barrier, inc=1, device_id=peer, device_id_type=MESH)
    pl.semaphore_wait(barrier, len(peers))

    def copy(src, dst, s, rcv, peer):
        return pltpu.make_async_remote_copy(
            src_ref=src, dst_ref=dst, send_sem=s, recv_sem=rcv, device_id=peer, device_id_type=MESH
        )

    def unit(v, rr, f, t):
        return srcs[v].at[pl.ds(rr * T + t * tc, tc), pl.ds(f * C, C)]

    def a_copy(v, h, f, t):
        return copy(
            unit(v, r12 if h else r1, f, t), abuf.at[v, h, f, t],
            a_s.at[v, h, f, t], a_r.at[v, h, f, t], {"row": r1},
        )

    def o_copy(v, h, f, t):
        return pltpu.make_async_copy(
            unit(v, r2 if h else r, f, t), obuf.at[v, h, f, t], o_l.at[v, h, f, t]
        )

    def y_copy(v, f, t):
        return copy(sbuf.at[v, f, t], bbuf.at[v, f, t], y_s.at[v, f, t], y_r.at[v, f, t],
                    {"row": r2})

    def z_copy(v, f, t, slot, step):
        return copy(zsb.at[v, f, t], zin.at[v, slot, t], z_s.at[v, f, t], z_r.at[v, slot, t],
                    {"col": c + step})

    for v in range(2):
        for i in range(n_col):
            for t in range(chunks):
                for h in (1, 0):
                    a_copy(v, h, forder[i], t).start()
                    o_copy(v, h, forder[i], t).start()

    qw, n_in, n_out = 3 * HF, 3 * HF + 2 * UT, HF + 2 * UT
    wide = (qw + UT, UT)
    lane0 = (0, qw + UT)
    tall = (HF, 2 * UT)
    row0 = (0, HF)

    def gi_src(own, cc):
        return dwi_ref.at[pl.ds(cc * C, C), pl.ds(lane0[own], wide[own])]

    def gf_src(own, cc):
        return dwf_ref.at[pl.ds(row0[own], tall[own]), pl.ds(cc * C, C)]

    def xi_copy(own, cc):
        return copy(gi_src(own, cc), gi.at[cc, :, pl.ds(0, wide[own])], x_s.at[0, cc],
                    x_r.at[0, cc], {"dp": 1 - d})

    def xf_copy(own, cc):
        return copy(gf_src(own, cc), gf.at[cc, pl.ds(0, tall[own]), :], x_s.at[1, cc],
                    x_r.at[1, cc], {"dp": 1 - d})

    def li_copy(own, cc):
        return pltpu.make_async_copy(gi_src(own, cc), oi.at[cc, :, pl.ds(0, wide[own])],
                                     g_l.at[0, cc])

    def lf_copy(own, cc):
        return pltpu.make_async_copy(gf_src(own, cc), of.at[cc, pl.ds(0, tall[own]), :],
                                     g_l.at[1, cc])

    def tile_parts(own, cc, source):
        half, odd = source // 2, lax.rem(source, 2)
        lw = 2 * HF
        if own == 0:
            parts = [
                (oi.at[cc, :, pl.ds(j * HF, HF)], tiles_ref.at[2 * j + half, :, pl.ds(odd * HF, HF)])
                for j in range(3)
            ]
            parts += [(oi.at[cc, :, pl.ds(qw, UT)], tiles_ref.at[8 + source])]
            parts += [
                (of.at[cc, pl.ds(0, HF), pl.ds(j * lw, lw)],
                 tiles_ref.at[6 + j, pl.ds(source * HF, HF), :])
                for j in range(2)
            ]
            return parts
        parts = [(oi.at[cc, :, pl.ds(0, UT)], tiles_ref.at[source])]
        for m in range(2):
            for j in range(2):
                parts.append(
                    (of.at[cc, pl.ds(m * UT, UT), pl.ds(j * lw, lw)],
                     tiles_ref.at[4 + 2 * (2 * m + half) + j, pl.ds(odd * UT, UT), :])
                )
        return parts

    def t_copies(own, cc):
        return [
            copy(src, dst, t_s.at[n, cc], t_r.at[n, c], {"col": cc})
            for n, (src, dst) in enumerate(tile_parts(own, cc, c))
        ]

    def t_waits(own, source):
        return [
            copy(src, dst, t_s.at[n, source], t_r.at[n, source], {"col": source})
            for n, (src, dst) in enumerate(tile_parts(own, source, source))
        ]

    def t_local(own):
        return [
            pltpu.make_async_copy(src, dst, t_s.at[n, c])
            for n, (src, dst) in enumerate(tile_parts(own, c, c))
        ]

    for i in range(n_col):
        for own in range(2):
            @pl.when(d == own)
            def _(own=own, i=i):
                xi_copy(1 - own, forder[i]).start()
                xf_copy(1 - own, forder[i]).start()
                li_copy(own, forder[i]).start()
                lf_copy(own, forder[i]).start()

    def looped(rows, fn):
        def one(k, carry):
            fn(pl.ds(pl.multiple_of(k * step_rows, step_rows), step_rows))
            return carry
        lax.fori_loop(0, rows // step_rows, one, 0)

    def first_sum(v, i):
        f = forder[i]
        for t in range(chunks):
            a_copy(v, 1, f, t).wait_recv()
            o_copy(v, 1, f, t).wait()

            def add(rows, t=t):
                sbuf[v, f, t, rows, :] = (
                    obuf[v, 1, f, t, rows, :].astype(F32) + abuf[v, 1, f, t, rows, :].astype(F32)
                ).astype(BF16)

            looped(tc, add)
            y_copy(v, f, t).start()

    def second_sum(v, i):
        f = forder[i]
        for t in range(chunks):
            a_copy(v, 0, f, t).wait_recv()
            o_copy(v, 0, f, t).wait()
            y_copy(v, f, t).wait_recv()

            def base(rows, t=t):
                return (
                    obuf[v, 0, f, t, rows, :].astype(F32)
                    + abuf[v, 0, f, t, rows, :].astype(F32)
                    + bbuf[v, f, t, rows, :].astype(F32)
                )

            if i < n_col - 1:
                right = f > c
                step = jnp.where(right, jnp.int32(1), jnp.int32(-1))
                landed = jnp.where(f == c + step, jnp.where(right, f, jnp.int32(n_col)), f)
                inner = jnp.where(right, c, n_col - 1 - c) > 0

                @pl.when(inner)
                def _(t=t):
                    z_copy(v, f, t, f, 0).wait_recv()

                    def add(rows):
                        zsb[v, f, t, rows, :] = (
                            base(rows) + zin[v, f, t, rows, :].astype(F32)
                        ).astype(BF16)

                    looped(tc, add)

                @pl.when(jnp.logical_not(inner))
                def _(t=t):
                    def add(rows):
                        zsb[v, f, t, rows, :] = base(rows).astype(BF16)

                    looped(tc, add)

                z_copy(v, f, t, landed, step).start()
            else:
                out = outs[v]

                def put(rows, value, t=t):
                    out[pl.ds(pl.multiple_of(rows.start + t * tc, step_rows), step_rows), :] = value

                @pl.when(c > 0)
                def _(t=t):
                    z_copy(v, f, t, f, 0).wait_recv()

                @pl.when(c < n_col - 1)
                def _(t=t):
                    z_copy(v, f, t, n_col, 0).wait_recv()

                @pl.when(c == 0)
                def _(t=t):
                    looped(tc, lambda rows: put(
                        rows, base(rows) + zin[v, n_col, t, rows, :].astype(F32)))

                @pl.when(c == n_col - 1)
                def _(t=t):
                    looped(tc, lambda rows: put(
                        rows, base(rows) + zin[v, f, t, rows, :].astype(F32)))

                @pl.when((c > 0) & (c < n_col - 1))
                def _(t=t):
                    looped(tc, lambda rows: put(
                        rows, base(rows) + zin[v, f, t, rows, :].astype(F32)
                        + zin[v, n_col, t, rows, :].astype(F32)))

    def grad_piece(i):
        cc = forder[i]
        for own in range(2):
            @pl.when(d == own)
            def _(own=own):
                xi_copy(own, cc).wait_recv()
                xf_copy(own, cc).wait_recv()
                li_copy(own, cc).wait()
                lf_copy(own, cc).wait()

                def add_i(rows):
                    at = (cc, rows, pl.ds(0, wide[own]))
                    oi[at] = (oi[at].astype(F32) + gi[at].astype(F32)).astype(BF16)

                def add_f(rows):
                    at = (cc, rows, slice(None))
                    of[at] = (of[at].astype(F32) + gf[at].astype(F32)).astype(BF16)

                looped(C, add_i)
                looped(tall[own], add_f)
                for item in t_local(own) if i == n_col - 1 else t_copies(own, cc):
                    item.start()

    for i in range(n_col):
        first_sum(0, i)
    for i in range(n_col):
        second_sum(0, i)
        first_sum(1, i)
        grad_piece(i)
    for i in range(n_col):
        second_sum(1, i)

    for own in range(2):
        @pl.when(d == own)
        def _(own=own):
            for k in range(1, n_col):
                for item in t_waits(own, lax.rem(c + k, n_col)):
                    item.wait_recv()
            for i in range(n_col - 1):
                for item in t_copies(own, forder[i]):
                    item.wait_send()
            for item in t_local(own):
                item.wait()
            for cc in range(n_col):
                xi_copy(1 - own, cc).wait_send()
                xf_copy(1 - own, cc).wait_send()
    for v in range(2):
        for t in range(chunks):
            for f in range(n_col):
                a_copy(v, 0, f, t).wait_send()
                a_copy(v, 1, f, t).wait_send()
                y_copy(v, f, t).wait_send()
            for i in range(n_col - 1):
                z_copy(v, forder[i], t, forder[i], 0).wait_send()


def reduce_all(p, q, dwi, dwf, T, C, HF, UT, n_row, n_col):
    dma = pltpu.SemaphoreType.DMA
    chunks = 2
    tc = T // chunks
    unit = (chunks, tc, C)
    vm = pl.BlockSpec(memory_space=pltpu.VMEM)
    return pl.pallas_call(
        functools.partial(reduce_kernel, n_row, n_col, (T, C, HF, UT, chunks)),
        name="reduce_all",
        out_shape=(
            jax.ShapeDtypeStruct((T, C), F32),
            jax.ShapeDtypeStruct((T, C), F32),
            jax.ShapeDtypeStruct((12, C, UT), BF16),
        ),
        in_specs=[ANY] * 4,
        out_specs=(vm, vm, ANY),
        scratch_shapes=[
            pltpu.VMEM((2, 2, n_col) + unit, BF16),
            pltpu.VMEM((2, 2, n_col) + unit, BF16),
            pltpu.VMEM((2, n_col) + unit, BF16),
            pltpu.VMEM((2, n_col) + unit, BF16),
            pltpu.VMEM((2, n_col) + unit, BF16),
            pltpu.VMEM((2, n_col + 1) + unit, BF16),
            pltpu.VMEM((n_col, C, 3 * HF + UT), BF16),
            pltpu.VMEM((n_col, 2 * UT, C), BF16),
            pltpu.VMEM((n_col, C, 3 * HF + UT), BF16),
            pltpu.VMEM((n_col, 2 * UT, C), BF16),
            dma((2, 2, n_col, chunks)),
            dma((2, 2, n_col, chunks)),
            dma((2, 2, n_col, chunks)),
            dma((2, n_col, chunks)),
            dma((2, n_col, chunks)),
            dma((2, n_col, chunks)),
            dma((2, n_col + 1, chunks)),
            dma((2, n_col)),
            dma((2, n_col)),
            dma((2, n_col)),
            dma((6, n_col)),
            dma((6, n_col)),
        ],
        compiler_params=pltpu.CompilerParams(
            collective_id=1, has_side_effects=True, vmem_limit_bytes=62 * 1024 * 1024
        ),
    )(p, q, dwi, dwf)


def finish_kernel(n_dp, n_row, n_col, width, gn_ref, x_ref, g_ref, mean_ref, rstd_ref, gain_ref, part_ref,
                  gx_ref, va_ref, vb_ref,
                  st, da, db, ra, rb,
                  st_s, st_r, d_s, d_r, r_s, r_r, c_s, c_r):
    d, r, c = lax.axis_index("dp"), lax.axis_index("row"), lax.axis_index("col")
    T, C = gn_ref.shape

    barrier = pltpu.get_barrier_semaphore()
    dps = [lax.rem(d + k, n_dp) for k in range(1, n_dp)]
    rows = [lax.rem(r + k, n_row) for k in range(1, n_row)]
    cols = [lax.rem(c + k, n_col) for k in range(1, n_col)]
    peers = [{"dp": k} for k in dps] + [{"row": k} for k in rows] + [{"col": k} for k in cols]
    for peer in peers:
        pl.semaphore_signal(barrier, inc=1, device_id=peer, device_id_type=MESH)
    pl.semaphore_wait(barrier, len(peers))

    def copy(src, dst, s, rcv, peer):
        return pltpu.make_async_remote_copy(
            src_ref=src, dst_ref=dst, send_sem=s, recv_sem=rcv, device_id=peer, device_id_type=MESH
        )

    gain = gain_ref[...]

    def fold(value):
        total = value[:, 0:128]
        for k in range(1, C // 128):
            total = total + value[:, k * 128 : (k + 1) * 128]
        return jnp.sum(jnp.transpose(total), axis=0, keepdims=True)

    gn = gn_ref[...]
    x_hat = (x_ref[...].astype(F32) - mean_ref[...]) * rstd_ref[...]
    gh = gn * gain
    st[c, 0:1, :] = fold(gh)
    st[c, 1:2, :] = fold(gh * x_hat)

    def st_copy(k):
        return copy(st.at[c], st.at[c], st_s.at[k], st_r.at[c], {"col": k})

    def st_wait(k):
        return copy(st.at[k], st.at[k], st_s.at[k], st_r.at[k], {"col": k})

    for k in cols:
        st_copy(k).start()

    da[d] = part_ref[...]
    db[d, 0:1, :] = jnp.sum(gn * x_hat, axis=0, keepdims=True)
    db[d, 1:2, :] = jnp.sum(gn, axis=0, keepdims=True)
    db[d, 2:3, :] = jnp.sum(g_ref[...].astype(F32), axis=0, keepdims=True)

    def pair(a_src, b_src, a_dst, b_dst, s, rcv, peer):
        return [copy(a_src, a_dst, s.at[0], rcv.at[0], peer),
                copy(b_src, b_dst, s.at[1], rcv.at[1], peer)]

    def d_pair(slot, peer):
        return pair(da.at[slot], db.at[slot], da.at[slot], db.at[slot],
                    d_s.at[peer], d_r.at[slot], {"dp": peer})

    def r_pair(slot, peer):
        return pair(ra.at[slot], rb.at[slot], ra.at[slot], rb.at[slot],
                    r_s.at[peer], r_r.at[slot], {"row": peer})

    def c_pair(slot, peer):
        return pair(va_ref.at[slot], vb_ref.at[slot], va_ref.at[slot], vb_ref.at[slot],
                    c_s.at[peer], c_r.at[slot], {"col": peer})

    for k in dps:
        for item in d_pair(d, k):
            item.start()
    for k in dps:
        for item in d_pair(k, k):
            item.wait_recv()
    a_sum, b_sum = da[0], db[0]
    for k in range(1, n_dp):
        a_sum = a_sum + da[k]
        b_sum = b_sum + db[k]
    ra[r] = a_sum
    rb[r] = b_sum
    for k in rows:
        for item in r_pair(r, k):
            item.start()

    for k in cols:
        st_wait(k).wait_recv()
    stats = st[0]
    for k in range(1, n_col):
        stats = stats + st[k]
    stats = stats / width
    m1 = jnp.transpose(jnp.broadcast_to(stats[0:1, :], (128, T)))[:, 0:1]
    m2 = jnp.transpose(jnp.broadcast_to(stats[1:2, :], (128, T)))[:, 0:1]
    gx_ref[...] = g_ref[...].astype(F32) + rstd_ref[...] * (gh - m1 - x_hat * m2)

    for k in rows:
        for item in r_pair(k, k):
            item.wait_recv()
    b_sum = rb[0]
    for k in range(1, n_row):
        b_sum = b_sum + rb[k]
    for k in range(n_row):
        va_ref[c, k] = ra[k]
    vb_ref[c] = b_sum
    for k in cols:
        for item in c_pair(c, k):
            item.start()
    for k in cols:
        for item in c_pair(k, k):
            item.wait_recv()
    for k in cols:
        st_copy(k).wait_send()
        for item in c_pair(c, k):
            item.wait_send()
    for k in dps:
        for item in d_pair(d, k):
            item.wait_send()
    for k in rows:
        for item in r_pair(r, k):
            item.wait_send()


def finish_all(gn, x, g, mean, rstd, gain, part, width, n_dp, n_row, n_col):
    T, C = gn.shape
    dma = pltpu.SemaphoreType.DMA
    vm = pl.BlockSpec(memory_space=pltpu.VMEM)
    return pl.pallas_call(
        functools.partial(finish_kernel, n_dp, n_row, n_col, width),
        name="finish_all",
        out_shape=(
            jax.ShapeDtypeStruct((T, C), F32),
            jax.ShapeDtypeStruct((n_col, n_row, 8, 128), F32),
            jax.ShapeDtypeStruct((n_col, 8, C), F32),
        ),
        in_specs=[vm] * 7,
        out_specs=(vm,) * 3,
        scratch_shapes=[
            pltpu.VMEM((n_col, 8, T), F32),
            pltpu.VMEM((n_dp, 8, 128), F32),
            pltpu.VMEM((n_dp, 8, C), F32),
            pltpu.VMEM((n_row, 8, 128), F32),
            pltpu.VMEM((n_row, 8, C), F32),
            dma((n_col,)),
            dma((n_col,)),
            dma((n_dp, 2)),
            dma((n_dp, 2)),
            dma((n_row, 2)),
            dma((n_row, 2)),
            dma((n_col, 2)),
            dma((n_col, 2)),
        ],
        compiler_params=pltpu.CompilerParams(
            collective_id=2, has_side_effects=True, vmem_limit_bytes=48 * 1024 * 1024
        ),
    )(gn, x, g, mean, rstd, gain, part)


def muon_kernel(owned, per_step, HF, UT, rate, grad_ref, mom_ref, wq_ref, wo_ref, wu_ref, wd_ref,
                og_ref, new_ref, nm_ref, wbuf, sem):
    first = lax.axis_index("dp") * owned
    step = pl.program_id(0)
    steps = owned // per_step
    n_qkv, n_out, n_up = 6, 2, 8

    def fetch(tile, slot, n, start):
        dst = wbuf.at[slot, n]

        def go(src, target, s):
            item = pltpu.make_async_copy(src, target, s)
            if start:
                item.start()
            else:
                item.wait()

        @pl.when(tile < n_qkv)
        def _():
            j, half = lax.div(tile, 2), lax.rem(tile, 2)
            for m in range(UT // HF):
                go(wq_ref.at[half * (UT // HF) + m, :, pl.ds(j * HF, HF)],
                   wbuf.at[slot, n, :, pl.ds(m * HF, HF)], sem.at[slot, n, m])

        @pl.when((tile >= n_qkv) & (tile < n_qkv + n_out))
        def _():
            go(wo_ref.at[:, pl.ds((tile - n_qkv) * UT, UT)], dst, sem.at[slot, n, 0])

        @pl.when((tile >= n_qkv + n_out) & (tile < n_qkv + n_out + n_up))
        def _():
            go(wu_ref.at[:, pl.ds((tile - n_qkv - n_out) * UT, UT)], dst, sem.at[slot, n, 0])

        @pl.when(tile >= n_qkv + n_out + n_up)
        def _():
            left = tile - (n_qkv + n_out + n_up)
            rows = dst.shape[0]
            go(wd_ref.at[pl.ds(lax.div(left, 2) * rows, rows), pl.ds(lax.rem(left, 2) * UT, UT)],
               dst, sem.at[slot, n, 0])

    def fetch_all(at, start):
        for n in range(per_step):
            fetch(first + at * per_step + n, lax.rem(at, 2), n, start)

    @pl.when(step == 0)
    def _():
        fetch_all(step, True)

    @pl.when(step + 1 < steps)
    def _():
        fetch_all(step + 1, True)

    iters = []
    for n in range(per_step):
        grad = grad_ref[n].astype(F32)
        og_ref[n] = grad
        moment = MOMENTUM_RATE * mom_ref[n] + grad
        nm_ref[n] = moment
        scale = lax.rsqrt(jnp.sum(moment * moment, keepdims=True) + STAT_EPS)
        iters.append((moment * scale).astype(BF16))
    contract = (((0,), (0,)), ((), ()))
    for _ in range(5):
        grams = [
            lax.dot_general(x, x, contract, preferred_element_type=F32).astype(BF16) for x in iters
        ]
        squares = [jnp.dot(g, g, preferred_element_type=F32) for g in grams]
        polys = [
            (NEWTON_B * g.astype(F32) + NEWTON_C * s).astype(BF16) for g, s in zip(grams, squares)
        ]
        iters = [
            (NEWTON_A * x.astype(F32) + jnp.dot(x, p, preferred_element_type=F32)).astype(BF16)
            for x, p in zip(iters, polys)
        ]
    fetch_all(step, False)
    for n in range(per_step):
        new_ref[n] = wbuf[lax.rem(step, 2), n].astype(F32) - rate * iters[n].astype(F32)


def muon_all(grads, moment, w_q, w_out, w_up, w_down, HF, UT):
    owned, rows, cols = moment.shape
    per_step = 3
    rate = MUON_RATE * math.sqrt(max(1.0, rows / cols))
    block = pl.BlockSpec((per_step, rows, cols), lambda i: (i, 0, 0))
    out = jax.ShapeDtypeStruct(moment.shape, F32)
    return pl.pallas_call(
        functools.partial(muon_kernel, owned, per_step, HF, UT, rate),
        name="muon_all",
        grid=(owned // per_step,),
        out_shape=(out, out, out),
        in_specs=[block, block, ANY, ANY, ANY, ANY],
        out_specs=(block, block, block),
        scratch_shapes=[
            pltpu.VMEM((2, per_step, rows, cols), BF16),
            pltpu.SemaphoreType.DMA((2, per_step, 2)),
        ],
        compiler_params=pltpu.CompilerParams(vmem_limit_bytes=56 * 1024 * 1024),
    )(grads, moment, w_q, w_out, w_up, w_down)


def reduce_plain(p, q, dwi, dwf, C, HF, UT, n_col, row_width):
    def block(part):
        part = lax.psum_scatter(part, "row", scatter_dimension=0, tiled=True)
        return lax.psum_scatter(part, "col", scatter_dimension=1, tiled=True).astype(F32)

    wi4 = lax.all_to_all(dwi.reshape(n_col, C, -1), "col", 0, 0)
    wf4 = lax.all_to_all(dwf.reshape(-1, n_col, C).transpose(1, 0, 2), "col", 0, 0)
    grad_qkv = (
        wi4[:, :, : 3 * HF].reshape(n_col, C, 3, HF).transpose(1, 2, 0, 3).reshape(C, 3, row_width)
    )
    grad_up_w = wi4[:, :, 3 * HF :].reshape(n_col, C, 2, UT).transpose(1, 2, 0, 3).reshape(C, -1)
    grad_w_out = wf4[:, :HF].reshape(-1, C)
    grad_w_down = wf4[:, HF:].reshape(n_col, 2, UT, C).transpose(1, 0, 2, 3).reshape(-1, C)
    grad_tiles = tile_blocks(grad_qkv, grad_w_out, grad_up_w, grad_w_down)
    owned = lax.psum_scatter(grad_tiles, "dp", scatter_dimension=0, tiled=True)
    return block(p), block(q), owned


def body(
    inputs,
    cotangent,
    segments,
    positions,
    w_qkv,
    w_out,
    w_up,
    w_down,
    vectors,
    tile_moment,
    vector_moment,
):
    d_index = lax.axis_index("dp")
    row_index = lax.axis_index("row")
    col_index = lax.axis_index("col")
    n_dp, n_row, n_col = lax.axis_size("dp"), lax.axis_size("row"), lax.axis_size("col")
    T, C = inputs.shape
    D = vectors.shape[1]
    row_width = w_qkv.shape[2]
    HF = row_width // n_col
    UT = w_up.shape[1] // (2 * n_col)
    score_scale = HEAD_DIM ** (-0.5)
    feat_start = (row_index * n_col + col_index) * HF
    unit_a = (row_index * 2 * n_col + col_index) * UT
    unit_b = unit_a + n_col * UT
    col_start = col_index * C
    gain, shift = vectors[5], vectors[6]
    norm_gain = lax.dynamic_slice_in_dim(gain, col_start, C)
    out_bias = lax.dynamic_slice_in_dim(vectors[3] + vectors[4], col_start, C)
    qkv_bias = lax.dynamic_slice_in_dim(vectors[0:3], feat_start, HF, axis=1)
    up_flat = vectors[7:].reshape(-1)
    up_bias = jnp.concatenate(
        [
            lax.dynamic_slice_in_dim(up_flat, unit_a, UT),
            lax.dynamic_slice_in_dim(up_flat, unit_b, UT),
        ]
    )
    w_q = (
        w_qkv.reshape(C, 3, n_col, HF).transpose(2, 0, 1, 3).reshape(n_col, C, 3 * HF)
    )
    x_full, cot_rows, w_in, w_fin = gather_all(
        inputs, cotangent, w_q, w_up, w_out, w_down, n_dp, n_row, n_col
    )
    seq_rows = x_full.shape[0]

    x_wide = x_full.astype(F32)
    mean_all = jnp.mean(x_wide, axis=1, keepdims=True)
    var_all = jnp.mean(x_wide * x_wide, axis=1, keepdims=True) - mean_all * mean_all
    rstd_all = lax.rsqrt(var_all + NORM_EPS)
    normed = ((x_wide - mean_all) * rstd_all * gain + shift).astype(BF16)

    mixed_out = jnp.dot(normed, w_in, preferred_element_type=F32)
    qkv_part = mixed_out[:, : 3 * HF].reshape(seq_rows, 3, HF) + qkv_bias[None]
    up_pre = mixed_out[:, 3 * HF :] + up_bias
    heads_here = HF // HEAD_DIM
    seq_count = seq_rows // SEQ_LEN

    def by_seq(tensor_in):
        return tensor_in.reshape((seq_count, SEQ_LEN) + tensor_in.shape[1:])

    cosine, sine_tab = rotary_tables(positions)
    queries = rotate(
        qkv_part[:, 0].reshape(seq_rows, heads_here, HEAD_DIM), cosine, sine_tab, 1.0
    ).astype(BF16)
    key_vecs = rotate(
        qkv_part[:, 1].reshape(seq_rows, heads_here, HEAD_DIM), cosine, sine_tab, 1.0
    ).astype(BF16)
    values = qkv_part[:, 2].reshape(seq_rows, heads_here, HEAD_DIM).astype(BF16)
    attended, logsum = jax.vmap(attend_forward, in_axes=(0, 0, 0, 0, None))(
        by_seq(queries), by_seq(key_vecs), by_seq(values), by_seq(segments), score_scale
    )
    attn_low = attended.reshape(seq_rows, HF).astype(BF16)
    act_low = gelu_value(up_pre).astype(BF16)
    hidden = jnp.concatenate([attn_low, act_low], axis=1)

    partial_out = jnp.dot(hidden, w_fin, preferred_element_type=F32).astype(BF16)
    x_val = inputs.astype(F32)

    grad_w_fin = jnp.einsum("ti,tj->ij", hidden, cot_rows, preferred_element_type=F32).astype(BF16)
    back = jnp.einsum("tj,ij->ti", cot_rows, w_fin, preferred_element_type=F32)
    grad_attn_low = back[:, :HF].astype(BF16)
    grad_up = back[:, HF:] * gelu_slope(up_pre)
    g_queries, g_keys, g_values = jax.vmap(attend_backward, in_axes=(0, 0, 0, 0, 0, 0, 0, None))(
        by_seq(queries),
        by_seq(key_vecs),
        by_seq(values),
        by_seq(attn_low.reshape(seq_rows, heads_here, HEAD_DIM)),
        by_seq(grad_attn_low.reshape(seq_rows, heads_here, HEAD_DIM)),
        logsum,
        by_seq(segments),
        score_scale,
    )
    g_queries = rotate(
        g_queries.reshape(seq_rows, heads_here, HEAD_DIM), cosine, sine_tab, -1.0
    ).reshape(seq_rows, HF)
    g_keys = rotate(g_keys.reshape(seq_rows, heads_here, HEAD_DIM), cosine, sine_tab, -1.0).reshape(
        seq_rows, HF
    )
    g_values = g_values.reshape(seq_rows, HF)
    grad_mixed = jnp.concatenate([g_queries, g_keys, g_values, grad_up], axis=1)
    grad_mixed_low = grad_mixed.astype(BF16)
    grad_w_in = jnp.einsum(
        "ti,tj->ij", normed, grad_mixed_low, preferred_element_type=F32
    ).astype(BF16)
    partial_norm = jnp.einsum(
        "tj,ij->ti", grad_mixed_low, w_in, preferred_element_type=F32
    ).astype(BF16)

    if n_dp == 2:
        branch, grad_norm, owned_low = reduce_all(
            partial_out, partial_norm, grad_w_in, grad_w_fin, T, C, HF, UT, n_row, n_col
        )
    else:
        branch, grad_norm, owned_low = reduce_plain(
            partial_out, partial_norm, grad_w_in, grad_w_fin, C, HF, UT, n_col, row_width
        )
    result = x_val + branch + out_bias

    sums = jnp.sum(grad_mixed, axis=0)
    part = jnp.pad(sums.reshape(-1, 128), ((0, 1), (0, 0)))
    grad_input, vec_a, vec_b = finish_all(
        grad_norm,
        inputs,
        cotangent,
        lax.dynamic_slice_in_dim(mean_all, row_index * T, T),
        lax.dynamic_slice_in_dim(rstd_all, row_index * T, T),
        norm_gain[None],
        part,
        D,
        n_dp,
        n_row,
        n_col,
    )
    vec_a = vec_a.transpose(2, 1, 0, 3)
    qkv_rows = vec_a[:3].reshape(3, D)
    up_rows = vec_a[3:7].reshape(2, UT // 128, n_row, n_col, 128).transpose(2, 0, 3, 1, 4)
    norm_rows = vec_b.transpose(1, 0, 2).reshape(8, D)
    vec_grad = jnp.concatenate(
        [qkv_rows, norm_rows[2:3], norm_rows[2:3], norm_rows[:2], up_rows.reshape(-1, D)], axis=0
    )
    scaled = vec_grad * lax.rsqrt(jnp.mean(vec_grad * vec_grad, axis=1, keepdims=True) + STAT_EPS)
    vec_moment_new = MOMENTUM_RATE * vector_moment + scaled
    vectors_new = vectors - VECTOR_RATE * vec_moment_new

    owned_grads, tiles_new, moment_new = muon_all(
        owned_low, tile_moment[0, 0], w_q, w_out, w_up, w_down, HF, UT
    )
    return (
        result,
        grad_input,
        owned_grads[None, None],
        tiles_new[None, None],
        moment_new[None, None],
        vec_grad,
        vectors_new,
        vec_moment_new,
    )


def solution(mesh):
    placed = (
        P(("dp", "row"), "col"),
        P(("dp", "row"), "col"),
        P("dp"),
        P("dp"),
        P("col", None, "row"),
        P("row", "col"),
        P("col", "row"),
        P("row", "col"),
        P(),
        P("row", "col", "dp", None, None),
        P(),
    )
    return jax.shard_map(
        body,
        mesh=mesh,
        in_specs=placed,
        out_specs=(
            P(("dp", "row"), "col"),
            P(("dp", "row"), "col"),
            P("row", "col", "dp", None, None),
            P("row", "col", "dp", None, None),
            P("row", "col", "dp", None, None),
            P(),
            P(),
            P(),
        ),
        check_vma=False,
    )
```

```python
import functools
import math

import jax
import jax.numpy as jnp
from jax import lax
from jax.experimental import pallas as pl
from jax.experimental.pallas import tpu as pltpu
from jax.sharding import PartitionSpec as P

HEAD_DIM = 64
ROTARY = 32
SEQ_LEN = 512

MOMENTUM_RATE = 0.95
MUON_RATE = 0.05
VECTOR_RATE = 0.12
NEWTON_A = 3.4445
NEWTON_B = -4.775
NEWTON_C = 2.0315
GELU_SCALE = 0.7978845608028654
GELU_CUBIC = 0.044715
NORM_EPS = 1e-05
STAT_EPS = 1e-06
MASKED_SCORE = -1e30

MESH = pl.DeviceIdType.MESH
ANY = pl.BlockSpec(memory_space=pl.ANY)
F32 = jnp.float32
BF16 = jnp.bfloat16


def to_low(tensor_in):
    return lax.optimization_barrier(tensor_in.astype(BF16))


def gelu_value(pre_act):
    inner_arg = GELU_SCALE * (pre_act + GELU_CUBIC * pre_act * pre_act * pre_act)
    return 0.5 * pre_act * (1.0 + jnp.tanh(inner_arg))


def gelu_slope(pre_act):
    tanh_val = jnp.tanh(GELU_SCALE * (pre_act + GELU_CUBIC * pre_act * pre_act * pre_act))
    return 0.5 * (1.0 + tanh_val) + 0.5 * pre_act * (1.0 - tanh_val * tanh_val) * GELU_SCALE * (
        1.0 + 3.0 * GELU_CUBIC * pre_act * pre_act
    )


def rotary_tables(positions):
    half_dims = ROTARY // 2
    frequency = jnp.exp(jnp.arange(half_dims, dtype=F32) * (-2.0 * math.log(10000.0) / ROTARY))
    angles = positions.astype(F32)[:, None] * frequency[None, :]
    return (jnp.cos(angles), jnp.sin(angles))


def rotate(tensor_in, cosine, sine_tab, direction_sign):
    half_dims = ROTARY // 2
    first_half = tensor_in[..., :half_dims]
    second_half = tensor_in[..., half_dims:ROTARY]
    cos_wide = cosine[:, None, :]
    sin_wide = sine_tab[:, None, :] * direction_sign
    return jnp.concatenate(
        [
            first_half * cos_wide - second_half * sin_wide,
            second_half * cos_wide + first_half * sin_wide,
            tensor_in[..., ROTARY:],
        ],
        axis=-1,
    )


def causal_allowed(segment):
    token_order = jnp.arange(segment.shape[0])
    return (segment[:, None] == segment[None, :]) & (token_order[:, None] >= token_order[None, :])


def masked_scores(queries, key_vecs, segment, score_scale):
    scores = (
        jnp.einsum("lhe,mhe->hlm", queries, key_vecs, preferred_element_type=F32) * score_scale
    )
    return jnp.where(causal_allowed(segment)[None], scores, MASKED_SCORE)


def attend_backward(queries, key_vecs, values, output_low, grad_low, logsum, segment, score_scale):
    scores = masked_scores(queries, key_vecs, segment, score_scale)
    probs = jnp.exp(scores - logsum[..., None])
    grad_values = jnp.einsum("hlm,lhe->mhe", to_low(probs), grad_low, preferred_element_type=F32)
    grad_probs = jnp.einsum("lhe,mhe->hlm", grad_low, values, preferred_element_type=F32)
    row_delta = jnp.sum(grad_low.astype(F32) * output_low.astype(F32), axis=-1)
    grad_scores = to_low(probs * (grad_probs - row_delta.T[:, :, None]) * score_scale)
    grad_queries = jnp.einsum("hlm,mhe->lhe", grad_scores, key_vecs, preferred_element_type=F32)
    grad_keys = jnp.einsum("hlm,lhe->mhe", grad_scores, queries, preferred_element_type=F32)
    return (grad_queries, grad_keys, grad_values)


def tile_blocks(qkv_block, out_block, up_block, down_block):
    tile_rows = qkv_block.shape[0]
    tile_cols = qkv_block.shape[2] // 2

    def split_cols(block_in):
        return block_in.reshape(
            block_in.shape[0], block_in.shape[1] // tile_cols, tile_cols
        ).transpose(1, 0, 2)

    down_part = down_block.reshape(
        down_block.shape[0] // tile_rows, tile_rows, down_block.shape[1] // tile_cols, tile_cols
    )
    down_part = down_part.transpose(0, 2, 1, 3).reshape(-1, tile_rows, tile_cols)
    return jnp.concatenate(
        [
            split_cols(qkv_block[:, 0]),
            split_cols(qkv_block[:, 1]),
            split_cols(qkv_block[:, 2]),
            split_cols(out_block),
            split_cols(up_block),
            down_part,
        ],
        axis=0,
    )


def forward_kernel(n_dp, n_row, n_col, dims,
                   x_ref, g_ref, wq_ref, wu_ref, wo_ref, wd_ref,
                   cos_ref, sin_ref, segc_ref, segr_ref, gain_ref, shift_ref, bias_ref,
                   gf, wi, wf, nrm, hid, qkv, up, lse, mean_ref, rstd_ref,
                   xv, nv, wv, stage_g, stage_o, stage_d,
                   zs, zr, ys, yr, cs, cr, ws, wr, ds, dr, ls, lo, no):
    T, C, HF, UT = dims
    d, r, c = lax.axis_index("dp"), lax.axis_index("row"), lax.axis_index("col")
    r1 = r + 1 - 2 * lax.rem(r, 2)
    r2 = lax.rem(r + 2, n_row)
    chunks = 2
    tc = T // chunks
    qw = 3 * HF
    rows_all, D = n_row * T, n_col * C
    seqs = rows_all // SEQ_LEN
    acts = ((x_ref, xv), (g_ref, gf))

    barrier = pltpu.get_barrier_semaphore()
    peers = [{"row": r1}, {"row": r2}]
    peers += [{"col": lax.rem(c + k, n_col)} for k in range(1, n_col)]
    peers += [{"dp": lax.rem(d + k, n_dp)} for k in range(1, n_dp)]
    for peer in peers:
        pl.semaphore_signal(barrier, inc=1, device_id=peer, device_id_type=MESH)
    pl.semaphore_wait(barrier, len(peers))

    def copy(src, dst, s, rcv, peer):
        return pltpu.make_async_remote_copy(
            src_ref=src, dst_ref=dst, send_sem=s, recv_sem=rcv, device_id=peer, device_id_type=MESH
        )

    def blk(a, rr, cc, t):
        return acts[a][1].at[pl.ds(pl.multiple_of(rr * T + t * tc, tc), tc),
                             pl.ds(pl.multiple_of(cc * C, C), C)]

    def own(a, t):
        return acts[a][0].at[pl.ds(t * tc, tc), :]

    def z_copy(a, t, cc, src, right):
        peer = {"col": c + 1} if right else {"col": c - 1}
        return copy(src, blk(a, r, cc, t), zs.at[a, t, int(right), cc], zr.at[a, t, cc], peer)

    def y_copy(a, t, cc, src):
        return copy(src, blk(a, r, cc, t), ys.at[a, t, cc], yr.at[a, t, cc], {"row": r2})

    def c_copy(a, t, cc, src, rr, which):
        return copy(
            src, blk(a, rr, cc, t), cs.at[a, t, which, cc], cr.at[a, t, which, cc], {"row": r1}
        )

    def send_own_z(a, t):
        @pl.when(c < n_col - 1)
        def _():
            z_copy(a, t, c, own(a, t), True).start()

        @pl.when(c > 0)
        def _():
            z_copy(a, t, c, own(a, t), False).start()

    def send_own_row(a, t):
        y_copy(a, t, c, own(a, t)).start()
        c_copy(a, t, c, own(a, t), r, 0).start()

    def relay(a, s, t):
        for right in (True, False):
            cc = c - s if right else c + s

            @pl.when((cc >= 0) & (cc < n_col))
            def _(cc=cc, right=right):
                z_copy(a, t, cc, blk(a, r, cc, t), right).wait_recv()

                @pl.when((c < n_col - 1) if right else (c > 0))
                def _():
                    z_copy(a, t, cc, blk(a, r, cc, t), right).start()

                y_copy(a, t, cc, blk(a, r, cc, t)).start()
                c_copy(a, t, cc, blk(a, r, cc, t), r, 0).start()

    def pass_row(a, s, t):
        for right in (True, False):
            cc = c - s if right else c + s
            ok = (cc >= 0) & (cc < n_col)
            if not right:
                ok = ok & (s > 0)

            @pl.when(ok)
            def _(cc=cc):
                y_copy(a, t, cc, blk(a, r, cc, t)).wait_recv()
                c_copy(a, t, cc, blk(a, r2, cc, t), r2, 1).start()

    ck, hk, uk = C // n_dp, HF // n_dp, UT // n_dp

    def w_dst(part, dd, cc):
        if part == 0:
            return wv.at[pl.ds(cc * C + dd * ck, ck), pl.ds(0, qw)]
        if part == 1:
            return wv.at[pl.ds(cc * C + dd * ck, ck), pl.ds(qw, UT)]
        if part == 2:
            return wv.at[pl.ds(cc * C + dd * ck, ck), pl.ds(qw + UT, UT)]
        if part == 3:
            return wf.at[pl.ds(dd * hk, hk), pl.ds(cc * C, C)]
        if part == 4:
            return wf.at[pl.ds(HF + dd * uk, uk), pl.ds(cc * C, C)]
        return wf.at[pl.ds(HF + UT + dd * uk, uk), pl.ds(cc * C, C)]

    def w_src(part, cc):
        if part == 0:
            return wq_ref.at[cc, pl.ds(d * ck, ck), :]
        if part == 1:
            return wu_ref.at[pl.ds(d * ck, ck), pl.ds(cc * UT, UT)]
        if part == 2:
            return wu_ref.at[pl.ds(d * ck, ck), pl.ds((n_col + cc) * UT, UT)]
        if part == 3:
            return wo_ref.at[pl.ds(cc * HF + d * hk, hk), :]
        if part == 4:
            return wd_ref.at[pl.ds(cc * UT + d * uk, uk), :]
        return wd_ref.at[pl.ds((n_col + cc) * UT + d * uk, uk), :]

    def w_copy(part, k):
        dest = lax.rem(c + k, n_col)
        return copy(
            w_src(part, dest), w_dst(part, d, c), ws.at[part, k], wr.at[part, k], {"col": dest}
        )

    def x_copy(part, k, j):
        got = w_dst(part, d, lax.rem(c + n_col - k, n_col))
        return copy(got, got, ds.at[part, k, j], dr.at[part, k, j], {"dp": lax.rem(d + j, n_dp)})

    def w_send(parts, k):
        for part in parts:
            w_copy(part, k).start()

    def w_pass(parts, k):
        for part in parts:
            w_copy(part, k).wait_recv()
            for j in range(1, n_dp):
                x_copy(part, k, j).start()

    def w_done(parts, k):
        for part in parts:
            for j in range(1, n_dp):
                x_copy(part, k, j).wait_recv()

    win, wfin = (0, 1, 2), (3, 4, 5)

    for t in range(chunks):
        send_own_z(0, t)
    for t in range(chunks):
        send_own_row(0, t)

    col_at = pl.ds(c * C, C)
    direct = [
        pltpu.make_async_copy(x_ref, xv.at[pl.ds(r * T, T), col_at], ls.at[0]),
        pltpu.make_async_copy(wq_ref.at[c], wv.at[col_at, pl.ds(0, qw)], ls.at[1]),
        pltpu.make_async_copy(wu_ref.at[:, pl.ds(c * UT, UT)], wv.at[col_at, pl.ds(qw, UT)],
                              ls.at[2]),
        pltpu.make_async_copy(wu_ref.at[:, pl.ds((n_col + c) * UT, UT)],
                              wv.at[col_at, pl.ds(qw + UT, UT)], ls.at[3]),
    ]
    loads = [
        pltpu.make_async_copy(g_ref, stage_g, ls.at[4]),
        pltpu.make_async_copy(wo_ref.at[pl.ds(c * HF, HF), :], stage_o, ls.at[5]),
        pltpu.make_async_copy(wd_ref.at[pl.ds(c * UT, UT), :], stage_d.at[0], ls.at[6]),
        pltpu.make_async_copy(wd_ref.at[pl.ds((n_col + c) * UT, UT), :], stage_d.at[1], ls.at[7]),
    ]
    stores = [
        pltpu.make_async_copy(stage_g, gf.at[pl.ds(r * T, T), col_at], lo.at[0]),
        pltpu.make_async_copy(stage_o, wf.at[pl.ds(0, HF), col_at], lo.at[1]),
        pltpu.make_async_copy(stage_d.at[0], wf.at[pl.ds(HF, UT), col_at], lo.at[2]),
        pltpu.make_async_copy(stage_d.at[1], wf.at[pl.ds(HF + UT, UT), col_at], lo.at[3]),
    ]
    for item in direct + loads:
        item.start()

    for t in range(chunks):
        relay(0, 1, t)
    w_send(win, 2)
    for t in range(chunks):
        relay(0, 2, t)
    w_send(win, 3)
    w_send(win, 1)
    for t in range(chunks):
        relay(0, 3, t)
    for t in range(chunks):
        send_own_z(1, t)
        send_own_row(1, t)
    for load, store in zip(loads, stores):
        load.wait()
        store.start()
    for s in range(n_col):
        for t in range(chunks):
            pass_row(0, s, t)
    for k in (2, 1, 3):
        w_pass(win, k)
    for t in range(chunks):
        relay(1, 1, t)
    w_send(wfin, 2)
    for item in direct:
        item.wait()
    for t in range(chunks):
        for cc in range(n_col):
            c_copy(0, t, cc, blk(0, r, cc, t), r, 0).wait_recv()
            c_copy(0, t, cc, blk(0, r, cc, t), r, 1).wait_recv()
    for k in (2, 1, 3):
        w_done(win, k)
    keep_w = pltpu.make_async_copy(wv, wi, no.at[0])
    keep_w.start()

    tile = 256
    tiles = rows_all // tile
    sub = 16

    def one_tile(i, carry):
        base = pl.multiple_of(i * tile, tile)

        def norm_rows(k, inner):
            at = pl.ds(pl.multiple_of(base + k * sub, sub), sub)
            val = xv[at, :].astype(F32)
            mean = jnp.sum(val, axis=1, keepdims=True) / D
            var = jnp.sum(val * val, axis=1, keepdims=True) / D - mean * mean
            rstd = lax.rsqrt(var + NORM_EPS)
            mean_ref[at, :] = mean
            rstd_ref[at, :] = rstd
            nv[at, :] = ((val - mean) * rstd * gain_ref[...] + shift_ref[...]).astype(BF16)
            return inner

        lax.fori_loop(0, tile // sub, norm_rows, 0)
        at = pl.ds(base, tile)
        mixed = jnp.dot(nv[at, :], wv[...], preferred_element_type=F32) + bias_ref[...]
        cos, sin = cos_ref[at, :], sin_ref[at, :]
        lane = lax.rem(lax.broadcasted_iota(jnp.int32, (tile, HF), 1), HEAD_DIM)
        low = lane < ROTARY // 2
        for j in range(2):
            part = mixed[:, j * HF : (j + 1) * HF]
            ahead = pltpu.roll(part, HF - ROTARY // 2, 1)
            behind = pltpu.roll(part, ROTARY // 2, 1)
            turned = part * cos + jnp.where(low, -ahead, behind) * sin
            qkv[at, j * HF : (j + 1) * HF] = turned.astype(BF16)
        qkv[at, 2 * HF : 3 * HF] = mixed[:, 2 * HF : 3 * HF].astype(BF16)
        pre = mixed[:, qw:]
        up[at, :] = pre
        hid[at, HF:] = gelu_value(pre).astype(BF16)

        s, t = 2 + lax.div(i, 2), lax.rem(i, 2)

        @pl.when(s < n_col)
        def _():
            relay(1, s, t)

        return carry

    lax.fori_loop(0, 2, one_tile, 0)
    w_send(wfin, 3)
    w_send(wfin, 1)
    lax.fori_loop(2, tiles, one_tile, 0)
    keep_norm = pltpu.make_async_copy(nv, nrm, no.at[1])
    keep_norm.start()

    heads = HF // HEAD_DIM
    qt = SEQ_LEN // 2

    def one_seq(s, carry):
        base = pl.multiple_of(s * SEQ_LEN, SEQ_LEN)
        lane = lax.broadcasted_iota(jnp.int32, (qt, HF), 1)
        for qi in range(2):
            width = (qi + 1) * qt
            q_at = pl.ds(base + qi * qt, qt)
            k_at = pl.ds(base, width)
            allowed = (segc_ref[q_at, :] == segr_ref[pl.ds(s, 1), 0:width]) & (
                lax.broadcasted_iota(jnp.int32, (qt, width), 0) + qi * qt
                >= lax.broadcasted_iota(jnp.int32, (qt, width), 1)
            )
            keys, vals = qkv[k_at, HF : 2 * HF], qkv[k_at, 2 * HF : 3 * HF]
            queries = qkv[q_at, 0:HF]
            total, logs = None, None
            for h in range(heads):
                mine = lax.div(lane, HEAD_DIM) == h
                scores = lax.dot_general(
                    jnp.where(mine, queries, jnp.zeros_like(queries)), keys,
                    (((1,), (1,)), ((), ())), preferred_element_type=F32,
                ) * (HEAD_DIM ** (-0.5))
                scores = jnp.where(allowed, scores, MASKED_SCORE)
                peak = jnp.max(scores, axis=1, keepdims=True)
                weight = jnp.exp(scores - peak)
                weight_sum = jnp.sum(weight, axis=1, keepdims=True)
                probs = (weight * (1.0 / weight_sum)).astype(BF16)
                out = jnp.dot(probs, vals, preferred_element_type=F32)
                log_h = peak + jnp.log(weight_sum)
                total = out if h == 0 else jnp.where(mine, out, total)
                logs = jnp.broadcast_to(log_h, (qt, HF)) if h == 0 else jnp.where(mine, log_h, logs)
            hid[q_at, 0:HF] = total.astype(BF16)
            lse[q_at, :] = logs

        @pl.when(s < n_col)
        def _():
            for t in range(chunks):
                pass_row(1, s, t)

        return carry

    lax.fori_loop(0, seqs, one_seq, 0)
    for k in (2, 3, 1):
        w_pass(wfin, k)

    for t in range(chunks):
        for cc in range(n_col):
            c_copy(1, t, cc, blk(1, r, cc, t), r, 0).wait_recv()
            c_copy(1, t, cc, blk(1, r, cc, t), r, 1).wait_recv()
    for k in range(1, n_col):
        w_done(wfin, k)
    for a in range(2):
        for t in range(chunks):
            for cc in range(n_col):
                @pl.when((cc <= c) & (c < n_col - 1))
                def _(a=a, t=t, cc=cc):
                    z_copy(a, t, cc, blk(a, r, cc, t), True).wait_send()

                @pl.when((cc >= c) & (c > 0))
                def _(a=a, t=t, cc=cc):
                    z_copy(a, t, cc, blk(a, r, cc, t), False).wait_send()

                y_copy(a, t, cc, blk(a, r, cc, t)).wait_send()
                c_copy(a, t, cc, blk(a, r, cc, t), r, 0).wait_send()
                c_copy(a, t, cc, blk(a, r, cc, t), r, 1).wait_send()
    for k in range(1, n_col):
        for part in win + wfin:
            w_copy(part, k).wait_send()
            for j in range(1, n_dp):
                x_copy(part, k, j).wait_send()
    for store in stores:
        store.wait()
    keep_w.wait()
    keep_norm.wait()


def forward_all(x, g, w_q, w_up, w_out, w_down, cos, sin, seg_col, seg_row, gain, shift, bias,
                n_dp, n_row, n_col):
    T, C = x.shape
    HF = w_q.shape[2] // 3
    UT = w_up.shape[1] // (2 * n_col)
    n_in, n_out = 3 * HF + 2 * UT, HF + 2 * UT
    rows, D = n_row * T, n_col * C
    dma = pltpu.SemaphoreType.DMA
    vm = pl.BlockSpec(memory_space=pltpu.VMEM)
    sds = jax.ShapeDtypeStruct
    return pl.pallas_call(
        functools.partial(forward_kernel, n_dp, n_row, n_col, (T, C, HF, UT)),
        name="forward_all",
        out_shape=(
            sds((rows, D), BF16),
            sds((D, n_in), BF16),
            sds((n_out, D), BF16),
            sds((rows, D), BF16),
            sds((rows, n_out), BF16),
            sds((rows, 3 * HF), BF16),
            sds((rows, 2 * UT), F32),
            sds((rows, HF), F32),
            sds((rows, 1), F32),
            sds((rows, 1), F32),
        ),
        in_specs=[ANY] * 6 + [vm] * 7,
        out_specs=(ANY,) * 4 + (vm,) * 6,
        scratch_shapes=[
            pltpu.VMEM((rows, D), BF16),
            pltpu.VMEM((rows, D), BF16),
            pltpu.VMEM((D, n_in), BF16),
            pltpu.VMEM((T, C), BF16),
            pltpu.VMEM((HF, C), BF16),
            pltpu.VMEM((2, UT, C), BF16),
            dma((2, 2, 2, n_col)),
            dma((2, 2, n_col)),
            dma((2, 2, n_col)),
            dma((2, 2, n_col)),
            dma((2, 2, 2, n_col)),
            dma((2, 2, 2, n_col)),
            dma((6, n_col)),
            dma((6, n_col)),
            dma((6, n_col, n_dp)),
            dma((6, n_col, n_dp)),
            dma((8,)),
            dma((4,)),
            dma((2,)),
        ],
        compiler_params=pltpu.CompilerParams(
            collective_id=0, has_side_effects=True, vmem_limit_bytes=60 * 1024 * 1024
        ),
    )(x, g, w_q, w_up, w_out, w_down, cos, sin, seg_col, seg_row, gain, shift, bias)


def pick(index, table):
    out = jnp.int32(table[0])
    for k in range(1, len(table)):
        out = jnp.where(index == k, jnp.int32(table[k]), out)
    return out


def reduce_kernel(n_row, n_col, dims, p_ref, q_ref, dwi_ref, dwf_ref,
                  res_ref, gn_ref, tiles_ref,
                  abuf, obuf, sbuf, bbuf, zsb, zin, gi, gf, oi, of,
                  a_s, a_r, o_l, y_s, y_r, z_s, z_r, x_s, x_r, g_l, t_s, t_r):
    T, C, HF, UT, chunks = dims
    tc = T // chunks
    step_rows = 64
    d, r, c = lax.axis_index("dp"), lax.axis_index("row"), lax.axis_index("col")
    r1 = r + 1 - 2 * lax.rem(r, 2)
    r2 = lax.rem(r + 2, n_row)
    r12 = lax.rem(r1 + 2, n_row)
    srcs = (p_ref, q_ref)
    outs = (res_ref, gn_ref)
    far = [
        sorted(range(n_col), key=lambda f: (-abs(f - cc), f < cc if cc < n_col // 2 else f > cc))
        for cc in range(n_col)
    ]
    forder = [pick(c, [far[cc][i] for cc in range(n_col)]) for i in range(n_col)]

    barrier = pltpu.get_barrier_semaphore()
    peers = [{"row": r1}, {"row": r2}, {"dp": 1 - d}]
    peers += [{"col": lax.rem(c + k, n_col)} for k in range(1, n_col)]
    for peer in peers:
        pl.semaphore_signal(barrier, inc=1, device_id=peer, device_id_type=MESH)
    pl.semaphore_wait(barrier, len(peers))

    def copy(src, dst, s, rcv, peer):
        return pltpu.make_async_remote_copy(
            src_ref=src, dst_ref=dst, send_sem=s, recv_sem=rcv, device_id=peer, device_id_type=MESH
        )

    def unit(v, rr, f, t):
        return srcs[v].at[pl.ds(rr * T + t * tc, tc), pl.ds(f * C, C)]

    def a_copy(v, h, f, t):
        return copy(
            unit(v, r12 if h else r1, f, t), abuf.at[v, h, f, t],
            a_s.at[v, h, f, t], a_r.at[v, h, f, t], {"row": r1},
        )

    def o_copy(v, h, f, t):
        return pltpu.make_async_copy(
            unit(v, r2 if h else r, f, t), obuf.at[v, h, f, t], o_l.at[v, h, f, t]
        )

    def y_copy(v, f, t):
        return copy(sbuf.at[v, f, t], bbuf.at[v, f, t], y_s.at[v, f, t], y_r.at[v, f, t],
                    {"row": r2})

    def z_copy(v, f, t, slot, step):
        return copy(zsb.at[v, f, t], zin.at[v, slot, t], z_s.at[v, f, t], z_r.at[v, slot, t],
                    {"col": c + step})

    for v in range(2):
        for i in range(n_col):
            for t in range(chunks):
                for h in (1, 0):
                    a_copy(v, h, forder[i], t).start()
                    o_copy(v, h, forder[i], t).start()

    qw, n_in, n_out = 3 * HF, 3 * HF + 2 * UT, HF + 2 * UT
    wide = (qw + UT, UT)
    lane0 = (0, qw + UT)
    tall = (HF, 2 * UT)
    row0 = (0, HF)

    def gi_src(own, cc):
        return dwi_ref.at[pl.ds(cc * C, C), pl.ds(lane0[own], wide[own])]

    def gf_src(own, cc):
        return dwf_ref.at[pl.ds(row0[own], tall[own]), pl.ds(cc * C, C)]

    def xi_copy(own, cc):
        return copy(gi_src(own, cc), gi.at[cc, :, pl.ds(0, wide[own])], x_s.at[0, cc],
                    x_r.at[0, cc], {"dp": 1 - d})

    def xf_copy(own, cc):
        return copy(gf_src(own, cc), gf.at[cc, pl.ds(0, tall[own]), :], x_s.at[1, cc],
                    x_r.at[1, cc], {"dp": 1 - d})

    def li_copy(own, cc):
        return pltpu.make_async_copy(gi_src(own, cc), oi.at[cc, :, pl.ds(0, wide[own])],
                                     g_l.at[0, cc])

    def lf_copy(own, cc):
        return pltpu.make_async_copy(gf_src(own, cc), of.at[cc, pl.ds(0, tall[own]), :],
                                     g_l.at[1, cc])

    def tile_parts(own, cc, source):
        half, odd = source // 2, lax.rem(source, 2)
        lw = 2 * HF
        if own == 0:
            parts = [
                (oi.at[cc, :, pl.ds(j * HF, HF)], tiles_ref.at[2 * j + half, :, pl.ds(odd * HF, HF)])
                for j in range(3)
            ]
            parts += [(oi.at[cc, :, pl.ds(qw, UT)], tiles_ref.at[8 + source])]
            parts += [
                (of.at[cc, pl.ds(0, HF), pl.ds(j * lw, lw)],
                 tiles_ref.at[6 + j, pl.ds(source * HF, HF), :])
                for j in range(2)
            ]
            return parts
        parts = [(oi.at[cc, :, pl.ds(0, UT)], tiles_ref.at[source])]
        for m in range(2):
            for j in range(2):
                parts.append(
                    (of.at[cc, pl.ds(m * UT, UT), pl.ds(j * lw, lw)],
                     tiles_ref.at[4 + 2 * (2 * m + half) + j, pl.ds(odd * UT, UT), :])
                )
        return parts

    def t_copies(own, cc):
        return [
            copy(src, dst, t_s.at[n, cc], t_r.at[n, c], {"col": cc})
            for n, (src, dst) in enumerate(tile_parts(own, cc, c))
        ]

    def t_waits(own, source):
        return [
            copy(src, dst, t_s.at[n, source], t_r.at[n, source], {"col": source})
            for n, (src, dst) in enumerate(tile_parts(own, source, source))
        ]

    def t_local(own):
        return [
            pltpu.make_async_copy(src, dst, t_s.at[n, c])
            for n, (src, dst) in enumerate(tile_parts(own, c, c))
        ]

    for i in range(n_col):
        for own in range(2):
            @pl.when(d == own)
            def _(own=own, i=i):
                xi_copy(1 - own, forder[i]).start()
                xf_copy(1 - own, forder[i]).start()
                li_copy(own, forder[i]).start()
                lf_copy(own, forder[i]).start()

    def looped(rows, fn):
        def one(k, carry):
            fn(pl.ds(pl.multiple_of(k * step_rows, step_rows), step_rows))
            return carry
        lax.fori_loop(0, rows // step_rows, one, 0)

    def first_sum(v, i):
        f = forder[i]
        for t in range(chunks):
            a_copy(v, 1, f, t).wait_recv()
            o_copy(v, 1, f, t).wait()

            def add(rows, t=t):
                sbuf[v, f, t, rows, :] = (
                    obuf[v, 1, f, t, rows, :].astype(F32) + abuf[v, 1, f, t, rows, :].astype(F32)
                ).astype(BF16)

            looped(tc, add)
            y_copy(v, f, t).start()

    def second_sum(v, i):
        f = forder[i]
        for t in range(chunks):
            a_copy(v, 0, f, t).wait_recv()
            o_copy(v, 0, f, t).wait()
            y_copy(v, f, t).wait_recv()

            def base(rows, t=t):
                return (
                    obuf[v, 0, f, t, rows, :].astype(F32)
                    + abuf[v, 0, f, t, rows, :].astype(F32)
                    + bbuf[v, f, t, rows, :].astype(F32)
                )

            if i < n_col - 1:
                right = f > c
                step = jnp.where(right, jnp.int32(1), jnp.int32(-1))
                landed = jnp.where(f == c + step, jnp.where(right, f, jnp.int32(n_col)), f)
                inner = jnp.where(right, c, n_col - 1 - c) > 0

                @pl.when(inner)
                def _(t=t):
                    z_copy(v, f, t, f, 0).wait_recv()

                    def add(rows):
                        zsb[v, f, t, rows, :] = (
                            base(rows) + zin[v, f, t, rows, :].astype(F32)
                        ).astype(BF16)

                    looped(tc, add)

                @pl.when(jnp.logical_not(inner))
                def _(t=t):
                    def add(rows):
                        zsb[v, f, t, rows, :] = base(rows).astype(BF16)

                    looped(tc, add)

                z_copy(v, f, t, landed, step).start()
            else:
                out = outs[v]

                def put(rows, value, t=t):
                    out[pl.ds(pl.multiple_of(rows.start + t * tc, step_rows), step_rows), :] = value

                @pl.when(c > 0)
                def _(t=t):
                    z_copy(v, f, t, f, 0).wait_recv()

                @pl.when(c < n_col - 1)
                def _(t=t):
                    z_copy(v, f, t, n_col, 0).wait_recv()

                @pl.when(c == 0)
                def _(t=t):
                    looped(tc, lambda rows: put(
                        rows, base(rows) + zin[v, n_col, t, rows, :].astype(F32)))

                @pl.when(c == n_col - 1)
                def _(t=t):
                    looped(tc, lambda rows: put(
                        rows, base(rows) + zin[v, f, t, rows, :].astype(F32)))

                @pl.when((c > 0) & (c < n_col - 1))
                def _(t=t):
                    looped(tc, lambda rows: put(
                        rows, base(rows) + zin[v, f, t, rows, :].astype(F32)
                        + zin[v, n_col, t, rows, :].astype(F32)))

    def grad_piece(i):
        cc = forder[i]
        for own in range(2):
            @pl.when(d == own)
            def _(own=own):
                xi_copy(own, cc).wait_recv()
                xf_copy(own, cc).wait_recv()
                li_copy(own, cc).wait()
                lf_copy(own, cc).wait()

                def add_i(rows):
                    at = (cc, rows, pl.ds(0, wide[own]))
                    oi[at] = (oi[at].astype(F32) + gi[at].astype(F32)).astype(BF16)

                def add_f(rows):
                    at = (cc, rows, slice(None))
                    of[at] = (of[at].astype(F32) + gf[at].astype(F32)).astype(BF16)

                looped(C, add_i)
                looped(tall[own], add_f)
                for item in t_local(own) if i == n_col - 1 else t_copies(own, cc):
                    item.start()

    for i in range(n_col):
        first_sum(0, i)
    for i in range(n_col):
        second_sum(0, i)
        first_sum(1, i)
        grad_piece(i)
    for i in range(n_col):
        second_sum(1, i)

    for own in range(2):
        @pl.when(d == own)
        def _(own=own):
            for k in range(1, n_col):
                for item in t_waits(own, lax.rem(c + k, n_col)):
                    item.wait_recv()
            for i in range(n_col - 1):
                for item in t_copies(own, forder[i]):
                    item.wait_send()
            for item in t_local(own):
                item.wait()
            for cc in range(n_col):
                xi_copy(1 - own, cc).wait_send()
                xf_copy(1 - own, cc).wait_send()
    for v in range(2):
        for t in range(chunks):
            for f in range(n_col):
                a_copy(v, 0, f, t).wait_send()
                a_copy(v, 1, f, t).wait_send()
                y_copy(v, f, t).wait_send()
            for i in range(n_col - 1):
                z_copy(v, forder[i], t, forder[i], 0).wait_send()


def reduce_all(p, q, dwi, dwf, T, C, HF, UT, n_row, n_col):
    dma = pltpu.SemaphoreType.DMA
    chunks = 2
    tc = T // chunks
    unit = (chunks, tc, C)
    vm = pl.BlockSpec(memory_space=pltpu.VMEM)
    return pl.pallas_call(
        functools.partial(reduce_kernel, n_row, n_col, (T, C, HF, UT, chunks)),
        name="reduce_all",
        out_shape=(
            jax.ShapeDtypeStruct((T, C), F32),
            jax.ShapeDtypeStruct((T, C), F32),
            jax.ShapeDtypeStruct((12, C, UT), BF16),
        ),
        in_specs=[ANY] * 4,
        out_specs=(vm, vm, ANY),
        scratch_shapes=[
            pltpu.VMEM((2, 2, n_col) + unit, BF16),
            pltpu.VMEM((2, 2, n_col) + unit, BF16),
            pltpu.VMEM((2, n_col) + unit, BF16),
            pltpu.VMEM((2, n_col) + unit, BF16),
            pltpu.VMEM((2, n_col) + unit, BF16),
            pltpu.VMEM((2, n_col + 1) + unit, BF16),
            pltpu.VMEM((n_col, C, 3 * HF + UT), BF16),
            pltpu.VMEM((n_col, 2 * UT, C), BF16),
            pltpu.VMEM((n_col, C, 3 * HF + UT), BF16),
            pltpu.VMEM((n_col, 2 * UT, C), BF16),
            dma((2, 2, n_col, chunks)),
            dma((2, 2, n_col, chunks)),
            dma((2, 2, n_col, chunks)),
            dma((2, n_col, chunks)),
            dma((2, n_col, chunks)),
            dma((2, n_col, chunks)),
            dma((2, n_col + 1, chunks)),
            dma((2, n_col)),
            dma((2, n_col)),
            dma((2, n_col)),
            dma((6, n_col)),
            dma((6, n_col)),
        ],
        compiler_params=pltpu.CompilerParams(
            collective_id=1, has_side_effects=True, vmem_limit_bytes=62 * 1024 * 1024
        ),
    )(p, q, dwi, dwf)


def finish_kernel(n_dp, n_row, n_col, width, gn_ref, x_ref, g_ref, mean_ref, rstd_ref, gain_ref, part_ref,
                  gx_ref, va_ref, vb_ref,
                  st, da, db, ra, rb,
                  st_s, st_r, d_s, d_r, r_s, r_r, c_s, c_r):
    d, r, c = lax.axis_index("dp"), lax.axis_index("row"), lax.axis_index("col")
    T, C = gn_ref.shape

    barrier = pltpu.get_barrier_semaphore()
    dps = [lax.rem(d + k, n_dp) for k in range(1, n_dp)]
    rows = [lax.rem(r + k, n_row) for k in range(1, n_row)]
    cols = [lax.rem(c + k, n_col) for k in range(1, n_col)]
    peers = [{"dp": k} for k in dps] + [{"row": k} for k in rows] + [{"col": k} for k in cols]
    for peer in peers:
        pl.semaphore_signal(barrier, inc=1, device_id=peer, device_id_type=MESH)
    pl.semaphore_wait(barrier, len(peers))

    def copy(src, dst, s, rcv, peer):
        return pltpu.make_async_remote_copy(
            src_ref=src, dst_ref=dst, send_sem=s, recv_sem=rcv, device_id=peer, device_id_type=MESH
        )

    gain = gain_ref[...]

    def fold(value):
        total = value[:, 0:128]
        for k in range(1, C // 128):
            total = total + value[:, k * 128 : (k + 1) * 128]
        return jnp.sum(jnp.transpose(total), axis=0, keepdims=True)

    gn = gn_ref[...]
    x_hat = (x_ref[...].astype(F32) - mean_ref[...]) * rstd_ref[...]
    gh = gn * gain
    st[c, 0:1, :] = fold(gh)
    st[c, 1:2, :] = fold(gh * x_hat)

    def st_copy(k):
        return copy(st.at[c], st.at[c], st_s.at[k], st_r.at[c], {"col": k})

    def st_wait(k):
        return copy(st.at[k], st.at[k], st_s.at[k], st_r.at[k], {"col": k})

    for k in cols:
        st_copy(k).start()

    da[d] = part_ref[...]
    db[d, 0:1, :] = jnp.sum(gn * x_hat, axis=0, keepdims=True)
    db[d, 1:2, :] = jnp.sum(gn, axis=0, keepdims=True)
    db[d, 2:3, :] = jnp.sum(g_ref[...].astype(F32), axis=0, keepdims=True)

    def pair(a_src, b_src, a_dst, b_dst, s, rcv, peer):
        return [copy(a_src, a_dst, s.at[0], rcv.at[0], peer),
                copy(b_src, b_dst, s.at[1], rcv.at[1], peer)]

    def d_pair(slot, peer):
        return pair(da.at[slot], db.at[slot], da.at[slot], db.at[slot],
                    d_s.at[peer], d_r.at[slot], {"dp": peer})

    def r_pair(slot, peer):
        return pair(ra.at[slot], rb.at[slot], ra.at[slot], rb.at[slot],
                    r_s.at[peer], r_r.at[slot], {"row": peer})

    def c_pair(slot, peer):
        return pair(va_ref.at[slot], vb_ref.at[slot], va_ref.at[slot], vb_ref.at[slot],
                    c_s.at[peer], c_r.at[slot], {"col": peer})

    for k in dps:
        for item in d_pair(d, k):
            item.start()
    for k in dps:
        for item in d_pair(k, k):
            item.wait_recv()
    a_sum, b_sum = da[0], db[0]
    for k in range(1, n_dp):
        a_sum = a_sum + da[k]
        b_sum = b_sum + db[k]
    ra[r] = a_sum
    rb[r] = b_sum
    for k in rows:
        for item in r_pair(r, k):
            item.start()

    for k in cols:
        st_wait(k).wait_recv()
    stats = st[0]
    for k in range(1, n_col):
        stats = stats + st[k]
    stats = stats / width
    m1 = jnp.transpose(jnp.broadcast_to(stats[0:1, :], (128, T)))[:, 0:1]
    m2 = jnp.transpose(jnp.broadcast_to(stats[1:2, :], (128, T)))[:, 0:1]
    gx_ref[...] = g_ref[...].astype(F32) + rstd_ref[...] * (gh - m1 - x_hat * m2)

    for k in rows:
        for item in r_pair(k, k):
            item.wait_recv()
    b_sum = rb[0]
    for k in range(1, n_row):
        b_sum = b_sum + rb[k]
    for k in range(n_row):
        va_ref[c, k] = ra[k]
    vb_ref[c] = b_sum
    for k in cols:
        for item in c_pair(c, k):
            item.start()
    for k in cols:
        for item in c_pair(k, k):
            item.wait_recv()
    for k in cols:
        st_copy(k).wait_send()
        for item in c_pair(c, k):
            item.wait_send()
    for k in dps:
        for item in d_pair(d, k):
            item.wait_send()
    for k in rows:
        for item in r_pair(r, k):
            item.wait_send()


def finish_all(gn, x, g, mean, rstd, gain, part, width, n_dp, n_row, n_col):
    T, C = gn.shape
    dma = pltpu.SemaphoreType.DMA
    vm = pl.BlockSpec(memory_space=pltpu.VMEM)
    return pl.pallas_call(
        functools.partial(finish_kernel, n_dp, n_row, n_col, width),
        name="finish_all",
        out_shape=(
            jax.ShapeDtypeStruct((T, C), F32),
            jax.ShapeDtypeStruct((n_col, n_row, 8, 128), F32),
            jax.ShapeDtypeStruct((n_col, 8, C), F32),
        ),
        in_specs=[vm] * 7,
        out_specs=(vm,) * 3,
        scratch_shapes=[
            pltpu.VMEM((n_col, 8, T), F32),
            pltpu.VMEM((n_dp, 8, 128), F32),
            pltpu.VMEM((n_dp, 8, C), F32),
            pltpu.VMEM((n_row, 8, 128), F32),
            pltpu.VMEM((n_row, 8, C), F32),
            dma((n_col,)),
            dma((n_col,)),
            dma((n_dp, 2)),
            dma((n_dp, 2)),
            dma((n_row, 2)),
            dma((n_row, 2)),
            dma((n_col, 2)),
            dma((n_col, 2)),
        ],
        compiler_params=pltpu.CompilerParams(
            collective_id=2, has_side_effects=True, vmem_limit_bytes=48 * 1024 * 1024
        ),
    )(gn, x, g, mean, rstd, gain, part)


def muon_kernel(owned, per_step, HF, UT, rate, grad_ref, mom_ref, wq_ref, wo_ref, wu_ref, wd_ref,
                og_ref, new_ref, nm_ref, wbuf, sem):
    first = lax.axis_index("dp") * owned
    step = pl.program_id(0)
    steps = owned // per_step
    n_qkv, n_out, n_up = 6, 2, 8

    def fetch(tile, slot, n, start):
        dst = wbuf.at[slot, n]

        def go(src, target, s):
            item = pltpu.make_async_copy(src, target, s)
            if start:
                item.start()
            else:
                item.wait()

        @pl.when(tile < n_qkv)
        def _():
            j, half = lax.div(tile, 2), lax.rem(tile, 2)
            for m in range(UT // HF):
                go(wq_ref.at[half * (UT // HF) + m, :, pl.ds(j * HF, HF)],
                   wbuf.at[slot, n, :, pl.ds(m * HF, HF)], sem.at[slot, n, m])

        @pl.when((tile >= n_qkv) & (tile < n_qkv + n_out))
        def _():
            go(wo_ref.at[:, pl.ds((tile - n_qkv) * UT, UT)], dst, sem.at[slot, n, 0])

        @pl.when((tile >= n_qkv + n_out) & (tile < n_qkv + n_out + n_up))
        def _():
            go(wu_ref.at[:, pl.ds((tile - n_qkv - n_out) * UT, UT)], dst, sem.at[slot, n, 0])

        @pl.when(tile >= n_qkv + n_out + n_up)
        def _():
            left = tile - (n_qkv + n_out + n_up)
            rows = dst.shape[0]
            go(wd_ref.at[pl.ds(lax.div(left, 2) * rows, rows), pl.ds(lax.rem(left, 2) * UT, UT)],
               dst, sem.at[slot, n, 0])

    def fetch_all(at, start):
        for n in range(per_step):
            fetch(first + at * per_step + n, lax.rem(at, 2), n, start)

    @pl.when(step == 0)
    def _():
        fetch_all(step, True)

    @pl.when(step + 1 < steps)
    def _():
        fetch_all(step + 1, True)

    iters = []
    for n in range(per_step):
        grad = grad_ref[n].astype(F32)
        og_ref[n] = grad
        moment = MOMENTUM_RATE * mom_ref[n] + grad
        nm_ref[n] = moment
        scale = lax.rsqrt(jnp.sum(moment * moment, keepdims=True) + STAT_EPS)
        iters.append((moment * scale).astype(BF16))
    contract = (((0,), (0,)), ((), ()))
    for _ in range(5):
        grams = [
            lax.dot_general(x, x, contract, preferred_element_type=F32).astype(BF16) for x in iters
        ]
        squares = [jnp.dot(g, g, preferred_element_type=F32) for g in grams]
        polys = [
            (NEWTON_B * g.astype(F32) + NEWTON_C * s).astype(BF16) for g, s in zip(grams, squares)
        ]
        iters = [
            (NEWTON_A * x.astype(F32) + jnp.dot(x, p, preferred_element_type=F32)).astype(BF16)
            for x, p in zip(iters, polys)
        ]
    fetch_all(step, False)
    for n in range(per_step):
        new_ref[n] = wbuf[lax.rem(step, 2), n].astype(F32) - rate * iters[n].astype(F32)


def muon_all(grads, moment, w_q, w_out, w_up, w_down, HF, UT):
    owned, rows, cols = moment.shape
    per_step = 3
    rate = MUON_RATE * math.sqrt(max(1.0, rows / cols))
    block = pl.BlockSpec((per_step, rows, cols), lambda i: (i, 0, 0))
    out = jax.ShapeDtypeStruct(moment.shape, F32)
    return pl.pallas_call(
        functools.partial(muon_kernel, owned, per_step, HF, UT, rate),
        name="muon_all",
        grid=(owned // per_step,),
        out_shape=(out, out, out),
        in_specs=[block, block, ANY, ANY, ANY, ANY],
        out_specs=(block, block, block),
        scratch_shapes=[
            pltpu.VMEM((2, per_step, rows, cols), BF16),
            pltpu.SemaphoreType.DMA((2, per_step, 2)),
        ],
        compiler_params=pltpu.CompilerParams(vmem_limit_bytes=56 * 1024 * 1024),
    )(grads, moment, w_q, w_out, w_up, w_down)


def reduce_plain(p, q, dwi, dwf, C, HF, UT, n_col, row_width):
    def block(part):
        part = lax.psum_scatter(part, "row", scatter_dimension=0, tiled=True)
        return lax.psum_scatter(part, "col", scatter_dimension=1, tiled=True).astype(F32)

    wi4 = lax.all_to_all(dwi.reshape(n_col, C, -1), "col", 0, 0)
    wf4 = lax.all_to_all(dwf.reshape(-1, n_col, C).transpose(1, 0, 2), "col", 0, 0)
    grad_qkv = (
        wi4[:, :, : 3 * HF].reshape(n_col, C, 3, HF).transpose(1, 2, 0, 3).reshape(C, 3, row_width)
    )
    grad_up_w = wi4[:, :, 3 * HF :].reshape(n_col, C, 2, UT).transpose(1, 2, 0, 3).reshape(C, -1)
    grad_w_out = wf4[:, :HF].reshape(-1, C)
    grad_w_down = wf4[:, HF:].reshape(n_col, 2, UT, C).transpose(1, 0, 2, 3).reshape(-1, C)
    grad_tiles = tile_blocks(grad_qkv, grad_w_out, grad_up_w, grad_w_down)
    owned = lax.psum_scatter(grad_tiles, "dp", scatter_dimension=0, tiled=True)
    return block(p), block(q), owned


def body(
    inputs,
    cotangent,
    segments,
    positions,
    w_qkv,
    w_out,
    w_up,
    w_down,
    vectors,
    tile_moment,
    vector_moment,
):
    d_index = lax.axis_index("dp")
    row_index = lax.axis_index("row")
    col_index = lax.axis_index("col")
    n_dp, n_row, n_col = lax.axis_size("dp"), lax.axis_size("row"), lax.axis_size("col")
    T, C = inputs.shape
    D = vectors.shape[1]
    row_width = w_qkv.shape[2]
    HF = row_width // n_col
    UT = w_up.shape[1] // (2 * n_col)
    score_scale = HEAD_DIM ** (-0.5)
    feat_start = (row_index * n_col + col_index) * HF
    unit_a = (row_index * 2 * n_col + col_index) * UT
    unit_b = unit_a + n_col * UT
    col_start = col_index * C
    gain, shift = vectors[5], vectors[6]
    norm_gain = lax.dynamic_slice_in_dim(gain, col_start, C)
    out_bias = lax.dynamic_slice_in_dim(vectors[3] + vectors[4], col_start, C)
    qkv_bias = lax.dynamic_slice_in_dim(vectors[0:3], feat_start, HF, axis=1)
    up_flat = vectors[7:].reshape(-1)
    up_bias = jnp.concatenate(
        [
            lax.dynamic_slice_in_dim(up_flat, unit_a, UT),
            lax.dynamic_slice_in_dim(up_flat, unit_b, UT),
        ]
    )
    w_q = (
        w_qkv.reshape(C, 3, n_col, HF).transpose(2, 0, 1, 3).reshape(n_col, C, 3 * HF)
    )
    cosine, sine_tab = rotary_tables(positions)
    rows_all = positions.shape[0]
    flat = jnp.ones((rows_all, HEAD_DIM - ROTARY), F32)
    heads_here = HF // HEAD_DIM
    cos_wide = jnp.tile(jnp.concatenate([cosine, cosine, flat], axis=1), (1, heads_here))
    sin_wide = jnp.tile(jnp.concatenate([sine_tab, sine_tab, 0.0 * flat], axis=1), (1, heads_here))
    seq_count = rows_all // SEQ_LEN
    cot_rows, w_in, w_fin, normed, hidden, qkv_low, up_pre, logs, mean_all, rstd_all = forward_all(
        inputs,
        cotangent,
        w_q,
        w_up,
        w_out,
        w_down,
        cos_wide,
        sin_wide,
        segments[:, None],
        segments.reshape(seq_count, SEQ_LEN),
        gain[None],
        shift[None],
        jnp.concatenate([qkv_bias.reshape(-1), up_bias])[None],
        n_dp,
        n_row,
        n_col,
    )
    seq_rows = rows_all

    def by_seq(tensor_in):
        return tensor_in.reshape((seq_count, SEQ_LEN) + tensor_in.shape[1:])

    queries = qkv_low[:, :HF].reshape(seq_rows, heads_here, HEAD_DIM)
    key_vecs = qkv_low[:, HF : 2 * HF].reshape(seq_rows, heads_here, HEAD_DIM)
    values = qkv_low[:, 2 * HF :].reshape(seq_rows, heads_here, HEAD_DIM)
    attn_low = hidden[:, :HF]
    logsum = by_seq(logs[:, ::HEAD_DIM]).transpose(0, 2, 1)

    partial_out = jnp.dot(hidden, w_fin, preferred_element_type=F32).astype(BF16)
    x_val = inputs.astype(F32)

    grad_w_fin = jnp.einsum("ti,tj->ij", hidden, cot_rows, preferred_element_type=F32).astype(BF16)
    back = jnp.einsum("tj,ij->ti", cot_rows, w_fin, preferred_element_type=F32)
    grad_attn_low = back[:, :HF].astype(BF16)
    grad_up = back[:, HF:] * gelu_slope(up_pre)
    g_queries, g_keys, g_values = jax.vmap(attend_backward, in_axes=(0, 0, 0, 0, 0, 0, 0, None))(
        by_seq(queries),
        by_seq(key_vecs),
        by_seq(values),
        by_seq(attn_low.reshape(seq_rows, heads_here, HEAD_DIM)),
        by_seq(grad_attn_low.reshape(seq_rows, heads_here, HEAD_DIM)),
        logsum,
        by_seq(segments),
        score_scale,
    )
    g_queries = rotate(
        g_queries.reshape(seq_rows, heads_here, HEAD_DIM), cosine, sine_tab, -1.0
    ).reshape(seq_rows, HF)
    g_keys = rotate(g_keys.reshape(seq_rows, heads_here, HEAD_DIM), cosine, sine_tab, -1.0).reshape(
        seq_rows, HF
    )
    g_values = g_values.reshape(seq_rows, HF)
    grad_mixed = jnp.concatenate([g_queries, g_keys, g_values, grad_up], axis=1)
    grad_mixed_low = grad_mixed.astype(BF16)
    grad_w_in = jnp.einsum(
        "ti,tj->ij", normed, grad_mixed_low, preferred_element_type=F32
    ).astype(BF16)
    partial_norm = jnp.einsum(
        "tj,ij->ti", grad_mixed_low, w_in, preferred_element_type=F32
    ).astype(BF16)

    if n_dp == 2:
        branch, grad_norm, owned_low = reduce_all(
            partial_out, partial_norm, grad_w_in, grad_w_fin, T, C, HF, UT, n_row, n_col
        )
    else:
        branch, grad_norm, owned_low = reduce_plain(
            partial_out, partial_norm, grad_w_in, grad_w_fin, C, HF, UT, n_col, row_width
        )
    result = x_val + branch + out_bias

    sums = jnp.sum(grad_mixed, axis=0)
    part = jnp.pad(sums.reshape(-1, 128), ((0, 1), (0, 0)))
    grad_input, vec_a, vec_b = finish_all(
        grad_norm,
        inputs,
        cotangent,
        lax.dynamic_slice_in_dim(mean_all, row_index * T, T),
        lax.dynamic_slice_in_dim(rstd_all, row_index * T, T),
        norm_gain[None],
        part,
        D,
        n_dp,
        n_row,
        n_col,
    )
    vec_a = vec_a.transpose(2, 1, 0, 3)
    qkv_rows = vec_a[:3].reshape(3, D)
    up_rows = vec_a[3:7].reshape(2, UT // 128, n_row, n_col, 128).transpose(2, 0, 3, 1, 4)
    norm_rows = vec_b.transpose(1, 0, 2).reshape(8, D)
    vec_grad = jnp.concatenate(
        [qkv_rows, norm_rows[2:3], norm_rows[2:3], norm_rows[:2], up_rows.reshape(-1, D)], axis=0
    )
    scaled = vec_grad * lax.rsqrt(jnp.mean(vec_grad * vec_grad, axis=1, keepdims=True) + STAT_EPS)
    vec_moment_new = MOMENTUM_RATE * vector_moment + scaled
    vectors_new = vectors - VECTOR_RATE * vec_moment_new

    owned_grads, tiles_new, moment_new = muon_all(
        owned_low, tile_moment[0, 0], w_q, w_out, w_up, w_down, HF, UT
    )
    return (
        result,
        grad_input,
        owned_grads[None, None],
        tiles_new[None, None],
        moment_new[None, None],
        vec_grad,
        vectors_new,
        vec_moment_new,
    )


def solution(mesh):
    placed = (
        P(("dp", "row"), "col"),
        P(("dp", "row"), "col"),
        P("dp"),
        P("dp"),
        P("col", None, "row"),
        P("row", "col"),
        P("col", "row"),
        P("row", "col"),
        P(),
        P("row", "col", "dp", None, None),
        P(),
    )
    return jax.shard_map(
        body,
        mesh=mesh,
        in_specs=placed,
        out_specs=(
            P(("dp", "row"), "col"),
            P(("dp", "row"), "col"),
            P("row", "col", "dp", None, None),
            P("row", "col", "dp", None, None),
            P("row", "col", "dp", None, None),
            P(),
            P(),
            P(),
        ),
        check_vma=False,
    )
```

```python
import functools
import math

import jax
import jax.numpy as jnp
from jax import lax
from jax.experimental import pallas as pl
from jax.experimental.pallas import tpu as pltpu
from jax.sharding import PartitionSpec as P

HEAD_DIM = 64
ROTARY = 32
SEQ_LEN = 512

MOMENTUM_RATE = 0.95
MUON_RATE = 0.05
VECTOR_RATE = 0.12
NEWTON_A = 3.4445
NEWTON_B = -4.775
NEWTON_C = 2.0315
GELU_SCALE = 0.7978845608028654
GELU_CUBIC = 0.044715
NORM_EPS = 1e-05
STAT_EPS = 1e-06
MASKED_SCORE = -1e30

MESH = pl.DeviceIdType.MESH
ANY = pl.BlockSpec(memory_space=pl.ANY)
F32 = jnp.float32
BF16 = jnp.bfloat16


def to_low(tensor_in):
    return lax.optimization_barrier(tensor_in.astype(BF16))


def gelu_value(pre_act):
    inner_arg = GELU_SCALE * (pre_act + GELU_CUBIC * pre_act * pre_act * pre_act)
    return 0.5 * pre_act * (1.0 + jnp.tanh(inner_arg))


def gelu_slope(pre_act):
    tanh_val = jnp.tanh(GELU_SCALE * (pre_act + GELU_CUBIC * pre_act * pre_act * pre_act))
    return 0.5 * (1.0 + tanh_val) + 0.5 * pre_act * (1.0 - tanh_val * tanh_val) * GELU_SCALE * (
        1.0 + 3.0 * GELU_CUBIC * pre_act * pre_act
    )


def rotary_tables(positions):
    half_dims = ROTARY // 2
    frequency = jnp.exp(jnp.arange(half_dims, dtype=F32) * (-2.0 * math.log(10000.0) / ROTARY))
    angles = positions.astype(F32)[:, None] * frequency[None, :]
    return (jnp.cos(angles), jnp.sin(angles))


def rotate(tensor_in, cosine, sine_tab, direction_sign):
    half_dims = ROTARY // 2
    first_half = tensor_in[..., :half_dims]
    second_half = tensor_in[..., half_dims:ROTARY]
    cos_wide = cosine[:, None, :]
    sin_wide = sine_tab[:, None, :] * direction_sign
    return jnp.concatenate(
        [
            first_half * cos_wide - second_half * sin_wide,
            second_half * cos_wide + first_half * sin_wide,
            tensor_in[..., ROTARY:],
        ],
        axis=-1,
    )


def causal_allowed(segment):
    token_order = jnp.arange(segment.shape[0])
    return (segment[:, None] == segment[None, :]) & (token_order[:, None] >= token_order[None, :])


def masked_scores(queries, key_vecs, segment, score_scale):
    scores = (
        jnp.einsum("lhe,mhe->hlm", queries, key_vecs, preferred_element_type=F32) * score_scale
    )
    return jnp.where(causal_allowed(segment)[None], scores, MASKED_SCORE)


def attend_backward(queries, key_vecs, values, output_low, grad_low, segment, score_scale):
    scores = masked_scores(queries, key_vecs, segment, score_scale)
    weight = jnp.exp(scores - jnp.max(scores, axis=-1, keepdims=True))
    probs = weight * (1.0 / jnp.sum(weight, axis=-1, keepdims=True))
    grad_values = jnp.einsum("hlm,lhe->mhe", to_low(probs), grad_low, preferred_element_type=F32)
    grad_probs = jnp.einsum("lhe,mhe->hlm", grad_low, values, preferred_element_type=F32)
    row_delta = jnp.sum(grad_low.astype(F32) * output_low.astype(F32), axis=-1)
    grad_scores = to_low(probs * (grad_probs - row_delta.T[:, :, None]) * score_scale)
    grad_queries = jnp.einsum("hlm,mhe->lhe", grad_scores, key_vecs, preferred_element_type=F32)
    grad_keys = jnp.einsum("hlm,lhe->mhe", grad_scores, queries, preferred_element_type=F32)
    return (grad_queries, grad_keys, grad_values)


def tile_blocks(qkv_block, out_block, up_block, down_block):
    tile_rows = qkv_block.shape[0]
    tile_cols = qkv_block.shape[2] // 2

    def split_cols(block_in):
        return block_in.reshape(
            block_in.shape[0], block_in.shape[1] // tile_cols, tile_cols
        ).transpose(1, 0, 2)

    down_part = down_block.reshape(
        down_block.shape[0] // tile_rows, tile_rows, down_block.shape[1] // tile_cols, tile_cols
    )
    down_part = down_part.transpose(0, 2, 1, 3).reshape(-1, tile_rows, tile_cols)
    return jnp.concatenate(
        [
            split_cols(qkv_block[:, 0]),
            split_cols(qkv_block[:, 1]),
            split_cols(qkv_block[:, 2]),
            split_cols(out_block),
            split_cols(up_block),
            down_part,
        ],
        axis=0,
    )


def forward_kernel(n_dp, n_row, n_col, dims,
                   x_ref, g_ref, wq_ref, wu_ref, wo_ref, wd_ref,
                   cs_ref, seg_ref, gain_ref, shift_ref, bias_ref,
                   gf, wi, wf, nt, hid, ht, qkv, up, mean_ref, rstd_ref,
                   xv, nb, ntv, wv, stage_g, stage_o, stage_d,
                   zs, zr, ys, yr, cs, cr, ws, wr, ds, dr, ls, lo, no):
    T, C, HF, UT = dims
    d, r, c = lax.axis_index("dp"), lax.axis_index("row"), lax.axis_index("col")
    r1 = r + 1 - 2 * lax.rem(r, 2)
    r2 = lax.rem(r + 2, n_row)
    chunks = 2
    tc = T // chunks
    qw = 3 * HF
    rows_all, D = n_row * T, n_col * C
    seqs = rows_all // SEQ_LEN
    acts = ((x_ref, xv), (g_ref, gf))

    barrier = pltpu.get_barrier_semaphore()
    peers = [{"row": r1}, {"row": r2}]
    peers += [{"col": lax.rem(c + k, n_col)} for k in range(1, n_col)]
    peers += [{"dp": lax.rem(d + k, n_dp)} for k in range(1, n_dp)]
    for peer in peers:
        pl.semaphore_signal(barrier, inc=1, device_id=peer, device_id_type=MESH)
    pl.semaphore_wait(barrier, len(peers))

    def copy(src, dst, s, rcv, peer):
        return pltpu.make_async_remote_copy(
            src_ref=src, dst_ref=dst, send_sem=s, recv_sem=rcv, device_id=peer, device_id_type=MESH
        )

    def blk(a, rr, cc, t):
        return acts[a][1].at[pl.ds(pl.multiple_of(rr * T + t * tc, tc), tc),
                             pl.ds(pl.multiple_of(cc * C, C), C)]

    def own(a, t):
        return acts[a][0].at[pl.ds(t * tc, tc), :]

    def z_copy(a, t, cc, src, right):
        peer = {"col": c + 1} if right else {"col": c - 1}
        return copy(src, blk(a, r, cc, t), zs.at[a, t, int(right), cc], zr.at[a, t, cc], peer)

    def y_copy(a, t, cc, src):
        return copy(src, blk(a, r, cc, t), ys.at[a, t, cc], yr.at[a, t, cc], {"row": r2})

    def c_copy(a, t, cc, src, rr, which):
        return copy(
            src, blk(a, rr, cc, t), cs.at[a, t, which, cc], cr.at[a, t, which, cc], {"row": r1}
        )

    def send_own_z(a, t):
        @pl.when(c < n_col - 1)
        def _():
            z_copy(a, t, c, own(a, t), True).start()

        @pl.when(c > 0)
        def _():
            z_copy(a, t, c, own(a, t), False).start()

    def send_own_row(a, t):
        y_copy(a, t, c, own(a, t)).start()
        c_copy(a, t, c, own(a, t), r, 0).start()

    def relay(a, s, t):
        for right in (True, False):
            cc = c - s if right else c + s

            @pl.when((cc >= 0) & (cc < n_col))
            def _(cc=cc, right=right):
                z_copy(a, t, cc, blk(a, r, cc, t), right).wait_recv()

                @pl.when((c < n_col - 1) if right else (c > 0))
                def _():
                    z_copy(a, t, cc, blk(a, r, cc, t), right).start()

                y_copy(a, t, cc, blk(a, r, cc, t)).start()
                c_copy(a, t, cc, blk(a, r, cc, t), r, 0).start()

    def pass_row(a, s, t):
        for right in (True, False):
            cc = c - s if right else c + s
            ok = (cc >= 0) & (cc < n_col)
            if not right:
                ok = ok & (s > 0)

            @pl.when(ok)
            def _(cc=cc):
                y_copy(a, t, cc, blk(a, r, cc, t)).wait_recv()
                c_copy(a, t, cc, blk(a, r2, cc, t), r2, 1).start()

    ck, hk, uk = C // n_dp, HF // n_dp, UT // n_dp

    def w_dst(part, dd, cc):
        if part == 0:
            return wv.at[pl.ds(cc * C + dd * ck, ck), pl.ds(0, qw)]
        if part == 1:
            return wv.at[pl.ds(cc * C + dd * ck, ck), pl.ds(qw, UT)]
        if part == 2:
            return wv.at[pl.ds(cc * C + dd * ck, ck), pl.ds(qw + UT, UT)]
        if part == 3:
            return wf.at[pl.ds(dd * hk, hk), pl.ds(cc * C, C)]
        if part == 4:
            return wf.at[pl.ds(HF + dd * uk, uk), pl.ds(cc * C, C)]
        return wf.at[pl.ds(HF + UT + dd * uk, uk), pl.ds(cc * C, C)]

    def w_src(part, cc):
        if part == 0:
            return wq_ref.at[cc, pl.ds(d * ck, ck), :]
        if part == 1:
            return wu_ref.at[pl.ds(d * ck, ck), pl.ds(cc * UT, UT)]
        if part == 2:
            return wu_ref.at[pl.ds(d * ck, ck), pl.ds((n_col + cc) * UT, UT)]
        if part == 3:
            return wo_ref.at[pl.ds(cc * HF + d * hk, hk), :]
        if part == 4:
            return wd_ref.at[pl.ds(cc * UT + d * uk, uk), :]
        return wd_ref.at[pl.ds((n_col + cc) * UT + d * uk, uk), :]

    def w_copy(part, k):
        dest = lax.rem(c + k, n_col)
        return copy(
            w_src(part, dest), w_dst(part, d, c), ws.at[part, k], wr.at[part, k], {"col": dest}
        )

    def x_copy(part, k, j):
        got = w_dst(part, d, lax.rem(c + n_col - k, n_col))
        return copy(got, got, ds.at[part, k, j], dr.at[part, k, j], {"dp": lax.rem(d + j, n_dp)})

    def w_send(parts, k):
        for part in parts:
            w_copy(part, k).start()

    def w_pass(parts, k):
        for part in parts:
            w_copy(part, k).wait_recv()
            for j in range(1, n_dp):
                x_copy(part, k, j).start()

    def w_done(parts, k):
        for part in parts:
            for j in range(1, n_dp):
                x_copy(part, k, j).wait_recv()

    win, wfin = (0, 1, 2), (3, 4, 5)

    for t in range(chunks):
        send_own_z(0, t)
    for t in range(chunks):
        send_own_row(0, t)

    col_at = pl.ds(c * C, C)
    direct = [
        pltpu.make_async_copy(x_ref, xv.at[pl.ds(r * T, T), col_at], ls.at[0]),
        pltpu.make_async_copy(wq_ref.at[c], wv.at[col_at, pl.ds(0, qw)], ls.at[1]),
        pltpu.make_async_copy(wu_ref.at[:, pl.ds(c * UT, UT)], wv.at[col_at, pl.ds(qw, UT)],
                              ls.at[2]),
        pltpu.make_async_copy(wu_ref.at[:, pl.ds((n_col + c) * UT, UT)],
                              wv.at[col_at, pl.ds(qw + UT, UT)], ls.at[3]),
    ]
    loads = [
        pltpu.make_async_copy(g_ref, stage_g, ls.at[4]),
        pltpu.make_async_copy(wo_ref.at[pl.ds(c * HF, HF), :], stage_o, ls.at[5]),
        pltpu.make_async_copy(wd_ref.at[pl.ds(c * UT, UT), :], stage_d.at[0], ls.at[6]),
        pltpu.make_async_copy(wd_ref.at[pl.ds((n_col + c) * UT, UT), :], stage_d.at[1], ls.at[7]),
    ]
    stores = [
        pltpu.make_async_copy(stage_g, gf.at[pl.ds(r * T, T), col_at], lo.at[0]),
        pltpu.make_async_copy(stage_o, wf.at[pl.ds(0, HF), col_at], lo.at[1]),
        pltpu.make_async_copy(stage_d.at[0], wf.at[pl.ds(HF, UT), col_at], lo.at[2]),
        pltpu.make_async_copy(stage_d.at[1], wf.at[pl.ds(HF + UT, UT), col_at], lo.at[3]),
    ]
    for item in direct + loads:
        item.start()

    for t in range(chunks):
        relay(0, 1, t)
    w_send(win, 2)
    for t in range(chunks):
        relay(0, 2, t)
    w_send(win, 3)
    w_send(win, 1)
    for t in range(chunks):
        relay(0, 3, t)
    for t in range(chunks):
        send_own_z(1, t)
        send_own_row(1, t)
    for load, store in zip(loads, stores):
        load.wait()
        store.start()
    for s in range(n_col):
        for t in range(chunks):
            pass_row(0, s, t)
    for k in (2, 1, 3):
        w_pass(win, k)
    for t in range(chunks):
        relay(1, 1, t)
    w_send(wfin, 2)
    for item in direct:
        item.wait()
    for t in range(chunks):
        for cc in range(n_col):
            c_copy(0, t, cc, blk(0, r, cc, t), r, 0).wait_recv()
            c_copy(0, t, cc, blk(0, r, cc, t), r, 1).wait_recv()
    for k in (2, 1, 3):
        w_done(win, k)
    keep_w = pltpu.make_async_copy(wv, wi, no.at[0])
    keep_w.start()

    tile = 256
    tiles = rows_all // tile
    sub = 16

    def one_tile(i, carry):
        base = pl.multiple_of(i * tile, tile)

        def norm_rows(k, inner):
            at = pl.ds(pl.multiple_of(base + k * sub, sub), sub)
            val = xv[at, :].astype(F32)
            mean = jnp.sum(val, axis=1, keepdims=True) / D
            var = jnp.sum(val * val, axis=1, keepdims=True) / D - mean * mean
            rstd = lax.rsqrt(var + NORM_EPS)
            mean_ref[at, :] = mean
            rstd_ref[at, :] = rstd
            nb[pl.ds(pl.multiple_of(k * sub, sub), sub), :] = (
                (val - mean) * rstd * gain_ref[...] + shift_ref[...]
            ).astype(BF16)
            return inner

        lax.fori_loop(0, tile // sub, norm_rows, 0)
        at = pl.ds(base, tile)
        mixed = jnp.dot(nb[...], wv[...], preferred_element_type=F32) + bias_ref[...]
        for k in range(D // tile):
            ntv[k * tile : (k + 1) * tile, at] = jnp.transpose(nb[:, k * tile : (k + 1) * tile])
        cos, sin = wide_tables(cs_ref[at, :])
        for j in range(2):
            part = mixed[:, j * HF : (j + 1) * HF]
            qkv[at, j * HF : (j + 1) * HF] = turn(part, cos, sin, 1.0).astype(BF16)
        qkv[at, 2 * HF : 3 * HF] = mixed[:, 2 * HF : 3 * HF].astype(BF16)
        pre = mixed[:, qw:]
        up[at, :] = pre
        act = gelu_value(pre).astype(BF16)
        hid[at, HF:] = act
        ht[HF:, at] = jnp.transpose(act)

        s, t = 2 + lax.div(i, 2), lax.rem(i, 2)

        @pl.when(s < n_col)
        def _():
            relay(1, s, t)

        return carry

    lax.fori_loop(0, 2, one_tile, 0)
    w_send(wfin, 3)
    w_send(wfin, 1)
    lax.fori_loop(2, tiles, one_tile, 0)
    keep_norm = pltpu.make_async_copy(ntv, nt, no.at[1])
    keep_norm.start()

    heads = HF // HEAD_DIM
    qt = SEQ_LEN // 2

    def one_seq(s, carry):
        base = pl.multiple_of(s * SEQ_LEN, SEQ_LEN)
        lane = lax.broadcasted_iota(jnp.int32, (qt, HF), 1)
        seg = seg_ref[pl.ds(s, 1), :]
        seg_col = jnp.transpose(jnp.broadcast_to(seg, (128, SEQ_LEN)))[:, 0:1]
        for qi in range(2):
            width = (qi + 1) * qt
            q_at = pl.ds(pl.multiple_of(base + qi * qt, qt), qt)
            k_at = pl.ds(base, width)
            allowed = (seg_col[qi * qt : (qi + 1) * qt, :] == seg[:, 0:width]) & (
                lax.broadcasted_iota(jnp.int32, (qt, width), 0) + qi * qt
                >= lax.broadcasted_iota(jnp.int32, (qt, width), 1)
            )
            keys, vals = qkv[k_at, HF : 2 * HF], qkv[k_at, 2 * HF : 3 * HF]
            queries = qkv[q_at, 0:HF]
            total = None
            for h in range(heads):
                mine = lax.div(lane, HEAD_DIM) == h
                scores = lax.dot_general(
                    jnp.where(mine, queries, jnp.zeros_like(queries)), keys,
                    (((1,), (1,)), ((), ())), preferred_element_type=F32,
                ) * (HEAD_DIM ** (-0.5))
                scores = jnp.where(allowed, scores, MASKED_SCORE)
                peak = jnp.max(scores, axis=1, keepdims=True)
                weight = jnp.exp(scores - peak)
                weight_sum = jnp.sum(weight, axis=1, keepdims=True)
                probs = (weight * (1.0 / weight_sum)).astype(BF16)
                out = jnp.dot(probs, vals, preferred_element_type=F32)
                total = out if h == 0 else jnp.where(mine, out, total)
            low = total.astype(BF16)
            hid[q_at, 0:HF] = low
            ht[0:HF, q_at] = jnp.transpose(low)

        @pl.when(s < n_col)
        def _():
            for t in range(chunks):
                pass_row(1, s, t)

        return carry

    lax.fori_loop(0, seqs, one_seq, 0)
    for k in (2, 3, 1):
        w_pass(wfin, k)

    for t in range(chunks):
        for cc in range(n_col):
            c_copy(1, t, cc, blk(1, r, cc, t), r, 0).wait_recv()
            c_copy(1, t, cc, blk(1, r, cc, t), r, 1).wait_recv()
    for k in range(1, n_col):
        w_done(wfin, k)
    for a in range(2):
        for t in range(chunks):
            for cc in range(n_col):
                @pl.when((cc <= c) & (c < n_col - 1))
                def _(a=a, t=t, cc=cc):
                    z_copy(a, t, cc, blk(a, r, cc, t), True).wait_send()

                @pl.when((cc >= c) & (c > 0))
                def _(a=a, t=t, cc=cc):
                    z_copy(a, t, cc, blk(a, r, cc, t), False).wait_send()

                y_copy(a, t, cc, blk(a, r, cc, t)).wait_send()
                c_copy(a, t, cc, blk(a, r, cc, t), r, 0).wait_send()
                c_copy(a, t, cc, blk(a, r, cc, t), r, 1).wait_send()
    for k in range(1, n_col):
        for part in win + wfin:
            w_copy(part, k).wait_send()
            for j in range(1, n_dp):
                x_copy(part, k, j).wait_send()
    for store in stores:
        store.wait()
    keep_w.wait()
    keep_norm.wait()


def forward_all(x, g, w_q, w_up, w_out, w_down, packed, seg_row, gain, shift, bias,
                n_dp, n_row, n_col):
    T, C = x.shape
    HF = w_q.shape[2] // 3
    UT = w_up.shape[1] // (2 * n_col)
    n_in, n_out = 3 * HF + 2 * UT, HF + 2 * UT
    rows, D = n_row * T, n_col * C
    dma = pltpu.SemaphoreType.DMA
    vm = pl.BlockSpec(memory_space=pltpu.VMEM)
    sds = jax.ShapeDtypeStruct
    return pl.pallas_call(
        functools.partial(forward_kernel, n_dp, n_row, n_col, (T, C, HF, UT)),
        name="forward_all",
        out_shape=(
            sds((rows, D), BF16),
            sds((D, n_in), BF16),
            sds((n_out, D), BF16),
            sds((D, rows), BF16),
            sds((rows, n_out), BF16),
            sds((n_out, rows), BF16),
            sds((rows, 3 * HF), BF16),
            sds((rows, 2 * UT), F32),
            sds((rows, 1), F32),
            sds((rows, 1), F32),
        ),
        in_specs=[ANY] * 6 + [vm] * 5,
        out_specs=(ANY,) * 4 + (vm,) * 6,
        scratch_shapes=[
            pltpu.VMEM((rows, D), BF16),
            pltpu.VMEM((256, D), BF16),
            pltpu.VMEM((D, rows), BF16),
            pltpu.VMEM((D, n_in), BF16),
            pltpu.VMEM((T, C), BF16),
            pltpu.VMEM((HF, C), BF16),
            pltpu.VMEM((2, UT, C), BF16),
            dma((2, 2, 2, n_col)),
            dma((2, 2, n_col)),
            dma((2, 2, n_col)),
            dma((2, 2, n_col)),
            dma((2, 2, 2, n_col)),
            dma((2, 2, 2, n_col)),
            dma((6, n_col)),
            dma((6, n_col)),
            dma((6, n_col, n_dp)),
            dma((6, n_col, n_dp)),
            dma((8,)),
            dma((4,)),
            dma((2,)),
        ],
        compiler_params=pltpu.CompilerParams(
            collective_id=0, has_side_effects=True, vmem_limit_bytes=60 * 1024 * 1024
        ),
    )(x, g, w_q, w_up, w_out, w_down, packed, seg_row, gain, shift, bias)


def pick(index, table):
    out = jnp.int32(table[0]) if isinstance(table[0], int) else table[0]
    for k in range(1, len(table)):
        out = jnp.where(index == k, table[k], out)
    return out


def wide_tables(packed):
    lane = lax.broadcasted_iota(jnp.int32, packed.shape, 1)
    turned = pltpu.roll(packed, HEAD_DIM, 1)
    first = lane < HEAD_DIM
    return jnp.where(first, packed, turned), jnp.where(first, turned, packed)


def turn(part, cos, sin, sign):
    lane = lax.rem(lax.broadcasted_iota(jnp.int32, part.shape, 1), HEAD_DIM)
    ahead = pltpu.roll(part, part.shape[1] - ROTARY // 2, 1)
    behind = pltpu.roll(part, ROTARY // 2, 1)
    return part * cos + jnp.where(lane < ROTARY // 2, -ahead, behind) * (sign * sin)


def backward_kernel(n_row, n_col, dims,
                    hid_ref, ht_ref, c_ref, wf_ref, wi_ref, nt_ref, qkv_ref, up_ref,
                    cs_ref, seg_ref,
                    res_ref, gn_ref, tiles_ref, part_ref,
                    hd, hts, big, wf, wi, qv, ups, ga,
                    abuf, obuf, asb, sbuf, bbuf, zsb, zin,
                    dwf, dwi, gf, gu, gk,
                    l_s, h_s, u_s, a_s, a_r, y_s, y_r, z_s, z_r, xf_s, xf_r, xu_s, xu_r, xk_s, xk_r,
                    t_s, t_r, free_row, free_col):
    T, C, HF, UT = dims
    rows_all, D = n_row * T, n_col * C
    qw, n_in, n_out = 3 * HF, 3 * HF + 2 * UT, HF + 2 * UT
    step_rows = 64
    d, r, c = lax.axis_index("dp"), lax.axis_index("row"), lax.axis_index("col")
    r1 = r + 1 - 2 * lax.rem(r, 2)
    r2 = lax.rem(r + 2, n_row)
    r12 = lax.rem(r1 + 2, n_row)
    far = [
        sorted(range(n_col), key=lambda f: (-abs(f - cc), f < cc if cc < n_col // 2 else f > cc))
        for cc in range(n_col)
    ]
    forder = [pick(c, [far[cc][i] for cc in range(n_col)]) for i in range(n_col)]
    outs = (res_ref, gn_ref)

    barrier = pltpu.get_barrier_semaphore()
    peers = [{"row": r1}, {"row": r2}, {"dp": 1 - d}]
    peers += [{"col": lax.rem(c + k, n_col)} for k in range(1, n_col)]
    for peer in peers:
        pl.semaphore_signal(barrier, inc=1, device_id=peer, device_id_type=MESH)

    loads = [
        pltpu.make_async_copy(hid_ref, hd.at[:, pl.ds(2 * HF, n_out)], l_s.at[0]),
        pltpu.make_async_copy(wf_ref, wf, l_s.at[1]),
        pltpu.make_async_copy(c_ref, big, l_s.at[2]),
        pltpu.make_async_copy(qkv_ref, qv, l_s.at[3]),
        pltpu.make_async_copy(wi_ref, wi, l_s.at[4]),
    ]
    for item in loads:
        item.start()
    load_nt = pltpu.make_async_copy(nt_ref, big, l_s.at[5])

    def load_ht(m, slot):
        return pltpu.make_async_copy(ht_ref.at[pl.ds(pl.multiple_of(m * HF, HF), HF), :],
                                     hts.at[slot], h_s.at[slot])

    tile = 256

    def load_up(i, slot):
        return pltpu.make_async_copy(up_ref.at[pl.ds(pl.multiple_of(i * tile, tile), tile), :],
                                     ups.at[slot], u_s.at[slot])

    load_ht(0, 0).start()
    load_up(0, 0).start()
    pl.semaphore_wait(barrier, len(peers))

    def copy(src, dst, s, rcv, peer):
        return pltpu.make_async_remote_copy(
            src_ref=src, dst_ref=dst, send_sem=s, recv_sem=rcv, device_id=peer, device_id_type=MESH
        )

    def a_copy(v, h, f):
        return copy(asb.at[h, f], abuf.at[v, h, f], a_s.at[h, f], a_r.at[v, h, f], {"row": r1})

    def y_copy(f):
        return copy(sbuf.at[f], bbuf.at[f], y_s.at[f], y_r.at[f], {"row": r2})

    def z_copy(f, slot, step):
        return copy(zsb.at[f], zin.at[slot], z_s.at[f], z_r.at[slot], {"col": c + step})

    def looped(rows, fn):
        def one(k, carry):
            fn(pl.ds(pl.multiple_of(k * step_rows, step_rows), step_rows))
            return carry
        lax.fori_loop(0, rows // step_rows, one, 0)

    def first_sum(v, f):
        a_copy(v, 1, f).wait_recv()

        def add(rows):
            sbuf[f, rows, :] = (
                obuf[1, f, rows, :].astype(F32) + abuf[v, 1, f, rows, :].astype(F32)
            ).astype(BF16)

        looped(T, add)
        y_copy(f).start()

    def second_sum(v, i):
        f = forder[i]
        a_copy(v, 0, f).wait_recv()
        y_copy(f).wait_recv()

        def base(rows):
            return (
                obuf[0, f, rows, :].astype(F32)
                + abuf[v, 0, f, rows, :].astype(F32)
                + bbuf[f, rows, :].astype(F32)
            )

        if i < n_col - 1:
            right = f > c
            step = jnp.where(right, jnp.int32(1), jnp.int32(-1))
            landed = jnp.where(f == c + step, jnp.where(right, f, jnp.int32(n_col)), f)
            inner = jnp.where(right, c, n_col - 1 - c) > 0

            @pl.when(inner)
            def _():
                z_copy(f, f, 0).wait_recv()

                def add(rows):
                    zsb[f, rows, :] = (base(rows) + zin[f, rows, :].astype(F32)).astype(BF16)

                looped(T, add)

            @pl.when(jnp.logical_not(inner))
            def _():
                def add(rows):
                    zsb[f, rows, :] = base(rows).astype(BF16)

                looped(T, add)

            z_copy(f, landed, step).start()
        else:
            out = outs[v]

            @pl.when(c > 0)
            def _():
                z_copy(f, f, 0).wait_recv()

            @pl.when(c < n_col - 1)
            def _():
                z_copy(f, n_col, 0).wait_recv()

            def put(rows, value):
                out[rows, :] = value

            @pl.when(c == 0)
            def _():
                looped(T, lambda rows: put(rows, base(rows) + zin[n_col, rows, :].astype(F32)))

            @pl.when(c == n_col - 1)
            def _():
                looped(T, lambda rows: put(rows, base(rows) + zin[f, rows, :].astype(F32)))

            @pl.when((c > 0) & (c < n_col - 1))
            def _():
                looped(T, lambda rows: put(
                    rows,
                    base(rows) + zin[f, rows, :].astype(F32) + zin[n_col, rows, :].astype(F32)))

    tall = (HF, 2 * UT)
    row0 = (0, HF)
    lane_u = (qw, qw + UT)
    lw = 2 * HF

    def xf_copy(own, b):
        return copy(dwf.at[pl.ds(row0[own] + b * HF, HF), :], gf.at[pl.ds(b * HF, HF), :],
                    xf_s.at[own, b], xf_r.at[b], {"dp": 1 - d})

    def xu_copy(own, cc):
        return copy(dwi.at[pl.ds(cc * C, C), pl.ds(lane_u[own], UT)], gu.at[cc],
                    xu_s.at[own, cc], xu_r.at[cc], {"dp": 1 - d})

    def xk_copy(cc):
        return copy(dwi.at[pl.ds(cc * C, C), pl.ds(0, qw)], gk.at[cc], xk_s.at[cc], xk_r.at[cc],
                    {"dp": 1 - d})

    def parts_f(own, cc, source):
        half, odd = lax.div(source, 2), lax.rem(source, 2)
        at = cc * C
        if own == 0:
            return [
                (dwf.at[pl.ds(0, HF), pl.ds(at + j * lw, lw)],
                 tiles_ref.at[6 + j, pl.ds(source * HF, HF), :])
                for j in range(2)
            ]
        return [
            (dwf.at[pl.ds(HF + m * UT, UT), pl.ds(at + j * lw, lw)],
             tiles_ref.at[4 + 2 * (2 * m + half) + j, pl.ds(odd * UT, UT), :])
            for m in range(2) for j in range(2)
        ]

    def parts_u(own, cc, source):
        dst = tiles_ref.at[8 + source] if own == 0 else tiles_ref.at[source]
        return [(dwi.at[pl.ds(cc * C, C), pl.ds(lane_u[own], UT)], dst)]

    def parts_k(own, cc, source):
        half, odd = lax.div(source, 2), lax.rem(source, 2)
        return [
            (dwi.at[pl.ds(cc * C, C), pl.ds(j * HF, HF)],
             tiles_ref.at[2 * j + half, :, pl.ds(odd * HF, HF)])
            for j in range(3)
        ]

    kinds = {"f": (parts_f, 0), "u": (parts_u, 4), "k": (parts_k, 5)}

    def t_send(kind, own, cc):
        parts, first = kinds[kind]
        return [
            copy(src, dst, t_s.at[first + n, cc], t_r.at[first + n, c], {"col": cc})
            for n, (src, dst) in enumerate(parts(own, cc, c))
        ]

    def t_wait(kind, own, source):
        parts, first = kinds[kind]
        return [
            copy(src, dst, t_s.at[first + n, source], t_r.at[first + n, source], {"col": source})
            for n, (src, dst) in enumerate(parts(own, source, source))
        ]

    def t_local(kind, own):
        parts, first = kinds[kind]
        return [
            pltpu.make_async_copy(src, dst, t_s.at[first + n, c])
            for n, (src, dst) in enumerate(parts(own, c, c))
        ]

    def owned_kinds(own):
        return ("f", "u", "k") if own == 0 else ("f", "u")

    def spread(kind, own):
        for k in range(1, n_col):
            for item in t_send(kind, own, lax.rem(c + k, n_col)):
                item.start()
        for item in t_local(kind, own):
            item.start()

    def add_f():
        for own in range(2):
            @pl.when(d == own)
            def _(own=own):
                for b in range(tall[own] // HF):
                    xf_copy(own, b).wait_recv()

                def add(rows):
                    at = (pl.ds(pl.multiple_of(rows.start + row0[own], step_rows), step_rows),
                          slice(None))
                    dwf[at] = (dwf[at].astype(F32) + gf[rows, :].astype(F32)).astype(BF16)

                looped(tall[own], add)
                spread("f", own)

    def add_piece(kind, own, cc):
        lane, width, buf, waiter = (
            (lane_u[own], UT, gu, xu_copy(own, cc)) if kind == "u" else (0, qw, gk, xk_copy(cc))
        )
        waiter.wait_recv()

        def add(rows):
            at = (pl.ds(pl.multiple_of(rows.start + cc * C, step_rows), step_rows),
                  pl.ds(lane, width))
            dwi[at] = (dwi[at].astype(F32) + buf[cc, rows, :].astype(F32)).astype(BF16)

        looped(C, add)

    def add_u(i):
        for own in range(2):
            @pl.when(d == own)
            def _(own=own):
                cc = forder[i]
                add_piece("u", own, cc)
                for item in t_local("u", own) if i == n_col - 1 else t_send("u", own, cc):
                    item.start()

    def add_k(i):
        @pl.when(d == 0)
        def _():
            cc = forder[i]
            add_piece("k", 0, cc)
            for item in t_local("k", 0) if i == n_col - 1 else t_send("k", 0, cc):
                item.start()

    loads[0].wait()
    loads[1].wait()

    def p_unit(rr, f):
        at = pl.ds(pl.multiple_of(rr * T, T), T)
        lanes = pl.ds(pl.multiple_of(f * C, C), C)
        return jnp.dot(hd[at, 2 * HF :], wf[:, lanes], preferred_element_type=F32).astype(BF16)

    def p_step(i, carry):
        f = pick(i, forder)
        for h, rr in ((1, r12), (0, r1)):
            asb[h, f] = p_unit(rr, f)
            a_copy(0, h, f).start()
        for h, rr in ((1, r2), (0, r)):
            obuf[h, f] = p_unit(rr, f)

        @pl.when(i > 0)
        def _():
            first_sum(0, pick(i - 1, forder))

        return carry

    lax.fori_loop(0, n_col, p_step, 0)

    loads[2].wait()
    blocks = n_out // HF

    def f_step(m, carry):
        slot = lax.rem(m, 2)
        load_ht(m, slot).wait()

        @pl.when(m + 1 < blocks)
        def _():
            load_ht(m + 1, 1 - slot).start()

        at = pl.ds(pl.multiple_of(m * HF, HF), HF)
        dwf[at, :] = jnp.dot(hts[slot], big[...], preferred_element_type=F32).astype(BF16)

        @pl.when((m == 0) & (d == 1))
        def _():
            xf_copy(0, 0).start()

        @pl.when((m > 0) & (d == 0))
        def _():
            xf_copy(1, m - 1).start()

        return carry

    lax.fori_loop(0, blocks, f_step, 0)
    first_sum(0, forder[n_col - 1])
    second_sum(0, 0)

    part_ref[...] = jnp.zeros_like(part_ref)
    tiles = rows_all // tile

    def b_step(i, carry):
        slot = lax.rem(i, 2)
        load_up(i, slot).wait()

        @pl.when(i + 1 < tiles)
        def _():
            load_up(i + 1, 1 - slot).start()

        at = pl.ds(pl.multiple_of(i * tile, tile), tile)
        back = lax.dot_general(
            big[at, :], wf[...], (((1,), (1,)), ((), ())), preferred_element_type=F32
        )
        ga[at, :] = back[:, :HF].astype(BF16)
        grad = back[:, HF:] * gelu_slope(ups[slot])
        hd[at, qw:] = grad.astype(BF16)
        sums = jnp.sum(grad, axis=0, keepdims=True)
        for k in range(2 * UT // 128):
            part_ref[3 + k : 4 + k, :] += sums[:, k * 128 : (k + 1) * 128]
        return carry

    lax.fori_loop(0, tiles, b_step, 0)
    load_nt.start()
    second_sum(0, 1)
    load_nt.wait()

    def u_step(i, carry):
        cc = pick(i, forder)
        at = pl.ds(pl.multiple_of(cc * C, C), C)
        dwi[at, qw:] = jnp.dot(big[at, :], hd[:, qw:], preferred_element_type=F32).astype(BF16)
        for own in range(2):
            @pl.when(d == own)
            def _(own=own):
                xu_copy(1 - own, cc).start()

        return carry

    lax.fori_loop(0, n_col, u_step, 0)
    second_sum(0, 2)

    loads[3].wait()
    loads[4].wait()
    heads = HF // HEAD_DIM
    qt = SEQ_LEN // 2
    scale = HEAD_DIM ** (-0.5)
    per_row = T // SEQ_LEN
    first_dim = (((0,), (0,)), ((), ()))
    last_dim = (((1,), (1,)), ((), ()))

    def attend_seq(s):
        base = pl.multiple_of(s * SEQ_LEN, SEQ_LEN)
        lane = lax.broadcasted_iota(jnp.int32, (qt, HF), 1)
        seg = seg_ref[pl.ds(s, 1), :]
        seg_col = jnp.transpose(jnp.broadcast_to(seg, (128, SEQ_LEN)))[:, 0:1]
        grad_q, grad_k, grad_v = [], None, None
        for qi in range(2):
            width = (qi + 1) * qt
            q_at = pl.ds(base + qi * qt, qt)
            k_at = pl.ds(base, width)
            allowed = (seg_col[qi * qt : (qi + 1) * qt, :] == seg[:, 0:width]) & (
                lax.broadcasted_iota(jnp.int32, (qt, width), 0) + qi * qt
                >= lax.broadcasted_iota(jnp.int32, (qt, width), 1)
            )
            queries, g_att = qv[q_at, 0:HF], ga[q_at, :]
            keys, vals = qv[k_at, HF : 2 * HF], qv[k_at, 2 * HF : 3 * HF]
            both = g_att.astype(F32) * hd[q_at, 2 * HF : 3 * HF].astype(F32)
            gq, gks, gvs = None, None, None
            for h in range(heads):
                mine = lax.div(lane, HEAD_DIM) == h
                q_h = jnp.where(mine, queries, jnp.zeros_like(queries))
                g_h = jnp.where(mine, g_att, jnp.zeros_like(g_att))
                scores = lax.dot_general(q_h, keys, last_dim, preferred_element_type=F32) * scale
                scores = jnp.where(allowed, scores, MASKED_SCORE)
                peak = jnp.max(scores, axis=1, keepdims=True)
                weight = jnp.exp(scores - peak)
                probs = weight * (1.0 / jnp.sum(weight, axis=1, keepdims=True))
                delta = jnp.sum(jnp.where(mine, both, 0.0), axis=1, keepdims=True)
                g_prob = lax.dot_general(g_h, vals, last_dim, preferred_element_type=F32)
                g_score = (probs * (g_prob - delta) * scale).astype(BF16)
                gq_h = jnp.dot(g_score, keys, preferred_element_type=F32)
                gk_h = lax.dot_general(g_score, q_h, first_dim, preferred_element_type=F32)
                gv_h = lax.dot_general(probs.astype(BF16), g_h, first_dim,
                                       preferred_element_type=F32)
                gq = gq_h if h == 0 else jnp.where(mine, gq_h, gq)
                gks = gk_h if h == 0 else gks + gk_h
                gvs = gv_h if h == 0 else gvs + gv_h
            grad_q.append(gq)
            if qi == 0:
                grad_k, grad_v = gks, gvs
            else:
                grad_k = jnp.concatenate([grad_k + gks[:qt], gks[qt:]], axis=0)
                grad_v = jnp.concatenate([grad_v + gvs[:qt], gvs[qt:]], axis=0)
        s_at = pl.ds(base, SEQ_LEN)
        cos, sin = wide_tables(cs_ref[s_at, :])
        grads = (
            turn(jnp.concatenate(grad_q, axis=0), cos, sin, -1.0),
            turn(grad_k, cos, sin, -1.0),
            grad_v,
        )
        for j, grad in enumerate(grads):
            part_ref[j : j + 1, :] += jnp.sum(grad, axis=0, keepdims=True)
            hd[s_at, j * HF : (j + 1) * HF] = grad.astype(BF16)

    def q_unit(rr, f):
        at = pl.ds(pl.multiple_of(rr * T, T), T)
        feats = pl.ds(pl.multiple_of(f * C, C), C)
        return lax.dot_general(
            hd[at, :], wi[feats, :], last_dim, preferred_element_type=F32
        ).astype(BF16)

    def credit(first):
        if first:
            pl.semaphore_signal(free_row, inc=1, device_id={"row": r2}, device_id_type=MESH)
        for n, step in enumerate((1, -1)):
            @pl.when((c + step >= 0) & (c + step < n_col))
            def _(n=n, step=step):
                if first:
                    pl.semaphore_signal(free_col.at[n], inc=1, device_id={"col": c + step},
                                        device_id_type=MESH)
                else:
                    pl.semaphore_wait(free_col.at[1 - n], 1)
        if not first:
            pl.semaphore_wait(free_row, 1)

    def s_step(m, carry):
        rr = pick(m, [r12, r2, r1, r])

        def seq(s, inner):
            attend_seq(rr * per_row + s)
            return inner

        lax.fori_loop(0, per_row, seq, 0)

        @pl.when(m == 1)
        def _():
            second_sum(0, n_col - 1)
            for f in range(n_col):
                y_copy(f).wait_send()
            for i in range(n_col - 1):
                z_copy(forder[i], forder[i], 0).wait_send()
            credit(True)
            credit(False)

        def units(i, inner):
            f = pick(i, forder)
            value = q_unit(rr, f)

            def to_peer(h):
                a_copy(0, h, f).wait_send()
                asb[h, f] = value
                a_copy(1, h, f).start()

            @pl.when(m == 0)
            def _():
                to_peer(1)

            @pl.when(m == 2)
            def _():
                to_peer(0)

            @pl.when(m == 1)
            def _():
                obuf[1, f] = value
                first_sum(1, f)

            @pl.when(m == 3)
            def _():
                obuf[0, f] = value

            return inner

        lax.fori_loop(0, n_col, units, 0)
        return carry

    lax.fori_loop(0, n_row, s_step, 0)
    add_f()

    def k_step(i, carry):
        cc = pick(i, forder)
        at = pl.ds(pl.multiple_of(cc * C, C), C)
        dwi[at, 0:qw] = jnp.dot(big[at, :], hd[:, 0:qw], preferred_element_type=F32).astype(BF16)

        @pl.when(d == 1)
        def _():
            xk_copy(cc).start()

        return carry

    lax.fori_loop(0, n_col, k_step, 0)
    for i in range(n_col):
        second_sum(1, i) if i < n_col - 1 else None
        add_u(i)
    for i in range(n_col):
        add_k(i)
    second_sum(1, n_col - 1)

    for own in range(2):
        @pl.when(d == own)
        def _(own=own):
            for kind in owned_kinds(own):
                for k in range(1, n_col):
                    for item in t_wait(kind, own, lax.rem(c + k, n_col)):
                        item.wait_recv()
                for k in range(1, n_col):
                    for item in t_send(kind, own, lax.rem(c + k, n_col)):
                        item.wait_send()
                for item in t_local(kind, own):
                    item.wait()
            for b in range(tall[1 - own] // HF):
                xf_copy(1 - own, b).wait_send()
            for cc in range(n_col):
                xu_copy(1 - own, cc).wait_send()
                if own == 1:
                    xk_copy(cc).wait_send()
    for f in range(n_col):
        a_copy(1, 0, f).wait_send()
        a_copy(1, 1, f).wait_send()
        y_copy(f).wait_send()
    for i in range(n_col - 1):
        z_copy(forder[i], forder[i], 0).wait_send()


def backward_all(hid, ht, cot, w_fin, w_in, nt, qkv, up, packed, seg_row, T, C, HF, UT, n_row, n_col):
    dma = pltpu.SemaphoreType.DMA
    vm = pl.BlockSpec(memory_space=pltpu.VMEM)
    rows, D = n_row * T, n_col * C
    n_in, n_out = 3 * HF + 2 * UT, HF + 2 * UT
    unit = (T, C)
    V = pltpu.VMEM
    return pl.pallas_call(
        functools.partial(backward_kernel, n_row, n_col, (T, C, HF, UT)),
        name="backward_all",
        out_shape=(
            jax.ShapeDtypeStruct(unit, F32),
            jax.ShapeDtypeStruct(unit, F32),
            jax.ShapeDtypeStruct((12, C, UT), BF16),
            jax.ShapeDtypeStruct((8, 128), F32),
        ),
        in_specs=[ANY] * 8 + [vm] * 2,
        out_specs=(vm, vm, ANY, vm),
        scratch_shapes=[
            V((rows, n_in), BF16),
            V((2, HF, rows), BF16),
            V((rows, D), BF16),
            V((n_out, D), BF16),
            V((D, n_in), BF16),
            V((rows, 3 * HF), BF16),
            V((2, 256, 2 * UT), F32),
            V((rows, HF), BF16),
            V((2, 2, n_col) + unit, BF16),
            V((2, n_col) + unit, BF16),
            V((2, n_col) + unit, BF16),
            V((n_col,) + unit, BF16),
            V((n_col,) + unit, BF16),
            V((n_col,) + unit, BF16),
            V((n_col + 1,) + unit, BF16),
            V((n_out, D), BF16),
            V((D, n_in), BF16),
            V((2 * UT, D), BF16),
            V((n_col, C, UT), BF16),
            V((n_col, C, 3 * HF), BF16),
            dma((6,)),
            dma((2,)),
            dma((2,)),
            dma((2, n_col)),
            dma((2, 2, n_col)),
            dma((n_col,)),
            dma((n_col,)),
            dma((n_col,)),
            dma((n_col + 1,)),
            dma((2, 2 * UT // HF)),
            dma((2 * UT // HF,)),
            dma((2, n_col)),
            dma((n_col,)),
            dma((n_col,)),
            dma((n_col,)),
            dma((8, n_col)),
            dma((8, n_col)),
            pltpu.SemaphoreType.REGULAR,
            pltpu.SemaphoreType.REGULAR((2,)),
        ],
        compiler_params=pltpu.CompilerParams(
            collective_id=1, has_side_effects=True, vmem_limit_bytes=67043328
        ),
    )(hid, ht, cot, w_fin, w_in, nt, qkv, up, packed, seg_row)


def finish_kernel(n_dp, n_row, n_col, width, gn_ref, x_ref, g_ref, mean_ref, rstd_ref, gain_ref, part_ref,
                  gx_ref, va_ref, vb_ref,
                  st, da, db, ra, rb,
                  st_s, st_r, d_s, d_r, r_s, r_r, c_s, c_r):
    d, r, c = lax.axis_index("dp"), lax.axis_index("row"), lax.axis_index("col")
    T, C = gn_ref.shape

    barrier = pltpu.get_barrier_semaphore()
    dps = [lax.rem(d + k, n_dp) for k in range(1, n_dp)]
    rows = [lax.rem(r + k, n_row) for k in range(1, n_row)]
    cols = [lax.rem(c + k, n_col) for k in range(1, n_col)]
    peers = [{"dp": k} for k in dps] + [{"row": k} for k in rows] + [{"col": k} for k in cols]
    for peer in peers:
        pl.semaphore_signal(barrier, inc=1, device_id=peer, device_id_type=MESH)
    pl.semaphore_wait(barrier, len(peers))

    def copy(src, dst, s, rcv, peer):
        return pltpu.make_async_remote_copy(
            src_ref=src, dst_ref=dst, send_sem=s, recv_sem=rcv, device_id=peer, device_id_type=MESH
        )

    gain = gain_ref[...]

    def fold(value):
        total = value[:, 0:128]
        for k in range(1, C // 128):
            total = total + value[:, k * 128 : (k + 1) * 128]
        return jnp.sum(jnp.transpose(total), axis=0, keepdims=True)

    gn = gn_ref[...]
    x_hat = (x_ref[...].astype(F32) - mean_ref[...]) * rstd_ref[...]
    gh = gn * gain
    st[c, 0:1, :] = fold(gh)
    st[c, 1:2, :] = fold(gh * x_hat)

    def st_copy(k):
        return copy(st.at[c], st.at[c], st_s.at[k], st_r.at[c], {"col": k})

    def st_wait(k):
        return copy(st.at[k], st.at[k], st_s.at[k], st_r.at[k], {"col": k})

    for k in cols:
        st_copy(k).start()

    da[d] = part_ref[...]
    db[d, 0:1, :] = jnp.sum(gn * x_hat, axis=0, keepdims=True)
    db[d, 1:2, :] = jnp.sum(gn, axis=0, keepdims=True)
    db[d, 2:3, :] = jnp.sum(g_ref[...].astype(F32), axis=0, keepdims=True)

    def pair(a_src, b_src, a_dst, b_dst, s, rcv, peer):
        return [copy(a_src, a_dst, s.at[0], rcv.at[0], peer),
                copy(b_src, b_dst, s.at[1], rcv.at[1], peer)]

    def d_pair(slot, peer):
        return pair(da.at[slot], db.at[slot], da.at[slot], db.at[slot],
                    d_s.at[peer], d_r.at[slot], {"dp": peer})

    def r_pair(slot, peer):
        return pair(ra.at[slot], rb.at[slot], ra.at[slot], rb.at[slot],
                    r_s.at[peer], r_r.at[slot], {"row": peer})

    def c_pair(slot, peer):
        return pair(va_ref.at[slot], vb_ref.at[slot], va_ref.at[slot], vb_ref.at[slot],
                    c_s.at[peer], c_r.at[slot], {"col": peer})

    for k in dps:
        for item in d_pair(d, k):
            item.start()
    for k in dps:
        for item in d_pair(k, k):
            item.wait_recv()
    a_sum, b_sum = da[0], db[0]
    for k in range(1, n_dp):
        a_sum = a_sum + da[k]
        b_sum = b_sum + db[k]
    ra[r] = a_sum
    rb[r] = b_sum
    for k in rows:
        for item in r_pair(r, k):
            item.start()

    for k in cols:
        st_wait(k).wait_recv()
    stats = st[0]
    for k in range(1, n_col):
        stats = stats + st[k]
    stats = stats / width
    m1 = jnp.transpose(jnp.broadcast_to(stats[0:1, :], (128, T)))[:, 0:1]
    m2 = jnp.transpose(jnp.broadcast_to(stats[1:2, :], (128, T)))[:, 0:1]
    gx_ref[...] = g_ref[...].astype(F32) + rstd_ref[...] * (gh - m1 - x_hat * m2)

    for k in rows:
        for item in r_pair(k, k):
            item.wait_recv()
    b_sum = rb[0]
    for k in range(1, n_row):
        b_sum = b_sum + rb[k]
    for k in range(n_row):
        va_ref[c, k] = ra[k]
    vb_ref[c] = b_sum
    for k in cols:
        for item in c_pair(c, k):
            item.start()
    for k in cols:
        for item in c_pair(k, k):
            item.wait_recv()
    for k in cols:
        st_copy(k).wait_send()
        for item in c_pair(c, k):
            item.wait_send()
    for k in dps:
        for item in d_pair(d, k):
            item.wait_send()
    for k in rows:
        for item in r_pair(r, k):
            item.wait_send()


def finish_all(gn, x, g, mean, rstd, gain, part, width, n_dp, n_row, n_col):
    T, C = gn.shape
    dma = pltpu.SemaphoreType.DMA
    vm = pl.BlockSpec(memory_space=pltpu.VMEM)
    return pl.pallas_call(
        functools.partial(finish_kernel, n_dp, n_row, n_col, width),
        name="finish_all",
        out_shape=(
            jax.ShapeDtypeStruct((T, C), F32),
            jax.ShapeDtypeStruct((n_col, n_row, 8, 128), F32),
            jax.ShapeDtypeStruct((n_col, 8, C), F32),
        ),
        in_specs=[vm] * 7,
        out_specs=(vm,) * 3,
        scratch_shapes=[
            pltpu.VMEM((n_col, 8, T), F32),
            pltpu.VMEM((n_dp, 8, 128), F32),
            pltpu.VMEM((n_dp, 8, C), F32),
            pltpu.VMEM((n_row, 8, 128), F32),
            pltpu.VMEM((n_row, 8, C), F32),
            dma((n_col,)),
            dma((n_col,)),
            dma((n_dp, 2)),
            dma((n_dp, 2)),
            dma((n_row, 2)),
            dma((n_row, 2)),
            dma((n_col, 2)),
            dma((n_col, 2)),
        ],
        compiler_params=pltpu.CompilerParams(
            collective_id=2, has_side_effects=True, vmem_limit_bytes=48 * 1024 * 1024
        ),
    )(gn, x, g, mean, rstd, gain, part)


def muon_kernel(owned, per_step, HF, UT, rate, grad_ref, mom_ref, wq_ref, wo_ref, wu_ref, wd_ref,
                og_ref, new_ref, nm_ref, wbuf, sem):
    first = lax.axis_index("dp") * owned
    step = pl.program_id(0)
    steps = owned // per_step
    n_qkv, n_out, n_up = 6, 2, 8

    def fetch(tile, slot, n, start):
        dst = wbuf.at[slot, n]

        def go(src, target, s):
            item = pltpu.make_async_copy(src, target, s)
            if start:
                item.start()
            else:
                item.wait()

        @pl.when(tile < n_qkv)
        def _():
            j, half = lax.div(tile, 2), lax.rem(tile, 2)
            for m in range(UT // HF):
                go(wq_ref.at[half * (UT // HF) + m, :, pl.ds(j * HF, HF)],
                   wbuf.at[slot, n, :, pl.ds(m * HF, HF)], sem.at[slot, n, m])

        @pl.when((tile >= n_qkv) & (tile < n_qkv + n_out))
        def _():
            go(wo_ref.at[:, pl.ds((tile - n_qkv) * UT, UT)], dst, sem.at[slot, n, 0])

        @pl.when((tile >= n_qkv + n_out) & (tile < n_qkv + n_out + n_up))
        def _():
            go(wu_ref.at[:, pl.ds((tile - n_qkv - n_out) * UT, UT)], dst, sem.at[slot, n, 0])

        @pl.when(tile >= n_qkv + n_out + n_up)
        def _():
            left = tile - (n_qkv + n_out + n_up)
            rows = dst.shape[0]
            go(wd_ref.at[pl.ds(lax.div(left, 2) * rows, rows), pl.ds(lax.rem(left, 2) * UT, UT)],
               dst, sem.at[slot, n, 0])

    def fetch_all(at, start):
        for n in range(per_step):
            fetch(first + at * per_step + n, lax.rem(at, 2), n, start)

    @pl.when(step == 0)
    def _():
        fetch_all(step, True)

    @pl.when(step + 1 < steps)
    def _():
        fetch_all(step + 1, True)

    iters = []
    for n in range(per_step):
        grad = grad_ref[n].astype(F32)
        og_ref[n] = grad
        moment = MOMENTUM_RATE * mom_ref[n] + grad
        nm_ref[n] = moment
        scale = lax.rsqrt(jnp.sum(moment * moment, keepdims=True) + STAT_EPS)
        iters.append((moment * scale).astype(BF16))
    contract = (((0,), (0,)), ((), ()))
    for _ in range(5):
        grams = [
            lax.dot_general(x, x, contract, preferred_element_type=F32).astype(BF16) for x in iters
        ]
        squares = [jnp.dot(g, g, preferred_element_type=F32) for g in grams]
        polys = [
            (NEWTON_B * g.astype(F32) + NEWTON_C * s).astype(BF16) for g, s in zip(grams, squares)
        ]
        iters = [
            (NEWTON_A * x.astype(F32) + jnp.dot(x, p, preferred_element_type=F32)).astype(BF16)
            for x, p in zip(iters, polys)
        ]
    fetch_all(step, False)
    for n in range(per_step):
        new_ref[n] = wbuf[lax.rem(step, 2), n].astype(F32) - rate * iters[n].astype(F32)


def muon_all(grads, moment, w_q, w_out, w_up, w_down, HF, UT):
    owned, rows, cols = moment.shape
    per_step = 3
    rate = MUON_RATE * math.sqrt(max(1.0, rows / cols))
    block = pl.BlockSpec((per_step, rows, cols), lambda i: (i, 0, 0))
    out = jax.ShapeDtypeStruct(moment.shape, F32)
    return pl.pallas_call(
        functools.partial(muon_kernel, owned, per_step, HF, UT, rate),
        name="muon_all",
        grid=(owned // per_step,),
        out_shape=(out, out, out),
        in_specs=[block, block, ANY, ANY, ANY, ANY],
        out_specs=(block, block, block),
        scratch_shapes=[
            pltpu.VMEM((2, per_step, rows, cols), BF16),
            pltpu.SemaphoreType.DMA((2, per_step, 2)),
        ],
        compiler_params=pltpu.CompilerParams(vmem_limit_bytes=56 * 1024 * 1024),
    )(grads, moment, w_q, w_out, w_up, w_down)


def reduce_plain(p, q, dwi, dwf, C, HF, UT, n_col, row_width):
    def block(part):
        part = lax.psum_scatter(part, "row", scatter_dimension=0, tiled=True)
        return lax.psum_scatter(part, "col", scatter_dimension=1, tiled=True).astype(F32)

    wi4 = lax.all_to_all(dwi.reshape(n_col, C, -1), "col", 0, 0)
    wf4 = lax.all_to_all(dwf.reshape(-1, n_col, C).transpose(1, 0, 2), "col", 0, 0)
    grad_qkv = (
        wi4[:, :, : 3 * HF].reshape(n_col, C, 3, HF).transpose(1, 2, 0, 3).reshape(C, 3, row_width)
    )
    grad_up_w = wi4[:, :, 3 * HF :].reshape(n_col, C, 2, UT).transpose(1, 2, 0, 3).reshape(C, -1)
    grad_w_out = wf4[:, :HF].reshape(-1, C)
    grad_w_down = wf4[:, HF:].reshape(n_col, 2, UT, C).transpose(1, 0, 2, 3).reshape(-1, C)
    grad_tiles = tile_blocks(grad_qkv, grad_w_out, grad_up_w, grad_w_down)
    owned = lax.psum_scatter(grad_tiles, "dp", scatter_dimension=0, tiled=True)
    return block(p), block(q), owned


def backward_plain(hidden, hidden_t, cot, w_fin, w_in, norm_t, qkv, up_pre, cosine, sine_tab, segments, HF):
    rows = cot.shape[0]
    seqs, heads = rows // SEQ_LEN, HF // HEAD_DIM

    def by_head(tensor_in):
        return tensor_in.reshape(seqs, SEQ_LEN, heads, HEAD_DIM)

    partial_out = jnp.dot(hidden, w_fin, preferred_element_type=F32).astype(BF16)
    grad_w_fin = jnp.dot(hidden_t, cot, preferred_element_type=F32).astype(BF16)
    back = jnp.einsum("tj,ij->ti", cot, w_fin, preferred_element_type=F32)
    grad_up = back[:, HF:] * gelu_slope(up_pre)
    grads = jax.vmap(attend_backward, in_axes=(0, 0, 0, 0, 0, 0, None))(
        by_head(qkv[:, :HF]),
        by_head(qkv[:, HF : 2 * HF]),
        by_head(qkv[:, 2 * HF :]),
        by_head(hidden[:, :HF]),
        by_head(back[:, :HF].astype(BF16)),
        segments.reshape(seqs, SEQ_LEN),
        HEAD_DIM ** (-0.5),
    )
    g_q, g_k, g_v = [item.reshape(rows, heads, HEAD_DIM) for item in grads]
    g_q = rotate(g_q, cosine, sine_tab, -1.0)
    g_k = rotate(g_k, cosine, sine_tab, -1.0)
    grad_mixed = jnp.concatenate(
        [item.reshape(rows, HF) for item in (g_q, g_k, g_v)] + [grad_up], axis=1
    )
    low = grad_mixed.astype(BF16)
    grad_w_in = jnp.dot(norm_t, low, preferred_element_type=F32).astype(BF16)
    partial_norm = jnp.einsum("tj,ij->ti", low, w_in, preferred_element_type=F32).astype(BF16)
    part = jnp.pad(jnp.sum(grad_mixed, axis=0).reshape(-1, 128), ((0, 1), (0, 0)))
    return (partial_out, partial_norm, grad_w_in, grad_w_fin), part


def body(
    inputs,
    cotangent,
    segments,
    positions,
    w_qkv,
    w_out,
    w_up,
    w_down,
    vectors,
    tile_moment,
    vector_moment,
):
    row_index = lax.axis_index("row")
    col_index = lax.axis_index("col")
    n_dp, n_row, n_col = lax.axis_size("dp"), lax.axis_size("row"), lax.axis_size("col")
    T, C = inputs.shape
    D = vectors.shape[1]
    row_width = w_qkv.shape[2]
    HF = row_width // n_col
    UT = w_up.shape[1] // (2 * n_col)
    feat_start = (row_index * n_col + col_index) * HF
    unit_a = (row_index * 2 * n_col + col_index) * UT
    unit_b = unit_a + n_col * UT
    col_start = col_index * C
    gain, shift = vectors[5], vectors[6]
    norm_gain = lax.dynamic_slice_in_dim(gain, col_start, C)
    out_bias = lax.dynamic_slice_in_dim(vectors[3] + vectors[4], col_start, C)
    qkv_bias = lax.dynamic_slice_in_dim(vectors[0:3], feat_start, HF, axis=1)
    up_flat = vectors[7:].reshape(-1)
    up_bias = jnp.concatenate(
        [
            lax.dynamic_slice_in_dim(up_flat, unit_a, UT),
            lax.dynamic_slice_in_dim(up_flat, unit_b, UT),
        ]
    )
    w_q = (
        w_qkv.reshape(C, 3, n_col, HF).transpose(2, 0, 1, 3).reshape(n_col, C, 3 * HF)
    )
    cosine, sine_tab = rotary_tables(positions)
    rows_all = positions.shape[0]
    flat = jnp.ones((rows_all, HEAD_DIM - ROTARY), F32)
    packed = jnp.concatenate(
        [cosine, cosine, flat, sine_tab, sine_tab, 0.0 * flat], axis=1
    )
    seq_count = rows_all // SEQ_LEN
    seg_row = segments.reshape(seq_count, SEQ_LEN)
    cot_rows, w_in, w_fin, norm_t, hidden, hidden_t, qkv_low, up_pre, mean_all, rstd_all = forward_all(
        inputs,
        cotangent,
        w_q,
        w_up,
        w_out,
        w_down,
        packed,
        seg_row,
        gain[None],
        shift[None],
        jnp.concatenate([qkv_bias.reshape(-1), up_bias])[None],
        n_dp,
        n_row,
        n_col,
    )
    if n_dp == 2:
        branch, grad_norm, owned_low, part = backward_all(
            hidden, hidden_t, cot_rows, w_fin, w_in, norm_t, qkv_low, up_pre, packed, seg_row,
            T, C, HF, UT, n_row, n_col,
        )
    else:
        partials, part = backward_plain(
            hidden, hidden_t, cot_rows, w_fin, w_in, norm_t, qkv_low, up_pre, cosine, sine_tab, segments, HF
        )
        branch, grad_norm, owned_low = reduce_plain(*partials, C, HF, UT, n_col, row_width)
    x_val = inputs.astype(F32)
    result = x_val + branch + out_bias

    grad_input, vec_a, vec_b = finish_all(
        grad_norm,
        inputs,
        cotangent,
        lax.dynamic_slice_in_dim(mean_all, row_index * T, T),
        lax.dynamic_slice_in_dim(rstd_all, row_index * T, T),
        norm_gain[None],
        part,
        D,
        n_dp,
        n_row,
        n_col,
    )
    vec_a = vec_a.transpose(2, 1, 0, 3)
    qkv_rows = vec_a[:3].reshape(3, D)
    up_rows = vec_a[3:7].reshape(2, UT // 128, n_row, n_col, 128).transpose(2, 0, 3, 1, 4)
    norm_rows = vec_b.transpose(1, 0, 2).reshape(8, D)
    vec_grad = jnp.concatenate(
        [qkv_rows, norm_rows[2:3], norm_rows[2:3], norm_rows[:2], up_rows.reshape(-1, D)], axis=0
    )
    scaled = vec_grad * lax.rsqrt(jnp.mean(vec_grad * vec_grad, axis=1, keepdims=True) + STAT_EPS)
    vec_moment_new = MOMENTUM_RATE * vector_moment + scaled
    vectors_new = vectors - VECTOR_RATE * vec_moment_new

    owned_grads, tiles_new, moment_new = muon_all(
        owned_low, tile_moment[0, 0], w_q, w_out, w_up, w_down, HF, UT
    )
    return (
        result,
        grad_input,
        owned_grads[None, None],
        tiles_new[None, None],
        moment_new[None, None],
        vec_grad,
        vectors_new,
        vec_moment_new,
    )


def solution(mesh):
    placed = (
        P(("dp", "row"), "col"),
        P(("dp", "row"), "col"),
        P("dp"),
        P("dp"),
        P("col", None, "row"),
        P("row", "col"),
        P("col", "row"),
        P("row", "col"),
        P(),
        P("row", "col", "dp", None, None),
        P(),
    )
    return jax.shard_map(
        body,
        mesh=mesh,
        in_specs=placed,
        out_specs=(
            P(("dp", "row"), "col"),
            P(("dp", "row"), "col"),
            P("row", "col", "dp", None, None),
            P("row", "col", "dp", None, None),
            P("row", "col", "dp", None, None),
            P(),
            P(),
            P(),
        ),
        check_vma=False,
    )
```

```python
import functools
import math

import jax
import jax.numpy as jnp
from jax import lax
from jax.experimental import pallas as pl
from jax.experimental.pallas import tpu as pltpu
from jax.sharding import PartitionSpec as P

HEAD_DIM = 64
ROTARY = 32
SEQ_LEN = 512

MOMENTUM_RATE = 0.95
MUON_RATE = 0.05
VECTOR_RATE = 0.12
NEWTON_A = 3.4445
NEWTON_B = -4.775
NEWTON_C = 2.0315
GELU_SCALE = 0.7978845608028654
GELU_CUBIC = 0.044715
NORM_EPS = 1e-05
STAT_EPS = 1e-06
MASKED_SCORE = -1e30

MESH = pl.DeviceIdType.MESH
ANY = pl.BlockSpec(memory_space=pl.ANY)
F32 = jnp.float32
BF16 = jnp.bfloat16


def to_low(tensor_in):
    return lax.optimization_barrier(tensor_in.astype(BF16))


def gelu_value(pre_act):
    inner_arg = GELU_SCALE * (pre_act + GELU_CUBIC * pre_act * pre_act * pre_act)
    return 0.5 * pre_act * (1.0 + jnp.tanh(inner_arg))


def gelu_slope(pre_act):
    tanh_val = jnp.tanh(GELU_SCALE * (pre_act + GELU_CUBIC * pre_act * pre_act * pre_act))
    return 0.5 * (1.0 + tanh_val) + 0.5 * pre_act * (1.0 - tanh_val * tanh_val) * GELU_SCALE * (
        1.0 + 3.0 * GELU_CUBIC * pre_act * pre_act
    )


def rotary_tables(positions):
    half_dims = ROTARY // 2
    frequency = jnp.exp(jnp.arange(half_dims, dtype=F32) * (-2.0 * math.log(10000.0) / ROTARY))
    angles = positions.astype(F32)[:, None] * frequency[None, :]
    return (jnp.cos(angles), jnp.sin(angles))


def rotate(tensor_in, cosine, sine_tab, direction_sign):
    half_dims = ROTARY // 2
    first_half = tensor_in[..., :half_dims]
    second_half = tensor_in[..., half_dims:ROTARY]
    cos_wide = cosine[:, None, :]
    sin_wide = sine_tab[:, None, :] * direction_sign
    return jnp.concatenate(
        [
            first_half * cos_wide - second_half * sin_wide,
            second_half * cos_wide + first_half * sin_wide,
            tensor_in[..., ROTARY:],
        ],
        axis=-1,
    )


def causal_allowed(segment):
    token_order = jnp.arange(segment.shape[0])
    return (segment[:, None] == segment[None, :]) & (token_order[:, None] >= token_order[None, :])


def masked_scores(queries, key_vecs, segment, score_scale):
    scores = (
        jnp.einsum("lhe,mhe->hlm", queries, key_vecs, preferred_element_type=F32) * score_scale
    )
    return jnp.where(causal_allowed(segment)[None], scores, MASKED_SCORE)


def attend_backward(queries, key_vecs, values, output_low, grad_low, segment, score_scale):
    scores = masked_scores(queries, key_vecs, segment, score_scale)
    weight = jnp.exp(scores - jnp.max(scores, axis=-1, keepdims=True))
    probs = weight * (1.0 / jnp.sum(weight, axis=-1, keepdims=True))
    grad_values = jnp.einsum("hlm,lhe->mhe", to_low(probs), grad_low, preferred_element_type=F32)
    grad_probs = jnp.einsum("lhe,mhe->hlm", grad_low, values, preferred_element_type=F32)
    row_delta = jnp.sum(grad_low.astype(F32) * output_low.astype(F32), axis=-1)
    grad_scores = to_low(probs * (grad_probs - row_delta.T[:, :, None]) * score_scale)
    grad_queries = jnp.einsum("hlm,mhe->lhe", grad_scores, key_vecs, preferred_element_type=F32)
    grad_keys = jnp.einsum("hlm,lhe->mhe", grad_scores, queries, preferred_element_type=F32)
    return (grad_queries, grad_keys, grad_values)


def tile_blocks(qkv_block, out_block, up_block, down_block):
    tile_rows = qkv_block.shape[0]
    tile_cols = qkv_block.shape[2] // 2

    def split_cols(block_in):
        return block_in.reshape(
            block_in.shape[0], block_in.shape[1] // tile_cols, tile_cols
        ).transpose(1, 0, 2)

    down_part = down_block.reshape(
        down_block.shape[0] // tile_rows, tile_rows, down_block.shape[1] // tile_cols, tile_cols
    )
    down_part = down_part.transpose(0, 2, 1, 3).reshape(-1, tile_rows, tile_cols)
    return jnp.concatenate(
        [
            split_cols(qkv_block[:, 0]),
            split_cols(qkv_block[:, 1]),
            split_cols(qkv_block[:, 2]),
            split_cols(out_block),
            split_cols(up_block),
            down_part,
        ],
        axis=0,
    )


def pick(index, table):
    out = jnp.int32(table[0]) if isinstance(table[0], int) else table[0]
    for k in range(1, len(table)):
        out = jnp.where(index == k, table[k], out)
    return out


def far_order(c, n_col):
    far = [
        sorted(range(n_col), key=lambda f: (-abs(f - cc), f < cc if cc < n_col // 2 else f > cc))
        for cc in range(n_col)
    ]
    return [pick(c, [far[cc][i] for cc in range(n_col)]) for i in range(n_col)]


def forward_kernel(n_dp, n_row, n_col, dims,
                   x_ref, g_ref, wq_ref, wu_ref, wo_ref, wd_ref,
                   pos_ref, seg_ref, freq_ref, vec_ref,
                   gf, wi, wf, nt, hid_out, ht_out, qkv_out, up_out, cs_out, mean_ref, rstd_ref,
                   xv, ntv, wv, hid, ht, qkv, up, tab, mean_v, rstd_v, stage_g, stage_o, stage_d,
                   zs, zr, ys, yr, cs, cr, ws, wr, ds, dr, ls, lo, no):
    T, C, HF, UT = dims
    d, r, c = lax.axis_index("dp"), lax.axis_index("row"), lax.axis_index("col")
    r1 = r + 1 - 2 * lax.rem(r, 2)
    r2 = lax.rem(r + 2, n_row)
    chunks = 2
    tc = T // chunks
    qw = 3 * HF
    rows_all, D = n_row * T, n_col * C
    seqs = rows_all // SEQ_LEN
    acts = ((x_ref, xv), (g_ref, gf))
    forder = far_order(c, n_col)

    barrier = pltpu.get_barrier_semaphore()
    peers = [{"row": r1}, {"row": r2}]
    peers += [{"col": lax.rem(c + k, n_col)} for k in range(1, n_col)]
    peers += [{"dp": lax.rem(d + k, n_dp)} for k in range(1, n_dp)]
    for peer in peers:
        pl.semaphore_signal(barrier, inc=1, device_id=peer, device_id_type=MESH)
    pl.semaphore_wait(barrier, len(peers))

    def copy(src, dst, s, rcv, peer):
        return pltpu.make_async_remote_copy(
            src_ref=src, dst_ref=dst, send_sem=s, recv_sem=rcv, device_id=peer, device_id_type=MESH
        )

    def blk(a, rr, cc, t):
        return acts[a][1].at[pl.ds(pl.multiple_of(rr * T + t * tc, tc), tc),
                             pl.ds(pl.multiple_of(cc * C, C), C)]

    def own(a, t):
        return acts[a][0].at[pl.ds(t * tc, tc), :]

    def z_copy(a, t, cc, src, right):
        peer = {"col": c + 1} if right else {"col": c - 1}
        return copy(src, blk(a, r, cc, t), zs.at[a, t, int(right), cc], zr.at[a, t, cc], peer)

    def y_copy(a, t, cc, src):
        return copy(src, blk(a, r, cc, t), ys.at[a, t, cc], yr.at[a, t, cc], {"row": r2})

    def c_copy(a, t, cc, src, rr, which):
        return copy(
            src, blk(a, rr, cc, t), cs.at[a, t, which, cc], cr.at[a, t, which, cc], {"row": r1}
        )

    def send_own_z(a, t):
        @pl.when(c < n_col - 1)
        def _():
            z_copy(a, t, c, own(a, t), True).start()

        @pl.when(c > 0)
        def _():
            z_copy(a, t, c, own(a, t), False).start()

    def send_own_row(a, t):
        y_copy(a, t, c, own(a, t)).start()
        c_copy(a, t, c, own(a, t), r, 0).start()

    def relay(a, s, t):
        for right in (True, False):
            cc = c - s if right else c + s

            @pl.when((cc >= 0) & (cc < n_col))
            def _(cc=cc, right=right):
                z_copy(a, t, cc, blk(a, r, cc, t), right).wait_recv()

                @pl.when((c < n_col - 1) if right else (c > 0))
                def _():
                    z_copy(a, t, cc, blk(a, r, cc, t), right).start()

                y_copy(a, t, cc, blk(a, r, cc, t)).start()
                c_copy(a, t, cc, blk(a, r, cc, t), r, 0).start()

    def pass_row(a, s, t):
        for right in (True, False):
            cc = c - s if right else c + s
            ok = (cc >= 0) & (cc < n_col)
            if not right:
                ok = ok & (s > 0)

            @pl.when(ok)
            def _(cc=cc):
                y_copy(a, t, cc, blk(a, r, cc, t)).wait_recv()
                c_copy(a, t, cc, blk(a, r2, cc, t), r2, 1).start()

    ck, hk, uk = C // n_dp, HF // n_dp, UT // n_dp

    def w_dst(part, dd, cc):
        if part == 0:
            return wv.at[pl.ds(cc * C + dd * ck, ck), pl.ds(0, qw)]
        if part == 1:
            return wv.at[pl.ds(cc * C + dd * ck, ck), pl.ds(qw, UT)]
        if part == 2:
            return wv.at[pl.ds(cc * C + dd * ck, ck), pl.ds(qw + UT, UT)]
        if part == 3:
            return wf.at[pl.ds(dd * hk, hk), pl.ds(cc * C, C)]
        if part == 4:
            return wf.at[pl.ds(HF + dd * uk, uk), pl.ds(cc * C, C)]
        return wf.at[pl.ds(HF + UT + dd * uk, uk), pl.ds(cc * C, C)]

    def w_src(part, cc):
        if part == 0:
            return wq_ref.at[cc, pl.ds(d * ck, ck), :]
        if part == 1:
            return wu_ref.at[pl.ds(d * ck, ck), pl.ds(cc * UT, UT)]
        if part == 2:
            return wu_ref.at[pl.ds(d * ck, ck), pl.ds((n_col + cc) * UT, UT)]
        if part == 3:
            return wo_ref.at[pl.ds(cc * HF + d * hk, hk), :]
        if part == 4:
            return wd_ref.at[pl.ds(cc * UT + d * uk, uk), :]
        return wd_ref.at[pl.ds((n_col + cc) * UT + d * uk, uk), :]

    def w_copy(part, dest):
        return copy(
            w_src(part, dest), w_dst(part, d, c), ws.at[part, dest], wr.at[part, c], {"col": dest}
        )

    def w_from(part, source):
        return copy(
            w_src(part, source), w_dst(part, d, source), ws.at[part, source], wr.at[part, source],
            {"col": source},
        )

    def x_copy(part, source, j):
        got = w_dst(part, d, source)
        return copy(got, got, ds.at[part, source, j], dr.at[part, source, j],
                    {"dp": lax.rem(d + j, n_dp)})

    others = forder[: n_col - 1]

    def w_send(part):
        for dest in others:
            w_copy(part, dest).start()

    def w_pass(part):
        for source in others[::-1]:
            w_from(part, source).wait_recv()
            for j in range(1, n_dp):
                x_copy(part, source, j).start()

    def w_done(part):
        for source in others:
            for j in range(1, n_dp):
                x_copy(part, source, j).wait_recv()

    win, wfin = (0, 1, 2), (3, 4, 5)

    for t in range(chunks):
        send_own_z(0, t)
    for t in range(chunks):
        send_own_row(0, t)

    col_at = pl.ds(c * C, C)
    direct = [
        pltpu.make_async_copy(x_ref, xv.at[pl.ds(r * T, T), col_at], ls.at[0]),
        pltpu.make_async_copy(wq_ref.at[c], wv.at[col_at, pl.ds(0, qw)], ls.at[1]),
        pltpu.make_async_copy(wu_ref.at[:, pl.ds(c * UT, UT)], wv.at[col_at, pl.ds(qw, UT)],
                              ls.at[2]),
        pltpu.make_async_copy(wu_ref.at[:, pl.ds((n_col + c) * UT, UT)],
                              wv.at[col_at, pl.ds(qw + UT, UT)], ls.at[3]),
    ]
    loads = [
        pltpu.make_async_copy(g_ref, stage_g, ls.at[4]),
        pltpu.make_async_copy(wo_ref.at[pl.ds(c * HF, HF), :], stage_o, ls.at[5]),
        pltpu.make_async_copy(wd_ref.at[pl.ds(c * UT, UT), :], stage_d.at[0], ls.at[6]),
        pltpu.make_async_copy(wd_ref.at[pl.ds((n_col + c) * UT, UT), :], stage_d.at[1], ls.at[7]),
    ]
    stores = [
        pltpu.make_async_copy(stage_g, gf.at[pl.ds(r * T, T), col_at], lo.at[0]),
        pltpu.make_async_copy(stage_o, wf.at[pl.ds(0, HF), col_at], lo.at[1]),
        pltpu.make_async_copy(stage_d.at[0], wf.at[pl.ds(HF, UT), col_at], lo.at[2]),
        pltpu.make_async_copy(stage_d.at[1], wf.at[pl.ds(HF + UT, UT), col_at], lo.at[3]),
    ]
    for item in direct + loads:
        item.start()

    for n in range(1, n_col):
        for t in range(chunks):
            relay(0, n, t)
        w_send(win[n - 1])
    for t in range(chunks):
        send_own_z(1, t)
        send_own_row(1, t)
    for load, store in zip(loads, stores):
        load.wait()
        store.start()
    w_pass(win[0])

    def one_table(n, carry):
        rows = jnp.broadcast_to(pos_ref[pl.ds(n, 1), :], (2 * HEAD_DIM, SEQ_LEN))
        angle = jnp.transpose(rows) * freq_ref[...]
        lane = lax.broadcasted_iota(jnp.int32, angle.shape, 1)
        turns = jnp.floor(angle * (2.0 / math.pi) + 0.5)
        rest = angle - turns * 1.5703125
        rest = rest - turns * 4.837512969970703125e-4
        rest = rest - turns * 7.54978994889188e-8
        sq = rest * rest
        sine = rest + rest * sq * (
            -1.6666654611e-1 + sq * (8.3321608736e-3 - sq * 1.9515295891e-4)
        )
        cosine = 1.0 - 0.5 * sq + sq * sq * (
            4.166664568298827e-2 + sq * (-1.388731625493765e-3 + sq * 2.443315711809948e-5)
        )
        quarter = jnp.where(lane < HEAD_DIM, turns, turns - 1.0)
        quarter = quarter - 4.0 * jnp.floor(quarter * 0.25)
        odd = (quarter == 1.0) | (quarter == 3.0)
        value = jnp.where(odd, sine, cosine)
        value = jnp.where((quarter == 1.0) | (quarter == 2.0), -value, value)
        tab[pl.ds(pl.multiple_of(n * SEQ_LEN, SEQ_LEN), SEQ_LEN), :] = value
        return carry

    lax.fori_loop(0, seqs, one_table, 0)
    keep_cs = pltpu.make_async_copy(tab, cs_out, no.at[2])
    keep_cs.start()
    for n in range(n_col):
        for t in range(chunks):
            pass_row(0, n, t)
    w_pass(win[1])
    for item in direct:
        item.wait()
    for t in range(chunks):
        for cc in range(n_col):
            c_copy(0, t, cc, blk(0, r, cc, t), r, 0).wait_recv()
            c_copy(0, t, cc, blk(0, r, cc, t), r, 1).wait_recv()

    def act_sent(a):
        for t in range(chunks):
            for cc in range(n_col):
                @pl.when((cc <= c) & (c < n_col - 1))
                def _(t=t, cc=cc):
                    z_copy(a, t, cc, blk(a, r, cc, t), True).wait_send()

                @pl.when((cc >= c) & (c > 0))
                def _(t=t, cc=cc):
                    z_copy(a, t, cc, blk(a, r, cc, t), False).wait_send()

                y_copy(a, t, cc, blk(a, r, cc, t)).wait_send()
                c_copy(a, t, cc, blk(a, r, cc, t), r, 0).wait_send()
                c_copy(a, t, cc, blk(a, r, cc, t), r, 1).wait_send()

    act_sent(0)

    tile = 256
    tiles = rows_all // tile
    sub = 16

    def norm_tile(i, carry):
        base = pl.multiple_of(i * tile, tile)

        def norm_rows(k, inner):
            at = pl.ds(pl.multiple_of(base + k * sub, sub), sub)
            val = xv[at, :].astype(F32)
            mean = jnp.sum(val, axis=1, keepdims=True) / D
            var = jnp.sum(val * val, axis=1, keepdims=True) / D - mean * mean
            rstd = lax.rsqrt(var + NORM_EPS)
            mean_v[at, :] = mean
            rstd_v[at, :] = rstd
            xv[at, :] = ((val - mean) * rstd * vec_ref[5:6, :] + vec_ref[6:7, :]).astype(BF16)
            return inner

        lax.fori_loop(0, tile // sub, norm_rows, 0)
        at = pl.ds(base, tile)
        for k in range(D // tile):
            ntv[k * tile : (k + 1) * tile, at] = jnp.transpose(xv[at, k * tile : (k + 1) * tile])
        return carry

    lax.fori_loop(0, tiles // 2, norm_tile, 0)
    w_pass(win[2])
    for t in range(chunks):
        relay(1, 1, t)
    w_send(wfin[0])
    lax.fori_loop(tiles // 2, tiles, norm_tile, 0)
    keep_norm = pltpu.make_async_copy(ntv, nt, no.at[1])
    keep_norm.start()
    own_rows = pl.ds(pl.multiple_of(r * T, T), T)
    mean_ref[...] = mean_v[own_rows, :]
    rstd_ref[...] = rstd_v[own_rows, :]
    for part in win:
        w_done(part)
    keep_w = pltpu.make_async_copy(wv, wi, no.at[0])
    keep_w.start()

    q_lanes = pl.ds(pl.multiple_of((r * n_col + c) * HF, HF), HF)
    biases = [vec_ref[j : j + 1, q_lanes] for j in range(3)]
    biases += [
        vec_ref[pl.ds(7 + r, 1), pl.ds(pl.multiple_of((m * n_col + c) * UT, UT), UT)]
        for m in range(2)
    ]
    bias = jnp.concatenate(biases, axis=1)

    def one_tile(i, carry):
        at = pl.ds(pl.multiple_of(i * tile, tile), tile)
        mixed = jnp.dot(xv[at, :], wv[...], preferred_element_type=F32) + bias
        cos, sin = wide_tables(tab[at, :])
        for j in range(2):
            part = mixed[:, j * HF : (j + 1) * HF]
            qkv[at, j * HF : (j + 1) * HF] = turn(part, cos, sin, 1.0).astype(BF16)
        qkv[at, 2 * HF : 3 * HF] = mixed[:, 2 * HF : 3 * HF].astype(BF16)
        pre = mixed[:, qw:]
        up[at, :] = pre
        act = gelu_value(pre).astype(BF16)
        hid[at, HF:] = act
        ht[HF:, at] = jnp.transpose(act)

        s, t = 2 + lax.div(i, 2), lax.rem(i, 2)

        @pl.when(s < n_col)
        def _():
            relay(1, s, t)

        return carry

    lax.fori_loop(0, 2, one_tile, 0)
    w_send(wfin[1])
    lax.fori_loop(2, 4, one_tile, 0)
    w_send(wfin[2])
    lax.fori_loop(4, tiles, one_tile, 0)
    keep_up = pltpu.make_async_copy(up, up_out, no.at[3])
    keep_qkv = pltpu.make_async_copy(qkv, qkv_out, no.at[4])
    keep_up.start()
    keep_qkv.start()

    heads = HF // HEAD_DIM
    qt = SEQ_LEN // 2

    def one_seq(s, carry):
        base = pl.multiple_of(s * SEQ_LEN, SEQ_LEN)
        lane = lax.broadcasted_iota(jnp.int32, (qt, HF), 1)
        seg = seg_ref[pl.ds(s, 1), :]
        seg_col = jnp.transpose(jnp.broadcast_to(seg, (128, SEQ_LEN)))[:, 0:1]
        for qi in range(2):
            width = (qi + 1) * qt
            q_at = pl.ds(pl.multiple_of(base + qi * qt, qt), qt)
            k_at = pl.ds(base, width)
            allowed = (seg_col[qi * qt : (qi + 1) * qt, :] == seg[:, 0:width]) & (
                lax.broadcasted_iota(jnp.int32, (qt, width), 0) + qi * qt
                >= lax.broadcasted_iota(jnp.int32, (qt, width), 1)
            )
            keys, vals = qkv[k_at, HF : 2 * HF], qkv[k_at, 2 * HF : 3 * HF]
            queries = qkv[q_at, 0:HF]
            total = None
            for h in range(heads):
                mine = lax.div(lane, HEAD_DIM) == h
                scores = lax.dot_general(
                    jnp.where(mine, queries, jnp.zeros_like(queries)), keys,
                    (((1,), (1,)), ((), ())), preferred_element_type=F32,
                ) * (HEAD_DIM ** (-0.5))
                scores = jnp.where(allowed, scores, MASKED_SCORE)
                peak = jnp.max(scores, axis=1, keepdims=True)
                weight = jnp.exp(scores - peak)
                weight_sum = jnp.sum(weight, axis=1, keepdims=True)
                probs = (weight * (1.0 / weight_sum)).astype(BF16)
                out = jnp.dot(probs, vals, preferred_element_type=F32)
                total = out if h == 0 else jnp.where(mine, out, total)
            low = total.astype(BF16)
            hid[q_at, 0:HF] = low
            ht[0:HF, q_at] = jnp.transpose(low)

        @pl.when(s < n_col)
        def _():
            for t in range(chunks):
                pass_row(1, s, t)

        return carry

    lax.fori_loop(0, seqs, one_seq, 0)
    keep_hid = pltpu.make_async_copy(hid, hid_out, no.at[5])
    keep_ht = pltpu.make_async_copy(ht, ht_out, no.at[6])
    keep_hid.start()
    keep_ht.start()
    for part in wfin:
        w_pass(part)

    for t in range(chunks):
        for cc in range(n_col):
            c_copy(1, t, cc, blk(1, r, cc, t), r, 0).wait_recv()
            c_copy(1, t, cc, blk(1, r, cc, t), r, 1).wait_recv()
    for part in wfin:
        w_done(part)
    act_sent(1)
    for part in win + wfin:
        for peer in others:
            w_copy(part, peer).wait_send()
            for j in range(1, n_dp):
                x_copy(part, peer, j).wait_send()
    for store in stores:
        store.wait()
    for item in (keep_w, keep_norm, keep_cs, keep_up, keep_qkv, keep_hid, keep_ht):
        item.wait()


def forward_all(x, g, w_q, w_up, w_out, w_down, pos_row, seg_row, freq, vectors,
                n_dp, n_row, n_col):
    T, C = x.shape
    HF = w_q.shape[2] // 3
    UT = w_up.shape[1] // (2 * n_col)
    n_in, n_out = 3 * HF + 2 * UT, HF + 2 * UT
    rows, D = n_row * T, n_col * C
    dma = pltpu.SemaphoreType.DMA
    vm = pl.BlockSpec(memory_space=pltpu.VMEM)
    sds = jax.ShapeDtypeStruct
    return pl.pallas_call(
        functools.partial(forward_kernel, n_dp, n_row, n_col, (T, C, HF, UT)),
        name="forward_all",
        out_shape=(
            sds((rows, D), BF16),
            sds((D, n_in), BF16),
            sds((n_out, D), BF16),
            sds((D, rows), BF16),
            sds((rows, n_out), BF16),
            sds((n_out, rows), BF16),
            sds((rows, 3 * HF), BF16),
            sds((rows, 2 * UT), F32),
            sds((rows, 2 * HEAD_DIM), F32),
            sds((T, 1), F32),
            sds((T, 1), F32),
        ),
        in_specs=[ANY] * 6 + [vm] * 4,
        out_specs=(ANY,) * 9 + (vm,) * 2,
        scratch_shapes=[
            pltpu.VMEM((rows, D), BF16),
            pltpu.VMEM((D, rows), BF16),
            pltpu.VMEM((D, n_in), BF16),
            pltpu.VMEM((rows, n_out), BF16),
            pltpu.VMEM((n_out, rows), BF16),
            pltpu.VMEM((rows, 3 * HF), BF16),
            pltpu.VMEM((rows, 2 * UT), F32),
            pltpu.VMEM((rows, 2 * HEAD_DIM), F32),
            pltpu.VMEM((rows, 1), F32),
            pltpu.VMEM((rows, 1), F32),
            pltpu.VMEM((T, C), BF16),
            pltpu.VMEM((HF, C), BF16),
            pltpu.VMEM((2, UT, C), BF16),
            dma((2, 2, 2, n_col)),
            dma((2, 2, n_col)),
            dma((2, 2, n_col)),
            dma((2, 2, n_col)),
            dma((2, 2, 2, n_col)),
            dma((2, 2, 2, n_col)),
            dma((6, n_col)),
            dma((6, n_col)),
            dma((6, n_col, n_dp)),
            dma((6, n_col, n_dp)),
            dma((8,)),
            dma((4,)),
            dma((7,)),
        ],
        compiler_params=pltpu.CompilerParams(
            collective_id=0, has_side_effects=True, vmem_limit_bytes=60 * 1024 * 1024
        ),
    )(x, g, w_q, w_up, w_out, w_down, pos_row, seg_row, freq, vectors)


def wide_tables(packed):
    lane = lax.broadcasted_iota(jnp.int32, packed.shape, 1)
    turned = pltpu.roll(packed, HEAD_DIM, 1)
    first = lane < HEAD_DIM
    return jnp.where(first, packed, turned), jnp.where(first, turned, packed)


def turn(part, cos, sin, sign):
    lane = lax.rem(lax.broadcasted_iota(jnp.int32, part.shape, 1), HEAD_DIM)
    ahead = pltpu.roll(part, part.shape[1] - ROTARY // 2, 1)
    behind = pltpu.roll(part, ROTARY // 2, 1)
    return part * cos + jnp.where(lane < ROTARY // 2, -ahead, behind) * (sign * sin)


def backward_kernel(n_row, n_col, dims,
                    hid_ref, ht_ref, c_ref, wf_ref, wi_ref, nt_ref, qkv_ref, up_ref,
                    cs_ref, seg_ref,
                    res_ref, gn_ref, tiles_ref, part_ref,
                    hd, hts, big, wf, wi, qv, ups, ga,
                    abuf, obuf, asb, sbuf, bbuf, zsb, zin,
                    dwf, dwi, gf, gu, gk,
                    l_s, h_s, u_s, a_s, a_r, y_s, y_r, z_s, z_r, xf_s, xf_r, xu_s, xu_r, xk_s, xk_r,
                    t_s, t_r, free_row, free_col):
    T, C, HF, UT = dims
    rows_all, D = n_row * T, n_col * C
    qw, n_in, n_out = 3 * HF, 3 * HF + 2 * UT, HF + 2 * UT
    step_rows = 64
    d, r, c = lax.axis_index("dp"), lax.axis_index("row"), lax.axis_index("col")
    r1 = r + 1 - 2 * lax.rem(r, 2)
    r2 = lax.rem(r + 2, n_row)
    r12 = lax.rem(r1 + 2, n_row)
    forder = far_order(c, n_col)
    outs = (res_ref, gn_ref)

    barrier = pltpu.get_barrier_semaphore()
    peers = [{"row": r1}, {"row": r2}, {"dp": 1 - d}]
    peers += [{"col": lax.rem(c + k, n_col)} for k in range(1, n_col)]
    for peer in peers:
        pl.semaphore_signal(barrier, inc=1, device_id=peer, device_id_type=MESH)

    loads = [
        pltpu.make_async_copy(hid_ref, hd.at[:, pl.ds(2 * HF, n_out)], l_s.at[0]),
        pltpu.make_async_copy(wf_ref, wf, l_s.at[1]),
        pltpu.make_async_copy(c_ref, big, l_s.at[2]),
        pltpu.make_async_copy(qkv_ref, qv, l_s.at[3]),
        pltpu.make_async_copy(wi_ref, wi, l_s.at[4]),
    ]
    for item in loads:
        item.start()
    load_nt = pltpu.make_async_copy(nt_ref, big, l_s.at[5])

    def load_ht(m, slot):
        return pltpu.make_async_copy(ht_ref.at[pl.ds(pl.multiple_of(m * HF, HF), HF), :],
                                     hts.at[slot], h_s.at[slot])

    tile = 256

    def load_up(i, slot):
        return pltpu.make_async_copy(up_ref.at[pl.ds(pl.multiple_of(i * tile, tile), tile), :],
                                     ups.at[slot], u_s.at[slot])

    load_ht(0, 0).start()
    load_up(0, 0).start()
    pl.semaphore_wait(barrier, len(peers))

    def copy(src, dst, s, rcv, peer):
        return pltpu.make_async_remote_copy(
            src_ref=src, dst_ref=dst, send_sem=s, recv_sem=rcv, device_id=peer, device_id_type=MESH
        )

    def a_copy(v, h, f):
        return copy(asb.at[h, f], abuf.at[v, h, f], a_s.at[h, f], a_r.at[v, h, f], {"row": r1})

    def y_copy(f):
        return copy(sbuf.at[f], bbuf.at[f], y_s.at[f], y_r.at[f], {"row": r2})

    def z_copy(f, slot, step):
        return copy(zsb.at[f], zin.at[slot], z_s.at[f], z_r.at[slot], {"col": c + step})

    def looped(rows, fn):
        def one(k, carry):
            fn(pl.ds(pl.multiple_of(k * step_rows, step_rows), step_rows))
            return carry
        lax.fori_loop(0, rows // step_rows, one, 0)

    def first_sum(v, f):
        a_copy(v, 1, f).wait_recv()

        def add(rows):
            sbuf[f, rows, :] = (
                obuf[1, f, rows, :].astype(F32) + abuf[v, 1, f, rows, :].astype(F32)
            ).astype(BF16)

        looped(T, add)
        y_copy(f).start()

    def second_sum(v, i):
        f = forder[i]
        a_copy(v, 0, f).wait_recv()
        y_copy(f).wait_recv()

        def base(rows):
            return (
                obuf[0, f, rows, :].astype(F32)
                + abuf[v, 0, f, rows, :].astype(F32)
                + bbuf[f, rows, :].astype(F32)
            )

        if i < n_col - 1:
            right = f > c
            step = jnp.where(right, jnp.int32(1), jnp.int32(-1))
            landed = jnp.where(f == c + step, jnp.where(right, f, jnp.int32(n_col)), f)
            inner = jnp.where(right, c, n_col - 1 - c) > 0

            @pl.when(inner)
            def _():
                z_copy(f, f, 0).wait_recv()

                def add(rows):
                    zsb[f, rows, :] = (base(rows) + zin[f, rows, :].astype(F32)).astype(BF16)

                looped(T, add)

            @pl.when(jnp.logical_not(inner))
            def _():
                def add(rows):
                    zsb[f, rows, :] = base(rows).astype(BF16)

                looped(T, add)

            z_copy(f, landed, step).start()
        else:
            out = outs[v]

            @pl.when(c > 0)
            def _():
                z_copy(f, f, 0).wait_recv()

            @pl.when(c < n_col - 1)
            def _():
                z_copy(f, n_col, 0).wait_recv()

            def put(rows, value):
                out[rows, :] = value

            @pl.when(c == 0)
            def _():
                looped(T, lambda rows: put(rows, base(rows) + zin[n_col, rows, :].astype(F32)))

            @pl.when(c == n_col - 1)
            def _():
                looped(T, lambda rows: put(rows, base(rows) + zin[f, rows, :].astype(F32)))

            @pl.when((c > 0) & (c < n_col - 1))
            def _():
                looped(T, lambda rows: put(
                    rows,
                    base(rows) + zin[f, rows, :].astype(F32) + zin[n_col, rows, :].astype(F32)))

    tall = (HF, 2 * UT)
    row0 = (0, HF)
    lane_u = (qw, qw + UT)
    lw = 2 * HF

    def xf_copy(own, b):
        return copy(dwf.at[pl.ds(row0[own] + b * HF, HF), :], gf.at[pl.ds(b * HF, HF), :],
                    xf_s.at[own, b], xf_r.at[b], {"dp": 1 - d})

    def xu_copy(own, cc):
        return copy(dwi.at[pl.ds(cc * C, C), pl.ds(lane_u[own], UT)], gu.at[cc],
                    xu_s.at[own, cc], xu_r.at[cc], {"dp": 1 - d})

    def xk_copy(cc):
        return copy(dwi.at[pl.ds(cc * C, C), pl.ds(0, qw)], gk.at[cc], xk_s.at[cc], xk_r.at[cc],
                    {"dp": 1 - d})

    def parts_f(own, cc, source):
        half, odd = lax.div(source, 2), lax.rem(source, 2)
        at = cc * C
        if own == 0:
            return [
                (dwf.at[pl.ds(0, HF), pl.ds(at + j * lw, lw)],
                 tiles_ref.at[6 + j, pl.ds(source * HF, HF), :])
                for j in range(2)
            ]
        return [
            (dwf.at[pl.ds(HF + m * UT, UT), pl.ds(at + j * lw, lw)],
             tiles_ref.at[4 + 2 * (2 * m + half) + j, pl.ds(odd * UT, UT), :])
            for m in range(2) for j in range(2)
        ]

    def parts_u(own, cc, source):
        dst = tiles_ref.at[8 + source] if own == 0 else tiles_ref.at[source]
        return [(dwi.at[pl.ds(cc * C, C), pl.ds(lane_u[own], UT)], dst)]

    def parts_k(own, cc, source):
        half, odd = lax.div(source, 2), lax.rem(source, 2)
        return [
            (dwi.at[pl.ds(cc * C, C), pl.ds(j * HF, HF)],
             tiles_ref.at[2 * j + half, :, pl.ds(odd * HF, HF)])
            for j in range(3)
        ]

    kinds = {"f": (parts_f, 0), "u": (parts_u, 4), "k": (parts_k, 5)}

    def t_send(kind, own, cc):
        parts, first = kinds[kind]
        return [
            copy(src, dst, t_s.at[first + n, cc], t_r.at[first + n, c], {"col": cc})
            for n, (src, dst) in enumerate(parts(own, cc, c))
        ]

    def t_wait(kind, own, source):
        parts, first = kinds[kind]
        return [
            copy(src, dst, t_s.at[first + n, source], t_r.at[first + n, source], {"col": source})
            for n, (src, dst) in enumerate(parts(own, source, source))
        ]

    def t_local(kind, own):
        parts, first = kinds[kind]
        return [
            pltpu.make_async_copy(src, dst, t_s.at[first + n, c])
            for n, (src, dst) in enumerate(parts(own, c, c))
        ]

    def owned_kinds(own):
        return ("f", "u", "k") if own == 0 else ("f", "u")

    def spread(kind, own):
        for k in range(1, n_col):
            for item in t_send(kind, own, lax.rem(c + k, n_col)):
                item.start()
        for item in t_local(kind, own):
            item.start()

    def add_f():
        for own in range(2):
            @pl.when(d == own)
            def _(own=own):
                for b in range(tall[own] // HF):
                    xf_copy(own, b).wait_recv()

                def add(rows):
                    at = (pl.ds(pl.multiple_of(rows.start + row0[own], step_rows), step_rows),
                          slice(None))
                    dwf[at] = (dwf[at].astype(F32) + gf[rows, :].astype(F32)).astype(BF16)

                looped(tall[own], add)
                spread("f", own)

    def add_piece(kind, own, cc):
        lane, width, buf, waiter = (
            (lane_u[own], UT, gu, xu_copy(own, cc)) if kind == "u" else (0, qw, gk, xk_copy(cc))
        )
        waiter.wait_recv()

        def add(rows):
            at = (pl.ds(pl.multiple_of(rows.start + cc * C, step_rows), step_rows),
                  pl.ds(lane, width))
            dwi[at] = (dwi[at].astype(F32) + buf[cc, rows, :].astype(F32)).astype(BF16)

        looped(C, add)

    def add_u(i):
        for own in range(2):
            @pl.when(d == own)
            def _(own=own):
                cc = forder[i]
                add_piece("u", own, cc)
                for item in t_local("u", own) if i == n_col - 1 else t_send("u", own, cc):
                    item.start()

    def add_k(i):
        @pl.when(d == 0)
        def _():
            cc = forder[i]
            add_piece("k", 0, cc)
            for item in t_local("k", 0) if i == n_col - 1 else t_send("k", 0, cc):
                item.start()

    loads[0].wait()
    loads[1].wait()

    def p_unit(rr, f):
        at = pl.ds(pl.multiple_of(rr * T, T), T)
        lanes = pl.ds(pl.multiple_of(f * C, C), C)
        return jnp.dot(hd[at, 2 * HF :], wf[:, lanes], preferred_element_type=F32).astype(BF16)

    def p_step(i, carry):
        f = pick(i, forder)
        for h, rr in ((1, r12), (0, r1)):
            asb[h, f] = p_unit(rr, f)
            a_copy(0, h, f).start()
        for h, rr in ((1, r2), (0, r)):
            obuf[h, f] = p_unit(rr, f)

        @pl.when(i > 0)
        def _():
            first_sum(0, pick(i - 1, forder))

        return carry

    lax.fori_loop(0, n_col, p_step, 0)

    loads[2].wait()
    blocks = n_out // HF

    def f_step(m, carry):
        slot = lax.rem(m, 2)
        load_ht(m, slot).wait()

        @pl.when(m + 1 < blocks)
        def _():
            load_ht(m + 1, 1 - slot).start()

        at = pl.ds(pl.multiple_of(m * HF, HF), HF)
        dwf[at, :] = jnp.dot(hts[slot], big[...], preferred_element_type=F32).astype(BF16)

        @pl.when((m == 0) & (d == 1))
        def _():
            xf_copy(0, 0).start()

        @pl.when((m > 0) & (d == 0))
        def _():
            xf_copy(1, m - 1).start()

        return carry

    lax.fori_loop(0, blocks, f_step, 0)
    first_sum(0, forder[n_col - 1])
    second_sum(0, 0)

    part_ref[...] = jnp.zeros_like(part_ref)
    tiles = rows_all // tile

    def b_step(i, carry):
        slot = lax.rem(i, 2)
        load_up(i, slot).wait()

        @pl.when(i + 1 < tiles)
        def _():
            load_up(i + 1, 1 - slot).start()

        at = pl.ds(pl.multiple_of(i * tile, tile), tile)
        back = lax.dot_general(
            big[at, :], wf[...], (((1,), (1,)), ((), ())), preferred_element_type=F32
        )
        ga[at, :] = back[:, :HF].astype(BF16)
        grad = back[:, HF:] * gelu_slope(ups[slot])
        hd[at, qw:] = grad.astype(BF16)
        sums = jnp.sum(grad, axis=0, keepdims=True)
        for k in range(2 * UT // 128):
            part_ref[3 + k : 4 + k, :] += sums[:, k * 128 : (k + 1) * 128]
        return carry

    lax.fori_loop(0, tiles, b_step, 0)
    load_nt.start()
    second_sum(0, 1)
    load_nt.wait()

    def u_step(i, carry):
        cc = pick(i, forder)
        at = pl.ds(pl.multiple_of(cc * C, C), C)
        dwi[at, qw:] = jnp.dot(big[at, :], hd[:, qw:], preferred_element_type=F32).astype(BF16)
        for own in range(2):
            @pl.when(d == own)
            def _(own=own):
                xu_copy(1 - own, cc).start()

        return carry

    lax.fori_loop(0, n_col, u_step, 0)
    second_sum(0, 2)

    loads[3].wait()
    loads[4].wait()
    heads = HF // HEAD_DIM
    qt = SEQ_LEN // 2
    scale = HEAD_DIM ** (-0.5)
    per_row = T // SEQ_LEN
    first_dim = (((0,), (0,)), ((), ()))
    last_dim = (((1,), (1,)), ((), ()))

    def attend_seq(s):
        base = pl.multiple_of(s * SEQ_LEN, SEQ_LEN)
        lane = lax.broadcasted_iota(jnp.int32, (qt, HF), 1)
        seg = seg_ref[pl.ds(s, 1), :]
        seg_col = jnp.transpose(jnp.broadcast_to(seg, (128, SEQ_LEN)))[:, 0:1]
        grad_q, grad_k, grad_v = [], None, None
        for qi in range(2):
            width = (qi + 1) * qt
            q_at = pl.ds(base + qi * qt, qt)
            k_at = pl.ds(base, width)
            allowed = (seg_col[qi * qt : (qi + 1) * qt, :] == seg[:, 0:width]) & (
                lax.broadcasted_iota(jnp.int32, (qt, width), 0) + qi * qt
                >= lax.broadcasted_iota(jnp.int32, (qt, width), 1)
            )
            queries, g_att = qv[q_at, 0:HF], ga[q_at, :]
            keys, vals = qv[k_at, HF : 2 * HF], qv[k_at, 2 * HF : 3 * HF]
            both = g_att.astype(F32) * hd[q_at, 2 * HF : 3 * HF].astype(F32)
            gq, gks, gvs = None, None, None
            for h in range(heads):
                mine = lax.div(lane, HEAD_DIM) == h
                q_h = jnp.where(mine, queries, jnp.zeros_like(queries))
                g_h = jnp.where(mine, g_att, jnp.zeros_like(g_att))
                scores = lax.dot_general(q_h, keys, last_dim, preferred_element_type=F32) * scale
                scores = jnp.where(allowed, scores, MASKED_SCORE)
                peak = jnp.max(scores, axis=1, keepdims=True)
                weight = jnp.exp(scores - peak)
                probs = weight * (1.0 / jnp.sum(weight, axis=1, keepdims=True))
                delta = jnp.sum(jnp.where(mine, both, 0.0), axis=1, keepdims=True)
                g_prob = lax.dot_general(g_h, vals, last_dim, preferred_element_type=F32)
                g_score = (probs * (g_prob - delta) * scale).astype(BF16)
                gq_h = jnp.dot(g_score, keys, preferred_element_type=F32)
                gk_h = lax.dot_general(g_score, q_h, first_dim, preferred_element_type=F32)
                gv_h = lax.dot_general(probs.astype(BF16), g_h, first_dim,
                                       preferred_element_type=F32)
                gq = gq_h if h == 0 else jnp.where(mine, gq_h, gq)
                gks = gk_h if h == 0 else gks + gk_h
                gvs = gv_h if h == 0 else gvs + gv_h
            grad_q.append(gq)
            if qi == 0:
                grad_k, grad_v = gks, gvs
            else:
                grad_k = jnp.concatenate([grad_k + gks[:qt], gks[qt:]], axis=0)
                grad_v = jnp.concatenate([grad_v + gvs[:qt], gvs[qt:]], axis=0)
        s_at = pl.ds(base, SEQ_LEN)
        cos, sin = wide_tables(cs_ref[s_at, :])
        grads = (
            turn(jnp.concatenate(grad_q, axis=0), cos, sin, -1.0),
            turn(grad_k, cos, sin, -1.0),
            grad_v,
        )
        for j, grad in enumerate(grads):
            part_ref[j : j + 1, :] += jnp.sum(grad, axis=0, keepdims=True)
            hd[s_at, j * HF : (j + 1) * HF] = grad.astype(BF16)

    def q_unit(rr, f):
        at = pl.ds(pl.multiple_of(rr * T, T), T)
        feats = pl.ds(pl.multiple_of(f * C, C), C)
        return lax.dot_general(
            hd[at, :], wi[feats, :], last_dim, preferred_element_type=F32
        ).astype(BF16)

    def credit(first):
        if first:
            pl.semaphore_signal(free_row, inc=1, device_id={"row": r2}, device_id_type=MESH)
        for n, step in enumerate((1, -1)):
            @pl.when((c + step >= 0) & (c + step < n_col))
            def _(n=n, step=step):
                if first:
                    pl.semaphore_signal(free_col.at[n], inc=1, device_id={"col": c + step},
                                        device_id_type=MESH)
                else:
                    pl.semaphore_wait(free_col.at[1 - n], 1)
        if not first:
            pl.semaphore_wait(free_row, 1)

    def s_step(m, carry):
        rr = pick(m, [r12, r2, r1, r])

        def seq(s, inner):
            attend_seq(rr * per_row + s)
            return inner

        lax.fori_loop(0, per_row, seq, 0)

        @pl.when(m == 1)
        def _():
            second_sum(0, n_col - 1)
            for f in range(n_col):
                y_copy(f).wait_send()
            for i in range(n_col - 1):
                z_copy(forder[i], forder[i], 0).wait_send()
            credit(True)
            credit(False)

        def units(i, inner):
            f = pick(i, forder)
            value = q_unit(rr, f)

            def to_peer(h):
                a_copy(0, h, f).wait_send()
                asb[h, f] = value
                a_copy(1, h, f).start()

            @pl.when(m == 0)
            def _():
                to_peer(1)

            @pl.when(m == 2)
            def _():
                to_peer(0)

            @pl.when(m == 1)
            def _():
                obuf[1, f] = value
                first_sum(1, f)

            @pl.when(m == 3)
            def _():
                obuf[0, f] = value

            return inner

        lax.fori_loop(0, n_col, units, 0)
        return carry

    lax.fori_loop(0, n_row, s_step, 0)
    add_f()

    def k_step(i, carry):
        cc = pick(i, forder)
        at = pl.ds(pl.multiple_of(cc * C, C), C)
        dwi[at, 0:qw] = jnp.dot(big[at, :], hd[:, 0:qw], preferred_element_type=F32).astype(BF16)

        @pl.when(d == 1)
        def _():
            xk_copy(cc).start()

        return carry

    lax.fori_loop(0, n_col, k_step, 0)
    for i in range(n_col):
        second_sum(1, i) if i < n_col - 1 else None
        add_u(i)
    for i in range(n_col):
        add_k(i)
    second_sum(1, n_col - 1)

    for own in range(2):
        @pl.when(d == own)
        def _(own=own):
            for kind in owned_kinds(own):
                for k in range(1, n_col):
                    for item in t_wait(kind, own, lax.rem(c + k, n_col)):
                        item.wait_recv()
                for k in range(1, n_col):
                    for item in t_send(kind, own, lax.rem(c + k, n_col)):
                        item.wait_send()
                for item in t_local(kind, own):
                    item.wait()
            for b in range(tall[1 - own] // HF):
                xf_copy(1 - own, b).wait_send()
            for cc in range(n_col):
                xu_copy(1 - own, cc).wait_send()
                if own == 1:
                    xk_copy(cc).wait_send()
    for f in range(n_col):
        a_copy(1, 0, f).wait_send()
        a_copy(1, 1, f).wait_send()
        y_copy(f).wait_send()
    for i in range(n_col - 1):
        z_copy(forder[i], forder[i], 0).wait_send()


def backward_all(hid, ht, cot, w_fin, w_in, nt, qkv, up, packed, seg_row, T, C, HF, UT, n_row, n_col):
    dma = pltpu.SemaphoreType.DMA
    vm = pl.BlockSpec(memory_space=pltpu.VMEM)
    rows, D = n_row * T, n_col * C
    n_in, n_out = 3 * HF + 2 * UT, HF + 2 * UT
    unit = (T, C)
    V = pltpu.VMEM
    return pl.pallas_call(
        functools.partial(backward_kernel, n_row, n_col, (T, C, HF, UT)),
        name="backward_all",
        out_shape=(
            jax.ShapeDtypeStruct(unit, F32),
            jax.ShapeDtypeStruct(unit, F32),
            jax.ShapeDtypeStruct((12, C, UT), BF16),
            jax.ShapeDtypeStruct((8, 128), F32),
        ),
        in_specs=[ANY] * 8 + [vm] * 2,
        out_specs=(vm, vm, ANY, vm),
        scratch_shapes=[
            V((rows, n_in), BF16),
            V((2, HF, rows), BF16),
            V((rows, D), BF16),
            V((n_out, D), BF16),
            V((D, n_in), BF16),
            V((rows, 3 * HF), BF16),
            V((2, 256, 2 * UT), F32),
            V((rows, HF), BF16),
            V((2, 2, n_col) + unit, BF16),
            V((2, n_col) + unit, BF16),
            V((2, n_col) + unit, BF16),
            V((n_col,) + unit, BF16),
            V((n_col,) + unit, BF16),
            V((n_col,) + unit, BF16),
            V((n_col + 1,) + unit, BF16),
            V((n_out, D), BF16),
            V((D, n_in), BF16),
            V((2 * UT, D), BF16),
            V((n_col, C, UT), BF16),
            V((n_col, C, 3 * HF), BF16),
            dma((6,)),
            dma((2,)),
            dma((2,)),
            dma((2, n_col)),
            dma((2, 2, n_col)),
            dma((n_col,)),
            dma((n_col,)),
            dma((n_col,)),
            dma((n_col + 1,)),
            dma((2, 2 * UT // HF)),
            dma((2 * UT // HF,)),
            dma((2, n_col)),
            dma((n_col,)),
            dma((n_col,)),
            dma((n_col,)),
            dma((8, n_col)),
            dma((8, n_col)),
            pltpu.SemaphoreType.REGULAR,
            pltpu.SemaphoreType.REGULAR((2,)),
        ],
        compiler_params=pltpu.CompilerParams(
            collective_id=1, has_side_effects=True, vmem_limit_bytes=67043328
        ),
    )(hid, ht, cot, w_fin, w_in, nt, qkv, up, packed, seg_row)


def finish_kernel(n_dp, n_row, n_col, width, gn_ref, x_ref, g_ref, mean_ref, rstd_ref, gain_ref, part_ref,
                  gx_ref, va_ref, vb_ref,
                  st, da, db, ra, rb,
                  st_s, st_r, d_s, d_r, r_s, r_r, c_s, c_r):
    d, r, c = lax.axis_index("dp"), lax.axis_index("row"), lax.axis_index("col")
    T, C = gn_ref.shape

    barrier = pltpu.get_barrier_semaphore()
    dps = [lax.rem(d + k, n_dp) for k in range(1, n_dp)]
    rows = [lax.rem(r + k, n_row) for k in range(1, n_row)]
    cols = [lax.rem(c + k, n_col) for k in range(1, n_col)]
    peers = [{"dp": k} for k in dps] + [{"row": k} for k in rows] + [{"col": k} for k in cols]
    for peer in peers:
        pl.semaphore_signal(barrier, inc=1, device_id=peer, device_id_type=MESH)
    pl.semaphore_wait(barrier, len(peers))

    def copy(src, dst, s, rcv, peer):
        return pltpu.make_async_remote_copy(
            src_ref=src, dst_ref=dst, send_sem=s, recv_sem=rcv, device_id=peer, device_id_type=MESH
        )

    gain = gain_ref[...]

    def fold(value):
        total = value[:, 0:128]
        for k in range(1, C // 128):
            total = total + value[:, k * 128 : (k + 1) * 128]
        return jnp.sum(jnp.transpose(total), axis=0, keepdims=True)

    gn = gn_ref[...]
    x_hat = (x_ref[...].astype(F32) - mean_ref[...]) * rstd_ref[...]
    gh = gn * gain
    st[c, 0:1, :] = fold(gh)
    st[c, 1:2, :] = fold(gh * x_hat)

    def st_copy(k):
        return copy(st.at[c], st.at[c], st_s.at[k], st_r.at[c], {"col": k})

    def st_wait(k):
        return copy(st.at[k], st.at[k], st_s.at[k], st_r.at[k], {"col": k})

    for k in cols:
        st_copy(k).start()

    da[d] = part_ref[...]
    db[d, 0:1, :] = jnp.sum(gn * x_hat, axis=0, keepdims=True)
    db[d, 1:2, :] = jnp.sum(gn, axis=0, keepdims=True)
    db[d, 2:3, :] = jnp.sum(g_ref[...].astype(F32), axis=0, keepdims=True)

    def pair(a_src, b_src, a_dst, b_dst, s, rcv, peer):
        return [copy(a_src, a_dst, s.at[0], rcv.at[0], peer),
                copy(b_src, b_dst, s.at[1], rcv.at[1], peer)]

    def d_pair(slot, peer):
        return pair(da.at[slot], db.at[slot], da.at[slot], db.at[slot],
                    d_s.at[peer], d_r.at[slot], {"dp": peer})

    def r_pair(slot, peer):
        return pair(ra.at[slot], rb.at[slot], ra.at[slot], rb.at[slot],
                    r_s.at[peer], r_r.at[slot], {"row": peer})

    def c_pair(slot, peer):
        return pair(va_ref.at[slot], vb_ref.at[slot], va_ref.at[slot], vb_ref.at[slot],
                    c_s.at[peer], c_r.at[slot], {"col": peer})

    for k in dps:
        for item in d_pair(d, k):
            item.start()
    for k in dps:
        for item in d_pair(k, k):
            item.wait_recv()
    a_sum, b_sum = da[0], db[0]
    for k in range(1, n_dp):
        a_sum = a_sum + da[k]
        b_sum = b_sum + db[k]
    ra[r] = a_sum
    rb[r] = b_sum
    for k in rows:
        for item in r_pair(r, k):
            item.start()

    for k in cols:
        st_wait(k).wait_recv()
    stats = st[0]
    for k in range(1, n_col):
        stats = stats + st[k]
    stats = stats / width
    m1 = jnp.transpose(jnp.broadcast_to(stats[0:1, :], (128, T)))[:, 0:1]
    m2 = jnp.transpose(jnp.broadcast_to(stats[1:2, :], (128, T)))[:, 0:1]
    gx_ref[...] = g_ref[...].astype(F32) + rstd_ref[...] * (gh - m1 - x_hat * m2)

    for k in rows:
        for item in r_pair(k, k):
            item.wait_recv()
    b_sum = rb[0]
    for k in range(1, n_row):
        b_sum = b_sum + rb[k]
    for k in range(n_row):
        va_ref[c, k] = ra[k]
    vb_ref[c] = b_sum
    for k in cols:
        for item in c_pair(c, k):
            item.start()
    for k in cols:
        for item in c_pair(k, k):
            item.wait_recv()
    for k in cols:
        st_copy(k).wait_send()
        for item in c_pair(c, k):
            item.wait_send()
    for k in dps:
        for item in d_pair(d, k):
            item.wait_send()
    for k in rows:
        for item in r_pair(r, k):
            item.wait_send()


def finish_all(gn, x, g, mean, rstd, gain, part, width, n_dp, n_row, n_col):
    T, C = gn.shape
    dma = pltpu.SemaphoreType.DMA
    vm = pl.BlockSpec(memory_space=pltpu.VMEM)
    return pl.pallas_call(
        functools.partial(finish_kernel, n_dp, n_row, n_col, width),
        name="finish_all",
        out_shape=(
            jax.ShapeDtypeStruct((T, C), F32),
            jax.ShapeDtypeStruct((n_col, n_row, 8, 128), F32),
            jax.ShapeDtypeStruct((n_col, 8, C), F32),
        ),
        in_specs=[vm] * 7,
        out_specs=(vm,) * 3,
        scratch_shapes=[
            pltpu.VMEM((n_col, 8, T), F32),
            pltpu.VMEM((n_dp, 8, 128), F32),
            pltpu.VMEM((n_dp, 8, C), F32),
            pltpu.VMEM((n_row, 8, 128), F32),
            pltpu.VMEM((n_row, 8, C), F32),
            dma((n_col,)),
            dma((n_col,)),
            dma((n_dp, 2)),
            dma((n_dp, 2)),
            dma((n_row, 2)),
            dma((n_row, 2)),
            dma((n_col, 2)),
            dma((n_col, 2)),
        ],
        compiler_params=pltpu.CompilerParams(
            collective_id=2, has_side_effects=True, vmem_limit_bytes=48 * 1024 * 1024
        ),
    )(gn, x, g, mean, rstd, gain, part)


def muon_kernel(owned, per_step, HF, UT, rate, grad_ref, mom_ref, wq_ref, wo_ref, wu_ref, wd_ref,
                og_ref, new_ref, nm_ref, wbuf, sem):
    first = lax.axis_index("dp") * owned
    step = pl.program_id(0)
    steps = owned // per_step
    n_qkv, n_out, n_up = 6, 2, 8

    def fetch(tile, slot, n, start):
        dst = wbuf.at[slot, n]

        def go(src, target, s):
            item = pltpu.make_async_copy(src, target, s)
            if start:
                item.start()
            else:
                item.wait()

        @pl.when(tile < n_qkv)
        def _():
            j, half = lax.div(tile, 2), lax.rem(tile, 2)
            for m in range(UT // HF):
                go(wq_ref.at[half * (UT // HF) + m, :, pl.ds(j * HF, HF)],
                   wbuf.at[slot, n, :, pl.ds(m * HF, HF)], sem.at[slot, n, m])

        @pl.when((tile >= n_qkv) & (tile < n_qkv + n_out))
        def _():
            go(wo_ref.at[:, pl.ds((tile - n_qkv) * UT, UT)], dst, sem.at[slot, n, 0])

        @pl.when((tile >= n_qkv + n_out) & (tile < n_qkv + n_out + n_up))
        def _():
            go(wu_ref.at[:, pl.ds((tile - n_qkv - n_out) * UT, UT)], dst, sem.at[slot, n, 0])

        @pl.when(tile >= n_qkv + n_out + n_up)
        def _():
            left = tile - (n_qkv + n_out + n_up)
            rows = dst.shape[0]
            go(wd_ref.at[pl.ds(lax.div(left, 2) * rows, rows), pl.ds(lax.rem(left, 2) * UT, UT)],
               dst, sem.at[slot, n, 0])

    def fetch_all(at, start):
        for n in range(per_step):
            fetch(first + at * per_step + n, lax.rem(at, 2), n, start)

    @pl.when(step == 0)
    def _():
        fetch_all(step, True)

    @pl.when(step + 1 < steps)
    def _():
        fetch_all(step + 1, True)

    iters = []
    for n in range(per_step):
        grad = grad_ref[n].astype(F32)
        og_ref[n] = grad
        moment = MOMENTUM_RATE * mom_ref[n] + grad
        nm_ref[n] = moment
        scale = lax.rsqrt(jnp.sum(moment * moment, keepdims=True) + STAT_EPS)
        iters.append((moment * scale).astype(BF16))
    contract = (((0,), (0,)), ((), ()))
    for _ in range(5):
        grams = [
            lax.dot_general(x, x, contract, preferred_element_type=F32).astype(BF16) for x in iters
        ]
        squares = [jnp.dot(g, g, preferred_element_type=F32) for g in grams]
        polys = [
            (NEWTON_B * g.astype(F32) + NEWTON_C * s).astype(BF16) for g, s in zip(grams, squares)
        ]
        iters = [
            (NEWTON_A * x.astype(F32) + jnp.dot(x, p, preferred_element_type=F32)).astype(BF16)
            for x, p in zip(iters, polys)
        ]
    fetch_all(step, False)
    for n in range(per_step):
        new_ref[n] = wbuf[lax.rem(step, 2), n].astype(F32) - rate * iters[n].astype(F32)


def muon_all(grads, moment, w_q, w_out, w_up, w_down, HF, UT):
    owned, rows, cols = moment.shape
    per_step = 3
    rate = MUON_RATE * math.sqrt(max(1.0, rows / cols))
    block = pl.BlockSpec((per_step, rows, cols), lambda i: (i, 0, 0))
    out = jax.ShapeDtypeStruct(moment.shape, F32)
    return pl.pallas_call(
        functools.partial(muon_kernel, owned, per_step, HF, UT, rate),
        name="muon_all",
        grid=(owned // per_step,),
        out_shape=(out, out, out),
        in_specs=[block, block, ANY, ANY, ANY, ANY],
        out_specs=(block, block, block),
        scratch_shapes=[
            pltpu.VMEM((2, per_step, rows, cols), BF16),
            pltpu.SemaphoreType.DMA((2, per_step, 2)),
        ],
        compiler_params=pltpu.CompilerParams(vmem_limit_bytes=56 * 1024 * 1024),
    )(grads, moment, w_q, w_out, w_up, w_down)


def reduce_plain(p, q, dwi, dwf, C, HF, UT, n_col, row_width):
    def block(part):
        part = lax.psum_scatter(part, "row", scatter_dimension=0, tiled=True)
        return lax.psum_scatter(part, "col", scatter_dimension=1, tiled=True).astype(F32)

    wi4 = lax.all_to_all(dwi.reshape(n_col, C, -1), "col", 0, 0)
    wf4 = lax.all_to_all(dwf.reshape(-1, n_col, C).transpose(1, 0, 2), "col", 0, 0)
    grad_qkv = (
        wi4[:, :, : 3 * HF].reshape(n_col, C, 3, HF).transpose(1, 2, 0, 3).reshape(C, 3, row_width)
    )
    grad_up_w = wi4[:, :, 3 * HF :].reshape(n_col, C, 2, UT).transpose(1, 2, 0, 3).reshape(C, -1)
    grad_w_out = wf4[:, :HF].reshape(-1, C)
    grad_w_down = wf4[:, HF:].reshape(n_col, 2, UT, C).transpose(1, 0, 2, 3).reshape(-1, C)
    grad_tiles = tile_blocks(grad_qkv, grad_w_out, grad_up_w, grad_w_down)
    owned = lax.psum_scatter(grad_tiles, "dp", scatter_dimension=0, tiled=True)
    return block(p), block(q), owned


def backward_plain(hidden, hidden_t, cot, w_fin, w_in, norm_t, qkv, up_pre, positions, segments, HF):
    cosine, sine_tab = rotary_tables(positions)
    rows = cot.shape[0]
    seqs, heads = rows // SEQ_LEN, HF // HEAD_DIM

    def by_head(tensor_in):
        return tensor_in.reshape(seqs, SEQ_LEN, heads, HEAD_DIM)

    partial_out = jnp.dot(hidden, w_fin, preferred_element_type=F32).astype(BF16)
    grad_w_fin = jnp.dot(hidden_t, cot, preferred_element_type=F32).astype(BF16)
    back = jnp.einsum("tj,ij->ti", cot, w_fin, preferred_element_type=F32)
    grad_up = back[:, HF:] * gelu_slope(up_pre)
    grads = jax.vmap(attend_backward, in_axes=(0, 0, 0, 0, 0, 0, None))(
        by_head(qkv[:, :HF]),
        by_head(qkv[:, HF : 2 * HF]),
        by_head(qkv[:, 2 * HF :]),
        by_head(hidden[:, :HF]),
        by_head(back[:, :HF].astype(BF16)),
        segments.reshape(seqs, SEQ_LEN),
        HEAD_DIM ** (-0.5),
    )
    g_q, g_k, g_v = [item.reshape(rows, heads, HEAD_DIM) for item in grads]
    g_q = rotate(g_q, cosine, sine_tab, -1.0)
    g_k = rotate(g_k, cosine, sine_tab, -1.0)
    grad_mixed = jnp.concatenate(
        [item.reshape(rows, HF) for item in (g_q, g_k, g_v)] + [grad_up], axis=1
    )
    low = grad_mixed.astype(BF16)
    grad_w_in = jnp.dot(norm_t, low, preferred_element_type=F32).astype(BF16)
    partial_norm = jnp.einsum("tj,ij->ti", low, w_in, preferred_element_type=F32).astype(BF16)
    part = jnp.pad(jnp.sum(grad_mixed, axis=0).reshape(-1, 128), ((0, 1), (0, 0)))
    return (partial_out, partial_norm, grad_w_in, grad_w_fin), part


def body(
    inputs,
    cotangent,
    segments,
    positions,
    w_qkv,
    w_out,
    w_up,
    w_down,
    vectors,
    tile_moment,
    vector_moment,
):
    col_index = lax.axis_index("col")
    n_dp, n_row, n_col = lax.axis_size("dp"), lax.axis_size("row"), lax.axis_size("col")
    T, C = inputs.shape
    D = vectors.shape[1]
    row_width = w_qkv.shape[2]
    HF = row_width // n_col
    UT = w_up.shape[1] // (2 * n_col)
    col_start = col_index * C
    norm_gain = lax.dynamic_slice_in_dim(vectors[5], col_start, C)
    out_bias = lax.dynamic_slice_in_dim(vectors[3] + vectors[4], col_start, C)
    w_q = (
        w_qkv.reshape(C, 3, n_col, HF).transpose(2, 0, 1, 3).reshape(n_col, C, 3 * HF)
    )
    rows_all = positions.shape[0]
    seq_count = rows_all // SEQ_LEN
    half = jnp.exp(
        jnp.arange(ROTARY // 2, dtype=F32) * (-2.0 * math.log(10000.0) / ROTARY)
    )
    freq = jnp.tile(jnp.concatenate([half, half, jnp.zeros((HEAD_DIM - ROTARY,), F32)]), 2)
    seg_row = segments.reshape(seq_count, SEQ_LEN)
    pos_row = positions.reshape(seq_count, SEQ_LEN).astype(F32)
    cot_rows, w_in, w_fin, norm_t, hidden, hidden_t, qkv_low, up_pre, packed, mean_own, rstd_own = (
        forward_all(
            inputs, cotangent, w_q, w_up, w_out, w_down, pos_row, seg_row, freq[None], vectors,
            n_dp, n_row, n_col,
        )
    )
    if n_dp == 2:
        branch, grad_norm, owned_low, part = backward_all(
            hidden, hidden_t, cot_rows, w_fin, w_in, norm_t, qkv_low, up_pre, packed, seg_row,
            T, C, HF, UT, n_row, n_col,
        )
    else:
        partials, part = backward_plain(
            hidden, hidden_t, cot_rows, w_fin, w_in, norm_t, qkv_low, up_pre, positions, segments, HF
        )
        branch, grad_norm, owned_low = reduce_plain(*partials, C, HF, UT, n_col, row_width)
    x_val = inputs.astype(F32)
    result = x_val + branch + out_bias

    grad_input, vec_a, vec_b = finish_all(
        grad_norm,
        inputs,
        cotangent,
        mean_own,
        rstd_own,
        norm_gain[None],
        part,
        D,
        n_dp,
        n_row,
        n_col,
    )
    vec_a = vec_a.transpose(2, 1, 0, 3)
    qkv_rows = vec_a[:3].reshape(3, D)
    up_rows = vec_a[3:7].reshape(2, UT // 128, n_row, n_col, 128).transpose(2, 0, 3, 1, 4)
    norm_rows = vec_b.transpose(1, 0, 2).reshape(8, D)
    vec_grad = jnp.concatenate(
        [qkv_rows, norm_rows[2:3], norm_rows[2:3], norm_rows[:2], up_rows.reshape(-1, D)], axis=0
    )
    scaled = vec_grad * lax.rsqrt(jnp.mean(vec_grad * vec_grad, axis=1, keepdims=True) + STAT_EPS)
    vec_moment_new = MOMENTUM_RATE * vector_moment + scaled
    vectors_new = vectors - VECTOR_RATE * vec_moment_new

    owned_grads, tiles_new, moment_new = muon_all(
        owned_low, tile_moment[0, 0], w_q, w_out, w_up, w_down, HF, UT
    )
    return (
        result,
        grad_input,
        owned_grads[None, None],
        tiles_new[None, None],
        moment_new[None, None],
        vec_grad,
        vectors_new,
        vec_moment_new,
    )


def solution(mesh):
    placed = (
        P(("dp", "row"), "col"),
        P(("dp", "row"), "col"),
        P("dp"),
        P("dp"),
        P("col", None, "row"),
        P("row", "col"),
        P("col", "row"),
        P("row", "col"),
        P(),
        P("row", "col", "dp", None, None),
        P(),
    )
    return jax.shard_map(
        body,
        mesh=mesh,
        in_specs=placed,
        out_specs=(
            P(("dp", "row"), "col"),
            P(("dp", "row"), "col"),
            P("row", "col", "dp", None, None),
            P("row", "col", "dp", None, None),
            P("row", "col", "dp", None, None),
            P(),
            P(),
            P(),
        ),
        check_vma=False,
    )
```

```python
import functools
import math

import jax
import jax.numpy as jnp
from jax import lax
from jax.experimental import pallas as pl
from jax.experimental.pallas import tpu as pltpu
from jax.sharding import PartitionSpec as P

HEAD_DIM = 64
ROTARY = 32
SEQ_LEN = 512

MOMENTUM_RATE = 0.95
MUON_RATE = 0.05
VECTOR_RATE = 0.12
NEWTON_A = 3.4445
NEWTON_B = -4.775
NEWTON_C = 2.0315
GELU_SCALE = 0.7978845608028654
GELU_CUBIC = 0.044715
NORM_EPS = 1e-05
STAT_EPS = 1e-06
MASKED_SCORE = -1e30

MESH = pl.DeviceIdType.MESH
ANY = pl.BlockSpec(memory_space=pl.ANY)
F32 = jnp.float32
BF16 = jnp.bfloat16


def to_low(tensor_in):
    return lax.optimization_barrier(tensor_in.astype(BF16))


def gelu_value(pre_act):
    inner_arg = GELU_SCALE * (pre_act + GELU_CUBIC * pre_act * pre_act * pre_act)
    return 0.5 * pre_act * (1.0 + jnp.tanh(inner_arg))


def gelu_slope(pre_act):
    tanh_val = jnp.tanh(GELU_SCALE * (pre_act + GELU_CUBIC * pre_act * pre_act * pre_act))
    return 0.5 * (1.0 + tanh_val) + 0.5 * pre_act * (1.0 - tanh_val * tanh_val) * GELU_SCALE * (
        1.0 + 3.0 * GELU_CUBIC * pre_act * pre_act
    )


def rotary_tables(positions):
    half_dims = ROTARY // 2
    frequency = jnp.exp(jnp.arange(half_dims, dtype=F32) * (-2.0 * math.log(10000.0) / ROTARY))
    angles = positions.astype(F32)[:, None] * frequency[None, :]
    return (jnp.cos(angles), jnp.sin(angles))


def rotate(tensor_in, cosine, sine_tab, direction_sign):
    half_dims = ROTARY // 2
    first_half = tensor_in[..., :half_dims]
    second_half = tensor_in[..., half_dims:ROTARY]
    cos_wide = cosine[:, None, :]
    sin_wide = sine_tab[:, None, :] * direction_sign
    return jnp.concatenate(
        [
            first_half * cos_wide - second_half * sin_wide,
            second_half * cos_wide + first_half * sin_wide,
            tensor_in[..., ROTARY:],
        ],
        axis=-1,
    )


def causal_allowed(segment):
    token_order = jnp.arange(segment.shape[0])
    return (segment[:, None] == segment[None, :]) & (token_order[:, None] >= token_order[None, :])


def masked_scores(queries, key_vecs, segment, score_scale):
    scores = (
        jnp.einsum("lhe,mhe->hlm", queries, key_vecs, preferred_element_type=F32) * score_scale
    )
    return jnp.where(causal_allowed(segment)[None], scores, MASKED_SCORE)


def attend_backward(queries, key_vecs, values, output_low, grad_low, segment, score_scale):
    scores = masked_scores(queries, key_vecs, segment, score_scale)
    weight = jnp.exp(scores - jnp.max(scores, axis=-1, keepdims=True))
    probs = weight * (1.0 / jnp.sum(weight, axis=-1, keepdims=True))
    grad_values = jnp.einsum("hlm,lhe->mhe", to_low(probs), grad_low, preferred_element_type=F32)
    grad_probs = jnp.einsum("lhe,mhe->hlm", grad_low, values, preferred_element_type=F32)
    row_delta = jnp.sum(grad_low.astype(F32) * output_low.astype(F32), axis=-1)
    grad_scores = to_low(probs * (grad_probs - row_delta.T[:, :, None]) * score_scale)
    grad_queries = jnp.einsum("hlm,mhe->lhe", grad_scores, key_vecs, preferred_element_type=F32)
    grad_keys = jnp.einsum("hlm,lhe->mhe", grad_scores, queries, preferred_element_type=F32)
    return (grad_queries, grad_keys, grad_values)


def tile_blocks(qkv_block, out_block, up_block, down_block):
    tile_rows = qkv_block.shape[0]
    tile_cols = qkv_block.shape[2] // 2

    def split_cols(block_in):
        return block_in.reshape(
            block_in.shape[0], block_in.shape[1] // tile_cols, tile_cols
        ).transpose(1, 0, 2)

    down_part = down_block.reshape(
        down_block.shape[0] // tile_rows, tile_rows, down_block.shape[1] // tile_cols, tile_cols
    )
    down_part = down_part.transpose(0, 2, 1, 3).reshape(-1, tile_rows, tile_cols)
    return jnp.concatenate(
        [
            split_cols(qkv_block[:, 0]),
            split_cols(qkv_block[:, 1]),
            split_cols(qkv_block[:, 2]),
            split_cols(out_block),
            split_cols(up_block),
            down_part,
        ],
        axis=0,
    )


def pick(index, table):
    out = jnp.int32(table[0]) if isinstance(table[0], int) else table[0]
    for k in range(1, len(table)):
        out = jnp.where(index == k, table[k], out)
    return out


def far_order(c, n_col):
    far = [
        sorted(range(n_col), key=lambda f: (-abs(f - cc), f < cc if cc < n_col // 2 else f > cc))
        for cc in range(n_col)
    ]
    return [pick(c, [far[cc][i] for cc in range(n_col)]) for i in range(n_col)]


def forward_kernel(n_dp, n_row, n_col, dims,
                   x_ref, g_ref, wq_ref, wu_ref, wo_ref, wd_ref,
                   pos_ref, seg_ref, freq_ref, vec_ref,
                   gf, wi, wf, nt, hid_out, ht_out, qkv_out, up_out, cs_out, mean_ref, rstd_ref,
                   xv, ntv, wv, hid, ht, qkv, up, tab, mean_v, rstd_v, stage_g, stage_o, stage_d,
                   zs, zr, ys, yr, cs, cr, ws, wr, ds, dr, ls, lo, no):
    T, C, HF, UT = dims
    d, r, c = lax.axis_index("dp"), lax.axis_index("row"), lax.axis_index("col")
    r1 = r + 1 - 2 * lax.rem(r, 2)
    r2 = lax.rem(r + 2, n_row)
    chunks = 2
    tc = T // chunks
    qw = 3 * HF
    rows_all, D = n_row * T, n_col * C
    seqs = rows_all // SEQ_LEN
    acts = ((x_ref, xv), (g_ref, gf))
    forder = far_order(c, n_col)

    barrier = pltpu.get_barrier_semaphore()
    peers = [{"row": r1}, {"row": r2}]
    peers += [{"col": lax.rem(c + k, n_col)} for k in range(1, n_col)]
    peers += [{"dp": lax.rem(d + k, n_dp)} for k in range(1, n_dp)]
    for peer in peers:
        pl.semaphore_signal(barrier, inc=1, device_id=peer, device_id_type=MESH)
    pl.semaphore_wait(barrier, len(peers))

    def copy(src, dst, s, rcv, peer):
        return pltpu.make_async_remote_copy(
            src_ref=src, dst_ref=dst, send_sem=s, recv_sem=rcv, device_id=peer, device_id_type=MESH
        )

    def blk(a, rr, cc, t):
        return acts[a][1].at[pl.ds(pl.multiple_of(rr * T + t * tc, tc), tc),
                             pl.ds(pl.multiple_of(cc * C, C), C)]

    def own(a, t):
        return acts[a][0].at[pl.ds(t * tc, tc), :]

    def z_copy(a, t, cc, src, right):
        peer = {"col": c + 1} if right else {"col": c - 1}
        return copy(src, blk(a, r, cc, t), zs.at[a, t, int(right), cc], zr.at[a, t, cc], peer)

    def y_copy(a, t, cc, src):
        return copy(src, blk(a, r, cc, t), ys.at[a, t, cc], yr.at[a, t, cc], {"row": r2})

    def c_copy(a, t, cc, src, rr, which):
        return copy(
            src, blk(a, rr, cc, t), cs.at[a, t, which, cc], cr.at[a, t, which, cc], {"row": r1}
        )

    def send_own_z(a, t):
        @pl.when(c < n_col - 1)
        def _():
            z_copy(a, t, c, own(a, t), True).start()

        @pl.when(c > 0)
        def _():
            z_copy(a, t, c, own(a, t), False).start()

    def send_own_row(a, t):
        y_copy(a, t, c, own(a, t)).start()
        c_copy(a, t, c, own(a, t), r, 0).start()

    def relay(a, s, t):
        for right in (True, False):
            cc = c - s if right else c + s

            @pl.when((cc >= 0) & (cc < n_col))
            def _(cc=cc, right=right):
                z_copy(a, t, cc, blk(a, r, cc, t), right).wait_recv()

                @pl.when((c < n_col - 1) if right else (c > 0))
                def _():
                    z_copy(a, t, cc, blk(a, r, cc, t), right).start()

                y_copy(a, t, cc, blk(a, r, cc, t)).start()
                c_copy(a, t, cc, blk(a, r, cc, t), r, 0).start()

    def pass_row(a, s, t):
        for right in (True, False):
            cc = c - s if right else c + s
            ok = (cc >= 0) & (cc < n_col)
            if not right:
                ok = ok & (s > 0)

            @pl.when(ok)
            def _(cc=cc):
                y_copy(a, t, cc, blk(a, r, cc, t)).wait_recv()
                c_copy(a, t, cc, blk(a, r2, cc, t), r2, 1).start()

    ck, hk, uk = C // n_dp, HF // n_dp, UT // n_dp

    def w_dst(part, dd, cc):
        if part == 0:
            return wv.at[pl.ds(cc * C + dd * ck, ck), pl.ds(0, qw)]
        if part == 1:
            return wv.at[pl.ds(cc * C + dd * ck, ck), pl.ds(qw, UT)]
        if part == 2:
            return wv.at[pl.ds(cc * C + dd * ck, ck), pl.ds(qw + UT, UT)]
        if part == 3:
            return wf.at[pl.ds(dd * hk, hk), pl.ds(cc * C, C)]
        if part == 4:
            return wf.at[pl.ds(HF + dd * uk, uk), pl.ds(cc * C, C)]
        return wf.at[pl.ds(HF + UT + dd * uk, uk), pl.ds(cc * C, C)]

    def w_src(part, cc):
        if part == 0:
            return wq_ref.at[cc, pl.ds(d * ck, ck), :]
        if part == 1:
            return wu_ref.at[pl.ds(d * ck, ck), pl.ds(cc * UT, UT)]
        if part == 2:
            return wu_ref.at[pl.ds(d * ck, ck), pl.ds((n_col + cc) * UT, UT)]
        if part == 3:
            return wo_ref.at[pl.ds(cc * HF + d * hk, hk), :]
        if part == 4:
            return wd_ref.at[pl.ds(cc * UT + d * uk, uk), :]
        return wd_ref.at[pl.ds((n_col + cc) * UT + d * uk, uk), :]

    def w_copy(part, dest):
        return copy(
            w_src(part, dest), w_dst(part, d, c), ws.at[part, dest], wr.at[part, c], {"col": dest}
        )

    def w_from(part, source):
        return copy(
            w_src(part, source), w_dst(part, d, source), ws.at[part, source], wr.at[part, source],
            {"col": source},
        )

    def x_copy(part, source, j):
        got = w_dst(part, d, source)
        return copy(got, got, ds.at[part, source, j], dr.at[part, source, j],
                    {"dp": lax.rem(d + j, n_dp)})

    others = forder[: n_col - 1]

    def w_send(part):
        for dest in others:
            w_copy(part, dest).start()

    def w_pass(part):
        for source in others[::-1]:
            w_from(part, source).wait_recv()
            for j in range(1, n_dp):
                x_copy(part, source, j).start()

    def w_done(part):
        for source in others:
            for j in range(1, n_dp):
                x_copy(part, source, j).wait_recv()

    win, wfin = (0, 1, 2), (3, 4, 5)

    for t in range(chunks):
        send_own_z(0, t)
    for t in range(chunks):
        send_own_row(0, t)

    col_at = pl.ds(c * C, C)
    direct = [
        pltpu.make_async_copy(x_ref, xv.at[pl.ds(r * T, T), col_at], ls.at[0]),
        pltpu.make_async_copy(wq_ref.at[c], wv.at[col_at, pl.ds(0, qw)], ls.at[1]),
        pltpu.make_async_copy(wu_ref.at[:, pl.ds(c * UT, UT)], wv.at[col_at, pl.ds(qw, UT)],
                              ls.at[2]),
        pltpu.make_async_copy(wu_ref.at[:, pl.ds((n_col + c) * UT, UT)],
                              wv.at[col_at, pl.ds(qw + UT, UT)], ls.at[3]),
    ]
    loads = [
        pltpu.make_async_copy(g_ref, stage_g, ls.at[4]),
        pltpu.make_async_copy(wo_ref.at[pl.ds(c * HF, HF), :], stage_o, ls.at[5]),
        pltpu.make_async_copy(wd_ref.at[pl.ds(c * UT, UT), :], stage_d.at[0], ls.at[6]),
        pltpu.make_async_copy(wd_ref.at[pl.ds((n_col + c) * UT, UT), :], stage_d.at[1], ls.at[7]),
    ]
    stores = [
        pltpu.make_async_copy(stage_g, gf.at[pl.ds(r * T, T), col_at], lo.at[0]),
        pltpu.make_async_copy(stage_o, wf.at[pl.ds(0, HF), col_at], lo.at[1]),
        pltpu.make_async_copy(stage_d.at[0], wf.at[pl.ds(HF, UT), col_at], lo.at[2]),
        pltpu.make_async_copy(stage_d.at[1], wf.at[pl.ds(HF + UT, UT), col_at], lo.at[3]),
    ]
    for item in direct + loads:
        item.start()

    for n in range(1, n_col):
        for t in range(chunks):
            relay(0, n, t)
        w_send(win[n - 1])
    for t in range(chunks):
        send_own_z(1, t)
        send_own_row(1, t)
    for load, store in zip(loads, stores):
        load.wait()
        store.start()
    w_pass(win[0])

    def one_table(n, carry):
        rows = jnp.broadcast_to(pos_ref[pl.ds(n, 1), :], (2 * HEAD_DIM, SEQ_LEN))
        angle = jnp.transpose(rows) * freq_ref[...]
        lane = lax.broadcasted_iota(jnp.int32, angle.shape, 1)
        turns = jnp.floor(angle * (2.0 / math.pi) + 0.5)
        rest = angle - turns * 1.5703125
        rest = rest - turns * 4.837512969970703125e-4
        rest = rest - turns * 7.54978994889188e-8
        sq = rest * rest
        sine = rest + rest * sq * (
            -1.6666654611e-1 + sq * (8.3321608736e-3 - sq * 1.9515295891e-4)
        )
        cosine = 1.0 - 0.5 * sq + sq * sq * (
            4.166664568298827e-2 + sq * (-1.388731625493765e-3 + sq * 2.443315711809948e-5)
        )
        quarter = jnp.where(lane < HEAD_DIM, turns, turns - 1.0)
        quarter = quarter - 4.0 * jnp.floor(quarter * 0.25)
        odd = (quarter == 1.0) | (quarter == 3.0)
        value = jnp.where(odd, sine, cosine)
        value = jnp.where((quarter == 1.0) | (quarter == 2.0), -value, value)
        tab[pl.ds(pl.multiple_of(n * SEQ_LEN, SEQ_LEN), SEQ_LEN), :] = value
        return carry

    lax.fori_loop(0, seqs, one_table, 0)
    keep_cs = pltpu.make_async_copy(tab, cs_out, no.at[2])
    keep_cs.start()
    for n in range(n_col):
        for t in range(chunks):
            pass_row(0, n, t)
    w_pass(win[1])
    for item in direct:
        item.wait()
    for t in range(chunks):
        for cc in range(n_col):
            c_copy(0, t, cc, blk(0, r, cc, t), r, 0).wait_recv()
            c_copy(0, t, cc, blk(0, r, cc, t), r, 1).wait_recv()

    def act_sent(a):
        for t in range(chunks):
            for cc in range(n_col):
                @pl.when((cc <= c) & (c < n_col - 1))
                def _(t=t, cc=cc):
                    z_copy(a, t, cc, blk(a, r, cc, t), True).wait_send()

                @pl.when((cc >= c) & (c > 0))
                def _(t=t, cc=cc):
                    z_copy(a, t, cc, blk(a, r, cc, t), False).wait_send()

                y_copy(a, t, cc, blk(a, r, cc, t)).wait_send()
                c_copy(a, t, cc, blk(a, r, cc, t), r, 0).wait_send()
                c_copy(a, t, cc, blk(a, r, cc, t), r, 1).wait_send()

    act_sent(0)

    tile = 256
    tiles = rows_all // tile
    sub = 16

    def norm_tile(i, carry):
        base = pl.multiple_of(i * tile, tile)

        def norm_rows(k, inner):
            at = pl.ds(pl.multiple_of(base + k * sub, sub), sub)
            val = xv[at, :].astype(F32)
            mean = jnp.sum(val, axis=1, keepdims=True) / D
            var = jnp.sum(val * val, axis=1, keepdims=True) / D - mean * mean
            rstd = lax.rsqrt(var + NORM_EPS)
            mean_v[at, :] = mean
            rstd_v[at, :] = rstd
            xv[at, :] = ((val - mean) * rstd * vec_ref[5:6, :] + vec_ref[6:7, :]).astype(BF16)
            return inner

        lax.fori_loop(0, tile // sub, norm_rows, 0)
        at = pl.ds(base, tile)
        for k in range(D // tile):
            ntv[k * tile : (k + 1) * tile, at] = jnp.transpose(xv[at, k * tile : (k + 1) * tile])
        return carry

    lax.fori_loop(0, tiles // 2, norm_tile, 0)
    w_pass(win[2])
    for t in range(chunks):
        relay(1, 1, t)
    w_send(wfin[0])
    lax.fori_loop(tiles // 2, tiles, norm_tile, 0)
    keep_norm = pltpu.make_async_copy(ntv, nt, no.at[1])
    keep_norm.start()
    own_rows = pl.ds(pl.multiple_of(r * T, T), T)
    mean_ref[...] = mean_v[own_rows, :]
    rstd_ref[...] = rstd_v[own_rows, :]
    for part in win:
        w_done(part)
    keep_w = pltpu.make_async_copy(wv, wi, no.at[0])
    keep_w.start()

    q_lanes = pl.ds(pl.multiple_of((r * n_col + c) * HF, HF), HF)
    biases = [vec_ref[j : j + 1, q_lanes] for j in range(3)]
    biases += [
        vec_ref[pl.ds(7 + r, 1), pl.ds(pl.multiple_of((m * n_col + c) * UT, UT), UT)]
        for m in range(2)
    ]
    bias = jnp.concatenate(biases, axis=1)

    def one_tile(i, carry):
        at = pl.ds(pl.multiple_of(i * tile, tile), tile)
        mixed = jnp.dot(xv[at, :], wv[...], preferred_element_type=F32) + bias
        cos, sin = wide_tables(tab[at, :])
        for j in range(2):
            part = mixed[:, j * HF : (j + 1) * HF]
            qkv[at, j * HF : (j + 1) * HF] = turn(part, cos, sin, 1.0).astype(BF16)
        qkv[at, 2 * HF : 3 * HF] = mixed[:, 2 * HF : 3 * HF].astype(BF16)
        pre = mixed[:, qw:]
        up[at, :] = pre
        act = gelu_value(pre).astype(BF16)
        hid[at, HF:] = act
        ht[HF:, at] = jnp.transpose(act)

        s, t = 2 + lax.div(i, 2), lax.rem(i, 2)

        @pl.when(s < n_col)
        def _():
            relay(1, s, t)

        return carry

    lax.fori_loop(0, 2, one_tile, 0)
    w_send(wfin[1])
    lax.fori_loop(2, 4, one_tile, 0)
    w_send(wfin[2])
    lax.fori_loop(4, tiles, one_tile, 0)
    keep_up = pltpu.make_async_copy(up, up_out, no.at[3])
    keep_qkv = pltpu.make_async_copy(qkv, qkv_out, no.at[4])
    keep_up.start()
    keep_qkv.start()

    heads = HF // HEAD_DIM
    qt = SEQ_LEN // 2

    def one_seq(s, carry):
        base = pl.multiple_of(s * SEQ_LEN, SEQ_LEN)
        lane = lax.broadcasted_iota(jnp.int32, (qt, HF), 1)
        seg = seg_ref[pl.ds(s, 1), :]
        seg_col = jnp.transpose(jnp.broadcast_to(seg, (128, SEQ_LEN)))[:, 0:1]
        for qi in range(2):
            width = (qi + 1) * qt
            q_at = pl.ds(pl.multiple_of(base + qi * qt, qt), qt)
            k_at = pl.ds(base, width)
            allowed = (seg_col[qi * qt : (qi + 1) * qt, :] == seg[:, 0:width]) & (
                lax.broadcasted_iota(jnp.int32, (qt, width), 0) + qi * qt
                >= lax.broadcasted_iota(jnp.int32, (qt, width), 1)
            )
            keys, vals = qkv[k_at, HF : 2 * HF], qkv[k_at, 2 * HF : 3 * HF]
            queries = qkv[q_at, 0:HF]
            total = None
            for h in range(heads):
                mine = lax.div(lane, HEAD_DIM) == h
                scores = lax.dot_general(
                    jnp.where(mine, queries, jnp.zeros_like(queries)), keys,
                    (((1,), (1,)), ((), ())), preferred_element_type=F32,
                ) * (HEAD_DIM ** (-0.5))
                scores = jnp.where(allowed, scores, MASKED_SCORE)
                peak = jnp.max(scores, axis=1, keepdims=True)
                weight = jnp.exp(scores - peak)
                weight_sum = jnp.sum(weight, axis=1, keepdims=True)
                probs = (weight * (1.0 / weight_sum)).astype(BF16)
                out = jnp.dot(probs, vals, preferred_element_type=F32)
                total = out if h == 0 else jnp.where(mine, out, total)
            low = total.astype(BF16)
            hid[q_at, 0:HF] = low
            ht[0:HF, q_at] = jnp.transpose(low)

        @pl.when(s < n_col)
        def _():
            for t in range(chunks):
                pass_row(1, s, t)

        return carry

    lax.fori_loop(0, seqs, one_seq, 0)
    keep_hid = pltpu.make_async_copy(hid, hid_out, no.at[5])
    keep_ht = pltpu.make_async_copy(ht, ht_out, no.at[6])
    keep_hid.start()
    keep_ht.start()
    for part in wfin:
        w_pass(part)

    for t in range(chunks):
        for cc in range(n_col):
            c_copy(1, t, cc, blk(1, r, cc, t), r, 0).wait_recv()
            c_copy(1, t, cc, blk(1, r, cc, t), r, 1).wait_recv()
    for part in wfin:
        w_done(part)
    act_sent(1)
    for part in win + wfin:
        for peer in others:
            w_copy(part, peer).wait_send()
            for j in range(1, n_dp):
                x_copy(part, peer, j).wait_send()
    for store in stores:
        store.wait()
    for item in (keep_w, keep_norm, keep_cs, keep_up, keep_qkv, keep_hid, keep_ht):
        item.wait()


def forward_all(x, g, w_q, w_up, w_out, w_down, pos_row, seg_row, freq, vectors,
                n_dp, n_row, n_col):
    T, C = x.shape
    HF = w_q.shape[2] // 3
    UT = w_up.shape[1] // (2 * n_col)
    n_in, n_out = 3 * HF + 2 * UT, HF + 2 * UT
    rows, D = n_row * T, n_col * C
    dma = pltpu.SemaphoreType.DMA
    vm = pl.BlockSpec(memory_space=pltpu.VMEM)
    sds = jax.ShapeDtypeStruct
    return pl.pallas_call(
        functools.partial(forward_kernel, n_dp, n_row, n_col, (T, C, HF, UT)),
        name="forward_all",
        out_shape=(
            sds((rows, D), BF16),
            sds((D, n_in), BF16),
            sds((n_out, D), BF16),
            sds((D, rows), BF16),
            sds((rows, n_out), BF16),
            sds((n_out, rows), BF16),
            sds((rows, 3 * HF), BF16),
            sds((rows, 2 * UT), F32),
            sds((rows, 2 * HEAD_DIM), F32),
            sds((T, 1), F32),
            sds((T, 1), F32),
        ),
        in_specs=[ANY] * 6 + [vm] * 4,
        out_specs=(ANY,) * 9 + (vm,) * 2,
        scratch_shapes=[
            pltpu.VMEM((rows, D), BF16),
            pltpu.VMEM((D, rows), BF16),
            pltpu.VMEM((D, n_in), BF16),
            pltpu.VMEM((rows, n_out), BF16),
            pltpu.VMEM((n_out, rows), BF16),
            pltpu.VMEM((rows, 3 * HF), BF16),
            pltpu.VMEM((rows, 2 * UT), F32),
            pltpu.VMEM((rows, 2 * HEAD_DIM), F32),
            pltpu.VMEM((rows, 1), F32),
            pltpu.VMEM((rows, 1), F32),
            pltpu.VMEM((T, C), BF16),
            pltpu.VMEM((HF, C), BF16),
            pltpu.VMEM((2, UT, C), BF16),
            dma((2, 2, 2, n_col)),
            dma((2, 2, n_col)),
            dma((2, 2, n_col)),
            dma((2, 2, n_col)),
            dma((2, 2, 2, n_col)),
            dma((2, 2, 2, n_col)),
            dma((6, n_col)),
            dma((6, n_col)),
            dma((6, n_col, n_dp)),
            dma((6, n_col, n_dp)),
            dma((8,)),
            dma((4,)),
            dma((7,)),
        ],
        compiler_params=pltpu.CompilerParams(
            collective_id=0, has_side_effects=True, vmem_limit_bytes=60 * 1024 * 1024
        ),
    )(x, g, w_q, w_up, w_out, w_down, pos_row, seg_row, freq, vectors)


def wide_tables(packed):
    lane = lax.broadcasted_iota(jnp.int32, packed.shape, 1)
    turned = pltpu.roll(packed, HEAD_DIM, 1)
    first = lane < HEAD_DIM
    return jnp.where(first, packed, turned), jnp.where(first, turned, packed)


def turn(part, cos, sin, sign):
    lane = lax.rem(lax.broadcasted_iota(jnp.int32, part.shape, 1), HEAD_DIM)
    ahead = pltpu.roll(part, part.shape[1] - ROTARY // 2, 1)
    behind = pltpu.roll(part, ROTARY // 2, 1)
    return part * cos + jnp.where(lane < ROTARY // 2, -ahead, behind) * (sign * sin)


def backward_kernel(n_row, n_col, dims,
                    hid_ref, ht_ref, c_ref, wf_ref, wi_ref, nt_ref, qkv_ref, up_ref,
                    cs_ref, seg_ref,
                    res_ref, gn_ref, tiles_ref, part_ref,
                    hd, hts, big, wf, wi, qv, ups, ga,
                    abuf, obuf, asb, sbuf, bbuf, zsb, zin,
                    dwf, dwi, gf, gu, gk,
                    l_s, h_s, u_s, a_s, a_r, y_s, y_r, z_s, z_r, xf_s, xf_r, xu_s, xu_r, xk_s, xk_r,
                    t_s, t_r, free_row, free_col):
    T, C, HF, UT = dims
    rows_all, D = n_row * T, n_col * C
    qw, n_in, n_out = 3 * HF, 3 * HF + 2 * UT, HF + 2 * UT
    step_rows = 64
    d, r, c = lax.axis_index("dp"), lax.axis_index("row"), lax.axis_index("col")
    r1 = r + 1 - 2 * lax.rem(r, 2)
    r2 = lax.rem(r + 2, n_row)
    r12 = lax.rem(r1 + 2, n_row)
    forder = far_order(c, n_col)
    outs = (res_ref, gn_ref)

    barrier = pltpu.get_barrier_semaphore()
    peers = [{"row": r1}, {"row": r2}, {"dp": 1 - d}]
    peers += [{"col": lax.rem(c + k, n_col)} for k in range(1, n_col)]
    for peer in peers:
        pl.semaphore_signal(barrier, inc=1, device_id=peer, device_id_type=MESH)

    loads = [
        pltpu.make_async_copy(hid_ref, hd.at[:, pl.ds(2 * HF, n_out)], l_s.at[0]),
        pltpu.make_async_copy(wf_ref, wf, l_s.at[1]),
        pltpu.make_async_copy(c_ref, big, l_s.at[2]),
        pltpu.make_async_copy(qkv_ref, qv, l_s.at[3]),
        pltpu.make_async_copy(wi_ref, wi, l_s.at[4]),
    ]
    for item in loads:
        item.start()
    load_nt = pltpu.make_async_copy(nt_ref, big, l_s.at[5])

    def load_ht(m, slot):
        return pltpu.make_async_copy(ht_ref.at[pl.ds(pl.multiple_of(m * HF, HF), HF), :],
                                     hts.at[slot], h_s.at[slot])

    tile = 256

    def load_up(i, slot):
        return pltpu.make_async_copy(up_ref.at[pl.ds(pl.multiple_of(i * tile, tile), tile), :],
                                     ups.at[slot], u_s.at[slot])

    load_ht(0, 0).start()
    load_up(0, 0).start()
    pl.semaphore_wait(barrier, len(peers))

    def copy(src, dst, s, rcv, peer):
        return pltpu.make_async_remote_copy(
            src_ref=src, dst_ref=dst, send_sem=s, recv_sem=rcv, device_id=peer, device_id_type=MESH
        )

    def a_copy(v, h, f):
        return copy(asb.at[h, f], abuf.at[v, h, f], a_s.at[h, f], a_r.at[v, h, f], {"row": r1})

    def y_copy(f):
        return copy(sbuf.at[f], bbuf.at[f], y_s.at[f], y_r.at[f], {"row": r2})

    def z_copy(f, slot, step):
        return copy(zsb.at[f], zin.at[slot], z_s.at[f], z_r.at[slot], {"col": c + step})

    def looped(rows, fn):
        def one(k, carry):
            fn(pl.ds(pl.multiple_of(k * step_rows, step_rows), step_rows))
            return carry
        lax.fori_loop(0, rows // step_rows, one, 0)

    def first_sum(v, f):
        a_copy(v, 1, f).wait_recv()
        if v == 1:
            y_copy(f).wait_send()

        def add(rows):
            sbuf[f, rows, :] = (
                obuf[1, f, rows, :].astype(F32) + abuf[v, 1, f, rows, :].astype(F32)
            ).astype(BF16)

        looped(T, add)
        if v == 1:
            pl.semaphore_wait(free_row.at[f], 1)
        y_copy(f).start()

    def release(f, peer):
        pl.semaphore_signal(free_col.at[f], inc=1, device_id={"col": peer}, device_id_type=MESH)

    def second_sum(v, i):
        f = forder[i]
        a_copy(v, 0, f).wait_recv()
        y_copy(f).wait_recv()

        def base(rows):
            return (
                obuf[0, f, rows, :].astype(F32)
                + abuf[v, 0, f, rows, :].astype(F32)
                + bbuf[f, rows, :].astype(F32)
            )

        if i < n_col - 1:
            right = f > c
            step = jnp.where(right, jnp.int32(1), jnp.int32(-1))
            landed = jnp.where(f == c + step, jnp.where(right, f, jnp.int32(n_col)), f)
            inner = jnp.where(right, c, n_col - 1 - c) > 0
            if v == 1:
                z_copy(f, f, 0).wait_send()

            @pl.when(inner)
            def _():
                z_copy(f, f, 0).wait_recv()

                def add(rows):
                    zsb[f, rows, :] = (base(rows) + zin[f, rows, :].astype(F32)).astype(BF16)

                looped(T, add)
                if v == 0:
                    release(f, c - step)

            @pl.when(jnp.logical_not(inner))
            def _():
                def add(rows):
                    zsb[f, rows, :] = base(rows).astype(BF16)

                looped(T, add)

            if v == 1:
                pl.semaphore_wait(free_col.at[f], 1)
            z_copy(f, landed, step).start()
        else:
            out = outs[v]

            @pl.when(c > 0)
            def _():
                z_copy(f, f, 0).wait_recv()

            @pl.when(c < n_col - 1)
            def _():
                z_copy(f, n_col, 0).wait_recv()

            def put(rows, value):
                out[rows, :] = value

            @pl.when(c == 0)
            def _():
                looped(T, lambda rows: put(rows, base(rows) + zin[n_col, rows, :].astype(F32)))

            @pl.when(c == n_col - 1)
            def _():
                looped(T, lambda rows: put(rows, base(rows) + zin[f, rows, :].astype(F32)))

            @pl.when((c > 0) & (c < n_col - 1))
            def _():
                looped(T, lambda rows: put(
                    rows,
                    base(rows) + zin[f, rows, :].astype(F32) + zin[n_col, rows, :].astype(F32)))

            if v == 0:
                @pl.when(c > 0)
                def _():
                    release(f, c - 1)

                @pl.when(c < n_col - 1)
                def _():
                    release(f, c + 1)

        if v == 0:
            pl.semaphore_signal(free_row.at[f], inc=1, device_id={"row": r2}, device_id_type=MESH)

    tall = (HF, 2 * UT)
    row0 = (0, HF)
    lane_u = (qw, qw + UT)
    lw = 2 * HF

    def xf_copy(own, b):
        return copy(dwf.at[pl.ds(row0[own] + b * HF, HF), :], gf.at[pl.ds(b * HF, HF), :],
                    xf_s.at[own, b], xf_r.at[b], {"dp": 1 - d})

    def xu_copy(own, cc):
        return copy(dwi.at[pl.ds(cc * C, C), pl.ds(lane_u[own], UT)], gu.at[cc],
                    xu_s.at[own, cc], xu_r.at[cc], {"dp": 1 - d})

    def xk_copy(cc):
        return copy(dwi.at[pl.ds(cc * C, C), pl.ds(0, qw)], gk.at[cc], xk_s.at[cc], xk_r.at[cc],
                    {"dp": 1 - d})

    def parts_f(own, cc, source):
        half, odd = lax.div(source, 2), lax.rem(source, 2)
        at = cc * C
        if own == 0:
            return [
                (dwf.at[pl.ds(0, HF), pl.ds(at + j * lw, lw)],
                 tiles_ref.at[6 + j, pl.ds(source * HF, HF), :])
                for j in range(2)
            ]
        return [
            (dwf.at[pl.ds(HF, UT), pl.ds(at + j * lw, lw)],
             tiles_ref.at[4 + 2 * half + j, pl.ds(odd * UT, UT), :])
            for j in range(2)
        ]

    def parts_e(own, cc, source):
        half, odd = lax.div(source, 2), lax.rem(source, 2)
        at = cc * C
        return [
            (dwf.at[pl.ds(HF + UT, UT), pl.ds(at + j * lw, lw)],
             tiles_ref.at[8 + 2 * half + j, pl.ds(odd * UT, UT), :])
            for j in range(2)
        ]

    def parts_u(own, cc, source):
        dst = tiles_ref.at[8 + source] if own == 0 else tiles_ref.at[source]
        return [(dwi.at[pl.ds(cc * C, C), pl.ds(lane_u[own], UT)], dst)]

    def parts_k(own, cc, source):
        half, odd = lax.div(source, 2), lax.rem(source, 2)
        return [
            (dwi.at[pl.ds(cc * C, C), pl.ds(j * HF, HF)],
             tiles_ref.at[2 * j + half, :, pl.ds(odd * HF, HF)])
            for j in range(3)
        ]

    kinds = {"f": (parts_f, 0), "e": (parts_e, 2), "u": (parts_u, 4), "k": (parts_k, 5)}

    def t_send(kind, own, cc):
        parts, first = kinds[kind]
        return [
            copy(src, dst, t_s.at[first + n, cc], t_r.at[first + n, c], {"col": cc})
            for n, (src, dst) in enumerate(parts(own, cc, c))
        ]

    def t_wait(kind, own, source):
        parts, first = kinds[kind]
        return [
            copy(src, dst, t_s.at[first + n, source], t_r.at[first + n, source], {"col": source})
            for n, (src, dst) in enumerate(parts(own, source, source))
        ]

    def t_local(kind, own):
        parts, first = kinds[kind]
        return [
            pltpu.make_async_copy(src, dst, t_s.at[first + n, c])
            for n, (src, dst) in enumerate(parts(own, c, c))
        ]

    def owned_kinds(own):
        return ("f", "u", "k") if own == 0 else ("f", "e", "u")

    def spread(kind, own):
        for k in range(1, n_col):
            for item in t_send(kind, own, lax.rem(c + k, n_col)):
                item.start()
        for item in t_local(kind, own):
            item.start()

    def add_rows(own, first, count):
        for b in range(first, first + count):
            xf_copy(own, b).wait_recv()

        def add(rows):
            here = pl.ds(pl.multiple_of(rows.start + first * HF, step_rows), step_rows)
            at = (pl.ds(pl.multiple_of(rows.start + row0[own] + first * HF, step_rows), step_rows),
                  slice(None))
            dwf[at] = (dwf[at].astype(F32) + gf[here, :].astype(F32)).astype(BF16)

        looped(count * HF, add)

    def add_f():
        for own in range(2):
            @pl.when(d == own)
            def _(own=own):
                add_rows(own, 0, 1 if own == 0 else UT // HF)
                spread("f", own)

    def add_e():
        @pl.when(d == 1)
        def _():
            add_rows(1, UT // HF, UT // HF)
            spread("e", 1)

    def add_piece(kind, own, cc):
        lane, width, buf, waiter = (
            (lane_u[own], UT, gu, xu_copy(own, cc)) if kind == "u" else (0, qw, gk, xk_copy(cc))
        )
        waiter.wait_recv()

        def add(rows):
            at = (pl.ds(pl.multiple_of(rows.start + cc * C, step_rows), step_rows),
                  pl.ds(lane, width))
            dwi[at] = (dwi[at].astype(F32) + buf[cc, rows, :].astype(F32)).astype(BF16)

        looped(C, add)

    def add_w(i):
        for own in range(2):
            @pl.when(d == own)
            def _(own=own):
                cc = forder[i]
                for kind in ("k", "u") if own == 0 else ("u",):
                    add_piece(kind, own, cc)
                    for item in t_local(kind, own) if i == n_col - 1 else t_send(kind, own, cc):
                        item.start()

    loads[0].wait()
    loads[1].wait()

    def p_unit(rr, f):
        at = pl.ds(pl.multiple_of(rr * T, T), T)
        lanes = pl.ds(pl.multiple_of(f * C, C), C)
        return jnp.dot(hd[at, 2 * HF :], wf[:, lanes], preferred_element_type=F32).astype(BF16)

    def p_step(i, carry):
        f = pick(i, forder)
        for h, rr in ((1, r12), (0, r1)):
            asb[h, f] = p_unit(rr, f)
            a_copy(0, h, f).start()
        for h, rr in ((1, r2), (0, r)):
            obuf[h, f] = p_unit(rr, f)

        @pl.when(i > 0)
        def _():
            first_sum(0, pick(i - 1, forder))

        return carry

    lax.fori_loop(0, n_col, p_step, 0)

    loads[2].wait()
    blocks = n_out // HF

    def f_step(m, carry):
        slot = lax.rem(m, 2)
        load_ht(m, slot).wait()

        @pl.when(m + 1 < blocks)
        def _():
            load_ht(m + 1, 1 - slot).start()

        at = pl.ds(pl.multiple_of(m * HF, HF), HF)
        dwf[at, :] = jnp.dot(hts[slot], big[...], preferred_element_type=F32).astype(BF16)

        @pl.when((m == 0) & (d == 1))
        def _():
            xf_copy(0, 0).start()

        @pl.when((m > 0) & (d == 0))
        def _():
            xf_copy(1, m - 1).start()

        return carry

    early = 1 + UT // HF
    first_sum(0, forder[n_col - 1])
    lax.fori_loop(0, early, f_step, 0)

    part_ref[...] = jnp.zeros_like(part_ref)
    tiles = rows_all // tile

    def b_step(i, carry):
        slot = lax.rem(i, 2)
        load_up(i, slot).wait()

        @pl.when(i + 1 < tiles)
        def _():
            load_up(i + 1, 1 - slot).start()

        at = pl.ds(pl.multiple_of(i * tile, tile), tile)
        back = lax.dot_general(
            big[at, :], wf[...], (((1,), (1,)), ((), ())), preferred_element_type=F32
        )
        ga[at, :] = back[:, :HF].astype(BF16)
        grad = back[:, HF:] * gelu_slope(ups[slot])
        hd[at, qw:] = grad.astype(BF16)
        sums = jnp.sum(grad, axis=0, keepdims=True)
        for k in range(2 * UT // 128):
            part_ref[3 + k : 4 + k, :] += sums[:, k * 128 : (k + 1) * 128]
        return carry

    lax.fori_loop(0, tiles, b_step, 0)
    load_nt.start()
    second_sum(0, 0)

    loads[3].wait()
    loads[4].wait()
    heads = HF // HEAD_DIM
    qt = SEQ_LEN // 2
    scale = HEAD_DIM ** (-0.5)
    per_row = T // SEQ_LEN
    first_dim = (((0,), (0,)), ((), ()))
    last_dim = (((1,), (1,)), ((), ()))

    def attend_seq(s):
        base = pl.multiple_of(s * SEQ_LEN, SEQ_LEN)
        lane = lax.broadcasted_iota(jnp.int32, (qt, HF), 1)
        seg = seg_ref[pl.ds(s, 1), :]
        seg_col = jnp.transpose(jnp.broadcast_to(seg, (128, SEQ_LEN)))[:, 0:1]
        grad_q, grad_k, grad_v = [], None, None
        for qi in range(2):
            width = (qi + 1) * qt
            q_at = pl.ds(base + qi * qt, qt)
            k_at = pl.ds(base, width)
            allowed = (seg_col[qi * qt : (qi + 1) * qt, :] == seg[:, 0:width]) & (
                lax.broadcasted_iota(jnp.int32, (qt, width), 0) + qi * qt
                >= lax.broadcasted_iota(jnp.int32, (qt, width), 1)
            )
            queries, g_att = qv[q_at, 0:HF], ga[q_at, :]
            keys, vals = qv[k_at, HF : 2 * HF], qv[k_at, 2 * HF : 3 * HF]
            both = g_att.astype(F32) * hd[q_at, 2 * HF : 3 * HF].astype(F32)
            gq, gks, gvs = None, None, None
            for h in range(heads):
                mine = lax.div(lane, HEAD_DIM) == h
                q_h = jnp.where(mine, queries, jnp.zeros_like(queries))
                g_h = jnp.where(mine, g_att, jnp.zeros_like(g_att))
                scores = lax.dot_general(q_h, keys, last_dim, preferred_element_type=F32) * scale
                scores = jnp.where(allowed, scores, MASKED_SCORE)
                peak = jnp.max(scores, axis=1, keepdims=True)
                weight = jnp.exp(scores - peak)
                probs = weight * (1.0 / jnp.sum(weight, axis=1, keepdims=True))
                delta = jnp.sum(jnp.where(mine, both, 0.0), axis=1, keepdims=True)
                g_prob = lax.dot_general(g_h, vals, last_dim, preferred_element_type=F32)
                g_score = (probs * (g_prob - delta) * scale).astype(BF16)
                gq_h = jnp.dot(g_score, keys, preferred_element_type=F32)
                gk_h = lax.dot_general(g_score, q_h, first_dim, preferred_element_type=F32)
                gv_h = lax.dot_general(probs.astype(BF16), g_h, first_dim,
                                       preferred_element_type=F32)
                gq = gq_h if h == 0 else jnp.where(mine, gq_h, gq)
                gks = gk_h if h == 0 else gks + gk_h
                gvs = gv_h if h == 0 else gvs + gv_h
            grad_q.append(gq)
            if qi == 0:
                grad_k, grad_v = gks, gvs
            else:
                grad_k = jnp.concatenate([grad_k + gks[:qt], gks[qt:]], axis=0)
                grad_v = jnp.concatenate([grad_v + gvs[:qt], gvs[qt:]], axis=0)
        s_at = pl.ds(base, SEQ_LEN)
        cos, sin = wide_tables(cs_ref[s_at, :])
        grads = (
            turn(jnp.concatenate(grad_q, axis=0), cos, sin, -1.0),
            turn(grad_k, cos, sin, -1.0),
            grad_v,
        )
        for j, grad in enumerate(grads):
            part_ref[j : j + 1, :] += jnp.sum(grad, axis=0, keepdims=True)
            hd[s_at, j * HF : (j + 1) * HF] = grad.astype(BF16)

    def q_unit(rr, f):
        at = pl.ds(pl.multiple_of(rr * T, T), T)
        feats = pl.ds(pl.multiple_of(f * C, C), C)
        return lax.dot_general(
            hd[at, :], wi[feats, :], last_dim, preferred_element_type=F32
        ).astype(BF16)

    def seq_step(s, carry):
        attend_seq(s)
        return carry

    lax.fori_loop(0, rows_all // SEQ_LEN, seq_step, 0)
    second_sum(0, 1)
    load_nt.wait()

    half_rows = C // 2

    def w_step(i, carry):
        cc = pick(lax.div(i, 2), forder)
        at = pl.ds(pl.multiple_of(cc * C + lax.rem(i, 2) * half_rows, half_rows), half_rows)
        dwi[at, :] = jnp.dot(big[at, :], hd[...], preferred_element_type=F32).astype(BF16)

        @pl.when(lax.rem(i, 2) == 1)
        def _():
            for own in range(2):
                @pl.when(d == own)
                def _(own=own):
                    if own == 1:
                        xk_copy(cc).start()
                    xu_copy(1 - own, cc).start()

        return carry

    lax.fori_loop(0, n_col, w_step, 0)
    second_sum(0, 2)
    lax.fori_loop(n_col, 2 * n_col, w_step, 0)
    load_c = pltpu.make_async_copy(c_ref, big, l_s.at[2])
    load_c.start()

    def q_step(h, rows_peer, rows_own):
        def units(i, carry):
            f = pick(i, forder)
            a_copy(0, h, f).wait_send()
            asb[h, f] = q_unit(rows_peer, f)
            a_copy(1, h, f).start()
            obuf[h, f] = q_unit(rows_own, f)
            return carry

        lax.fori_loop(0, n_col, units, 0)

    q_step(1, r12, r2)
    for i in range(n_col - 1):
        first_sum(1, forder[i])
    add_f()
    load_c.wait()
    lax.fori_loop(early, blocks, f_step, 0)
    second_sum(0, n_col - 1)
    first_sum(1, forder[n_col - 1])
    add_w(0)
    q_step(0, r1, r)
    add_w(1)
    second_sum(1, 0)
    add_w(2)
    second_sum(1, 1)
    add_e()
    second_sum(1, 2)
    add_w(3)
    second_sum(1, n_col - 1)

    for own in range(2):
        @pl.when(d == own)
        def _(own=own):
            for kind in owned_kinds(own):
                for k in range(1, n_col):
                    for item in t_wait(kind, own, lax.rem(c + k, n_col)):
                        item.wait_recv()
                for k in range(1, n_col):
                    for item in t_send(kind, own, lax.rem(c + k, n_col)):
                        item.wait_send()
                for item in t_local(kind, own):
                    item.wait()
            for b in range(tall[1 - own] // HF):
                xf_copy(1 - own, b).wait_send()
            for cc in range(n_col):
                xu_copy(1 - own, cc).wait_send()
                if own == 1:
                    xk_copy(cc).wait_send()
    for f in range(n_col):
        a_copy(1, 0, f).wait_send()
        a_copy(1, 1, f).wait_send()
        y_copy(f).wait_send()
    for i in range(n_col - 1):
        z_copy(forder[i], forder[i], 0).wait_send()


def backward_all(hid, ht, cot, w_fin, w_in, nt, qkv, up, packed, seg_row, T, C, HF, UT, n_row, n_col):
    dma = pltpu.SemaphoreType.DMA
    vm = pl.BlockSpec(memory_space=pltpu.VMEM)
    rows, D = n_row * T, n_col * C
    n_in, n_out = 3 * HF + 2 * UT, HF + 2 * UT
    unit = (T, C)
    V = pltpu.VMEM
    return pl.pallas_call(
        functools.partial(backward_kernel, n_row, n_col, (T, C, HF, UT)),
        name="backward_all",
        out_shape=(
            jax.ShapeDtypeStruct(unit, F32),
            jax.ShapeDtypeStruct(unit, F32),
            jax.ShapeDtypeStruct((12, C, UT), BF16),
            jax.ShapeDtypeStruct((8, 128), F32),
        ),
        in_specs=[ANY] * 8 + [vm] * 2,
        out_specs=(vm, vm, ANY, vm),
        scratch_shapes=[
            V((rows, n_in), BF16),
            V((2, HF, rows), BF16),
            V((rows, D), BF16),
            V((n_out, D), BF16),
            V((D, n_in), BF16),
            V((rows, 3 * HF), BF16),
            V((2, 256, 2 * UT), F32),
            V((rows, HF), BF16),
            V((2, 2, n_col) + unit, BF16),
            V((2, n_col) + unit, BF16),
            V((2, n_col) + unit, BF16),
            V((n_col,) + unit, BF16),
            V((n_col,) + unit, BF16),
            V((n_col,) + unit, BF16),
            V((n_col + 1,) + unit, BF16),
            V((n_out, D), BF16),
            V((D, n_in), BF16),
            V((2 * UT, D), BF16),
            V((n_col, C, UT), BF16),
            V((n_col, C, 3 * HF), BF16),
            dma((6,)),
            dma((2,)),
            dma((2,)),
            dma((2, n_col)),
            dma((2, 2, n_col)),
            dma((n_col,)),
            dma((n_col,)),
            dma((n_col,)),
            dma((n_col + 1,)),
            dma((2, 2 * UT // HF)),
            dma((2 * UT // HF,)),
            dma((2, n_col)),
            dma((n_col,)),
            dma((n_col,)),
            dma((n_col,)),
            dma((8, n_col)),
            dma((8, n_col)),
            pltpu.SemaphoreType.REGULAR((n_col,)),
            pltpu.SemaphoreType.REGULAR((n_col,)),
        ],
        compiler_params=pltpu.CompilerParams(
            collective_id=1, has_side_effects=True, vmem_limit_bytes=67043328
        ),
    )(hid, ht, cot, w_fin, w_in, nt, qkv, up, packed, seg_row)


def finish_kernel(n_dp, n_row, n_col, width, *refs):
    hbm, (gx_ref, va_ref, vb_ref), local = refs[:7], refs[7:10], refs[10:17]
    gn_ref, x_ref, g_ref, mean_ref, rstd_ref, gain_ref, part_ref = local
    l_s, st, da, db, ra, rb, st_s, st_r, d_s, d_r, r_s, r_r, c_s, c_r = refs[17:]
    loads = [
        pltpu.make_async_copy(src, dst, l_s.at[n]) for n, (src, dst) in enumerate(zip(hbm, local))
    ]
    for item in loads:
        item.start()
    d, r, c = lax.axis_index("dp"), lax.axis_index("row"), lax.axis_index("col")
    T, C = gn_ref.shape

    barrier = pltpu.get_barrier_semaphore()
    dps = [lax.rem(d + k, n_dp) for k in range(1, n_dp)]
    rows = [lax.rem(r + k, n_row) for k in range(1, n_row)]
    cols = [lax.rem(c + k, n_col) for k in range(1, n_col)]
    peers = [{"dp": k} for k in dps] + [{"row": k} for k in rows] + [{"col": k} for k in cols]
    for peer in peers:
        pl.semaphore_signal(barrier, inc=1, device_id=peer, device_id_type=MESH)

    def copy(src, dst, s, rcv, peer):
        return pltpu.make_async_remote_copy(
            src_ref=src, dst_ref=dst, send_sem=s, recv_sem=rcv, device_id=peer, device_id_type=MESH
        )

    for item in loads:
        item.wait()
    gain = gain_ref[...]

    def fold(value):
        total = value[:, 0:128]
        for k in range(1, C // 128):
            total = total + value[:, k * 128 : (k + 1) * 128]
        return jnp.sum(jnp.transpose(total), axis=0, keepdims=True)

    gn = gn_ref[...]
    x_hat = (x_ref[...].astype(F32) - mean_ref[...]) * rstd_ref[...]
    gh = gn * gain
    st[c, 0:1, :] = fold(gh)
    st[c, 1:2, :] = fold(gh * x_hat)

    def st_copy(k):
        return copy(st.at[c], st.at[c], st_s.at[k], st_r.at[c], {"col": k})

    def st_wait(k):
        return copy(st.at[k], st.at[k], st_s.at[k], st_r.at[k], {"col": k})

    pl.semaphore_wait(barrier, len(peers))
    for k in cols:
        st_copy(k).start()

    da[d] = part_ref[...]
    db[d, 0:1, :] = jnp.sum(gn * x_hat, axis=0, keepdims=True)
    db[d, 1:2, :] = jnp.sum(gn, axis=0, keepdims=True)
    db[d, 2:3, :] = jnp.sum(g_ref[...].astype(F32), axis=0, keepdims=True)

    def pair(a_src, b_src, a_dst, b_dst, s, rcv, peer):
        return [copy(a_src, a_dst, s.at[0], rcv.at[0], peer),
                copy(b_src, b_dst, s.at[1], rcv.at[1], peer)]

    def d_pair(slot, peer):
        return pair(da.at[slot], db.at[slot], da.at[slot], db.at[slot],
                    d_s.at[peer], d_r.at[slot], {"dp": peer})

    def r_pair(slot, peer):
        return pair(ra.at[slot], rb.at[slot], ra.at[slot], rb.at[slot],
                    r_s.at[peer], r_r.at[slot], {"row": peer})

    def c_pair(slot, peer):
        return pair(va_ref.at[slot], vb_ref.at[slot], va_ref.at[slot], vb_ref.at[slot],
                    c_s.at[peer], c_r.at[slot], {"col": peer})

    for k in dps:
        for item in d_pair(d, k):
            item.start()
    for k in dps:
        for item in d_pair(k, k):
            item.wait_recv()
    a_sum, b_sum = da[0], db[0]
    for k in range(1, n_dp):
        a_sum = a_sum + da[k]
        b_sum = b_sum + db[k]
    ra[r] = a_sum
    rb[r] = b_sum
    for k in rows:
        for item in r_pair(r, k):
            item.start()

    for k in cols:
        st_wait(k).wait_recv()
    stats = st[0]
    for k in range(1, n_col):
        stats = stats + st[k]
    stats = stats / width
    m1 = jnp.transpose(jnp.broadcast_to(stats[0:1, :], (128, T)))[:, 0:1]
    m2 = jnp.transpose(jnp.broadcast_to(stats[1:2, :], (128, T)))[:, 0:1]
    gx_ref[...] = g_ref[...].astype(F32) + rstd_ref[...] * (gh - m1 - x_hat * m2)

    for k in rows:
        for item in r_pair(k, k):
            item.wait_recv()
    b_sum = rb[0]
    for k in range(1, n_row):
        b_sum = b_sum + rb[k]
    for k in range(n_row):
        va_ref[c, k] = ra[k]
    vb_ref[c] = b_sum
    for k in cols:
        for item in c_pair(c, k):
            item.start()
    for k in cols:
        for item in c_pair(k, k):
            item.wait_recv()
    for k in cols:
        st_copy(k).wait_send()
        for item in c_pair(c, k):
            item.wait_send()
    for k in dps:
        for item in d_pair(d, k):
            item.wait_send()
    for k in rows:
        for item in r_pair(r, k):
            item.wait_send()


def finish_all(gn, x, g, mean, rstd, gain, part, width, n_dp, n_row, n_col):
    args = (gn, x, g, mean, rstd, gain, part)
    T, C = gn.shape
    dma = pltpu.SemaphoreType.DMA
    vm = pl.BlockSpec(memory_space=pltpu.VMEM)
    return pl.pallas_call(
        functools.partial(finish_kernel, n_dp, n_row, n_col, width),
        name="finish_all",
        out_shape=(
            jax.ShapeDtypeStruct((T, C), F32),
            jax.ShapeDtypeStruct((n_col, n_row, 8, 128), F32),
            jax.ShapeDtypeStruct((n_col, 8, C), F32),
        ),
        in_specs=[ANY] * 7,
        out_specs=(vm,) * 3,
        scratch_shapes=[pltpu.VMEM(item.shape, item.dtype) for item in args]
        + [
            dma((7,)),
            pltpu.VMEM((n_col, 8, T), F32),
            pltpu.VMEM((n_dp, 8, 128), F32),
            pltpu.VMEM((n_dp, 8, C), F32),
            pltpu.VMEM((n_row, 8, 128), F32),
            pltpu.VMEM((n_row, 8, C), F32),
            dma((n_col,)),
            dma((n_col,)),
            dma((n_dp, 2)),
            dma((n_dp, 2)),
            dma((n_row, 2)),
            dma((n_row, 2)),
            dma((n_col, 2)),
            dma((n_col, 2)),
        ],
        compiler_params=pltpu.CompilerParams(
            collective_id=2, has_side_effects=True, vmem_limit_bytes=48 * 1024 * 1024
        ),
    )(*args)


def muon_kernel(owned, per_step, HF, UT, rate, grad_ref, mom_ref, wq_ref, wo_ref, wu_ref, wd_ref,
                og_ref, new_ref, nm_ref, wbuf, sem):
    first = lax.axis_index("dp") * owned
    step = pl.program_id(0)
    steps = owned // per_step
    n_qkv, n_out, n_up = 6, 2, 8

    def fetch(tile, slot, n, start):
        dst = wbuf.at[slot, n]

        def go(src, target, s):
            item = pltpu.make_async_copy(src, target, s)
            if start:
                item.start()
            else:
                item.wait()

        @pl.when(tile < n_qkv)
        def _():
            j, half = lax.div(tile, 2), lax.rem(tile, 2)
            for m in range(UT // HF):
                go(wq_ref.at[half * (UT // HF) + m, :, pl.ds(j * HF, HF)],
                   wbuf.at[slot, n, :, pl.ds(m * HF, HF)], sem.at[slot, n, m])

        @pl.when((tile >= n_qkv) & (tile < n_qkv + n_out))
        def _():
            go(wo_ref.at[:, pl.ds((tile - n_qkv) * UT, UT)], dst, sem.at[slot, n, 0])

        @pl.when((tile >= n_qkv + n_out) & (tile < n_qkv + n_out + n_up))
        def _():
            go(wu_ref.at[:, pl.ds((tile - n_qkv - n_out) * UT, UT)], dst, sem.at[slot, n, 0])

        @pl.when(tile >= n_qkv + n_out + n_up)
        def _():
            left = tile - (n_qkv + n_out + n_up)
            rows = dst.shape[0]
            go(wd_ref.at[pl.ds(lax.div(left, 2) * rows, rows), pl.ds(lax.rem(left, 2) * UT, UT)],
               dst, sem.at[slot, n, 0])

    def fetch_all(at, start):
        for n in range(per_step):
            fetch(first + at * per_step + n, lax.rem(at, 2), n, start)

    @pl.when(step == 0)
    def _():
        fetch_all(step, True)

    @pl.when(step + 1 < steps)
    def _():
        fetch_all(step + 1, True)

    iters = []
    for n in range(per_step):
        grad = grad_ref[n].astype(F32)
        og_ref[n] = grad
        moment = MOMENTUM_RATE * mom_ref[n] + grad
        nm_ref[n] = moment
        scale = lax.rsqrt(jnp.sum(moment * moment, keepdims=True) + STAT_EPS)
        iters.append((moment * scale).astype(BF16))
    contract = (((0,), (0,)), ((), ()))
    for _ in range(5):
        grams = [
            lax.dot_general(x, x, contract, preferred_element_type=F32).astype(BF16) for x in iters
        ]
        squares = [jnp.dot(g, g, preferred_element_type=F32) for g in grams]
        polys = [
            (NEWTON_B * g.astype(F32) + NEWTON_C * s).astype(BF16) for g, s in zip(grams, squares)
        ]
        iters = [
            (NEWTON_A * x.astype(F32) + jnp.dot(x, p, preferred_element_type=F32)).astype(BF16)
            for x, p in zip(iters, polys)
        ]
    fetch_all(step, False)
    for n in range(per_step):
        new_ref[n] = wbuf[lax.rem(step, 2), n].astype(F32) - rate * iters[n].astype(F32)


def muon_all(grads, moment, w_q, w_out, w_up, w_down, HF, UT):
    owned, rows, cols = moment.shape
    per_step = 4 if owned % 4 == 0 else 3
    rate = MUON_RATE * math.sqrt(max(1.0, rows / cols))
    block = pl.BlockSpec((per_step, rows, cols), lambda i: (i, 0, 0))
    out = jax.ShapeDtypeStruct(moment.shape, F32)
    return pl.pallas_call(
        functools.partial(muon_kernel, owned, per_step, HF, UT, rate),
        name="muon_all",
        grid=(owned // per_step,),
        out_shape=(out, out, out),
        in_specs=[block, block, ANY, ANY, ANY, ANY],
        out_specs=(block, block, block),
        scratch_shapes=[
            pltpu.VMEM((2, per_step, rows, cols), BF16),
            pltpu.SemaphoreType.DMA((2, per_step, 2)),
        ],
        compiler_params=pltpu.CompilerParams(vmem_limit_bytes=56 * 1024 * 1024),
    )(grads, moment, w_q, w_out, w_up, w_down)


def reduce_plain(p, q, dwi, dwf, C, HF, UT, n_col, row_width):
    def block(part):
        part = lax.psum_scatter(part, "row", scatter_dimension=0, tiled=True)
        return lax.psum_scatter(part, "col", scatter_dimension=1, tiled=True).astype(F32)

    wi4 = lax.all_to_all(dwi.reshape(n_col, C, -1), "col", 0, 0)
    wf4 = lax.all_to_all(dwf.reshape(-1, n_col, C).transpose(1, 0, 2), "col", 0, 0)
    grad_qkv = (
        wi4[:, :, : 3 * HF].reshape(n_col, C, 3, HF).transpose(1, 2, 0, 3).reshape(C, 3, row_width)
    )
    grad_up_w = wi4[:, :, 3 * HF :].reshape(n_col, C, 2, UT).transpose(1, 2, 0, 3).reshape(C, -1)
    grad_w_out = wf4[:, :HF].reshape(-1, C)
    grad_w_down = wf4[:, HF:].reshape(n_col, 2, UT, C).transpose(1, 0, 2, 3).reshape(-1, C)
    grad_tiles = tile_blocks(grad_qkv, grad_w_out, grad_up_w, grad_w_down)
    owned = lax.psum_scatter(grad_tiles, "dp", scatter_dimension=0, tiled=True)
    return block(p), block(q), owned


def backward_plain(hidden, hidden_t, cot, w_fin, w_in, norm_t, qkv, up_pre, positions, segments, HF):
    cosine, sine_tab = rotary_tables(positions)
    rows = cot.shape[0]
    seqs, heads = rows // SEQ_LEN, HF // HEAD_DIM

    def by_head(tensor_in):
        return tensor_in.reshape(seqs, SEQ_LEN, heads, HEAD_DIM)

    partial_out = jnp.dot(hidden, w_fin, preferred_element_type=F32).astype(BF16)
    grad_w_fin = jnp.dot(hidden_t, cot, preferred_element_type=F32).astype(BF16)
    back = jnp.einsum("tj,ij->ti", cot, w_fin, preferred_element_type=F32)
    grad_up = back[:, HF:] * gelu_slope(up_pre)
    grads = jax.vmap(attend_backward, in_axes=(0, 0, 0, 0, 0, 0, None))(
        by_head(qkv[:, :HF]),
        by_head(qkv[:, HF : 2 * HF]),
        by_head(qkv[:, 2 * HF :]),
        by_head(hidden[:, :HF]),
        by_head(back[:, :HF].astype(BF16)),
        segments.reshape(seqs, SEQ_LEN),
        HEAD_DIM ** (-0.5),
    )
    g_q, g_k, g_v = [item.reshape(rows, heads, HEAD_DIM) for item in grads]
    g_q = rotate(g_q, cosine, sine_tab, -1.0)
    g_k = rotate(g_k, cosine, sine_tab, -1.0)
    grad_mixed = jnp.concatenate(
        [item.reshape(rows, HF) for item in (g_q, g_k, g_v)] + [grad_up], axis=1
    )
    low = grad_mixed.astype(BF16)
    grad_w_in = jnp.dot(norm_t, low, preferred_element_type=F32).astype(BF16)
    partial_norm = jnp.einsum("tj,ij->ti", low, w_in, preferred_element_type=F32).astype(BF16)
    part = jnp.pad(jnp.sum(grad_mixed, axis=0).reshape(-1, 128), ((0, 1), (0, 0)))
    return (partial_out, partial_norm, grad_w_in, grad_w_fin), part


def body(
    inputs,
    cotangent,
    segments,
    positions,
    w_qkv,
    w_out,
    w_up,
    w_down,
    vectors,
    tile_moment,
    vector_moment,
):
    col_index = lax.axis_index("col")
    n_dp, n_row, n_col = lax.axis_size("dp"), lax.axis_size("row"), lax.axis_size("col")
    T, C = inputs.shape
    D = vectors.shape[1]
    row_width = w_qkv.shape[2]
    HF = row_width // n_col
    UT = w_up.shape[1] // (2 * n_col)
    col_start = col_index * C
    norm_gain = lax.dynamic_slice_in_dim(vectors[5], col_start, C)
    out_bias = lax.dynamic_slice_in_dim(vectors[3] + vectors[4], col_start, C)
    w_q = (
        w_qkv.reshape(C, 3, n_col, HF).transpose(2, 0, 1, 3).reshape(n_col, C, 3 * HF)
    )
    rows_all = positions.shape[0]
    seq_count = rows_all // SEQ_LEN
    half = jnp.exp(
        jnp.arange(ROTARY // 2, dtype=F32) * (-2.0 * math.log(10000.0) / ROTARY)
    )
    freq = jnp.tile(jnp.concatenate([half, half, jnp.zeros((HEAD_DIM - ROTARY,), F32)]), 2)
    seg_row = segments.reshape(seq_count, SEQ_LEN)
    pos_row = positions.reshape(seq_count, SEQ_LEN).astype(F32)
    cot_rows, w_in, w_fin, norm_t, hidden, hidden_t, qkv_low, up_pre, packed, mean_own, rstd_own = (
        forward_all(
            inputs, cotangent, w_q, w_up, w_out, w_down, pos_row, seg_row, freq[None], vectors,
            n_dp, n_row, n_col,
        )
    )
    if n_dp == 2:
        branch, grad_norm, owned_low, part = backward_all(
            hidden, hidden_t, cot_rows, w_fin, w_in, norm_t, qkv_low, up_pre, packed, seg_row,
            T, C, HF, UT, n_row, n_col,
        )
    else:
        partials, part = backward_plain(
            hidden, hidden_t, cot_rows, w_fin, w_in, norm_t, qkv_low, up_pre, positions, segments, HF
        )
        branch, grad_norm, owned_low = reduce_plain(*partials, C, HF, UT, n_col, row_width)
    x_val = inputs.astype(F32)
    result = x_val + branch + out_bias

    grad_input, vec_a, vec_b = finish_all(
        grad_norm,
        inputs,
        cotangent,
        mean_own,
        rstd_own,
        norm_gain[None],
        part,
        D,
        n_dp,
        n_row,
        n_col,
    )
    vec_a = vec_a.transpose(2, 1, 0, 3)
    qkv_rows = vec_a[:3].reshape(3, D)
    up_rows = vec_a[3:7].reshape(2, UT // 128, n_row, n_col, 128).transpose(2, 0, 3, 1, 4)
    norm_rows = vec_b.transpose(1, 0, 2).reshape(8, D)
    vec_grad = jnp.concatenate(
        [qkv_rows, norm_rows[2:3], norm_rows[2:3], norm_rows[:2], up_rows.reshape(-1, D)], axis=0
    )
    scaled = vec_grad * lax.rsqrt(jnp.mean(vec_grad * vec_grad, axis=1, keepdims=True) + STAT_EPS)
    vec_moment_new = MOMENTUM_RATE * vector_moment + scaled
    vectors_new = vectors - VECTOR_RATE * vec_moment_new

    owned_grads, tiles_new, moment_new = muon_all(
        owned_low, tile_moment[0, 0], w_q, w_out, w_up, w_down, HF, UT
    )
    return (
        result,
        grad_input,
        owned_grads[None, None],
        tiles_new[None, None],
        moment_new[None, None],
        vec_grad,
        vectors_new,
        vec_moment_new,
    )


def solution(mesh):
    placed = (
        P(("dp", "row"), "col"),
        P(("dp", "row"), "col"),
        P("dp"),
        P("dp"),
        P("col", None, "row"),
        P("row", "col"),
        P("col", "row"),
        P("row", "col"),
        P(),
        P("row", "col", "dp", None, None),
        P(),
    )
    return jax.shard_map(
        body,
        mesh=mesh,
        in_specs=placed,
        out_specs=(
            P(("dp", "row"), "col"),
            P(("dp", "row"), "col"),
            P("row", "col", "dp", None, None),
            P("row", "col", "dp", None, None),
            P("row", "col", "dp", None, None),
            P(),
            P(),
            P(),
        ),
        check_vma=False,
    )
```

```python
import functools
import math

import jax
import jax.numpy as jnp
from jax import lax
from jax.experimental import pallas as pl
from jax.experimental.pallas import tpu as pltpu
from jax.sharding import PartitionSpec as P

HEAD_DIM = 64
ROTARY = 32
SEQ_LEN = 512

MOMENTUM_RATE = 0.95
MUON_RATE = 0.05
VECTOR_RATE = 0.12
NEWTON_A = 3.4445
NEWTON_B = -4.775
NEWTON_C = 2.0315
GELU_SCALE = 0.7978845608028654
GELU_CUBIC = 0.044715
NORM_EPS = 1e-05
STAT_EPS = 1e-06
MASKED_SCORE = -1e30

MESH = pl.DeviceIdType.MESH
ANY = pl.BlockSpec(memory_space=pl.ANY)
F32 = jnp.float32
BF16 = jnp.bfloat16


def to_low(tensor_in):
    return lax.optimization_barrier(tensor_in.astype(BF16))


def gelu_value(pre_act):
    inner_arg = GELU_SCALE * (pre_act + GELU_CUBIC * pre_act * pre_act * pre_act)
    return 0.5 * pre_act * (1.0 + jnp.tanh(inner_arg))


def gelu_slope(pre_act):
    tanh_val = jnp.tanh(GELU_SCALE * (pre_act + GELU_CUBIC * pre_act * pre_act * pre_act))
    return 0.5 * (1.0 + tanh_val) + 0.5 * pre_act * (1.0 - tanh_val * tanh_val) * GELU_SCALE * (
        1.0 + 3.0 * GELU_CUBIC * pre_act * pre_act
    )


def rotary_tables(positions):
    half_dims = ROTARY // 2
    frequency = jnp.exp(jnp.arange(half_dims, dtype=F32) * (-2.0 * math.log(10000.0) / ROTARY))
    angles = positions.astype(F32)[:, None] * frequency[None, :]
    return (jnp.cos(angles), jnp.sin(angles))


def rotate(tensor_in, cosine, sine_tab, direction_sign):
    half_dims = ROTARY // 2
    first_half = tensor_in[..., :half_dims]
    second_half = tensor_in[..., half_dims:ROTARY]
    cos_wide = cosine[:, None, :]
    sin_wide = sine_tab[:, None, :] * direction_sign
    return jnp.concatenate(
        [
            first_half * cos_wide - second_half * sin_wide,
            second_half * cos_wide + first_half * sin_wide,
            tensor_in[..., ROTARY:],
        ],
        axis=-1,
    )


def causal_allowed(segment):
    token_order = jnp.arange(segment.shape[0])
    return (segment[:, None] == segment[None, :]) & (token_order[:, None] >= token_order[None, :])


def masked_scores(queries, key_vecs, segment, score_scale):
    scores = (
        jnp.einsum("lhe,mhe->hlm", queries, key_vecs, preferred_element_type=F32) * score_scale
    )
    return jnp.where(causal_allowed(segment)[None], scores, MASKED_SCORE)


def attend_backward(queries, key_vecs, values, output_low, grad_low, segment, score_scale):
    scores = masked_scores(queries, key_vecs, segment, score_scale)
    weight = jnp.exp(scores - jnp.max(scores, axis=-1, keepdims=True))
    probs = weight * (1.0 / jnp.sum(weight, axis=-1, keepdims=True))
    grad_values = jnp.einsum("hlm,lhe->mhe", to_low(probs), grad_low, preferred_element_type=F32)
    grad_probs = jnp.einsum("lhe,mhe->hlm", grad_low, values, preferred_element_type=F32)
    row_delta = jnp.sum(grad_low.astype(F32) * output_low.astype(F32), axis=-1)
    grad_scores = to_low(probs * (grad_probs - row_delta.T[:, :, None]) * score_scale)
    grad_queries = jnp.einsum("hlm,mhe->lhe", grad_scores, key_vecs, preferred_element_type=F32)
    grad_keys = jnp.einsum("hlm,lhe->mhe", grad_scores, queries, preferred_element_type=F32)
    return (grad_queries, grad_keys, grad_values)


def tile_blocks(qkv_block, out_block, up_block, down_block):
    tile_rows = qkv_block.shape[0]
    tile_cols = qkv_block.shape[2] // 2

    def split_cols(block_in):
        return block_in.reshape(
            block_in.shape[0], block_in.shape[1] // tile_cols, tile_cols
        ).transpose(1, 0, 2)

    down_part = down_block.reshape(
        down_block.shape[0] // tile_rows, tile_rows, down_block.shape[1] // tile_cols, tile_cols
    )
    down_part = down_part.transpose(0, 2, 1, 3).reshape(-1, tile_rows, tile_cols)
    return jnp.concatenate(
        [
            split_cols(qkv_block[:, 0]),
            split_cols(qkv_block[:, 1]),
            split_cols(qkv_block[:, 2]),
            split_cols(out_block),
            split_cols(up_block),
            down_part,
        ],
        axis=0,
    )


def pick(index, table):
    out = jnp.int32(table[0]) if isinstance(table[0], int) else table[0]
    for k in range(1, len(table)):
        out = jnp.where(index == k, table[k], out)
    return out


def far_order(c, n_col):
    far = [
        sorted(range(n_col), key=lambda f: (-abs(f - cc), f < cc if cc < n_col // 2 else f > cc))
        for cc in range(n_col)
    ]
    return [pick(c, [far[cc][i] for cc in range(n_col)]) for i in range(n_col)]


def forward_kernel(n_dp, n_row, n_col, dims,
                   x_ref, g_ref, wq_ref, wu_ref, wo_ref, wd_ref,
                   pos_ref, seg_ref, vec_ref,
                   gf, wi, wf, nt, hid_out, ht_out, qkv_out, up_out, cs_out, mean_ref, rstd_ref,
                   xv, ntv, wv, hid, ht, qkv, up, tab, mean_v, rstd_v, stage_g, stage_o, stage_d,
                   zs, zr, ys, yr, cs, cr, ws, wr, ds, dr, ls, lo, no):
    T, C, HF, UT = dims
    d, r, c = lax.axis_index("dp"), lax.axis_index("row"), lax.axis_index("col")
    r1 = r + 1 - 2 * lax.rem(r, 2)
    r2 = lax.rem(r + 2, n_row)
    chunks = 2
    tc = T // chunks
    qw = 3 * HF
    rows_all, D = n_row * T, n_col * C
    seqs = rows_all // SEQ_LEN
    acts = ((x_ref, xv), (g_ref, gf))
    forder = far_order(c, n_col)

    barrier = pltpu.get_barrier_semaphore()
    peers = [{"row": r1}, {"row": r2}]
    peers += [{"col": lax.rem(c + k, n_col)} for k in range(1, n_col)]
    peers += [{"dp": lax.rem(d + k, n_dp)} for k in range(1, n_dp)]
    for peer in peers:
        pl.semaphore_signal(barrier, inc=1, device_id=peer, device_id_type=MESH)
    pl.semaphore_wait(barrier, len(peers))

    def copy(src, dst, s, rcv, peer):
        return pltpu.make_async_remote_copy(
            src_ref=src, dst_ref=dst, send_sem=s, recv_sem=rcv, device_id=peer, device_id_type=MESH
        )

    def blk(a, rr, cc, t):
        return acts[a][1].at[pl.ds(pl.multiple_of(rr * T + t * tc, tc), tc),
                             pl.ds(pl.multiple_of(cc * C, C), C)]

    def own(a, t):
        return acts[a][0].at[pl.ds(t * tc, tc), :]

    def z_copy(a, t, cc, src, right):
        peer = {"col": c + 1} if right else {"col": c - 1}
        return copy(src, blk(a, r, cc, t), zs.at[a, t, int(right), cc], zr.at[a, t, cc], peer)

    def y_copy(a, t, cc, src):
        return copy(src, blk(a, r, cc, t), ys.at[a, t, cc], yr.at[a, t, cc], {"row": r2})

    def c_copy(a, t, cc, src, rr, which):
        return copy(
            src, blk(a, rr, cc, t), cs.at[a, t, which, cc], cr.at[a, t, which, cc], {"row": r1}
        )

    def send_own_z(a, t):
        @pl.when(c < n_col - 1)
        def _():
            z_copy(a, t, c, own(a, t), True).start()

        @pl.when(c > 0)
        def _():
            z_copy(a, t, c, own(a, t), False).start()

    def send_own_row(a, t):
        y_copy(a, t, c, own(a, t)).start()
        c_copy(a, t, c, own(a, t), r, 0).start()

    def relay(a, s, t):
        for right in (True, False):
            cc = c - s if right else c + s

            @pl.when((cc >= 0) & (cc < n_col))
            def _(cc=cc, right=right):
                z_copy(a, t, cc, blk(a, r, cc, t), right).wait_recv()

                @pl.when((c < n_col - 1) if right else (c > 0))
                def _():
                    z_copy(a, t, cc, blk(a, r, cc, t), right).start()

                y_copy(a, t, cc, blk(a, r, cc, t)).start()
                c_copy(a, t, cc, blk(a, r, cc, t), r, 0).start()

    def pass_row(a, s, t):
        for right in (True, False):
            cc = c - s if right else c + s
            ok = (cc >= 0) & (cc < n_col)
            if not right:
                ok = ok & (s > 0)

            @pl.when(ok)
            def _(cc=cc):
                y_copy(a, t, cc, blk(a, r, cc, t)).wait_recv()
                c_copy(a, t, cc, blk(a, r2, cc, t), r2, 1).start()

    ck, hk, uk = C // n_dp, HF // n_dp, UT // n_dp

    def w_dst(part, dd, cc):
        if part == 0:
            return wv.at[pl.ds(cc * C + dd * ck, ck), pl.ds(0, qw)]
        if part == 1:
            return wv.at[pl.ds(cc * C + dd * ck, ck), pl.ds(qw, UT)]
        if part == 2:
            return wv.at[pl.ds(cc * C + dd * ck, ck), pl.ds(qw + UT, UT)]
        if part == 3:
            return wf.at[pl.ds(dd * hk, hk), pl.ds(cc * C, C)]
        if part == 4:
            return wf.at[pl.ds(HF + dd * uk, uk), pl.ds(cc * C, C)]
        return wf.at[pl.ds(HF + UT + dd * uk, uk), pl.ds(cc * C, C)]

    def w_src(part, cc):
        if part == 0:
            return wq_ref.at[cc, pl.ds(d * ck, ck), :]
        if part == 1:
            return wu_ref.at[pl.ds(d * ck, ck), pl.ds(cc * UT, UT)]
        if part == 2:
            return wu_ref.at[pl.ds(d * ck, ck), pl.ds((n_col + cc) * UT, UT)]
        if part == 3:
            return wo_ref.at[pl.ds(cc * HF + d * hk, hk), :]
        if part == 4:
            return wd_ref.at[pl.ds(cc * UT + d * uk, uk), :]
        return wd_ref.at[pl.ds((n_col + cc) * UT + d * uk, uk), :]

    def w_copy(part, dest):
        return copy(
            w_src(part, dest), w_dst(part, d, c), ws.at[part, dest], wr.at[part, c], {"col": dest}
        )

    def w_from(part, source):
        return copy(
            w_src(part, source), w_dst(part, d, source), ws.at[part, source], wr.at[part, source],
            {"col": source},
        )

    def x_copy(part, source, j):
        got = w_dst(part, d, source)
        return copy(got, got, ds.at[part, source, j], dr.at[part, source, j],
                    {"dp": lax.rem(d + j, n_dp)})

    others = forder[: n_col - 1]

    def w_send(part):
        for dest in others:
            w_copy(part, dest).start()

    def w_pass(part):
        for source in others[::-1]:
            w_from(part, source).wait_recv()
            for j in range(1, n_dp):
                x_copy(part, source, j).start()

    def w_done(part):
        for source in others:
            for j in range(1, n_dp):
                x_copy(part, source, j).wait_recv()

    win, wfin = (0, 1, 2), (3, 4, 5)

    for t in range(chunks):
        send_own_z(0, t)
    for t in range(chunks):
        send_own_row(0, t)

    col_at = pl.ds(c * C, C)
    direct = [
        pltpu.make_async_copy(x_ref, xv.at[pl.ds(r * T, T), col_at], ls.at[0]),
        pltpu.make_async_copy(wq_ref.at[c], wv.at[col_at, pl.ds(0, qw)], ls.at[1]),
        pltpu.make_async_copy(wu_ref.at[:, pl.ds(c * UT, UT)], wv.at[col_at, pl.ds(qw, UT)],
                              ls.at[2]),
        pltpu.make_async_copy(wu_ref.at[:, pl.ds((n_col + c) * UT, UT)],
                              wv.at[col_at, pl.ds(qw + UT, UT)], ls.at[3]),
    ]
    loads = [
        pltpu.make_async_copy(g_ref, stage_g, ls.at[4]),
        pltpu.make_async_copy(wo_ref.at[pl.ds(c * HF, HF), :], stage_o, ls.at[5]),
        pltpu.make_async_copy(wd_ref.at[pl.ds(c * UT, UT), :], stage_d.at[0], ls.at[6]),
        pltpu.make_async_copy(wd_ref.at[pl.ds((n_col + c) * UT, UT), :], stage_d.at[1], ls.at[7]),
    ]
    stores = [
        pltpu.make_async_copy(stage_g, gf.at[pl.ds(r * T, T), col_at], lo.at[0]),
        pltpu.make_async_copy(stage_o, wf.at[pl.ds(0, HF), col_at], lo.at[1]),
        pltpu.make_async_copy(stage_d.at[0], wf.at[pl.ds(HF, UT), col_at], lo.at[2]),
        pltpu.make_async_copy(stage_d.at[1], wf.at[pl.ds(HF + UT, UT), col_at], lo.at[3]),
    ]
    for item in direct + loads:
        item.start()

    for n in range(1, n_col):
        for t in range(chunks):
            relay(0, n, t)
        w_send(win[n - 1])
    for t in range(chunks):
        send_own_z(1, t)
        send_own_row(1, t)
    for load, store in zip(loads, stores):
        load.wait()
        store.start()
    w_pass(win[0])

    place = lax.rem(lax.broadcasted_iota(jnp.int32, (1, 2 * HEAD_DIM), 1), HEAD_DIM)
    power = jnp.exp(
        lax.rem(place, ROTARY // 2).astype(F32) * (-2.0 * math.log(10000.0) / ROTARY)
    )
    freq = jnp.where(place < ROTARY, power, 0.0)

    def one_table(n, carry):
        rows = jnp.broadcast_to(pos_ref[pl.ds(n, 1), :].astype(F32), (2 * HEAD_DIM, SEQ_LEN))
        angle = jnp.transpose(rows) * freq
        lane = lax.broadcasted_iota(jnp.int32, angle.shape, 1)
        turns = jnp.floor(angle * (2.0 / math.pi) + 0.5)
        rest = angle - turns * 1.5703125
        rest = rest - turns * 4.837512969970703125e-4
        rest = rest - turns * 7.54978994889188e-8
        sq = rest * rest
        sine = rest + rest * sq * (
            -1.6666654611e-1 + sq * (8.3321608736e-3 - sq * 1.9515295891e-4)
        )
        cosine = 1.0 - 0.5 * sq + sq * sq * (
            4.166664568298827e-2 + sq * (-1.388731625493765e-3 + sq * 2.443315711809948e-5)
        )
        quarter = jnp.where(lane < HEAD_DIM, turns, turns - 1.0)
        quarter = quarter - 4.0 * jnp.floor(quarter * 0.25)
        odd = (quarter == 1.0) | (quarter == 3.0)
        value = jnp.where(odd, sine, cosine)
        value = jnp.where((quarter == 1.0) | (quarter == 2.0), -value, value)
        tab[pl.ds(pl.multiple_of(n * SEQ_LEN, SEQ_LEN), SEQ_LEN), :] = value
        return carry

    lax.fori_loop(0, seqs, one_table, 0)
    keep_cs = pltpu.make_async_copy(tab, cs_out, no.at[2])
    keep_cs.start()
    for n in range(n_col):
        for t in range(chunks):
            pass_row(0, n, t)
    w_pass(win[1])
    for item in direct:
        item.wait()
    for t in range(chunks):
        for cc in range(n_col):
            c_copy(0, t, cc, blk(0, r, cc, t), r, 0).wait_recv()
            c_copy(0, t, cc, blk(0, r, cc, t), r, 1).wait_recv()

    def act_sent(a):
        for t in range(chunks):
            for cc in range(n_col):
                @pl.when((cc <= c) & (c < n_col - 1))
                def _(t=t, cc=cc):
                    z_copy(a, t, cc, blk(a, r, cc, t), True).wait_send()

                @pl.when((cc >= c) & (c > 0))
                def _(t=t, cc=cc):
                    z_copy(a, t, cc, blk(a, r, cc, t), False).wait_send()

                y_copy(a, t, cc, blk(a, r, cc, t)).wait_send()
                c_copy(a, t, cc, blk(a, r, cc, t), r, 0).wait_send()
                c_copy(a, t, cc, blk(a, r, cc, t), r, 1).wait_send()

    act_sent(0)

    tile = 256
    tiles = rows_all // tile
    sub = 16

    def norm_tile(i, carry):
        base = pl.multiple_of(i * tile, tile)

        def norm_rows(k, inner):
            at = pl.ds(pl.multiple_of(base + k * sub, sub), sub)
            val = xv[at, :].astype(F32)
            mean = jnp.sum(val, axis=1, keepdims=True) / D
            var = jnp.sum(val * val, axis=1, keepdims=True) / D - mean * mean
            rstd = lax.rsqrt(var + NORM_EPS)
            mean_v[at, :] = mean
            rstd_v[at, :] = rstd
            xv[at, :] = ((val - mean) * rstd * vec_ref[5:6, :] + vec_ref[6:7, :]).astype(BF16)
            return inner

        lax.fori_loop(0, tile // sub, norm_rows, 0)
        at = pl.ds(base, tile)
        for k in range(D // tile):
            ntv[k * tile : (k + 1) * tile, at] = jnp.transpose(xv[at, k * tile : (k + 1) * tile])
        return carry

    lax.fori_loop(0, tiles // 2, norm_tile, 0)
    w_pass(win[2])
    for t in range(chunks):
        relay(1, 1, t)
    w_send(wfin[0])
    lax.fori_loop(tiles // 2, tiles, norm_tile, 0)
    keep_norm = pltpu.make_async_copy(ntv, nt, no.at[1])
    keep_norm.start()
    own_rows = pl.ds(pl.multiple_of(r * T, T), T)
    mean_ref[...] = mean_v[own_rows, :]
    rstd_ref[...] = rstd_v[own_rows, :]
    for part in win:
        w_done(part)
    keep_w = pltpu.make_async_copy(wv, wi, no.at[0])
    keep_w.start()

    q_lanes = pl.ds(pl.multiple_of((r * n_col + c) * HF, HF), HF)
    biases = [vec_ref[j : j + 1, q_lanes] for j in range(3)]
    biases += [
        vec_ref[pl.ds(7 + r, 1), pl.ds(pl.multiple_of((m * n_col + c) * UT, UT), UT)]
        for m in range(2)
    ]
    bias = jnp.concatenate(biases, axis=1)

    def one_tile(i, carry):
        at = pl.ds(pl.multiple_of(i * tile, tile), tile)
        mixed = jnp.dot(xv[at, :], wv[...], preferred_element_type=F32) + bias
        cos, sin = wide_tables(tab[at, :])
        for j in range(2):
            part = mixed[:, j * HF : (j + 1) * HF]
            qkv[at, j * HF : (j + 1) * HF] = turn(part, cos, sin, 1.0).astype(BF16)
        qkv[at, 2 * HF : 3 * HF] = mixed[:, 2 * HF : 3 * HF].astype(BF16)
        pre = mixed[:, qw:]
        up[at, :] = pre
        act = gelu_value(pre).astype(BF16)
        hid[at, HF:] = act
        ht[HF:, at] = jnp.transpose(act)

        s, t = 2 + lax.div(i, 2), lax.rem(i, 2)

        @pl.when(s < n_col)
        def _():
            relay(1, s, t)

        return carry

    lax.fori_loop(0, 2, one_tile, 0)
    w_send(wfin[1])
    lax.fori_loop(2, 4, one_tile, 0)
    w_send(wfin[2])
    lax.fori_loop(4, tiles, one_tile, 0)
    keep_up = pltpu.make_async_copy(up, up_out, no.at[3])
    keep_qkv = pltpu.make_async_copy(qkv, qkv_out, no.at[4])
    keep_up.start()
    keep_qkv.start()

    heads = HF // HEAD_DIM
    qt = SEQ_LEN // 2

    def one_seq(s, carry):
        base = pl.multiple_of(s * SEQ_LEN, SEQ_LEN)
        lane = lax.broadcasted_iota(jnp.int32, (qt, HF), 1)
        seg = seg_ref[pl.ds(s, 1), :]
        seg_col = jnp.transpose(jnp.broadcast_to(seg, (128, SEQ_LEN)))[:, 0:1]
        for qi in range(2):
            width = (qi + 1) * qt
            q_at = pl.ds(pl.multiple_of(base + qi * qt, qt), qt)
            k_at = pl.ds(base, width)
            allowed = (seg_col[qi * qt : (qi + 1) * qt, :] == seg[:, 0:width]) & (
                lax.broadcasted_iota(jnp.int32, (qt, width), 0) + qi * qt
                >= lax.broadcasted_iota(jnp.int32, (qt, width), 1)
            )
            keys, vals = qkv[k_at, HF : 2 * HF], qkv[k_at, 2 * HF : 3 * HF]
            queries = qkv[q_at, 0:HF]
            total = None
            for h in range(heads):
                mine = lax.div(lane, HEAD_DIM) == h
                scores = lax.dot_general(
                    jnp.where(mine, queries, jnp.zeros_like(queries)), keys,
                    (((1,), (1,)), ((), ())), preferred_element_type=F32,
                ) * (HEAD_DIM ** (-0.5))
                scores = jnp.where(allowed, scores, MASKED_SCORE)
                peak = jnp.max(scores, axis=1, keepdims=True)
                weight = jnp.exp(scores - peak)
                weight_sum = jnp.sum(weight, axis=1, keepdims=True)
                probs = (weight * (1.0 / weight_sum)).astype(BF16)
                out = jnp.dot(probs, vals, preferred_element_type=F32)
                total = out if h == 0 else jnp.where(mine, out, total)
            low = total.astype(BF16)
            hid[q_at, 0:HF] = low
            ht[0:HF, q_at] = jnp.transpose(low)

        @pl.when(s < n_col)
        def _():
            for t in range(chunks):
                pass_row(1, s, t)

        return carry

    lax.fori_loop(0, seqs, one_seq, 0)
    keep_hid = pltpu.make_async_copy(hid, hid_out, no.at[5])
    keep_ht = pltpu.make_async_copy(ht, ht_out, no.at[6])
    keep_hid.start()
    keep_ht.start()
    for part in wfin:
        w_pass(part)

    for t in range(chunks):
        for cc in range(n_col):
            c_copy(1, t, cc, blk(1, r, cc, t), r, 0).wait_recv()
            c_copy(1, t, cc, blk(1, r, cc, t), r, 1).wait_recv()
    for part in wfin:
        w_done(part)
    act_sent(1)
    for part in win + wfin:
        for peer in others:
            w_copy(part, peer).wait_send()
            for j in range(1, n_dp):
                x_copy(part, peer, j).wait_send()
    for store in stores:
        store.wait()
    for item in (keep_w, keep_norm, keep_cs, keep_up, keep_qkv, keep_hid, keep_ht):
        item.wait()


def forward_all(x, g, w_q, w_up, w_out, w_down, pos_row, seg_row, vectors,
                n_dp, n_row, n_col):
    T, C = x.shape
    HF = w_q.shape[2] // 3
    UT = w_up.shape[1] // (2 * n_col)
    n_in, n_out = 3 * HF + 2 * UT, HF + 2 * UT
    rows, D = n_row * T, n_col * C
    dma = pltpu.SemaphoreType.DMA
    vm = pl.BlockSpec(memory_space=pltpu.VMEM)
    sds = jax.ShapeDtypeStruct
    return pl.pallas_call(
        functools.partial(forward_kernel, n_dp, n_row, n_col, (T, C, HF, UT)),
        name="forward_all",
        out_shape=(
            sds((rows, D), BF16),
            sds((D, n_in), BF16),
            sds((n_out, D), BF16),
            sds((D, rows), BF16),
            sds((rows, n_out), BF16),
            sds((n_out, rows), BF16),
            sds((rows, 3 * HF), BF16),
            sds((rows, 2 * UT), F32),
            sds((rows, 2 * HEAD_DIM), F32),
            sds((T, 1), F32),
            sds((T, 1), F32),
        ),
        in_specs=[ANY] * 6 + [vm] * 3,
        out_specs=(ANY,) * 9 + (vm,) * 2,
        scratch_shapes=[
            pltpu.VMEM((rows, D), BF16),
            pltpu.VMEM((D, rows), BF16),
            pltpu.VMEM((D, n_in), BF16),
            pltpu.VMEM((rows, n_out), BF16),
            pltpu.VMEM((n_out, rows), BF16),
            pltpu.VMEM((rows, 3 * HF), BF16),
            pltpu.VMEM((rows, 2 * UT), F32),
            pltpu.VMEM((rows, 2 * HEAD_DIM), F32),
            pltpu.VMEM((rows, 1), F32),
            pltpu.VMEM((rows, 1), F32),
            pltpu.VMEM((T, C), BF16),
            pltpu.VMEM((HF, C), BF16),
            pltpu.VMEM((2, UT, C), BF16),
            dma((2, 2, 2, n_col)),
            dma((2, 2, n_col)),
            dma((2, 2, n_col)),
            dma((2, 2, n_col)),
            dma((2, 2, 2, n_col)),
            dma((2, 2, 2, n_col)),
            dma((6, n_col)),
            dma((6, n_col)),
            dma((6, n_col, n_dp)),
            dma((6, n_col, n_dp)),
            dma((8,)),
            dma((4,)),
            dma((7,)),
        ],
        compiler_params=pltpu.CompilerParams(
            collective_id=0, has_side_effects=True, vmem_limit_bytes=60 * 1024 * 1024
        ),
    )(x, g, w_q, w_up, w_out, w_down, pos_row, seg_row, vectors)


def wide_tables(packed):
    lane = lax.broadcasted_iota(jnp.int32, packed.shape, 1)
    turned = pltpu.roll(packed, HEAD_DIM, 1)
    first = lane < HEAD_DIM
    return jnp.where(first, packed, turned), jnp.where(first, turned, packed)


def turn(part, cos, sin, sign):
    lane = lax.rem(lax.broadcasted_iota(jnp.int32, part.shape, 1), HEAD_DIM)
    ahead = pltpu.roll(part, part.shape[1] - ROTARY // 2, 1)
    behind = pltpu.roll(part, ROTARY // 2, 1)
    return part * cos + jnp.where(lane < ROTARY // 2, -ahead, behind) * (sign * sin)


def backward_kernel(n_row, n_col, dims,
                    hid_ref, ht_ref, c_ref, wf_ref, wi_ref, nt_ref, qkv_ref, up_ref,
                    cs_ref, seg_ref,
                    res_ref, gn_ref, tiles_ref, part_ref,
                    hd, hts, big, wf, wi, qv, ups, ga,
                    abuf, obuf, asb, sbuf, bbuf, zsb, zin,
                    dwf, dwi, gf, gu, gk,
                    l_s, h_s, u_s, a_s, a_r, y_s, y_r, z_s, z_r, xf_s, xf_r, xu_s, xu_r, xk_s, xk_r,
                    t_s, t_r, free_row, free_col):
    T, C, HF, UT = dims
    rows_all, D = n_row * T, n_col * C
    qw, n_in, n_out = 3 * HF, 3 * HF + 2 * UT, HF + 2 * UT
    step_rows = 64
    d, r, c = lax.axis_index("dp"), lax.axis_index("row"), lax.axis_index("col")
    r1 = r + 1 - 2 * lax.rem(r, 2)
    r2 = lax.rem(r + 2, n_row)
    r12 = lax.rem(r1 + 2, n_row)
    forder = far_order(c, n_col)
    outs = (res_ref, gn_ref)

    barrier = pltpu.get_barrier_semaphore()
    peers = [{"row": r1}, {"row": r2}, {"dp": 1 - d}]
    peers += [{"col": lax.rem(c + k, n_col)} for k in range(1, n_col)]
    for peer in peers:
        pl.semaphore_signal(barrier, inc=1, device_id=peer, device_id_type=MESH)

    loads = [
        pltpu.make_async_copy(hid_ref, hd.at[:, pl.ds(2 * HF, n_out)], l_s.at[0]),
        pltpu.make_async_copy(wf_ref, wf, l_s.at[1]),
        pltpu.make_async_copy(c_ref, big, l_s.at[2]),
        pltpu.make_async_copy(qkv_ref, qv, l_s.at[3]),
        pltpu.make_async_copy(wi_ref, wi, l_s.at[4]),
    ]
    for item in loads:
        item.start()
    load_nt = pltpu.make_async_copy(nt_ref, big, l_s.at[5])

    def load_ht(m, slot):
        return pltpu.make_async_copy(ht_ref.at[pl.ds(pl.multiple_of(m * HF, HF), HF), :],
                                     hts.at[slot], h_s.at[slot])

    tile = 256

    def load_up(i, slot):
        return pltpu.make_async_copy(up_ref.at[pl.ds(pl.multiple_of(i * tile, tile), tile), :],
                                     ups.at[slot], u_s.at[slot])

    load_ht(0, 0).start()
    load_up(0, 0).start()
    pl.semaphore_wait(barrier, len(peers))

    def copy(src, dst, s, rcv, peer):
        return pltpu.make_async_remote_copy(
            src_ref=src, dst_ref=dst, send_sem=s, recv_sem=rcv, device_id=peer, device_id_type=MESH
        )

    def a_copy(v, h, f):
        return copy(asb.at[h, f], abuf.at[v, h, f], a_s.at[h, f], a_r.at[v, h, f], {"row": r1})

    def y_copy(f):
        return copy(sbuf.at[f], bbuf.at[f], y_s.at[f], y_r.at[f], {"row": r2})

    def z_copy(f, slot, step):
        return copy(zsb.at[f], zin.at[slot], z_s.at[f], z_r.at[slot], {"col": c + step})

    def looped(rows, fn):
        def one(k, carry):
            fn(pl.ds(pl.multiple_of(k * step_rows, step_rows), step_rows))
            return carry
        lax.fori_loop(0, rows // step_rows, one, 0)

    def first_sum(v, f):
        a_copy(v, 1, f).wait_recv()
        if v == 1:
            y_copy(f).wait_send()

        def add(rows):
            sbuf[f, rows, :] = (
                obuf[1, f, rows, :].astype(F32) + abuf[v, 1, f, rows, :].astype(F32)
            ).astype(BF16)

        looped(T, add)
        if v == 1:
            pl.semaphore_wait(free_row.at[f], 1)
        y_copy(f).start()

    def release(f, peer):
        pl.semaphore_signal(free_col.at[f], inc=1, device_id={"col": peer}, device_id_type=MESH)

    def second_sum(v, i):
        f = forder[i]
        a_copy(v, 0, f).wait_recv()
        y_copy(f).wait_recv()

        def base(rows):
            return (
                obuf[0, f, rows, :].astype(F32)
                + abuf[v, 0, f, rows, :].astype(F32)
                + bbuf[f, rows, :].astype(F32)
            )

        if i < n_col - 1:
            right = f > c
            step = jnp.where(right, jnp.int32(1), jnp.int32(-1))
            landed = jnp.where(f == c + step, jnp.where(right, f, jnp.int32(n_col)), f)
            inner = jnp.where(right, c, n_col - 1 - c) > 0
            if v == 1:
                z_copy(f, f, 0).wait_send()

            @pl.when(inner)
            def _():
                z_copy(f, f, 0).wait_recv()

                def add(rows):
                    zsb[f, rows, :] = (base(rows) + zin[f, rows, :].astype(F32)).astype(BF16)

                looped(T, add)
                if v == 0:
                    release(f, c - step)

            @pl.when(jnp.logical_not(inner))
            def _():
                def add(rows):
                    zsb[f, rows, :] = base(rows).astype(BF16)

                looped(T, add)

            if v == 1:
                pl.semaphore_wait(free_col.at[f], 1)
            z_copy(f, landed, step).start()
        else:
            out = outs[v]

            @pl.when(c > 0)
            def _():
                z_copy(f, f, 0).wait_recv()

            @pl.when(c < n_col - 1)
            def _():
                z_copy(f, n_col, 0).wait_recv()

            def put(rows, value):
                out[rows, :] = value

            @pl.when(c == 0)
            def _():
                looped(T, lambda rows: put(rows, base(rows) + zin[n_col, rows, :].astype(F32)))

            @pl.when(c == n_col - 1)
            def _():
                looped(T, lambda rows: put(rows, base(rows) + zin[f, rows, :].astype(F32)))

            @pl.when((c > 0) & (c < n_col - 1))
            def _():
                looped(T, lambda rows: put(
                    rows,
                    base(rows) + zin[f, rows, :].astype(F32) + zin[n_col, rows, :].astype(F32)))

            if v == 0:
                @pl.when(c > 0)
                def _():
                    release(f, c - 1)

                @pl.when(c < n_col - 1)
                def _():
                    release(f, c + 1)

        if v == 0:
            pl.semaphore_signal(free_row.at[f], inc=1, device_id={"row": r2}, device_id_type=MESH)

    tall = (HF, 2 * UT)
    row0 = (0, HF)
    lane_u = (qw, qw + UT)
    lw = 2 * HF

    def xf_copy(own, b):
        return copy(dwf.at[pl.ds(row0[own] + b * HF, HF), :], gf.at[pl.ds(b * HF, HF), :],
                    xf_s.at[own, b], xf_r.at[b], {"dp": 1 - d})

    def xu_copy(own, cc):
        return copy(dwi.at[pl.ds(cc * C, C), pl.ds(lane_u[own], UT)], gu.at[cc],
                    xu_s.at[own, cc], xu_r.at[cc], {"dp": 1 - d})

    def xk_copy(cc):
        return copy(dwi.at[pl.ds(cc * C, C), pl.ds(0, qw)], gk.at[cc], xk_s.at[cc], xk_r.at[cc],
                    {"dp": 1 - d})

    def parts_f(own, cc, source):
        half, odd = lax.div(source, 2), lax.rem(source, 2)
        at = cc * C
        if own == 0:
            return [
                (dwf.at[pl.ds(0, HF), pl.ds(at + j * lw, lw)],
                 tiles_ref.at[6 + j, pl.ds(source * HF, HF), :])
                for j in range(2)
            ]
        return [
            (dwf.at[pl.ds(HF, UT), pl.ds(at + j * lw, lw)],
             tiles_ref.at[4 + 2 * half + j, pl.ds(odd * UT, UT), :])
            for j in range(2)
        ]

    def parts_e(own, cc, source):
        half, odd = lax.div(source, 2), lax.rem(source, 2)
        at = cc * C
        return [
            (dwf.at[pl.ds(HF + UT, UT), pl.ds(at + j * lw, lw)],
             tiles_ref.at[8 + 2 * half + j, pl.ds(odd * UT, UT), :])
            for j in range(2)
        ]

    def parts_u(own, cc, source):
        dst = tiles_ref.at[8 + source] if own == 0 else tiles_ref.at[source]
        return [(dwi.at[pl.ds(cc * C, C), pl.ds(lane_u[own], UT)], dst)]

    def parts_k(own, cc, source):
        half, odd = lax.div(source, 2), lax.rem(source, 2)
        return [
            (dwi.at[pl.ds(cc * C, C), pl.ds(j * HF, HF)],
             tiles_ref.at[2 * j + half, :, pl.ds(odd * HF, HF)])
            for j in range(3)
        ]

    kinds = {"f": (parts_f, 0), "e": (parts_e, 2), "u": (parts_u, 4), "k": (parts_k, 5)}

    def t_send(kind, own, cc):
        parts, first = kinds[kind]
        return [
            copy(src, dst, t_s.at[first + n, cc], t_r.at[first + n, c], {"col": cc})
            for n, (src, dst) in enumerate(parts(own, cc, c))
        ]

    def t_wait(kind, own, source):
        parts, first = kinds[kind]
        return [
            copy(src, dst, t_s.at[first + n, source], t_r.at[first + n, source], {"col": source})
            for n, (src, dst) in enumerate(parts(own, source, source))
        ]

    def t_local(kind, own):
        parts, first = kinds[kind]
        return [
            pltpu.make_async_copy(src, dst, t_s.at[first + n, c])
            for n, (src, dst) in enumerate(parts(own, c, c))
        ]

    def owned_kinds(own):
        return ("f", "u", "k") if own == 0 else ("f", "e", "u")

    def spread(kind, own):
        for k in range(1, n_col):
            for item in t_send(kind, own, lax.rem(c + k, n_col)):
                item.start()
        for item in t_local(kind, own):
            item.start()

    def add_rows(own, first, count):
        for b in range(first, first + count):
            xf_copy(own, b).wait_recv()

        def add(rows):
            here = pl.ds(pl.multiple_of(rows.start + first * HF, step_rows), step_rows)
            at = (pl.ds(pl.multiple_of(rows.start + row0[own] + first * HF, step_rows), step_rows),
                  slice(None))
            dwf[at] = (dwf[at].astype(F32) + gf[here, :].astype(F32)).astype(BF16)

        looped(count * HF, add)

    def add_f():
        for own in range(2):
            @pl.when(d == own)
            def _(own=own):
                add_rows(own, 0, 1 if own == 0 else UT // HF)
                spread("f", own)

    def add_e():
        @pl.when(d == 1)
        def _():
            add_rows(1, UT // HF, UT // HF)
            spread("e", 1)

    def add_piece(kind, own, cc):
        lane, width, buf, waiter = (
            (lane_u[own], UT, gu, xu_copy(own, cc)) if kind == "u" else (0, qw, gk, xk_copy(cc))
        )
        waiter.wait_recv()

        def add(rows):
            at = (pl.ds(pl.multiple_of(rows.start + cc * C, step_rows), step_rows),
                  pl.ds(lane, width))
            dwi[at] = (dwi[at].astype(F32) + buf[cc, rows, :].astype(F32)).astype(BF16)

        looped(C, add)

    def add_w(i):
        for own in range(2):
            @pl.when(d == own)
            def _(own=own):
                cc = forder[i]
                for kind in ("k", "u") if own == 0 else ("u",):
                    add_piece(kind, own, cc)
                    for item in t_local(kind, own) if i == n_col - 1 else t_send(kind, own, cc):
                        item.start()

    loads[0].wait()
    loads[1].wait()

    def p_unit(rr, f):
        at = pl.ds(pl.multiple_of(rr * T, T), T)
        lanes = pl.ds(pl.multiple_of(f * C, C), C)
        return jnp.dot(hd[at, 2 * HF :], wf[:, lanes], preferred_element_type=F32).astype(BF16)

    def p_step(i, carry):
        f = pick(i, forder)
        for h, rr in ((1, r12), (0, r1)):
            asb[h, f] = p_unit(rr, f)
            a_copy(0, h, f).start()
        for h, rr in ((1, r2), (0, r)):
            obuf[h, f] = p_unit(rr, f)

        @pl.when(i > 0)
        def _():
            first_sum(0, pick(i - 1, forder))

        return carry

    lax.fori_loop(0, n_col, p_step, 0)

    loads[2].wait()
    blocks = n_out // HF

    def f_step(m, carry):
        slot = lax.rem(m, 2)
        load_ht(m, slot).wait()

        @pl.when(m + 1 < blocks)
        def _():
            load_ht(m + 1, 1 - slot).start()

        at = pl.ds(pl.multiple_of(m * HF, HF), HF)
        dwf[at, :] = jnp.dot(hts[slot], big[...], preferred_element_type=F32).astype(BF16)

        @pl.when((m == 0) & (d == 1))
        def _():
            xf_copy(0, 0).start()

        @pl.when((m > 0) & (d == 0))
        def _():
            xf_copy(1, m - 1).start()

        return carry

    early = 1 + UT // HF
    first_sum(0, forder[n_col - 1])
    lax.fori_loop(0, early, f_step, 0)

    part_ref[...] = jnp.zeros_like(part_ref)
    tiles = rows_all // tile

    def b_step(i, carry):
        slot = lax.rem(i, 2)
        load_up(i, slot).wait()

        @pl.when(i + 1 < tiles)
        def _():
            load_up(i + 1, 1 - slot).start()

        at = pl.ds(pl.multiple_of(i * tile, tile), tile)
        back = lax.dot_general(
            big[at, :], wf[...], (((1,), (1,)), ((), ())), preferred_element_type=F32
        )
        ga[at, :] = back[:, :HF].astype(BF16)
        grad = back[:, HF:] * gelu_slope(ups[slot])
        hd[at, qw:] = grad.astype(BF16)
        sums = jnp.sum(grad, axis=0, keepdims=True)
        for k in range(2 * UT // 128):
            part_ref[3 + k : 4 + k, :] += sums[:, k * 128 : (k + 1) * 128]
        return carry

    lax.fori_loop(0, tiles, b_step, 0)
    load_nt.start()
    second_sum(0, 0)

    loads[3].wait()
    loads[4].wait()
    heads = HF // HEAD_DIM
    qt = SEQ_LEN // 2
    scale = HEAD_DIM ** (-0.5)
    per_row = T // SEQ_LEN
    first_dim = (((0,), (0,)), ((), ()))
    last_dim = (((1,), (1,)), ((), ()))

    def attend_seq(s):
        base = pl.multiple_of(s * SEQ_LEN, SEQ_LEN)
        lane = lax.broadcasted_iota(jnp.int32, (qt, HF), 1)
        seg = seg_ref[pl.ds(s, 1), :]
        seg_col = jnp.transpose(jnp.broadcast_to(seg, (128, SEQ_LEN)))[:, 0:1]
        grad_q, grad_k, grad_v = [], None, None
        for qi in range(2):
            width = (qi + 1) * qt
            q_at = pl.ds(base + qi * qt, qt)
            k_at = pl.ds(base, width)
            allowed = (seg_col[qi * qt : (qi + 1) * qt, :] == seg[:, 0:width]) & (
                lax.broadcasted_iota(jnp.int32, (qt, width), 0) + qi * qt
                >= lax.broadcasted_iota(jnp.int32, (qt, width), 1)
            )
            queries, g_att = qv[q_at, 0:HF], ga[q_at, :]
            keys, vals = qv[k_at, HF : 2 * HF], qv[k_at, 2 * HF : 3 * HF]
            both = g_att.astype(F32) * hd[q_at, 2 * HF : 3 * HF].astype(F32)
            gq, gks, gvs = None, None, None
            for h in range(heads):
                mine = lax.div(lane, HEAD_DIM) == h
                q_h = jnp.where(mine, queries, jnp.zeros_like(queries))
                g_h = jnp.where(mine, g_att, jnp.zeros_like(g_att))
                scores = lax.dot_general(q_h, keys, last_dim, preferred_element_type=F32) * scale
                scores = jnp.where(allowed, scores, MASKED_SCORE)
                peak = jnp.max(scores, axis=1, keepdims=True)
                weight = jnp.exp(scores - peak)
                probs = weight * (1.0 / jnp.sum(weight, axis=1, keepdims=True))
                delta = jnp.sum(jnp.where(mine, both, 0.0), axis=1, keepdims=True)
                g_prob = lax.dot_general(g_h, vals, last_dim, preferred_element_type=F32)
                g_score = (probs * (g_prob - delta) * scale).astype(BF16)
                gq_h = jnp.dot(g_score, keys, preferred_element_type=F32)
                gk_h = lax.dot_general(g_score, q_h, first_dim, preferred_element_type=F32)
                gv_h = lax.dot_general(probs.astype(BF16), g_h, first_dim,
                                       preferred_element_type=F32)
                gq = gq_h if h == 0 else jnp.where(mine, gq_h, gq)
                gks = gk_h if h == 0 else gks + gk_h
                gvs = gv_h if h == 0 else gvs + gv_h
            grad_q.append(gq)
            if qi == 0:
                grad_k, grad_v = gks, gvs
            else:
                grad_k = jnp.concatenate([grad_k + gks[:qt], gks[qt:]], axis=0)
                grad_v = jnp.concatenate([grad_v + gvs[:qt], gvs[qt:]], axis=0)
        s_at = pl.ds(base, SEQ_LEN)
        cos, sin = wide_tables(cs_ref[s_at, :])
        grads = (
            turn(jnp.concatenate(grad_q, axis=0), cos, sin, -1.0),
            turn(grad_k, cos, sin, -1.0),
            grad_v,
        )
        for j, grad in enumerate(grads):
            part_ref[j : j + 1, :] += jnp.sum(grad, axis=0, keepdims=True)
            hd[s_at, j * HF : (j + 1) * HF] = grad.astype(BF16)

    def q_unit(rr, f):
        at = pl.ds(pl.multiple_of(rr * T, T), T)
        feats = pl.ds(pl.multiple_of(f * C, C), C)
        return lax.dot_general(
            hd[at, :], wi[feats, :], last_dim, preferred_element_type=F32
        ).astype(BF16)

    def seq_step(s, carry):
        attend_seq(s)
        return carry

    lax.fori_loop(0, rows_all // SEQ_LEN, seq_step, 0)
    second_sum(0, 1)
    load_nt.wait()

    half_rows = C // 2

    def w_step(i, carry):
        cc = pick(lax.div(i, 2), forder)
        at = pl.ds(pl.multiple_of(cc * C + lax.rem(i, 2) * half_rows, half_rows), half_rows)
        dwi[at, :] = jnp.dot(big[at, :], hd[...], preferred_element_type=F32).astype(BF16)

        @pl.when(lax.rem(i, 2) == 1)
        def _():
            for own in range(2):
                @pl.when(d == own)
                def _(own=own):
                    if own == 1:
                        xk_copy(cc).start()
                    xu_copy(1 - own, cc).start()

        return carry

    lax.fori_loop(0, n_col, w_step, 0)
    second_sum(0, 2)
    lax.fori_loop(n_col, 2 * n_col, w_step, 0)
    load_c = pltpu.make_async_copy(c_ref, big, l_s.at[2])
    load_c.start()

    def q_step(h, rows_peer, rows_own):
        def units(i, carry):
            f = pick(i, forder)
            a_copy(0, h, f).wait_send()
            asb[h, f] = q_unit(rows_peer, f)
            a_copy(1, h, f).start()
            obuf[h, f] = q_unit(rows_own, f)
            return carry

        lax.fori_loop(0, n_col, units, 0)

    q_step(1, r12, r2)
    for i in range(n_col - 1):
        first_sum(1, forder[i])
    add_f()
    load_c.wait()
    lax.fori_loop(early, blocks, f_step, 0)
    second_sum(0, n_col - 1)
    first_sum(1, forder[n_col - 1])
    add_w(0)
    q_step(0, r1, r)
    add_w(1)
    second_sum(1, 0)
    add_w(2)
    second_sum(1, 1)
    add_e()
    second_sum(1, 2)
    add_w(3)
    second_sum(1, n_col - 1)

    for own in range(2):
        @pl.when(d == own)
        def _(own=own):
            for kind in owned_kinds(own):
                for k in range(1, n_col):
                    for item in t_wait(kind, own, lax.rem(c + k, n_col)):
                        item.wait_recv()
                for k in range(1, n_col):
                    for item in t_send(kind, own, lax.rem(c + k, n_col)):
                        item.wait_send()
                for item in t_local(kind, own):
                    item.wait()
            for b in range(tall[1 - own] // HF):
                xf_copy(1 - own, b).wait_send()
            for cc in range(n_col):
                xu_copy(1 - own, cc).wait_send()
                if own == 1:
                    xk_copy(cc).wait_send()
    for f in range(n_col):
        a_copy(1, 0, f).wait_send()
        a_copy(1, 1, f).wait_send()
        y_copy(f).wait_send()
    for i in range(n_col - 1):
        z_copy(forder[i], forder[i], 0).wait_send()


def backward_all(hid, ht, cot, w_fin, w_in, nt, qkv, up, packed, seg_row, T, C, HF, UT, n_row, n_col):
    dma = pltpu.SemaphoreType.DMA
    vm = pl.BlockSpec(memory_space=pltpu.VMEM)
    rows, D = n_row * T, n_col * C
    n_in, n_out = 3 * HF + 2 * UT, HF + 2 * UT
    unit = (T, C)
    V = pltpu.VMEM
    return pl.pallas_call(
        functools.partial(backward_kernel, n_row, n_col, (T, C, HF, UT)),
        name="backward_all",
        out_shape=(
            jax.ShapeDtypeStruct(unit, F32),
            jax.ShapeDtypeStruct(unit, F32),
            jax.ShapeDtypeStruct((12, C, UT), BF16),
            jax.ShapeDtypeStruct((8, 128), F32),
        ),
        in_specs=[ANY] * 8 + [vm] * 2,
        out_specs=(vm, vm, ANY, vm),
        scratch_shapes=[
            V((rows, n_in), BF16),
            V((2, HF, rows), BF16),
            V((rows, D), BF16),
            V((n_out, D), BF16),
            V((D, n_in), BF16),
            V((rows, 3 * HF), BF16),
            V((2, 256, 2 * UT), F32),
            V((rows, HF), BF16),
            V((2, 2, n_col) + unit, BF16),
            V((2, n_col) + unit, BF16),
            V((2, n_col) + unit, BF16),
            V((n_col,) + unit, BF16),
            V((n_col,) + unit, BF16),
            V((n_col,) + unit, BF16),
            V((n_col + 1,) + unit, BF16),
            V((n_out, D), BF16),
            V((D, n_in), BF16),
            V((2 * UT, D), BF16),
            V((n_col, C, UT), BF16),
            V((n_col, C, 3 * HF), BF16),
            dma((6,)),
            dma((2,)),
            dma((2,)),
            dma((2, n_col)),
            dma((2, 2, n_col)),
            dma((n_col,)),
            dma((n_col,)),
            dma((n_col,)),
            dma((n_col + 1,)),
            dma((2, 2 * UT // HF)),
            dma((2 * UT // HF,)),
            dma((2, n_col)),
            dma((n_col,)),
            dma((n_col,)),
            dma((n_col,)),
            dma((8, n_col)),
            dma((8, n_col)),
            pltpu.SemaphoreType.REGULAR((n_col,)),
            pltpu.SemaphoreType.REGULAR((n_col,)),
        ],
        compiler_params=pltpu.CompilerParams(
            collective_id=1, has_side_effects=True, vmem_limit_bytes=67043328
        ),
    )(hid, ht, cot, w_fin, w_in, nt, qkv, up, packed, seg_row)


def finish_kernel(n_dp, n_row, n_col, width, *refs):
    hbm, (gx_ref, va_ref, vb_ref), local = refs[:7], refs[7:10], refs[10:17]
    gn_ref, x_ref, g_ref, mean_ref, rstd_ref, gain_ref, part_ref = local
    l_s, st, da, db, ra, rb, st_s, st_r, d_s, d_r, r_s, r_r, c_s, c_r = refs[17:]
    loads = [
        pltpu.make_async_copy(src, dst, l_s.at[n]) for n, (src, dst) in enumerate(zip(hbm, local))
    ]
    for item in loads:
        item.start()
    d, r, c = lax.axis_index("dp"), lax.axis_index("row"), lax.axis_index("col")
    T, C = gn_ref.shape

    barrier = pltpu.get_barrier_semaphore()
    dps = [lax.rem(d + k, n_dp) for k in range(1, n_dp)]
    rows = [lax.rem(r + k, n_row) for k in range(1, n_row)]
    cols = [lax.rem(c + k, n_col) for k in range(1, n_col)]
    peers = [{"dp": k} for k in dps] + [{"row": k} for k in rows] + [{"col": k} for k in cols]
    for peer in peers:
        pl.semaphore_signal(barrier, inc=1, device_id=peer, device_id_type=MESH)

    def copy(src, dst, s, rcv, peer):
        return pltpu.make_async_remote_copy(
            src_ref=src, dst_ref=dst, send_sem=s, recv_sem=rcv, device_id=peer, device_id_type=MESH
        )

    for item in loads:
        item.wait()
    gain = gain_ref[...]

    def fold(value):
        total = value[:, 0:128]
        for k in range(1, C // 128):
            total = total + value[:, k * 128 : (k + 1) * 128]
        return jnp.sum(jnp.transpose(total), axis=0, keepdims=True)

    gn = gn_ref[...]
    x_hat = (x_ref[...].astype(F32) - mean_ref[...]) * rstd_ref[...]
    gh = gn * gain
    st[c, 0:1, :] = fold(gh)
    st[c, 1:2, :] = fold(gh * x_hat)

    def st_copy(k):
        return copy(st.at[c], st.at[c], st_s.at[k], st_r.at[c], {"col": k})

    def st_wait(k):
        return copy(st.at[k], st.at[k], st_s.at[k], st_r.at[k], {"col": k})

    pl.semaphore_wait(barrier, len(peers))
    for k in cols:
        st_copy(k).start()

    da[d] = part_ref[...]
    db[d, 0:1, :] = jnp.sum(gn * x_hat, axis=0, keepdims=True)
    db[d, 1:2, :] = jnp.sum(gn, axis=0, keepdims=True)
    db[d, 2:3, :] = jnp.sum(g_ref[...].astype(F32), axis=0, keepdims=True)

    def pair(a_src, b_src, a_dst, b_dst, s, rcv, peer):
        return [copy(a_src, a_dst, s.at[0], rcv.at[0], peer),
                copy(b_src, b_dst, s.at[1], rcv.at[1], peer)]

    def d_pair(slot, peer):
        return pair(da.at[slot], db.at[slot], da.at[slot], db.at[slot],
                    d_s.at[peer], d_r.at[slot], {"dp": peer})

    def r_pair(slot, peer):
        return pair(ra.at[slot], rb.at[slot], ra.at[slot], rb.at[slot],
                    r_s.at[peer], r_r.at[slot], {"row": peer})

    def c_pair(slot, peer):
        return pair(va_ref.at[slot], vb_ref.at[slot], va_ref.at[slot], vb_ref.at[slot],
                    c_s.at[peer], c_r.at[slot], {"col": peer})

    for k in dps:
        for item in d_pair(d, k):
            item.start()
    for k in dps:
        for item in d_pair(k, k):
            item.wait_recv()
    a_sum, b_sum = da[0], db[0]
    for k in range(1, n_dp):
        a_sum = a_sum + da[k]
        b_sum = b_sum + db[k]
    ra[r] = a_sum
    rb[r] = b_sum
    for k in rows:
        for item in r_pair(r, k):
            item.start()

    for k in cols:
        st_wait(k).wait_recv()
    stats = st[0]
    for k in range(1, n_col):
        stats = stats + st[k]
    stats = stats / width
    m1 = jnp.transpose(jnp.broadcast_to(stats[0:1, :], (128, T)))[:, 0:1]
    m2 = jnp.transpose(jnp.broadcast_to(stats[1:2, :], (128, T)))[:, 0:1]
    gx_ref[...] = g_ref[...].astype(F32) + rstd_ref[...] * (gh - m1 - x_hat * m2)

    for k in rows:
        for item in r_pair(k, k):
            item.wait_recv()
    b_sum = rb[0]
    for k in range(1, n_row):
        b_sum = b_sum + rb[k]
    for k in range(n_row):
        va_ref[c, k] = ra[k]
    vb_ref[c] = b_sum
    for k in cols:
        for item in c_pair(c, k):
            item.start()
    for k in cols:
        for item in c_pair(k, k):
            item.wait_recv()
    for k in cols:
        st_copy(k).wait_send()
        for item in c_pair(c, k):
            item.wait_send()
    for k in dps:
        for item in d_pair(d, k):
            item.wait_send()
    for k in rows:
        for item in r_pair(r, k):
            item.wait_send()


def finish_all(gn, x, g, mean, rstd, gain, part, width, n_dp, n_row, n_col):
    args = (gn, x, g, mean, rstd, gain, part)
    T, C = gn.shape
    dma = pltpu.SemaphoreType.DMA
    vm = pl.BlockSpec(memory_space=pltpu.VMEM)
    return pl.pallas_call(
        functools.partial(finish_kernel, n_dp, n_row, n_col, width),
        name="finish_all",
        out_shape=(
            jax.ShapeDtypeStruct((T, C), F32),
            jax.ShapeDtypeStruct((n_col, n_row, 8, 128), F32),
            jax.ShapeDtypeStruct((n_col, 8, C), F32),
        ),
        in_specs=[ANY] * 7,
        out_specs=(vm,) * 3,
        scratch_shapes=[pltpu.VMEM(item.shape, item.dtype) for item in args]
        + [
            dma((7,)),
            pltpu.VMEM((n_col, 8, T), F32),
            pltpu.VMEM((n_dp, 8, 128), F32),
            pltpu.VMEM((n_dp, 8, C), F32),
            pltpu.VMEM((n_row, 8, 128), F32),
            pltpu.VMEM((n_row, 8, C), F32),
            dma((n_col,)),
            dma((n_col,)),
            dma((n_dp, 2)),
            dma((n_dp, 2)),
            dma((n_row, 2)),
            dma((n_row, 2)),
            dma((n_col, 2)),
            dma((n_col, 2)),
        ],
        compiler_params=pltpu.CompilerParams(
            collective_id=2, has_side_effects=True, vmem_limit_bytes=67043328
        ),
    )(*args)


def muon_kernel(owned, per_step, HF, UT, rate, grad_ref, mom_ref, wq_ref, wo_ref, wu_ref, wd_ref,
                og_ref, new_ref, nm_ref, wbuf, sem):
    first = lax.axis_index("dp") * owned
    step = pl.program_id(0)
    steps = owned // per_step
    n_qkv, n_out, n_up = 6, 2, 8

    def fetch(tile, slot, n, start):
        dst = wbuf.at[slot, n]

        def go(src, target, s):
            item = pltpu.make_async_copy(src, target, s)
            if start:
                item.start()
            else:
                item.wait()

        @pl.when(tile < n_qkv)
        def _():
            j, half = lax.div(tile, 2), lax.rem(tile, 2)
            for m in range(UT // HF):
                go(wq_ref.at[half * (UT // HF) + m, :, pl.ds(j * HF, HF)],
                   wbuf.at[slot, n, :, pl.ds(m * HF, HF)], sem.at[slot, n, m])

        @pl.when((tile >= n_qkv) & (tile < n_qkv + n_out))
        def _():
            go(wo_ref.at[:, pl.ds((tile - n_qkv) * UT, UT)], dst, sem.at[slot, n, 0])

        @pl.when((tile >= n_qkv + n_out) & (tile < n_qkv + n_out + n_up))
        def _():
            go(wu_ref.at[:, pl.ds((tile - n_qkv - n_out) * UT, UT)], dst, sem.at[slot, n, 0])

        @pl.when(tile >= n_qkv + n_out + n_up)
        def _():
            left = tile - (n_qkv + n_out + n_up)
            rows = dst.shape[0]
            go(wd_ref.at[pl.ds(lax.div(left, 2) * rows, rows), pl.ds(lax.rem(left, 2) * UT, UT)],
               dst, sem.at[slot, n, 0])

    def fetch_all(at, start):
        for n in range(per_step):
            fetch(first + at * per_step + n, lax.rem(at, 2), n, start)

    @pl.when(step == 0)
    def _():
        fetch_all(step, True)

    @pl.when(step + 1 < steps)
    def _():
        fetch_all(step + 1, True)

    iters = []
    for n in range(per_step):
        grad = grad_ref[n].astype(F32)
        og_ref[n] = grad
        moment = MOMENTUM_RATE * mom_ref[n] + grad
        nm_ref[n] = moment
        scale = lax.rsqrt(jnp.sum(moment * moment, keepdims=True) + STAT_EPS)
        iters.append((moment * scale).astype(BF16))
    contract = (((0,), (0,)), ((), ()))
    for _ in range(5):
        grams = [
            lax.dot_general(x, x, contract, preferred_element_type=F32).astype(BF16) for x in iters
        ]
        squares = [jnp.dot(g, g, preferred_element_type=F32) for g in grams]
        polys = [
            (NEWTON_B * g.astype(F32) + NEWTON_C * s).astype(BF16) for g, s in zip(grams, squares)
        ]
        iters = [
            (NEWTON_A * x.astype(F32) + jnp.dot(x, p, preferred_element_type=F32)).astype(BF16)
            for x, p in zip(iters, polys)
        ]
    fetch_all(step, False)
    for n in range(per_step):
        new_ref[n] = wbuf[lax.rem(step, 2), n].astype(F32) - rate * iters[n].astype(F32)


def muon_all(grads, moment, w_q, w_out, w_up, w_down, HF, UT):
    owned, rows, cols = moment.shape
    per_step = 4 if owned % 4 == 0 else 3
    rate = MUON_RATE * math.sqrt(max(1.0, rows / cols))
    block = pl.BlockSpec((per_step, rows, cols), lambda i: (i, 0, 0))
    out = jax.ShapeDtypeStruct(moment.shape, F32)
    return pl.pallas_call(
        functools.partial(muon_kernel, owned, per_step, HF, UT, rate),
        name="muon_all",
        grid=(owned // per_step,),
        out_shape=(out, out, out),
        in_specs=[block, block, ANY, ANY, ANY, ANY],
        out_specs=(block, block, block),
        scratch_shapes=[
            pltpu.VMEM((2, per_step, rows, cols), BF16),
            pltpu.SemaphoreType.DMA((2, per_step, 2)),
        ],
        compiler_params=pltpu.CompilerParams(vmem_limit_bytes=56 * 1024 * 1024),
    )(grads, moment, w_q, w_out, w_up, w_down)


def reduce_plain(p, q, dwi, dwf, C, HF, UT, n_col, row_width):
    def block(part):
        part = lax.psum_scatter(part, "row", scatter_dimension=0, tiled=True)
        return lax.psum_scatter(part, "col", scatter_dimension=1, tiled=True).astype(F32)

    wi4 = lax.all_to_all(dwi.reshape(n_col, C, -1), "col", 0, 0)
    wf4 = lax.all_to_all(dwf.reshape(-1, n_col, C).transpose(1, 0, 2), "col", 0, 0)
    grad_qkv = (
        wi4[:, :, : 3 * HF].reshape(n_col, C, 3, HF).transpose(1, 2, 0, 3).reshape(C, 3, row_width)
    )
    grad_up_w = wi4[:, :, 3 * HF :].reshape(n_col, C, 2, UT).transpose(1, 2, 0, 3).reshape(C, -1)
    grad_w_out = wf4[:, :HF].reshape(-1, C)
    grad_w_down = wf4[:, HF:].reshape(n_col, 2, UT, C).transpose(1, 0, 2, 3).reshape(-1, C)
    grad_tiles = tile_blocks(grad_qkv, grad_w_out, grad_up_w, grad_w_down)
    owned = lax.psum_scatter(grad_tiles, "dp", scatter_dimension=0, tiled=True)
    return block(p), block(q), owned


def backward_plain(hidden, hidden_t, cot, w_fin, w_in, norm_t, qkv, up_pre, positions, segments, HF):
    cosine, sine_tab = rotary_tables(positions)
    rows = cot.shape[0]
    seqs, heads = rows // SEQ_LEN, HF // HEAD_DIM

    def by_head(tensor_in):
        return tensor_in.reshape(seqs, SEQ_LEN, heads, HEAD_DIM)

    partial_out = jnp.dot(hidden, w_fin, preferred_element_type=F32).astype(BF16)
    grad_w_fin = jnp.dot(hidden_t, cot, preferred_element_type=F32).astype(BF16)
    back = jnp.einsum("tj,ij->ti", cot, w_fin, preferred_element_type=F32)
    grad_up = back[:, HF:] * gelu_slope(up_pre)
    grads = jax.vmap(attend_backward, in_axes=(0, 0, 0, 0, 0, 0, None))(
        by_head(qkv[:, :HF]),
        by_head(qkv[:, HF : 2 * HF]),
        by_head(qkv[:, 2 * HF :]),
        by_head(hidden[:, :HF]),
        by_head(back[:, :HF].astype(BF16)),
        segments.reshape(seqs, SEQ_LEN),
        HEAD_DIM ** (-0.5),
    )
    g_q, g_k, g_v = [item.reshape(rows, heads, HEAD_DIM) for item in grads]
    g_q = rotate(g_q, cosine, sine_tab, -1.0)
    g_k = rotate(g_k, cosine, sine_tab, -1.0)
    grad_mixed = jnp.concatenate(
        [item.reshape(rows, HF) for item in (g_q, g_k, g_v)] + [grad_up], axis=1
    )
    low = grad_mixed.astype(BF16)
    grad_w_in = jnp.dot(norm_t, low, preferred_element_type=F32).astype(BF16)
    partial_norm = jnp.einsum("tj,ij->ti", low, w_in, preferred_element_type=F32).astype(BF16)
    part = jnp.pad(jnp.sum(grad_mixed, axis=0).reshape(-1, 128), ((0, 1), (0, 0)))
    return (partial_out, partial_norm, grad_w_in, grad_w_fin), part


def body(
    inputs,
    cotangent,
    segments,
    positions,
    w_qkv,
    w_out,
    w_up,
    w_down,
    vectors,
    tile_moment,
    vector_moment,
):
    col_index = lax.axis_index("col")
    n_dp, n_row, n_col = lax.axis_size("dp"), lax.axis_size("row"), lax.axis_size("col")
    T, C = inputs.shape
    D = vectors.shape[1]
    row_width = w_qkv.shape[2]
    HF = row_width // n_col
    UT = w_up.shape[1] // (2 * n_col)
    col_start = col_index * C
    norm_gain = lax.dynamic_slice_in_dim(vectors[5], col_start, C)
    out_bias = lax.dynamic_slice_in_dim(vectors[3] + vectors[4], col_start, C)
    w_q = (
        w_qkv.reshape(C, 3, n_col, HF).transpose(2, 0, 1, 3).reshape(n_col, C, 3 * HF)
    )
    rows_all = positions.shape[0]
    seq_count = rows_all // SEQ_LEN
    seg_row = segments.reshape(seq_count, SEQ_LEN)
    pos_row = positions.reshape(seq_count, SEQ_LEN)
    cot_rows, w_in, w_fin, norm_t, hidden, hidden_t, qkv_low, up_pre, packed, mean_own, rstd_own = (
        forward_all(
            inputs, cotangent, w_q, w_up, w_out, w_down, pos_row, seg_row, vectors,
            n_dp, n_row, n_col,
        )
    )
    if n_dp == 2:
        branch, grad_norm, owned_low, part = backward_all(
            hidden, hidden_t, cot_rows, w_fin, w_in, norm_t, qkv_low, up_pre, packed, seg_row,
            T, C, HF, UT, n_row, n_col,
        )
    else:
        partials, part = backward_plain(
            hidden, hidden_t, cot_rows, w_fin, w_in, norm_t, qkv_low, up_pre, positions, segments, HF
        )
        branch, grad_norm, owned_low = reduce_plain(*partials, C, HF, UT, n_col, row_width)
    x_val = inputs.astype(F32)
    result = x_val + branch + out_bias

    grad_input, vec_a, vec_b = finish_all(
        grad_norm,
        inputs,
        cotangent,
        mean_own,
        rstd_own,
        norm_gain[None],
        part,
        D,
        n_dp,
        n_row,
        n_col,
    )
    vec_a = vec_a.transpose(2, 1, 0, 3)
    qkv_rows = vec_a[:3].reshape(3, D)
    up_rows = vec_a[3:7].reshape(2, UT // 128, n_row, n_col, 128).transpose(2, 0, 3, 1, 4)
    norm_rows = vec_b.transpose(1, 0, 2).reshape(8, D)
    vec_grad = jnp.concatenate(
        [qkv_rows, norm_rows[2:3], norm_rows[2:3], norm_rows[:2], up_rows.reshape(-1, D)], axis=0
    )
    scaled = vec_grad * lax.rsqrt(jnp.mean(vec_grad * vec_grad, axis=1, keepdims=True) + STAT_EPS)
    vec_moment_new = MOMENTUM_RATE * vector_moment + scaled
    vectors_new = vectors - VECTOR_RATE * vec_moment_new

    owned_grads, tiles_new, moment_new = muon_all(
        owned_low, tile_moment[0, 0], w_q, w_out, w_up, w_down, HF, UT
    )
    return (
        result,
        grad_input,
        owned_grads[None, None],
        tiles_new[None, None],
        moment_new[None, None],
        vec_grad,
        vectors_new,
        vec_moment_new,
    )


def solution(mesh):
    placed = (
        P(("dp", "row"), "col"),
        P(("dp", "row"), "col"),
        P("dp"),
        P("dp"),
        P("col", None, "row"),
        P("row", "col"),
        P("col", "row"),
        P("row", "col"),
        P(),
        P("row", "col", "dp", None, None),
        P(),
    )
    return jax.shard_map(
        body,
        mesh=mesh,
        in_specs=placed,
        out_specs=(
            P(("dp", "row"), "col"),
            P(("dp", "row"), "col"),
            P("row", "col", "dp", None, None),
            P("row", "col", "dp", None, None),
            P("row", "col", "dp", None, None),
            P(),
            P(),
            P(),
        ),
        check_vma=False,
    )
```

```python
import functools
import math

import jax
import jax.numpy as jnp
from jax import lax
from jax.experimental import pallas as pl
from jax.experimental.pallas import tpu as pltpu
from jax.sharding import PartitionSpec as P

HEAD_DIM = 64
ROTARY = 32
SEQ_LEN = 512

MOMENTUM_RATE = 0.95
MUON_RATE = 0.05
VECTOR_RATE = 0.12
NEWTON_A = 3.4445
NEWTON_B = -4.775
NEWTON_C = 2.0315
GELU_SCALE = 0.7978845608028654
GELU_CUBIC = 0.044715
NORM_EPS = 1e-05
STAT_EPS = 1e-06
MASKED_SCORE = -1e30

MESH = pl.DeviceIdType.MESH
ANY = pl.BlockSpec(memory_space=pl.ANY)
F32 = jnp.float32
BF16 = jnp.bfloat16


def to_low(tensor_in):
    return lax.optimization_barrier(tensor_in.astype(BF16))


def gelu_value(pre_act):
    inner_arg = GELU_SCALE * (pre_act + GELU_CUBIC * pre_act * pre_act * pre_act)
    return 0.5 * pre_act * (1.0 + jnp.tanh(inner_arg))


def gelu_slope(pre_act):
    tanh_val = jnp.tanh(GELU_SCALE * (pre_act + GELU_CUBIC * pre_act * pre_act * pre_act))
    return 0.5 * (1.0 + tanh_val) + 0.5 * pre_act * (1.0 - tanh_val * tanh_val) * GELU_SCALE * (
        1.0 + 3.0 * GELU_CUBIC * pre_act * pre_act
    )


def rotary_tables(positions):
    half_dims = ROTARY // 2
    frequency = jnp.exp(jnp.arange(half_dims, dtype=F32) * (-2.0 * math.log(10000.0) / ROTARY))
    angles = positions.astype(F32)[:, None] * frequency[None, :]
    return (jnp.cos(angles), jnp.sin(angles))


def rotate(tensor_in, cosine, sine_tab, direction_sign):
    half_dims = ROTARY // 2
    first_half = tensor_in[..., :half_dims]
    second_half = tensor_in[..., half_dims:ROTARY]
    cos_wide = cosine[:, None, :]
    sin_wide = sine_tab[:, None, :] * direction_sign
    return jnp.concatenate(
        [
            first_half * cos_wide - second_half * sin_wide,
            second_half * cos_wide + first_half * sin_wide,
            tensor_in[..., ROTARY:],
        ],
        axis=-1,
    )


def causal_allowed(segment):
    token_order = jnp.arange(segment.shape[0])
    return (segment[:, None] == segment[None, :]) & (token_order[:, None] >= token_order[None, :])


def masked_scores(queries, key_vecs, segment, score_scale):
    scores = (
        jnp.einsum("lhe,mhe->hlm", queries, key_vecs, preferred_element_type=F32) * score_scale
    )
    return jnp.where(causal_allowed(segment)[None], scores, MASKED_SCORE)


def attend_backward(queries, key_vecs, values, output_low, grad_low, segment, score_scale):
    scores = masked_scores(queries, key_vecs, segment, score_scale)
    weight = jnp.exp(scores - jnp.max(scores, axis=-1, keepdims=True))
    probs = weight * (1.0 / jnp.sum(weight, axis=-1, keepdims=True))
    grad_values = jnp.einsum("hlm,lhe->mhe", to_low(probs), grad_low, preferred_element_type=F32)
    grad_probs = jnp.einsum("lhe,mhe->hlm", grad_low, values, preferred_element_type=F32)
    row_delta = jnp.sum(grad_low.astype(F32) * output_low.astype(F32), axis=-1)
    grad_scores = to_low(probs * (grad_probs - row_delta.T[:, :, None]) * score_scale)
    grad_queries = jnp.einsum("hlm,mhe->lhe", grad_scores, key_vecs, preferred_element_type=F32)
    grad_keys = jnp.einsum("hlm,lhe->mhe", grad_scores, queries, preferred_element_type=F32)
    return (grad_queries, grad_keys, grad_values)


def tile_blocks(qkv_block, out_block, up_block, down_block):
    tile_rows = qkv_block.shape[0]
    tile_cols = qkv_block.shape[2] // 2

    def split_cols(block_in):
        return block_in.reshape(
            block_in.shape[0], block_in.shape[1] // tile_cols, tile_cols
        ).transpose(1, 0, 2)

    down_part = down_block.reshape(
        down_block.shape[0] // tile_rows, tile_rows, down_block.shape[1] // tile_cols, tile_cols
    )
    down_part = down_part.transpose(0, 2, 1, 3).reshape(-1, tile_rows, tile_cols)
    return jnp.concatenate(
        [
            split_cols(qkv_block[:, 0]),
            split_cols(qkv_block[:, 1]),
            split_cols(qkv_block[:, 2]),
            split_cols(out_block),
            split_cols(up_block),
            down_part,
        ],
        axis=0,
    )


def pick(index, table):
    out = jnp.int32(table[0]) if isinstance(table[0], int) else table[0]
    for k in range(1, len(table)):
        out = jnp.where(index == k, table[k], out)
    return out


def far_order(c, n_col):
    far = [
        sorted(range(n_col), key=lambda f: (-abs(f - cc), f < cc if cc < n_col // 2 else f > cc))
        for cc in range(n_col)
    ]
    return [pick(c, [far[cc][i] for cc in range(n_col)]) for i in range(n_col)]


def forward_kernel(n_dp, n_row, n_col, dims,
                   x_ref, g_ref, wq_ref, wu_ref, wo_ref, wd_ref,
                   pos_ref, seg_ref, vec_ref,
                   gf, wi, wf, nt, hid_out, ht_out, qkv_out, up_out, cs_out, mean_ref, rstd_ref,
                   xv, ntv, wv, hid, ht, qkv, up, tab, mean_v, rstd_v, stage_g, stage_o, stage_d,
                   zs, zr, ys, yr, cs, cr, ws, wr, ds, dr, ls, lo, no):
    T, C, HF, UT = dims
    d, r, c = lax.axis_index("dp"), lax.axis_index("row"), lax.axis_index("col")
    r1 = r + 1 - 2 * lax.rem(r, 2)
    r2 = lax.rem(r + 2, n_row)
    chunks = 2
    tc = T // chunks
    qw = 3 * HF
    rows_all, D = n_row * T, n_col * C
    seqs = rows_all // SEQ_LEN
    acts = ((x_ref, xv), (g_ref, gf))
    forder = far_order(c, n_col)

    barrier = pltpu.get_barrier_semaphore()
    peers = [{"row": r1}, {"row": r2}]
    peers += [{"col": lax.rem(c + k, n_col)} for k in range(1, n_col)]
    peers += [{"dp": lax.rem(d + k, n_dp)} for k in range(1, n_dp)]
    for peer in peers:
        pl.semaphore_signal(barrier, inc=1, device_id=peer, device_id_type=MESH)
    pl.semaphore_wait(barrier, len(peers))

    def copy(src, dst, s, rcv, peer):
        return pltpu.make_async_remote_copy(
            src_ref=src, dst_ref=dst, send_sem=s, recv_sem=rcv, device_id=peer, device_id_type=MESH
        )

    def blk(a, rr, cc, t):
        return acts[a][1].at[pl.ds(pl.multiple_of(rr * T + t * tc, tc), tc),
                             pl.ds(pl.multiple_of(cc * C, C), C)]

    def own(a, t):
        return acts[a][0].at[pl.ds(t * tc, tc), :]

    def z_copy(a, t, cc, src, right):
        peer = {"col": c + 1} if right else {"col": c - 1}
        return copy(src, blk(a, r, cc, t), zs.at[a, t, int(right), cc], zr.at[a, t, cc], peer)

    def y_copy(a, t, cc, src):
        return copy(src, blk(a, r, cc, t), ys.at[a, t, cc], yr.at[a, t, cc], {"row": r2})

    def c_copy(a, t, cc, src, rr, which):
        return copy(
            src, blk(a, rr, cc, t), cs.at[a, t, which, cc], cr.at[a, t, which, cc], {"row": r1}
        )

    def send_own_z(a, t):
        @pl.when(c < n_col - 1)
        def _():
            z_copy(a, t, c, own(a, t), True).start()

        @pl.when(c > 0)
        def _():
            z_copy(a, t, c, own(a, t), False).start()

    def send_own_row(a, t):
        y_copy(a, t, c, own(a, t)).start()
        c_copy(a, t, c, own(a, t), r, 0).start()

    def relay(a, s, t):
        for right in (True, False):
            cc = c - s if right else c + s

            @pl.when((cc >= 0) & (cc < n_col))
            def _(cc=cc, right=right):
                z_copy(a, t, cc, blk(a, r, cc, t), right).wait_recv()

                @pl.when((c < n_col - 1) if right else (c > 0))
                def _():
                    z_copy(a, t, cc, blk(a, r, cc, t), right).start()

                y_copy(a, t, cc, blk(a, r, cc, t)).start()
                c_copy(a, t, cc, blk(a, r, cc, t), r, 0).start()

    def pass_row(a, s, t):
        for right in (True, False):
            cc = c - s if right else c + s
            ok = (cc >= 0) & (cc < n_col)
            if not right:
                ok = ok & (s > 0)

            @pl.when(ok)
            def _(cc=cc):
                y_copy(a, t, cc, blk(a, r, cc, t)).wait_recv()
                c_copy(a, t, cc, blk(a, r2, cc, t), r2, 1).start()

    ck, hk, uk = C // n_dp, HF // n_dp, UT // n_dp

    def w_dst(part, dd, cc):
        if part == 0:
            return wv.at[pl.ds(cc * C + dd * ck, ck), pl.ds(0, qw)]
        if part == 1:
            return wv.at[pl.ds(cc * C + dd * ck, ck), pl.ds(qw, UT)]
        if part == 2:
            return wv.at[pl.ds(cc * C + dd * ck, ck), pl.ds(qw + UT, UT)]
        if part == 3:
            return wf.at[pl.ds(dd * hk, hk), pl.ds(cc * C, C)]
        if part == 4:
            return wf.at[pl.ds(HF + dd * uk, uk), pl.ds(cc * C, C)]
        return wf.at[pl.ds(HF + UT + dd * uk, uk), pl.ds(cc * C, C)]

    def w_src(part, cc):
        if part == 0:
            return wq_ref.at[cc, pl.ds(d * ck, ck), :]
        if part == 1:
            return wu_ref.at[pl.ds(d * ck, ck), pl.ds(cc * UT, UT)]
        if part == 2:
            return wu_ref.at[pl.ds(d * ck, ck), pl.ds((n_col + cc) * UT, UT)]
        if part == 3:
            return wo_ref.at[pl.ds(cc * HF + d * hk, hk), :]
        if part == 4:
            return wd_ref.at[pl.ds(cc * UT + d * uk, uk), :]
        return wd_ref.at[pl.ds((n_col + cc) * UT + d * uk, uk), :]

    def w_copy(part, dest):
        return copy(
            w_src(part, dest), w_dst(part, d, c), ws.at[part, dest], wr.at[part, c], {"col": dest}
        )

    def w_from(part, source):
        return copy(
            w_src(part, source), w_dst(part, d, source), ws.at[part, source], wr.at[part, source],
            {"col": source},
        )

    def x_copy(part, source, j):
        got = w_dst(part, d, source)
        return copy(got, got, ds.at[part, source, j], dr.at[part, source, j],
                    {"dp": lax.rem(d + j, n_dp)})

    others = forder[: n_col - 1]

    def w_send(part):
        for dest in others:
            w_copy(part, dest).start()

    def w_pass(part):
        for source in others[::-1]:
            w_from(part, source).wait_recv()
            for j in range(1, n_dp):
                x_copy(part, source, j).start()

    def w_done(part):
        for source in others:
            for j in range(1, n_dp):
                x_copy(part, source, j).wait_recv()

    win, wfin = (0, 1, 2), (3, 4, 5)

    for t in range(chunks):
        send_own_z(0, t)
    for t in range(chunks):
        send_own_row(0, t)

    col_at = pl.ds(c * C, C)
    direct = [
        pltpu.make_async_copy(x_ref, xv.at[pl.ds(r * T, T), col_at], ls.at[0]),
        pltpu.make_async_copy(wq_ref.at[c], wv.at[col_at, pl.ds(0, qw)], ls.at[1]),
        pltpu.make_async_copy(wu_ref.at[:, pl.ds(c * UT, UT)], wv.at[col_at, pl.ds(qw, UT)],
                              ls.at[2]),
        pltpu.make_async_copy(wu_ref.at[:, pl.ds((n_col + c) * UT, UT)],
                              wv.at[col_at, pl.ds(qw + UT, UT)], ls.at[3]),
    ]
    loads = [
        pltpu.make_async_copy(g_ref, stage_g, ls.at[4]),
        pltpu.make_async_copy(wo_ref.at[pl.ds(c * HF, HF), :], stage_o, ls.at[5]),
        pltpu.make_async_copy(wd_ref.at[pl.ds(c * UT, UT), :], stage_d.at[0], ls.at[6]),
        pltpu.make_async_copy(wd_ref.at[pl.ds((n_col + c) * UT, UT), :], stage_d.at[1], ls.at[7]),
    ]
    stores = [
        pltpu.make_async_copy(stage_g, gf.at[pl.ds(r * T, T), col_at], lo.at[0]),
        pltpu.make_async_copy(stage_o, wf.at[pl.ds(0, HF), col_at], lo.at[1]),
        pltpu.make_async_copy(stage_d.at[0], wf.at[pl.ds(HF, UT), col_at], lo.at[2]),
        pltpu.make_async_copy(stage_d.at[1], wf.at[pl.ds(HF + UT, UT), col_at], lo.at[3]),
    ]
    for item in direct + loads:
        item.start()

    for n in range(1, n_col):
        for t in range(chunks):
            relay(0, n, t)
        w_send(win[n - 1])
    for t in range(chunks):
        send_own_z(1, t)
        send_own_row(1, t)
    for load, store in zip(loads, stores):
        load.wait()
        store.start()
    w_pass(win[0])

    place = lax.rem(lax.broadcasted_iota(jnp.int32, (1, 2 * HEAD_DIM), 1), HEAD_DIM)
    power = jnp.exp(
        lax.rem(place, ROTARY // 2).astype(F32) * (-2.0 * math.log(10000.0) / ROTARY)
    )
    freq = jnp.where(place < ROTARY, power, 0.0)

    def one_table(n, carry):
        rows = jnp.broadcast_to(pos_ref[pl.ds(n, 1), :].astype(F32), (2 * HEAD_DIM, SEQ_LEN))
        angle = jnp.transpose(rows) * freq
        lane = lax.broadcasted_iota(jnp.int32, angle.shape, 1)
        turns = jnp.floor(angle * (2.0 / math.pi) + 0.5)
        rest = angle - turns * 1.5703125
        rest = rest - turns * 4.837512969970703125e-4
        rest = rest - turns * 7.54978994889188e-8
        sq = rest * rest
        sine = rest + rest * sq * (
            -1.6666654611e-1 + sq * (8.3321608736e-3 - sq * 1.9515295891e-4)
        )
        cosine = 1.0 - 0.5 * sq + sq * sq * (
            4.166664568298827e-2 + sq * (-1.388731625493765e-3 + sq * 2.443315711809948e-5)
        )
        quarter = jnp.where(lane < HEAD_DIM, turns, turns - 1.0)
        quarter = quarter - 4.0 * jnp.floor(quarter * 0.25)
        odd = (quarter == 1.0) | (quarter == 3.0)
        value = jnp.where(odd, sine, cosine)
        value = jnp.where((quarter == 1.0) | (quarter == 2.0), -value, value)
        tab[pl.ds(pl.multiple_of(n * SEQ_LEN, SEQ_LEN), SEQ_LEN), :] = value
        return carry

    lax.fori_loop(0, seqs, one_table, 0)
    keep_cs = pltpu.make_async_copy(tab, cs_out, no.at[2])
    keep_cs.start()
    for n in range(n_col):
        for t in range(chunks):
            pass_row(0, n, t)
    w_pass(win[1])
    for item in direct:
        item.wait()
    for t in range(chunks):
        for cc in range(n_col):
            c_copy(0, t, cc, blk(0, r, cc, t), r, 0).wait_recv()
            c_copy(0, t, cc, blk(0, r, cc, t), r, 1).wait_recv()

    def act_sent(a):
        for t in range(chunks):
            for cc in range(n_col):
                @pl.when((cc <= c) & (c < n_col - 1))
                def _(t=t, cc=cc):
                    z_copy(a, t, cc, blk(a, r, cc, t), True).wait_send()

                @pl.when((cc >= c) & (c > 0))
                def _(t=t, cc=cc):
                    z_copy(a, t, cc, blk(a, r, cc, t), False).wait_send()

                y_copy(a, t, cc, blk(a, r, cc, t)).wait_send()
                c_copy(a, t, cc, blk(a, r, cc, t), r, 0).wait_send()
                c_copy(a, t, cc, blk(a, r, cc, t), r, 1).wait_send()

    act_sent(0)

    tile = 256
    tiles = rows_all // tile
    sub = 16

    def norm_tile(i, carry):
        base = pl.multiple_of(i * tile, tile)

        def norm_rows(k, inner):
            at = pl.ds(pl.multiple_of(base + k * sub, sub), sub)
            val = xv[at, :].astype(F32)
            mean = jnp.sum(val, axis=1, keepdims=True) / D
            var = jnp.sum(val * val, axis=1, keepdims=True) / D - mean * mean
            rstd = lax.rsqrt(var + NORM_EPS)
            mean_v[at, :] = mean
            rstd_v[at, :] = rstd
            xv[at, :] = ((val - mean) * rstd * vec_ref[5:6, :] + vec_ref[6:7, :]).astype(BF16)
            return inner

        lax.fori_loop(0, tile // sub, norm_rows, 0)
        at = pl.ds(base, tile)
        for k in range(D // tile):
            ntv[k * tile : (k + 1) * tile, at] = jnp.transpose(xv[at, k * tile : (k + 1) * tile])
        return carry

    lax.fori_loop(0, tiles // 2, norm_tile, 0)
    w_pass(win[2])
    for t in range(chunks):
        relay(1, 1, t)
    w_send(wfin[0])
    lax.fori_loop(tiles // 2, tiles, norm_tile, 0)
    keep_norm = pltpu.make_async_copy(ntv, nt, no.at[1])
    keep_norm.start()
    own_rows = pl.ds(pl.multiple_of(r * T, T), T)
    mean_ref[...] = mean_v[own_rows, :]
    rstd_ref[...] = rstd_v[own_rows, :]
    for part in win:
        w_done(part)
    keep_w = pltpu.make_async_copy(wv, wi, no.at[0])
    keep_w.start()

    q_lanes = pl.ds(pl.multiple_of((r * n_col + c) * HF, HF), HF)
    biases = [vec_ref[j : j + 1, q_lanes] for j in range(3)]
    biases += [
        vec_ref[pl.ds(7 + r, 1), pl.ds(pl.multiple_of((m * n_col + c) * UT, UT), UT)]
        for m in range(2)
    ]
    bias = jnp.concatenate(biases, axis=1)

    def one_tile(i, carry):
        at = pl.ds(pl.multiple_of(i * tile, tile), tile)
        mixed = jnp.dot(xv[at, :], wv[...], preferred_element_type=F32) + bias
        cos, sin = wide_tables(tab[at, :])
        for j in range(2):
            part = mixed[:, j * HF : (j + 1) * HF]
            qkv[at, j * HF : (j + 1) * HF] = turn(part, cos, sin, 1.0).astype(BF16)
        qkv[at, 2 * HF : 3 * HF] = mixed[:, 2 * HF : 3 * HF].astype(BF16)
        pre = mixed[:, qw:]
        up[at, :] = pre
        act = gelu_value(pre).astype(BF16)
        hid[at, HF:] = act
        ht[HF:, at] = jnp.transpose(act)

        s, t = 2 + lax.div(i, 2), lax.rem(i, 2)

        @pl.when(s < n_col)
        def _():
            relay(1, s, t)

        return carry

    lax.fori_loop(0, 2, one_tile, 0)
    w_send(wfin[1])
    lax.fori_loop(2, 4, one_tile, 0)
    w_send(wfin[2])
    lax.fori_loop(4, tiles, one_tile, 0)
    keep_up = pltpu.make_async_copy(up, up_out, no.at[3])
    keep_qkv = pltpu.make_async_copy(qkv, qkv_out, no.at[4])
    keep_up.start()
    keep_qkv.start()

    heads = HF // HEAD_DIM
    qt = SEQ_LEN // 2

    def one_seq(s, carry):
        base = pl.multiple_of(s * SEQ_LEN, SEQ_LEN)
        lane = lax.broadcasted_iota(jnp.int32, (qt, HF), 1)
        seg = seg_ref[pl.ds(s, 1), :]
        seg_col = jnp.transpose(jnp.broadcast_to(seg, (128, SEQ_LEN)))[:, 0:1]
        for qi in range(2):
            width = (qi + 1) * qt
            q_at = pl.ds(pl.multiple_of(base + qi * qt, qt), qt)
            k_at = pl.ds(base, width)
            allowed = (seg_col[qi * qt : (qi + 1) * qt, :] == seg[:, 0:width]) & (
                lax.broadcasted_iota(jnp.int32, (qt, width), 0) + qi * qt
                >= lax.broadcasted_iota(jnp.int32, (qt, width), 1)
            )
            keys, vals = qkv[k_at, HF : 2 * HF], qkv[k_at, 2 * HF : 3 * HF]
            queries = qkv[q_at, 0:HF]
            total = None
            for h in range(heads):
                mine = lax.div(lane, HEAD_DIM) == h
                scores = lax.dot_general(
                    jnp.where(mine, queries, jnp.zeros_like(queries)), keys,
                    (((1,), (1,)), ((), ())), preferred_element_type=F32,
                ) * (HEAD_DIM ** (-0.5))
                scores = jnp.where(allowed, scores, MASKED_SCORE)
                peak = jnp.max(scores, axis=1, keepdims=True)
                weight = jnp.exp(scores - peak)
                weight_sum = jnp.sum(weight, axis=1, keepdims=True)
                probs = (weight * (1.0 / weight_sum)).astype(BF16)
                out = jnp.dot(probs, vals, preferred_element_type=F32)
                total = out if h == 0 else jnp.where(mine, out, total)
            low = total.astype(BF16)
            hid[q_at, 0:HF] = low
            ht[0:HF, q_at] = jnp.transpose(low)

        @pl.when(s < n_col)
        def _():
            for t in range(chunks):
                pass_row(1, s, t)

        return carry

    lax.fori_loop(0, seqs, one_seq, 0)
    keep_hid = pltpu.make_async_copy(hid, hid_out, no.at[5])
    keep_ht = pltpu.make_async_copy(ht, ht_out, no.at[6])
    keep_hid.start()
    keep_ht.start()
    for part in wfin:
        w_pass(part)

    for t in range(chunks):
        for cc in range(n_col):
            c_copy(1, t, cc, blk(1, r, cc, t), r, 0).wait_recv()
            c_copy(1, t, cc, blk(1, r, cc, t), r, 1).wait_recv()
    for part in wfin:
        w_done(part)
    act_sent(1)
    for part in win + wfin:
        for peer in others:
            w_copy(part, peer).wait_send()
            for j in range(1, n_dp):
                x_copy(part, peer, j).wait_send()
    for store in stores:
        store.wait()
    for item in (keep_w, keep_norm, keep_cs, keep_up, keep_qkv, keep_hid, keep_ht):
        item.wait()


def forward_all(x, g, w_q, w_up, w_out, w_down, pos_row, seg_row, vectors,
                n_dp, n_row, n_col):
    T, C = x.shape
    HF = w_q.shape[2] // 3
    UT = w_up.shape[1] // (2 * n_col)
    n_in, n_out = 3 * HF + 2 * UT, HF + 2 * UT
    rows, D = n_row * T, n_col * C
    dma = pltpu.SemaphoreType.DMA
    vm = pl.BlockSpec(memory_space=pltpu.VMEM)
    sds = jax.ShapeDtypeStruct
    return pl.pallas_call(
        functools.partial(forward_kernel, n_dp, n_row, n_col, (T, C, HF, UT)),
        name="forward_all",
        out_shape=(
            sds((rows, D), BF16),
            sds((D, n_in), BF16),
            sds((n_out, D), BF16),
            sds((D, rows), BF16),
            sds((rows, n_out), BF16),
            sds((n_out, rows), BF16),
            sds((rows, 3 * HF), BF16),
            sds((rows, 2 * UT), F32),
            sds((rows, 2 * HEAD_DIM), F32),
            sds((T, 1), F32),
            sds((T, 1), F32),
        ),
        in_specs=[ANY] * 6 + [vm] * 3,
        out_specs=(ANY,) * 9 + (vm,) * 2,
        scratch_shapes=[
            pltpu.VMEM((rows, D), BF16),
            pltpu.VMEM((D, rows), BF16),
            pltpu.VMEM((D, n_in), BF16),
            pltpu.VMEM((rows, n_out), BF16),
            pltpu.VMEM((n_out, rows), BF16),
            pltpu.VMEM((rows, 3 * HF), BF16),
            pltpu.VMEM((rows, 2 * UT), F32),
            pltpu.VMEM((rows, 2 * HEAD_DIM), F32),
            pltpu.VMEM((rows, 1), F32),
            pltpu.VMEM((rows, 1), F32),
            pltpu.VMEM((T, C), BF16),
            pltpu.VMEM((HF, C), BF16),
            pltpu.VMEM((2, UT, C), BF16),
            dma((2, 2, 2, n_col)),
            dma((2, 2, n_col)),
            dma((2, 2, n_col)),
            dma((2, 2, n_col)),
            dma((2, 2, 2, n_col)),
            dma((2, 2, 2, n_col)),
            dma((6, n_col)),
            dma((6, n_col)),
            dma((6, n_col, n_dp)),
            dma((6, n_col, n_dp)),
            dma((8,)),
            dma((4,)),
            dma((7,)),
        ],
        compiler_params=pltpu.CompilerParams(
            collective_id=0, has_side_effects=True, vmem_limit_bytes=60 * 1024 * 1024
        ),
    )(x, g, w_q, w_up, w_out, w_down, pos_row, seg_row, vectors)


def wide_tables(packed):
    lane = lax.broadcasted_iota(jnp.int32, packed.shape, 1)
    turned = pltpu.roll(packed, HEAD_DIM, 1)
    first = lane < HEAD_DIM
    return jnp.where(first, packed, turned), jnp.where(first, turned, packed)


def turn(part, cos, sin, sign):
    lane = lax.rem(lax.broadcasted_iota(jnp.int32, part.shape, 1), HEAD_DIM)
    ahead = pltpu.roll(part, part.shape[1] - ROTARY // 2, 1)
    behind = pltpu.roll(part, ROTARY // 2, 1)
    return part * cos + jnp.where(lane < ROTARY // 2, -ahead, behind) * (sign * sin)


def backward_kernel(n_row, n_col, dims,
                    hid_ref, ht_ref, c_ref, wf_ref, wi_ref, nt_ref, qkv_ref, up_ref,
                    cs_ref, seg_ref,
                    res_ref, gn_ref, tiles_ref, part_ref,
                    hd, hts, big, wf, wi, qv, ups, ga,
                    abuf, obuf, asb, sbuf, bbuf, zsb, zin,
                    dwf, dwi, gf, gu, gk,
                    l_s, h_s, u_s, a_s, a_r, y_s, y_r, z_s, z_r, xf_s, xf_r, xu_s, xu_r, xk_s, xk_r,
                    t_s, t_r, free_row, free_col):
    T, C, HF, UT = dims
    rows_all, D = n_row * T, n_col * C
    qw, n_in, n_out = 3 * HF, 3 * HF + 2 * UT, HF + 2 * UT
    step_rows = 64
    d, r, c = lax.axis_index("dp"), lax.axis_index("row"), lax.axis_index("col")
    r1 = r + 1 - 2 * lax.rem(r, 2)
    r2 = lax.rem(r + 2, n_row)
    r12 = lax.rem(r1 + 2, n_row)
    forder = far_order(c, n_col)
    outs = (res_ref, gn_ref)

    barrier = pltpu.get_barrier_semaphore()
    peers = [{"row": r1}, {"row": r2}, {"dp": 1 - d}]
    peers += [{"col": lax.rem(c + k, n_col)} for k in range(1, n_col)]
    for peer in peers:
        pl.semaphore_signal(barrier, inc=1, device_id=peer, device_id_type=MESH)

    loads = [
        pltpu.make_async_copy(hid_ref, hd.at[:, pl.ds(2 * HF, n_out)], l_s.at[0]),
        pltpu.make_async_copy(wf_ref, wf, l_s.at[1]),
        pltpu.make_async_copy(c_ref, big, l_s.at[2]),
        pltpu.make_async_copy(qkv_ref, qv, l_s.at[3]),
        pltpu.make_async_copy(wi_ref, wi, l_s.at[4]),
    ]
    for item in loads:
        item.start()
    load_nt = pltpu.make_async_copy(nt_ref, big, l_s.at[5])

    def load_ht(m, slot):
        return pltpu.make_async_copy(ht_ref.at[pl.ds(pl.multiple_of(m * HF, HF), HF), :],
                                     hts.at[slot], h_s.at[slot])

    tile = 256

    def load_up(i, slot):
        return pltpu.make_async_copy(up_ref.at[pl.ds(pl.multiple_of(i * tile, tile), tile), :],
                                     ups.at[slot], u_s.at[slot])

    load_ht(0, 0).start()
    load_up(0, 0).start()
    pl.semaphore_wait(barrier, len(peers))

    def copy(src, dst, s, rcv, peer):
        return pltpu.make_async_remote_copy(
            src_ref=src, dst_ref=dst, send_sem=s, recv_sem=rcv, device_id=peer, device_id_type=MESH
        )

    def a_copy(v, h, f):
        return copy(asb.at[h, f], abuf.at[v, h, f], a_s.at[h, f], a_r.at[v, h, f], {"row": r1})

    def y_copy(f):
        return copy(sbuf.at[f], bbuf.at[f], y_s.at[f], y_r.at[f], {"row": r2})

    def z_copy(f, slot, step):
        return copy(zsb.at[f], zin.at[slot], z_s.at[f], z_r.at[slot], {"col": c + step})

    def looped(rows, fn):
        def one(k, carry):
            fn(pl.ds(pl.multiple_of(k * step_rows, step_rows), step_rows))
            return carry
        lax.fori_loop(0, rows // step_rows, one, 0)

    def first_sum(v, f):
        a_copy(v, 1, f).wait_recv()
        if v == 1:
            y_copy(f).wait_send()

        def add(rows):
            sbuf[f, rows, :] = (
                obuf[1, f, rows, :].astype(F32) + abuf[v, 1, f, rows, :].astype(F32)
            ).astype(BF16)

        looped(T, add)
        if v == 1:
            pl.semaphore_wait(free_row.at[f], 1)
        y_copy(f).start()

    def release(f, peer):
        pl.semaphore_signal(free_col.at[f], inc=1, device_id={"col": peer}, device_id_type=MESH)

    def second_sum(v, i):
        f = forder[i]
        a_copy(v, 0, f).wait_recv()
        y_copy(f).wait_recv()

        def base(rows):
            return (
                obuf[0, f, rows, :].astype(F32)
                + abuf[v, 0, f, rows, :].astype(F32)
                + bbuf[f, rows, :].astype(F32)
            )

        if i < n_col - 1:
            right = f > c
            step = jnp.where(right, jnp.int32(1), jnp.int32(-1))
            landed = jnp.where(f == c + step, jnp.where(right, f, jnp.int32(n_col)), f)
            inner = jnp.where(right, c, n_col - 1 - c) > 0
            if v == 1:
                z_copy(f, f, 0).wait_send()

            @pl.when(inner)
            def _():
                z_copy(f, f, 0).wait_recv()

                def add(rows):
                    zsb[f, rows, :] = (base(rows) + zin[f, rows, :].astype(F32)).astype(BF16)

                looped(T, add)
                if v == 0:
                    release(f, c - step)

            @pl.when(jnp.logical_not(inner))
            def _():
                def add(rows):
                    zsb[f, rows, :] = base(rows).astype(BF16)

                looped(T, add)

            if v == 1:
                pl.semaphore_wait(free_col.at[f], 1)
            z_copy(f, landed, step).start()
        else:
            out = outs[v]

            @pl.when(c > 0)
            def _():
                z_copy(f, f, 0).wait_recv()

            @pl.when(c < n_col - 1)
            def _():
                z_copy(f, n_col, 0).wait_recv()

            def put(rows, value):
                out[rows, :] = value

            @pl.when(c == 0)
            def _():
                looped(T, lambda rows: put(rows, base(rows) + zin[n_col, rows, :].astype(F32)))

            @pl.when(c == n_col - 1)
            def _():
                looped(T, lambda rows: put(rows, base(rows) + zin[f, rows, :].astype(F32)))

            @pl.when((c > 0) & (c < n_col - 1))
            def _():
                looped(T, lambda rows: put(
                    rows,
                    base(rows) + zin[f, rows, :].astype(F32) + zin[n_col, rows, :].astype(F32)))

            if v == 0:
                @pl.when(c > 0)
                def _():
                    release(f, c - 1)

                @pl.when(c < n_col - 1)
                def _():
                    release(f, c + 1)

        if v == 0:
            pl.semaphore_signal(free_row.at[f], inc=1, device_id={"row": r2}, device_id_type=MESH)

    tall = (HF, 2 * UT)
    row0 = (0, HF)
    lane_u = (qw, qw + UT)
    lw = 2 * HF

    def xf_copy(own, b):
        return copy(dwf.at[pl.ds(row0[own] + b * HF, HF), :], gf.at[pl.ds(b * HF, HF), :],
                    xf_s.at[own, b], xf_r.at[b], {"dp": 1 - d})

    def xu_copy(own, cc):
        return copy(dwi.at[pl.ds(cc * C, C), pl.ds(lane_u[own], UT)], gu.at[cc],
                    xu_s.at[own, cc], xu_r.at[cc], {"dp": 1 - d})

    def xk_copy(cc):
        return copy(dwi.at[pl.ds(cc * C, C), pl.ds(0, qw)], gk.at[cc], xk_s.at[cc], xk_r.at[cc],
                    {"dp": 1 - d})

    def parts_f(own, cc, source):
        half, odd = lax.div(source, 2), lax.rem(source, 2)
        at = cc * C
        if own == 0:
            return [
                (dwf.at[pl.ds(0, HF), pl.ds(at + j * lw, lw)],
                 tiles_ref.at[6 + j, pl.ds(source * HF, HF), :])
                for j in range(2)
            ]
        return [
            (dwf.at[pl.ds(HF, UT), pl.ds(at + j * lw, lw)],
             tiles_ref.at[4 + 2 * half + j, pl.ds(odd * UT, UT), :])
            for j in range(2)
        ]

    def parts_e(own, cc, source):
        half, odd = lax.div(source, 2), lax.rem(source, 2)
        at = cc * C
        return [
            (dwf.at[pl.ds(HF + UT, UT), pl.ds(at + j * lw, lw)],
             tiles_ref.at[8 + 2 * half + j, pl.ds(odd * UT, UT), :])
            for j in range(2)
        ]

    def parts_u(own, cc, source):
        dst = tiles_ref.at[8 + source] if own == 0 else tiles_ref.at[source]
        return [(dwi.at[pl.ds(cc * C, C), pl.ds(lane_u[own], UT)], dst)]

    def parts_k(own, cc, source):
        half, odd = lax.div(source, 2), lax.rem(source, 2)
        return [
            (dwi.at[pl.ds(cc * C, C), pl.ds(j * HF, HF)],
             tiles_ref.at[2 * j + half, :, pl.ds(odd * HF, HF)])
            for j in range(3)
        ]

    kinds = {"f": (parts_f, 0), "e": (parts_e, 2), "u": (parts_u, 4), "k": (parts_k, 5)}

    def t_send(kind, own, cc):
        parts, first = kinds[kind]
        return [
            copy(src, dst, t_s.at[first + n, cc], t_r.at[first + n, c], {"col": cc})
            for n, (src, dst) in enumerate(parts(own, cc, c))
        ]

    def t_wait(kind, own, source):
        parts, first = kinds[kind]
        return [
            copy(src, dst, t_s.at[first + n, source], t_r.at[first + n, source], {"col": source})
            for n, (src, dst) in enumerate(parts(own, source, source))
        ]

    def t_local(kind, own):
        parts, first = kinds[kind]
        return [
            pltpu.make_async_copy(src, dst, t_s.at[first + n, c])
            for n, (src, dst) in enumerate(parts(own, c, c))
        ]

    def owned_kinds(own):
        return ("f", "u", "k") if own == 0 else ("f", "e", "u")

    def spread(kind, own):
        for k in range(1, n_col):
            for item in t_send(kind, own, lax.rem(c + k, n_col)):
                item.start()
        for item in t_local(kind, own):
            item.start()

    def add_rows(own, first, count):
        for b in range(first, first + count):
            xf_copy(own, b).wait_recv()

        def add(rows):
            here = pl.ds(pl.multiple_of(rows.start + first * HF, step_rows), step_rows)
            at = (pl.ds(pl.multiple_of(rows.start + row0[own] + first * HF, step_rows), step_rows),
                  slice(None))
            dwf[at] = (dwf[at].astype(F32) + gf[here, :].astype(F32)).astype(BF16)

        looped(count * HF, add)

    def add_f():
        for own in range(2):
            @pl.when(d == own)
            def _(own=own):
                add_rows(own, 0, 1 if own == 0 else UT // HF)
                spread("f", own)

    def add_e():
        @pl.when(d == 1)
        def _():
            add_rows(1, UT // HF, UT // HF)
            spread("e", 1)

    def add_piece(kind, own, cc):
        lane, width, buf, waiter = (
            (lane_u[own], UT, gu, xu_copy(own, cc)) if kind == "u" else (0, qw, gk, xk_copy(cc))
        )
        waiter.wait_recv()

        def add(rows):
            at = (pl.ds(pl.multiple_of(rows.start + cc * C, step_rows), step_rows),
                  pl.ds(lane, width))
            dwi[at] = (dwi[at].astype(F32) + buf[cc, rows, :].astype(F32)).astype(BF16)

        looped(C, add)

    def add_w(i):
        for own in range(2):
            @pl.when(d == own)
            def _(own=own):
                cc = forder[i]
                for kind in ("k", "u") if own == 0 else ("u",):
                    add_piece(kind, own, cc)
                    for item in t_local(kind, own) if i == n_col - 1 else t_send(kind, own, cc):
                        item.start()

    loads[0].wait()
    loads[1].wait()

    def p_unit(rr, f):
        at = pl.ds(pl.multiple_of(rr * T, T), T)
        lanes = pl.ds(pl.multiple_of(f * C, C), C)
        return jnp.dot(hd[at, 2 * HF :], wf[:, lanes], preferred_element_type=F32).astype(BF16)

    def p_step(i, carry):
        f = pick(i, forder)
        for h, rr in ((1, r12), (0, r1)):
            asb[h, f] = p_unit(rr, f)
            a_copy(0, h, f).start()
        for h, rr in ((1, r2), (0, r)):
            obuf[h, f] = p_unit(rr, f)

        @pl.when(i > 0)
        def _():
            first_sum(0, pick(i - 1, forder))

        return carry

    lax.fori_loop(0, n_col, p_step, 0)

    loads[2].wait()
    blocks = n_out // HF

    def f_step(m, carry):
        slot = lax.rem(m, 2)
        load_ht(m, slot).wait()

        @pl.when(m + 1 < blocks)
        def _():
            load_ht(m + 1, 1 - slot).start()

        at = pl.ds(pl.multiple_of(m * HF, HF), HF)
        dwf[at, :] = jnp.dot(hts[slot], big[...], preferred_element_type=F32).astype(BF16)

        @pl.when((m == 0) & (d == 1))
        def _():
            xf_copy(0, 0).start()

        @pl.when((m > 0) & (d == 0))
        def _():
            xf_copy(1, m - 1).start()

        return carry

    early = 1 + UT // HF
    first_sum(0, forder[n_col - 1])
    lax.fori_loop(0, early, f_step, 0)

    part_ref[...] = jnp.zeros_like(part_ref)
    tiles = rows_all // tile

    def b_step(i, carry):
        slot = lax.rem(i, 2)
        load_up(i, slot).wait()

        @pl.when(i + 1 < tiles)
        def _():
            load_up(i + 1, 1 - slot).start()

        at = pl.ds(pl.multiple_of(i * tile, tile), tile)
        back = lax.dot_general(
            big[at, :], wf[...], (((1,), (1,)), ((), ())), preferred_element_type=F32
        )
        ga[at, :] = back[:, :HF].astype(BF16)
        grad = back[:, HF:] * gelu_slope(ups[slot])
        hd[at, qw:] = grad.astype(BF16)
        sums = jnp.sum(grad, axis=0, keepdims=True)
        for k in range(2 * UT // 128):
            part_ref[3 + k : 4 + k, :] += sums[:, k * 128 : (k + 1) * 128]
        return carry

    lax.fori_loop(0, tiles, b_step, 0)
    load_nt.start()
    second_sum(0, 0)

    loads[3].wait()
    loads[4].wait()
    heads = HF // HEAD_DIM
    qt = SEQ_LEN // 2
    scale = HEAD_DIM ** (-0.5)
    per_row = T // SEQ_LEN
    first_dim = (((0,), (0,)), ((), ()))
    last_dim = (((1,), (1,)), ((), ()))

    def attend_seq(s):
        base = pl.multiple_of(s * SEQ_LEN, SEQ_LEN)
        lane = lax.broadcasted_iota(jnp.int32, (qt, HF), 1)
        seg = seg_ref[pl.ds(s, 1), :]
        seg_col = jnp.transpose(jnp.broadcast_to(seg, (128, SEQ_LEN)))[:, 0:1]
        grad_q, grad_k, grad_v = [], None, None
        for qi in range(2):
            width = (qi + 1) * qt
            q_at = pl.ds(base + qi * qt, qt)
            k_at = pl.ds(base, width)
            allowed = (seg_col[qi * qt : (qi + 1) * qt, :] == seg[:, 0:width]) & (
                lax.broadcasted_iota(jnp.int32, (qt, width), 0) + qi * qt
                >= lax.broadcasted_iota(jnp.int32, (qt, width), 1)
            )
            queries, g_att = qv[q_at, 0:HF], ga[q_at, :]
            keys, vals = qv[k_at, HF : 2 * HF], qv[k_at, 2 * HF : 3 * HF]
            both = g_att.astype(F32) * hd[q_at, 2 * HF : 3 * HF].astype(F32)
            gq, gks, gvs = None, None, None
            for h in range(heads):
                mine = lax.div(lane, HEAD_DIM) == h
                q_h = jnp.where(mine, queries, jnp.zeros_like(queries))
                g_h = jnp.where(mine, g_att, jnp.zeros_like(g_att))
                scores = lax.dot_general(q_h, keys, last_dim, preferred_element_type=F32) * scale
                scores = jnp.where(allowed, scores, MASKED_SCORE)
                peak = jnp.max(scores, axis=1, keepdims=True)
                weight = jnp.exp(scores - peak)
                probs = weight * (1.0 / jnp.sum(weight, axis=1, keepdims=True))
                delta = jnp.sum(jnp.where(mine, both, 0.0), axis=1, keepdims=True)
                g_prob = lax.dot_general(g_h, vals, last_dim, preferred_element_type=F32)
                g_score = (probs * (g_prob - delta) * scale).astype(BF16)
                gq_h = jnp.dot(g_score, keys, preferred_element_type=F32)
                gk_h = lax.dot_general(g_score, q_h, first_dim, preferred_element_type=F32)
                gv_h = lax.dot_general(probs.astype(BF16), g_h, first_dim,
                                       preferred_element_type=F32)
                gq = gq_h if h == 0 else jnp.where(mine, gq_h, gq)
                gks = gk_h if h == 0 else gks + gk_h
                gvs = gv_h if h == 0 else gvs + gv_h
            grad_q.append(gq)
            if qi == 0:
                grad_k, grad_v = gks, gvs
            else:
                grad_k = jnp.concatenate([grad_k + gks[:qt], gks[qt:]], axis=0)
                grad_v = jnp.concatenate([grad_v + gvs[:qt], gvs[qt:]], axis=0)
        s_at = pl.ds(base, SEQ_LEN)
        cos, sin = wide_tables(cs_ref[s_at, :])
        grads = (
            turn(jnp.concatenate(grad_q, axis=0), cos, sin, -1.0),
            turn(grad_k, cos, sin, -1.0),
            grad_v,
        )
        for j, grad in enumerate(grads):
            part_ref[j : j + 1, :] += jnp.sum(grad, axis=0, keepdims=True)
            hd[s_at, j * HF : (j + 1) * HF] = grad.astype(BF16)

    def q_unit(rr, f):
        at = pl.ds(pl.multiple_of(rr * T, T), T)
        feats = pl.ds(pl.multiple_of(f * C, C), C)
        return lax.dot_general(
            hd[at, :], wi[feats, :], last_dim, preferred_element_type=F32
        ).astype(BF16)

    def seq_step(s, carry):
        attend_seq(s)
        return carry

    lax.fori_loop(0, rows_all // SEQ_LEN, seq_step, 0)
    second_sum(0, 1)
    load_nt.wait()

    half_rows = C // 2

    def w_step(i, carry):
        cc = pick(lax.div(i, 2), forder)
        at = pl.ds(pl.multiple_of(cc * C + lax.rem(i, 2) * half_rows, half_rows), half_rows)
        dwi[at, :] = jnp.dot(big[at, :], hd[...], preferred_element_type=F32).astype(BF16)

        @pl.when(lax.rem(i, 2) == 1)
        def _():
            for own in range(2):
                @pl.when(d == own)
                def _(own=own):
                    if own == 1:
                        xk_copy(cc).start()
                    xu_copy(1 - own, cc).start()

        return carry

    lax.fori_loop(0, n_col, w_step, 0)
    second_sum(0, 2)
    lax.fori_loop(n_col, 2 * n_col, w_step, 0)
    load_c = pltpu.make_async_copy(c_ref, big, l_s.at[2])
    load_c.start()

    def q_step(h, rows_peer, rows_own):
        def units(i, carry):
            f = pick(i, forder)
            a_copy(0, h, f).wait_send()
            asb[h, f] = q_unit(rows_peer, f)
            a_copy(1, h, f).start()
            obuf[h, f] = q_unit(rows_own, f)
            return carry

        lax.fori_loop(0, n_col, units, 0)

    q_step(1, r12, r2)
    for i in range(n_col - 1):
        first_sum(1, forder[i])
    add_f()
    load_c.wait()
    lax.fori_loop(early, blocks, f_step, 0)
    second_sum(0, n_col - 1)
    first_sum(1, forder[n_col - 1])
    add_w(0)
    q_step(0, r1, r)
    add_w(1)
    second_sum(1, 0)
    add_w(2)
    second_sum(1, 1)
    add_e()
    second_sum(1, 2)
    add_w(3)
    second_sum(1, n_col - 1)

    for own in range(2):
        @pl.when(d == own)
        def _(own=own):
            for kind in owned_kinds(own):
                for k in range(1, n_col):
                    for item in t_wait(kind, own, lax.rem(c + k, n_col)):
                        item.wait_recv()
                for k in range(1, n_col):
                    for item in t_send(kind, own, lax.rem(c + k, n_col)):
                        item.wait_send()
                for item in t_local(kind, own):
                    item.wait()
            for b in range(tall[1 - own] // HF):
                xf_copy(1 - own, b).wait_send()
            for cc in range(n_col):
                xu_copy(1 - own, cc).wait_send()
                if own == 1:
                    xk_copy(cc).wait_send()
    for f in range(n_col):
        a_copy(1, 0, f).wait_send()
        a_copy(1, 1, f).wait_send()
        y_copy(f).wait_send()
    for i in range(n_col - 1):
        z_copy(forder[i], forder[i], 0).wait_send()


def backward_all(hid, ht, cot, w_fin, w_in, nt, qkv, up, packed, seg_row, T, C, HF, UT, n_row, n_col):
    dma = pltpu.SemaphoreType.DMA
    vm = pl.BlockSpec(memory_space=pltpu.VMEM)
    rows, D = n_row * T, n_col * C
    n_in, n_out = 3 * HF + 2 * UT, HF + 2 * UT
    unit = (T, C)
    V = pltpu.VMEM
    return pl.pallas_call(
        functools.partial(backward_kernel, n_row, n_col, (T, C, HF, UT)),
        name="backward_all",
        out_shape=(
            jax.ShapeDtypeStruct(unit, F32),
            jax.ShapeDtypeStruct(unit, F32),
            jax.ShapeDtypeStruct((12, C, UT), BF16),
            jax.ShapeDtypeStruct((8, 128), F32),
        ),
        in_specs=[ANY] * 8 + [vm] * 2,
        out_specs=(vm, vm, ANY, vm),
        scratch_shapes=[
            V((rows, n_in), BF16),
            V((2, HF, rows), BF16),
            V((rows, D), BF16),
            V((n_out, D), BF16),
            V((D, n_in), BF16),
            V((rows, 3 * HF), BF16),
            V((2, 256, 2 * UT), F32),
            V((rows, HF), BF16),
            V((2, 2, n_col) + unit, BF16),
            V((2, n_col) + unit, BF16),
            V((2, n_col) + unit, BF16),
            V((n_col,) + unit, BF16),
            V((n_col,) + unit, BF16),
            V((n_col,) + unit, BF16),
            V((n_col + 1,) + unit, BF16),
            V((n_out, D), BF16),
            V((D, n_in), BF16),
            V((2 * UT, D), BF16),
            V((n_col, C, UT), BF16),
            V((n_col, C, 3 * HF), BF16),
            dma((6,)),
            dma((2,)),
            dma((2,)),
            dma((2, n_col)),
            dma((2, 2, n_col)),
            dma((n_col,)),
            dma((n_col,)),
            dma((n_col,)),
            dma((n_col + 1,)),
            dma((2, 2 * UT // HF)),
            dma((2 * UT // HF,)),
            dma((2, n_col)),
            dma((n_col,)),
            dma((n_col,)),
            dma((n_col,)),
            dma((8, n_col)),
            dma((8, n_col)),
            pltpu.SemaphoreType.REGULAR((n_col,)),
            pltpu.SemaphoreType.REGULAR((n_col,)),
        ],
        compiler_params=pltpu.CompilerParams(
            collective_id=1, has_side_effects=True, vmem_limit_bytes=67043328
        ),
    )(hid, ht, cot, w_fin, w_in, nt, qkv, up, packed, seg_row)


def finish_kernel(n_dp, n_row, n_col, width, *refs):
    hbm, (gx_ref, vec_ref), local = refs[:7], refs[7:9], refs[9:16]
    gn_ref, x_ref, g_ref, mean_ref, rstd_ref, gain_ref, part_ref = local
    l_s, st, da, db, ra, rb, va_ref, vb_ref, st_s, st_r, d_s, d_r, r_s, r_r, c_s, c_r = refs[16:]
    loads = [
        pltpu.make_async_copy(src, dst, l_s.at[n]) for n, (src, dst) in enumerate(zip(hbm, local))
    ]
    for item in loads:
        item.start()
    d, r, c = lax.axis_index("dp"), lax.axis_index("row"), lax.axis_index("col")
    T, C = gn_ref.shape

    barrier = pltpu.get_barrier_semaphore()
    dps = [lax.rem(d + k, n_dp) for k in range(1, n_dp)]
    rows = [lax.rem(r + k, n_row) for k in range(1, n_row)]
    cols = [lax.rem(c + k, n_col) for k in range(1, n_col)]
    peers = [{"dp": k} for k in dps] + [{"row": k} for k in rows] + [{"col": k} for k in cols]
    for peer in peers:
        pl.semaphore_signal(barrier, inc=1, device_id=peer, device_id_type=MESH)

    def copy(src, dst, s, rcv, peer):
        return pltpu.make_async_remote_copy(
            src_ref=src, dst_ref=dst, send_sem=s, recv_sem=rcv, device_id=peer, device_id_type=MESH
        )

    for item in loads:
        item.wait()
    gain = gain_ref[...]

    def fold(value):
        total = value[:, 0:128]
        for k in range(1, C // 128):
            total = total + value[:, k * 128 : (k + 1) * 128]
        return jnp.sum(jnp.transpose(total), axis=0, keepdims=True)

    gn = gn_ref[...]
    x_hat = (x_ref[...].astype(F32) - mean_ref[...]) * rstd_ref[...]
    gh = gn * gain
    st[c, 0:1, :] = fold(gh)
    st[c, 1:2, :] = fold(gh * x_hat)

    def st_copy(k):
        return copy(st.at[c], st.at[c], st_s.at[k], st_r.at[c], {"col": k})

    def st_wait(k):
        return copy(st.at[k], st.at[k], st_s.at[k], st_r.at[k], {"col": k})

    pl.semaphore_wait(barrier, len(peers))
    for k in cols:
        st_copy(k).start()

    da[d] = part_ref[...]
    db[d, 0:1, :] = jnp.sum(gn * x_hat, axis=0, keepdims=True)
    db[d, 1:2, :] = jnp.sum(gn, axis=0, keepdims=True)
    db[d, 2:3, :] = jnp.sum(g_ref[...].astype(F32), axis=0, keepdims=True)

    def pair(a_src, b_src, a_dst, b_dst, s, rcv, peer):
        return [copy(a_src, a_dst, s.at[0], rcv.at[0], peer),
                copy(b_src, b_dst, s.at[1], rcv.at[1], peer)]

    def d_pair(slot, peer):
        return pair(da.at[slot], db.at[slot], da.at[slot], db.at[slot],
                    d_s.at[peer], d_r.at[slot], {"dp": peer})

    def r_pair(slot, peer):
        return pair(ra.at[slot], rb.at[slot], ra.at[slot], rb.at[slot],
                    r_s.at[peer], r_r.at[slot], {"row": peer})

    def c_pair(slot, peer):
        return pair(va_ref.at[slot], vb_ref.at[slot], va_ref.at[slot], vb_ref.at[slot],
                    c_s.at[peer], c_r.at[slot], {"col": peer})

    for k in dps:
        for item in d_pair(d, k):
            item.start()
    for k in dps:
        for item in d_pair(k, k):
            item.wait_recv()
    a_sum, b_sum = da[0], db[0]
    for k in range(1, n_dp):
        a_sum = a_sum + da[k]
        b_sum = b_sum + db[k]
    ra[r] = a_sum
    rb[r] = b_sum
    for k in rows:
        for item in r_pair(r, k):
            item.start()

    for k in cols:
        st_wait(k).wait_recv()
    stats = st[0]
    for k in range(1, n_col):
        stats = stats + st[k]
    stats = stats / width
    m1 = jnp.transpose(jnp.broadcast_to(stats[0:1, :], (128, T)))[:, 0:1]
    m2 = jnp.transpose(jnp.broadcast_to(stats[1:2, :], (128, T)))[:, 0:1]
    gx_ref[...] = g_ref[...].astype(F32) + rstd_ref[...] * (gh - m1 - x_hat * m2)

    for k in rows:
        for item in r_pair(k, k):
            item.wait_recv()
    b_sum = rb[0]
    for k in range(1, n_row):
        b_sum = b_sum + rb[k]
    for k in range(n_row):
        va_ref[c, k] = ra[k]
    vb_ref[c] = b_sum
    for k in cols:
        for item in c_pair(c, k):
            item.start()
    for k in cols:
        for item in c_pair(k, k):
            item.wait_recv()
    unit = 128
    units = (vec_ref.shape[1] // unit) // (2 * n_col)
    for cc in range(n_col):
        lanes = slice(cc * C, (cc + 1) * C)
        vec_ref[5:7, lanes] = vb_ref[cc, 0:2, :]
        for row in (3, 4):
            vec_ref[row : row + 1, lanes] = vb_ref[cc, 2:3, :]
        for rr in range(n_row):
            at = (rr * n_col + cc) * unit
            vec_ref[0:3, at : at + unit] = va_ref[cc, rr, 0:3, :]
            for half in range(2):
                for k in range(units):
                    to = ((half * n_col + cc) * units + k) * unit
                    src = 3 + half * units + k
                    vec_ref[7 + rr : 8 + rr, to : to + unit] = va_ref[cc, rr, src : src + 1, :]
    for k in cols:
        st_copy(k).wait_send()
        for item in c_pair(c, k):
            item.wait_send()
    for k in dps:
        for item in d_pair(d, k):
            item.wait_send()
    for k in rows:
        for item in r_pair(r, k):
            item.wait_send()


def finish_all(gn, x, g, mean, rstd, gain, part, width, n_dp, n_row, n_col):
    args = (gn, x, g, mean, rstd, gain, part)
    T, C = gn.shape
    dma = pltpu.SemaphoreType.DMA
    vm = pl.BlockSpec(memory_space=pltpu.VMEM)
    return pl.pallas_call(
        functools.partial(finish_kernel, n_dp, n_row, n_col, width),
        name="finish_all",
        out_shape=(
            jax.ShapeDtypeStruct((T, C), F32),
            jax.ShapeDtypeStruct((7 + n_row, n_col * C), F32),
        ),
        in_specs=[ANY] * 7,
        out_specs=(vm,) * 2,
        scratch_shapes=[pltpu.VMEM(item.shape, item.dtype) for item in args]
        + [
            dma((7,)),
            pltpu.VMEM((n_col, 8, T), F32),
            pltpu.VMEM((n_dp, 8, 128), F32),
            pltpu.VMEM((n_dp, 8, C), F32),
            pltpu.VMEM((n_row, 8, 128), F32),
            pltpu.VMEM((n_row, 8, C), F32),
            pltpu.VMEM((n_col, n_row, 8, 128), F32),
            pltpu.VMEM((n_col, 8, C), F32),
            dma((n_col,)),
            dma((n_col,)),
            dma((n_dp, 2)),
            dma((n_dp, 2)),
            dma((n_row, 2)),
            dma((n_row, 2)),
            dma((n_col, 2)),
            dma((n_col, 2)),
        ],
        compiler_params=pltpu.CompilerParams(
            collective_id=2, has_side_effects=True, vmem_limit_bytes=67043328
        ),
    )(*args)


def muon_kernel(owned, per_step, HF, UT, rate, grad_ref, mom_ref, wq_ref, wo_ref, wu_ref, wd_ref,
                og_ref, new_ref, nm_ref, wbuf, sem):
    first = lax.axis_index("dp") * owned
    step = pl.program_id(0)
    steps = owned // per_step
    n_qkv, n_out, n_up = 6, 2, 8

    def fetch(tile, slot, n, start):
        dst = wbuf.at[slot, n]

        def go(src, target, s):
            item = pltpu.make_async_copy(src, target, s)
            if start:
                item.start()
            else:
                item.wait()

        @pl.when(tile < n_qkv)
        def _():
            j, half = lax.div(tile, 2), lax.rem(tile, 2)
            for m in range(UT // HF):
                go(wq_ref.at[half * (UT // HF) + m, :, pl.ds(j * HF, HF)],
                   wbuf.at[slot, n, :, pl.ds(m * HF, HF)], sem.at[slot, n, m])

        @pl.when((tile >= n_qkv) & (tile < n_qkv + n_out))
        def _():
            go(wo_ref.at[:, pl.ds((tile - n_qkv) * UT, UT)], dst, sem.at[slot, n, 0])

        @pl.when((tile >= n_qkv + n_out) & (tile < n_qkv + n_out + n_up))
        def _():
            go(wu_ref.at[:, pl.ds((tile - n_qkv - n_out) * UT, UT)], dst, sem.at[slot, n, 0])

        @pl.when(tile >= n_qkv + n_out + n_up)
        def _():
            left = tile - (n_qkv + n_out + n_up)
            rows = dst.shape[0]
            go(wd_ref.at[pl.ds(lax.div(left, 2) * rows, rows), pl.ds(lax.rem(left, 2) * UT, UT)],
               dst, sem.at[slot, n, 0])

    def fetch_all(at, start):
        for n in range(per_step):
            fetch(first + at * per_step + n, lax.rem(at, 2), n, start)

    @pl.when(step == 0)
    def _():
        fetch_all(step, True)

    @pl.when(step + 1 < steps)
    def _():
        fetch_all(step + 1, True)

    iters = []
    for n in range(per_step):
        grad = grad_ref[n].astype(F32)
        og_ref[n] = grad
        moment = MOMENTUM_RATE * mom_ref[n] + grad
        nm_ref[n] = moment
        scale = lax.rsqrt(jnp.sum(moment * moment, keepdims=True) + STAT_EPS)
        iters.append((moment * scale).astype(BF16))
    contract = (((0,), (0,)), ((), ()))
    for _ in range(5):
        grams = [
            lax.dot_general(x, x, contract, preferred_element_type=F32).astype(BF16) for x in iters
        ]
        squares = [jnp.dot(g, g, preferred_element_type=F32) for g in grams]
        polys = [
            (NEWTON_B * g.astype(F32) + NEWTON_C * s).astype(BF16) for g, s in zip(grams, squares)
        ]
        iters = [
            (NEWTON_A * x.astype(F32) + jnp.dot(x, p, preferred_element_type=F32)).astype(BF16)
            for x, p in zip(iters, polys)
        ]
    fetch_all(step, False)
    for n in range(per_step):
        new_ref[n] = wbuf[lax.rem(step, 2), n].astype(F32) - rate * iters[n].astype(F32)


def muon_all(grads, moment, w_q, w_out, w_up, w_down, HF, UT):
    owned, rows, cols = moment.shape
    per_step = 4 if owned % 4 == 0 else 3
    rate = MUON_RATE * math.sqrt(max(1.0, rows / cols))
    block = pl.BlockSpec((per_step, rows, cols), lambda i: (i, 0, 0))
    out = jax.ShapeDtypeStruct(moment.shape, F32)
    return pl.pallas_call(
        functools.partial(muon_kernel, owned, per_step, HF, UT, rate),
        name="muon_all",
        grid=(owned // per_step,),
        out_shape=(out, out, out),
        in_specs=[block, block, ANY, ANY, ANY, ANY],
        out_specs=(block, block, block),
        scratch_shapes=[
            pltpu.VMEM((2, per_step, rows, cols), BF16),
            pltpu.SemaphoreType.DMA((2, per_step, 2)),
        ],
        compiler_params=pltpu.CompilerParams(vmem_limit_bytes=56 * 1024 * 1024),
    )(grads, moment, w_q, w_out, w_up, w_down)


def reduce_plain(p, q, dwi, dwf, C, HF, UT, n_col, row_width):
    def block(part):
        part = lax.psum_scatter(part, "row", scatter_dimension=0, tiled=True)
        return lax.psum_scatter(part, "col", scatter_dimension=1, tiled=True).astype(F32)

    wi4 = lax.all_to_all(dwi.reshape(n_col, C, -1), "col", 0, 0)
    wf4 = lax.all_to_all(dwf.reshape(-1, n_col, C).transpose(1, 0, 2), "col", 0, 0)
    grad_qkv = (
        wi4[:, :, : 3 * HF].reshape(n_col, C, 3, HF).transpose(1, 2, 0, 3).reshape(C, 3, row_width)
    )
    grad_up_w = wi4[:, :, 3 * HF :].reshape(n_col, C, 2, UT).transpose(1, 2, 0, 3).reshape(C, -1)
    grad_w_out = wf4[:, :HF].reshape(-1, C)
    grad_w_down = wf4[:, HF:].reshape(n_col, 2, UT, C).transpose(1, 0, 2, 3).reshape(-1, C)
    grad_tiles = tile_blocks(grad_qkv, grad_w_out, grad_up_w, grad_w_down)
    owned = lax.psum_scatter(grad_tiles, "dp", scatter_dimension=0, tiled=True)
    return block(p), block(q), owned


def backward_plain(hidden, hidden_t, cot, w_fin, w_in, norm_t, qkv, up_pre, positions, segments, HF):
    cosine, sine_tab = rotary_tables(positions)
    rows = cot.shape[0]
    seqs, heads = rows // SEQ_LEN, HF // HEAD_DIM

    def by_head(tensor_in):
        return tensor_in.reshape(seqs, SEQ_LEN, heads, HEAD_DIM)

    partial_out = jnp.dot(hidden, w_fin, preferred_element_type=F32).astype(BF16)
    grad_w_fin = jnp.dot(hidden_t, cot, preferred_element_type=F32).astype(BF16)
    back = jnp.einsum("tj,ij->ti", cot, w_fin, preferred_element_type=F32)
    grad_up = back[:, HF:] * gelu_slope(up_pre)
    grads = jax.vmap(attend_backward, in_axes=(0, 0, 0, 0, 0, 0, None))(
        by_head(qkv[:, :HF]),
        by_head(qkv[:, HF : 2 * HF]),
        by_head(qkv[:, 2 * HF :]),
        by_head(hidden[:, :HF]),
        by_head(back[:, :HF].astype(BF16)),
        segments.reshape(seqs, SEQ_LEN),
        HEAD_DIM ** (-0.5),
    )
    g_q, g_k, g_v = [item.reshape(rows, heads, HEAD_DIM) for item in grads]
    g_q = rotate(g_q, cosine, sine_tab, -1.0)
    g_k = rotate(g_k, cosine, sine_tab, -1.0)
    grad_mixed = jnp.concatenate(
        [item.reshape(rows, HF) for item in (g_q, g_k, g_v)] + [grad_up], axis=1
    )
    low = grad_mixed.astype(BF16)
    grad_w_in = jnp.dot(norm_t, low, preferred_element_type=F32).astype(BF16)
    partial_norm = jnp.einsum("tj,ij->ti", low, w_in, preferred_element_type=F32).astype(BF16)
    part = jnp.pad(jnp.sum(grad_mixed, axis=0).reshape(-1, 128), ((0, 1), (0, 0)))
    return (partial_out, partial_norm, grad_w_in, grad_w_fin), part


def body(
    inputs,
    cotangent,
    segments,
    positions,
    w_qkv,
    w_out,
    w_up,
    w_down,
    vectors,
    tile_moment,
    vector_moment,
):
    col_index = lax.axis_index("col")
    n_dp, n_row, n_col = lax.axis_size("dp"), lax.axis_size("row"), lax.axis_size("col")
    T, C = inputs.shape
    D = vectors.shape[1]
    row_width = w_qkv.shape[2]
    HF = row_width // n_col
    UT = w_up.shape[1] // (2 * n_col)
    col_start = col_index * C
    norm_gain = lax.dynamic_slice_in_dim(vectors[5], col_start, C)
    out_bias = lax.dynamic_slice_in_dim(vectors[3] + vectors[4], col_start, C)
    w_q = (
        w_qkv.reshape(C, 3, n_col, HF).transpose(2, 0, 1, 3).reshape(n_col, C, 3 * HF)
    )
    rows_all = positions.shape[0]
    seq_count = rows_all // SEQ_LEN
    seg_row = segments.reshape(seq_count, SEQ_LEN)
    pos_row = positions.reshape(seq_count, SEQ_LEN)
    cot_rows, w_in, w_fin, norm_t, hidden, hidden_t, qkv_low, up_pre, packed, mean_own, rstd_own = (
        forward_all(
            inputs, cotangent, w_q, w_up, w_out, w_down, pos_row, seg_row, vectors,
            n_dp, n_row, n_col,
        )
    )
    if n_dp == 2:
        branch, grad_norm, owned_low, part = backward_all(
            hidden, hidden_t, cot_rows, w_fin, w_in, norm_t, qkv_low, up_pre, packed, seg_row,
            T, C, HF, UT, n_row, n_col,
        )
    else:
        partials, part = backward_plain(
            hidden, hidden_t, cot_rows, w_fin, w_in, norm_t, qkv_low, up_pre, positions, segments, HF
        )
        branch, grad_norm, owned_low = reduce_plain(*partials, C, HF, UT, n_col, row_width)
    x_val = inputs.astype(F32)
    result = x_val + branch + out_bias

    grad_input, vec_grad = finish_all(
        grad_norm,
        inputs,
        cotangent,
        mean_own,
        rstd_own,
        norm_gain[None],
        part,
        D,
        n_dp,
        n_row,
        n_col,
    )
    scaled = vec_grad * lax.rsqrt(jnp.mean(vec_grad * vec_grad, axis=1, keepdims=True) + STAT_EPS)
    vec_moment_new = MOMENTUM_RATE * vector_moment + scaled
    vectors_new = vectors - VECTOR_RATE * vec_moment_new

    owned_grads, tiles_new, moment_new = muon_all(
        owned_low, tile_moment[0, 0], w_q, w_out, w_up, w_down, HF, UT
    )
    return (
        result,
        grad_input,
        owned_grads[None, None],
        tiles_new[None, None],
        moment_new[None, None],
        vec_grad,
        vectors_new,
        vec_moment_new,
    )


def solution(mesh):
    placed = (
        P(("dp", "row"), "col"),
        P(("dp", "row"), "col"),
        P("dp"),
        P("dp"),
        P("col", None, "row"),
        P("row", "col"),
        P("col", "row"),
        P("row", "col"),
        P(),
        P("row", "col", "dp", None, None),
        P(),
    )
    return jax.shard_map(
        body,
        mesh=mesh,
        in_specs=placed,
        out_specs=(
            P(("dp", "row"), "col"),
            P(("dp", "row"), "col"),
            P("row", "col", "dp", None, None),
            P("row", "col", "dp", None, None),
            P("row", "col", "dp", None, None),
            P(),
            P(),
            P(),
        ),
        check_vma=False,
    )
```
